64 devices in a mesh: dp: 4 (over x, y), tp: 16 (over z, core).
Axes of the slice: x: 2, y: 2, z: 8, core: 2. Of those that a mesh axis runs over, the one named last changes fastest.
The devices are a block of a 4x4x8 slice.
Arguments:
- tok_ids: int32 [16, 512], P('dp'), parts along dimension 0
- embed: bfloat16 [2048, 4096], P('tp')
- norm_gain: float32 [4096], replicated
- q_gain: float32 [128], replicated
- k_gain: float32 [128], replicated
- w_query: bfloat16 [4096, 8192], P(None, 'tp')
- w_key: bfloat16 [4096, 512], P(None, 'tp')
- w_value: bfloat16 [4096, 512], P(None, 'tp')
- w_out: bfloat16 [8192, 4096], P('tp')
- grad_y: bfloat16 [16, 512, 4096], P('dp', 'tp'), parts along dimension 0
Outputs:
- output 1: bfloat16 [16, 512, 4096], P('dp', 'tp'), parts along dimension 0
- output 2: float32 [8192, 4096], P(('dp', 'tp')), parts along dimension 0
- output 3: float32 [16384], P('dp'), parts along dimension 0
- output 4: float32 [512], P('dp'), parts along dimension 0
- output 5: float32 [512], P('dp'), parts along dimension 0
- output 6: float32 [16384, 8192], P('dp', 'tp'), parts along dimension 0
- output 7: float32 [16384, 512], P('dp', 'tp'), parts along dimension 0
- output 8: float32 [16384, 512], P('dp', 'tp'), parts along dimension 0
- output 9: float32 [32768, 4096], P(('dp', 'tp')), parts along dimension 0
There are 4 independent parts. The reference program is written for one: setup_inputs(seed, part) draws one part's arguments, and reference() takes and returns one part's arrays. A program takes and returns all parts, laid end to end along the dimension named above; an argument that names none is the same for every part.
All inputs are finite; a program needn't handle non-finite values.
Results may differ from the reference program's by a relative error of at most 0.02.
Values are sent between devices in bfloat16 or wider.
A program may use at most 768 MiB of HBM per device.

```python
import jax
import jax.numpy as jnp
from jax import lax

D_MODEL = 4096
Q_HEADS = 64
KV_HEADS = 4
HEAD_DIM = 128
BATCH_ROWS = 4
SEQ_LEN = 512
VOCAB_SIZE = 2048
VOCAB_SHARDS = 16

EPS = 1.0e-6
ROPE_BASE = 1.0e6
NEG_BIG = -1.0e30


def draw_ids(id_keys):
    shard_rows = VOCAB_SIZE // VOCAB_SHARDS
    first_ids = jax.random.randint(id_keys[0], (BATCH_ROWS, SEQ_LEN), 0, VOCAB_SIZE)
    second_ids = jax.random.randint(id_keys[1], (BATCH_ROWS, SEQ_LEN), 0, VOCAB_SIZE)
    coin_flip = jax.random.randint(id_keys[2], (BATCH_ROWS, SEQ_LEN), 0, 2)
    tok_ids = jnp.where(coin_flip == 1, jnp.minimum(first_ids, second_ids), first_ids)
    cover_ids = jnp.arange(VOCAB_SHARDS) * shard_rows + jax.random.randint(id_keys[3], (VOCAB_SHARDS,), 0, shard_rows)
    return tok_ids.at[0, :VOCAB_SHARDS].set(cover_ids).astype(jnp.int32)


def setup_inputs(seed: int = 0, part: int = 0) -> dict:
    base_key = jax.random.key(seed)
    own_keys = jax.random.split(jax.random.fold_in(base_key, part), 5)
    shared_keys = jax.random.split(base_key, 8)
    tok_ids = draw_ids(own_keys)
    embed = 0.5 * jax.random.normal(shared_keys[0], (VOCAB_SIZE, D_MODEL), jnp.float32)
    norm_gain = 1.0 + 0.3 * jax.random.normal(shared_keys[1], (D_MODEL,), jnp.float32)
    q_gain = 1.5 + 0.5 * jax.random.uniform(shared_keys[2], (HEAD_DIM,), jnp.float32, -1.0, 1.0)
    k_gain = 1.5 + 0.5 * jax.random.uniform(shared_keys[3], (HEAD_DIM,), jnp.float32, -1.0, 1.0)
    w_query = jax.random.normal(shared_keys[4], (D_MODEL, Q_HEADS * HEAD_DIM), jnp.float32) * D_MODEL ** -0.5
    w_key = jax.random.normal(shared_keys[5], (D_MODEL, KV_HEADS * HEAD_DIM), jnp.float32) * D_MODEL ** -0.5
    w_value = jax.random.normal(shared_keys[6], (D_MODEL, KV_HEADS * HEAD_DIM), jnp.float32) * D_MODEL ** -0.5
    w_out = jax.random.normal(shared_keys[7], (Q_HEADS * HEAD_DIM, D_MODEL), jnp.float32) * (Q_HEADS * HEAD_DIM) ** -0.5
    grad_y = jax.random.normal(own_keys[4], (BATCH_ROWS, SEQ_LEN, D_MODEL), jnp.float32)
    return {'tok_ids': tok_ids, 'embed': embed.astype(jnp.bfloat16), 'norm_gain': norm_gain, 'q_gain': q_gain, 'k_gain': k_gain, 'w_query': w_query.astype(jnp.bfloat16), 'w_key': w_key.astype(jnp.bfloat16), 'w_value': w_value.astype(jnp.bfloat16), 'w_out': w_out.astype(jnp.bfloat16), 'grad_y': grad_y.astype(jnp.bfloat16)}


def rope_tables(seq_len, head_dim):
    half_dim = head_dim // 2
    inv_freq = ROPE_BASE ** (-2.0 * jnp.arange(half_dim, dtype=jnp.float32) / head_dim)
    angles = jnp.arange(seq_len, dtype=jnp.float32)[:, None] * inv_freq[None, :]
    angles = jnp.concatenate([angles, angles], axis=-1)
    return jnp.cos(angles), jnp.sin(angles)


def rms_scale(wide_in, gain_vec):
    return wide_in * lax.rsqrt(jnp.mean(wide_in * wide_in, axis=-1, keepdims=True) + EPS) * gain_vec


def norm_rope(raw_heads, gain_vec, cos_tab, sin_tab):
    normed = rms_scale(raw_heads.astype(jnp.float32), gain_vec)
    half_dim = normed.shape[-1] // 2
    rotated = jnp.concatenate([-normed[..., half_dim:], normed[..., :half_dim]], axis=-1)
    return normed * cos_tab[:, None, :] + rotated * sin_tab[:, None, :]


def block_forward(x_emb, norm_gain, q_gain, k_gain, w_query, w_key, w_value, w_out):
    x_wide = x_emb.astype(jnp.float32)
    hidden = rms_scale(x_wide, norm_gain).astype(jnp.bfloat16).astype(jnp.float32)
    queries = jnp.einsum('bsd,dn->bsn', hidden, w_query).astype(jnp.bfloat16).astype(jnp.float32)
    keys_raw = jnp.einsum('bsd,dn->bsn', hidden, w_key).astype(jnp.bfloat16).astype(jnp.float32)
    values = jnp.einsum('bsd,dn->bsn', hidden, w_value).astype(jnp.bfloat16).astype(jnp.float32)
    cos_tab, sin_tab = rope_tables(SEQ_LEN, HEAD_DIM)
    q_rot = norm_rope(queries.reshape(BATCH_ROWS, SEQ_LEN, Q_HEADS, HEAD_DIM), q_gain, cos_tab, sin_tab).astype(jnp.bfloat16).astype(jnp.float32)
    k_rot = norm_rope(keys_raw.reshape(BATCH_ROWS, SEQ_LEN, KV_HEADS, HEAD_DIM), k_gain, cos_tab, sin_tab).astype(jnp.bfloat16).astype(jnp.float32)
    group_size = Q_HEADS // KV_HEADS
    k_heads = jnp.repeat(k_rot, group_size, axis=2)
    v_heads = jnp.repeat(values.reshape(BATCH_ROWS, SEQ_LEN, KV_HEADS, HEAD_DIM), group_size, axis=2)
    causal = jnp.arange(SEQ_LEN)[:, None] >= jnp.arange(SEQ_LEN)[None, :]
    attn_scale = HEAD_DIM ** -0.5

    def one_head(operands):
        q_head, k_head, v_head = operands
        scores = jnp.einsum('bqh,bsh->bqs', q_head, k_head) * attn_scale
        scores = jnp.where(causal, scores, NEG_BIG)
        attn_prob = jax.nn.softmax(scores, axis=-1).astype(jnp.bfloat16).astype(jnp.float32)
        return jnp.einsum('bqs,bsh->bqh', attn_prob, v_head).astype(jnp.bfloat16).astype(jnp.float32)

    head_out = lax.map(jax.checkpoint(one_head), (jnp.moveaxis(q_rot, 2, 0), jnp.moveaxis(k_heads, 2, 0), jnp.moveaxis(v_heads, 2, 0)))
    attn_flat = jnp.moveaxis(head_out, 0, 2).reshape(BATCH_ROWS, SEQ_LEN, Q_HEADS * HEAD_DIM)
    attn_proj = jnp.einsum('bsn,nd->bsd', attn_flat, w_out)
    return (x_wide + attn_proj).astype(jnp.bfloat16)


def reference(tok_ids, embed, norm_gain, q_gain, k_gain, w_query, w_key, w_value, w_out, grad_y):
    x_emb = jnp.take(embed, tok_ids, axis=0)
    y_out, pull_back = jax.vjp(block_forward, x_emb, norm_gain.astype(jnp.float32), q_gain.astype(jnp.float32), k_gain.astype(jnp.float32), w_query.astype(jnp.float32), w_key.astype(jnp.float32), w_value.astype(jnp.float32), w_out.astype(jnp.float32))
    grad_x, grad_norm_gain, grad_q_gain, grad_k_gain, grad_w_query, grad_w_key, grad_w_value, grad_w_out = pull_back(grad_y)
    grad_embed = jax.ops.segment_sum(grad_x.astype(jnp.float32).reshape(-1, D_MODEL), tok_ids.reshape(-1), num_segments=VOCAB_SIZE)
    return (y_out, grad_embed, grad_norm_gain, grad_q_gain, grad_k_gain, grad_w_query, grad_w_key, grad_w_value, grad_w_out)
```

```python
import functools
import jax
import jax.numpy as jnp
from jax import lax
from jax.sharding import PartitionSpec as P

EPS = 1.0e-6
ROPE_BASE = 1.0e6
NEG_BIG = -1.0e30
BF = jnp.bfloat16
F32 = jnp.float32


def rope_tables(seq_len, head_dim):
    half_dim = head_dim // 2
    inv_freq = ROPE_BASE ** (-2.0 * jnp.arange(half_dim, dtype=F32) / head_dim)
    angles = jnp.arange(seq_len, dtype=F32)[:, None] * inv_freq[None, :]
    angles = jnp.concatenate([angles, angles], axis=-1)
    return jnp.cos(angles), jnp.sin(angles)


def rms_scale(wide_in, gain_vec):
    return wide_in * lax.rsqrt(jnp.mean(wide_in * wide_in, axis=-1, keepdims=True) + EPS) * gain_vec


def norm_rope(raw_heads, gain_vec, cos_tab, sin_tab):
    normed = rms_scale(raw_heads.astype(F32), gain_vec)
    half_dim = normed.shape[-1] // 2
    rotated = jnp.concatenate([-normed[..., half_dim:], normed[..., :half_dim]], axis=-1)
    return normed * cos_tab[:, None, :] + rotated * sin_tab[:, None, :]


def mm(spec, a, b):
    return jnp.einsum(spec, a, b, preferred_element_type=F32)


def attention_core(q_four, k_rot, v_three):
    seq_len = q_four.shape[1]
    scores = mm('bqgh,bsh->bgqs', q_four, k_rot) * q_four.shape[-1] ** -0.5
    causal = jnp.arange(seq_len)[:, None] >= jnp.arange(seq_len)[None, :]
    attn_prob = jax.nn.softmax(jnp.where(causal, scores, NEG_BIG), axis=-1)
    prob_bf = attn_prob.astype(BF)
    attn_out = mm('bgqs,bsh->bqgh', prob_bf, v_three).astype(BF)
    return attn_prob, prob_bf, attn_out


def attention_grad(attn_prob, prob_bf, q_four, k_rot, v_three, grad_four):
    attn_scale = q_four.shape[-1] ** -0.5
    grad_prob = mm('bqgh,bsh->bgqs', grad_four, v_three)
    grad_values = mm('bgqs,bqgh->bsh', prob_bf, grad_four).astype(BF)
    grad_scores = (attn_prob * (grad_prob - jnp.sum(attn_prob * grad_prob, axis=-1, keepdims=True)) * attn_scale).astype(BF)
    grad_q_rot = mm('bgqs,bsh->bqgh', grad_scores, k_rot)
    grad_k_rot = mm('bgqs,bqgh->bsh', grad_scores, q_four)
    return grad_q_rot, grad_k_rot, grad_values


def solution(mesh):
    tp = mesh.shape['tp']

    def local_step(tok_ids, embed_loc, norm_gain, q_gain, k_gain, wq, wk, wv, wo, gy_loc):
        rank = lax.axis_index('tp')
        vrows, d_model = embed_loc.shape
        batch, seq = tok_ids.shape
        seq_dev = seq // tp
        vocab = vrows * tp
        hd = q_gain.shape[0]
        qn = wq.shape[1]
        heads = qn // hd
        kn = wk.shape[1]
        share = hd // kn
        toks = batch * seq
        tok_flat = tok_ids.reshape(toks)

        table = lax.all_gather(embed_loc, 'tp', axis=0, tiled=True)
        gy_in = gy_loc
        gy_all = lax.all_gather(gy_in, 'tp', axis=0, tiled=False).reshape(toks, d_model)
        used = jnp.any(tok_flat[None, :] == jnp.arange(vocab, dtype=tok_ids.dtype)[:, None], axis=1)
        hidden = jnp.where(used[:, None], rms_scale(table.astype(F32), norm_gain), 0.0).astype(BF)
        w_all = jnp.concatenate([wq, wk, wv], axis=1)
        rows_all = mm('rd,dn->rn', hidden, w_all).astype(BF)
        onehot = (tok_flat[:, None] == jnp.arange(vocab, dtype=tok_ids.dtype)[None, :]).astype(BF)
        q_tok = mm('tr,rn->tn', onehot, rows_all[:, :qn]).astype(BF)
        kv_t = rows_all[:, qn:].T
        swap1 = [(i, i ^ 1) for i in range(tp)]
        swap2 = [(i, i ^ 2) for i in range(tp)]
        odd = (rank & 1) == 1
        far = (rank & 2) == 2
        kv_s = lax.ppermute(kv_t, 'tp', swap1)
        pair = jnp.where(odd, jnp.stack([kv_s, kv_t]), jnp.stack([kv_t, kv_s]))
        pair_o = lax.ppermute(pair, 'tp', swap2)
        quad = jnp.where(far, jnp.stack([pair_o, pair]), jnp.stack([pair, pair_o]))
        quad = quad.reshape(share, 2, kn, vocab).transpose(1, 0, 2, 3).reshape(2 * hd, vocab)
        kv_tok = mm('tr,nr->tn', onehot, quad).astype(BF)

        cos_tab, sin_tab = rope_tables(seq, hd)
        rope_fn = functools.partial(norm_rope, cos_tab=cos_tab, sin_tab=sin_tab)
        q_wide, q_pull = jax.vjp(rope_fn, q_tok.reshape(batch, seq, heads, hd), q_gain)
        k_wide, k_pull = jax.vjp(rope_fn, kv_tok[:, :hd].reshape(batch, seq, 1, hd), k_gain)
        q_four = q_wide.astype(BF)
        k_rot = k_wide.astype(BF)[:, :, 0]
        v_three = kv_tok[:, hd:].reshape(batch, seq, hd)
        attn_prob, prob_bf, attn_out = attention_core(q_four, k_rot, v_three)
        attn_dev = attn_out.reshape(batch, tp, seq_dev, qn).transpose(1, 0, 2, 3).reshape(toks, qn)

        out_part = mm('tn,nd->td', attn_dev, wo).astype(BF)
        attn_sum = lax.psum_scatter(out_part, 'tp', scatter_dimension=0, tiled=True)
        my_ids = lax.dynamic_slice_in_dim(tok_ids, rank * seq_dev, seq_dev, axis=1)
        x_mine = jnp.take(table, my_ids.reshape(-1), axis=0)
        y_loc = (x_mine.astype(F32) + attn_sum.astype(F32)).astype(BF).reshape(batch, seq_dev, d_model)

        gw_out = mm('tn,td->nd', attn_dev, gy_all)
        grad_attn = mm('td,nd->tn', gy_all, wo).astype(BF)
        grad_four = grad_attn.reshape(tp, batch, seq_dev, qn).transpose(1, 0, 2, 3).reshape(batch, seq, heads, hd)
        gq_rot, gk_rot, g_val = attention_grad(attn_prob, prob_bf, q_four, k_rot, v_three, grad_four)
        gq_raw, gq_gain = q_pull(gq_rot.astype(BF).astype(F32))
        gk_raw, gk_gain = k_pull(gk_rot.astype(BF).astype(F32)[:, :, None])
        gkv_tok = jnp.concatenate([gk_raw.reshape(toks, hd), g_val.reshape(toks, hd)], axis=1)
        gq_rows = mm('tr,tn->rn', onehot, gq_raw.reshape(toks, qn)).astype(BF)
        gkv_t = mm('tn,tr->nr', gkv_tok, onehot).reshape(2, share, kn, vocab).transpose(1, 0, 2, 3)
        gkv_t = gkv_t.reshape(2, 2, 2 * kn, vocab)
        mine1 = jnp.where(odd, gkv_t[:, 1], gkv_t[:, 0])
        send1 = jnp.where(odd, gkv_t[:, 0], gkv_t[:, 1]).astype(BF)
        half = mine1 + lax.ppermute(send1, 'tp', swap1).astype(F32)
        mine2 = jnp.where(far, half[1], half[0])
        send2 = jnp.where(far, half[0], half[1]).astype(BF)
        gkv_rows = (mine2 + lax.ppermute(send2, 'tp', swap2).astype(F32)).astype(BF).T
        g_rows = jnp.concatenate([gq_rows, gkv_rows], axis=1)
        gh_part = mm('rn,dn->rd', g_rows, w_all).astype(BF)
        gh = lax.psum_scatter(gh_part, 'tp', scatter_dimension=0, tiled=True)
        gw_query = mm('rd,rn->dn', hidden, gq_rows)
        gw_kv = mm('rd,rn->dn', hidden, gkv_rows)
        dev_ids = tok_ids.reshape(batch, tp, seq_dev).transpose(1, 0, 2).reshape(toks)
        my_rows = rank * vrows + jnp.arange(vrows, dtype=tok_ids.dtype)
        mine_hot = (my_rows[:, None] == dev_ids[None, :]).astype(BF)
        gy_rows = lax.optimization_barrier(mm('rt,td->rd', mine_hot, gy_all))
        _, norm_pull = jax.vjp(rms_scale, embed_loc.astype(F32), norm_gain)
        gx_norm, gn_gain = norm_pull(gh.astype(F32))
        g_embed = lax.optimization_barrier(gy_rows) + gx_norm
        gains = jnp.concatenate([gn_gain, gq_gain, gk_gain])
        gains = jnp.sum(lax.all_gather(gains, 'tp', axis=0, tiled=False), axis=0)
        return (y_loc, g_embed, gains[:d_model], gains[d_model:d_model + hd], gains[d_model + hd:], gw_query, gw_kv[:, :kn], gw_kv[:, kn:], gw_out)

    in_specs = (P('dp', None), P('tp', None), P(), P(), P(), P(None, 'tp'), P(None, 'tp'), P(None, 'tp'), P('tp', None), P('dp', 'tp', None))
    out_specs = (P('dp', 'tp', None), P(('dp', 'tp'), None), P('dp'), P('dp'), P('dp'), P('dp', 'tp'), P('dp', 'tp'), P('dp', 'tp'), P(('dp', 'tp'), None))
    return jax.shard_map(local_step, mesh=mesh, in_specs=in_specs, out_specs=out_specs, check_vma=False)
```

```python
import functools
import jax
import jax.numpy as jnp
from jax import lax
from jax.experimental import pallas as pl
from jax.experimental.pallas import tpu as pltpu
from jax.sharding import PartitionSpec as P

ROPE_BASE = 1.0e6
NEG_BIG = -1.0e30


BF = jnp.bfloat16
F32 = jnp.float32
EPS = 1.0e-6
MESH = pl.DeviceIdType.MESH
NT = (((1,), (1,)), ((), ()))
NN = (((1,), (0,)), ((), ()))
TN = (((0,), (0,)), ((), ()))


def dotf(a, b, dims=NN):
    return lax.dot_general(a, b, dims, preferred_element_type=F32)


def seat():
    rank = lax.axis_index('tp')
    core = lax.rem(rank, 2)
    return rank, rank // 2, core


def rdma(src, dst, ssem, rsem, dev):
    return pltpu.make_async_remote_copy(src_ref=src, dst_ref=dst, send_sem=ssem, recv_sem=rsem, device_id={'tp': dev}, device_id_type=MESH)


def enter(devs):
    barrier = pltpu.get_barrier_semaphore()
    for dev in devs:
        pl.semaphore_signal(barrier, inc=1, device_id={'tp': dev}, device_id_type=MESH)
    pl.semaphore_wait(barrier, len(devs))


def rms_f32(x, gain):
    return x * lax.rsqrt(jnp.mean(x * x, axis=-1, keepdims=True) + EPS) * gain


def k1_body(nz, embed, wq, wk_t, wv_t, gain, tok_dev, h_out, q_out, kv_out, x_out, table, hbuf, wq_v, wkv_v, kvx, in_sem, h_sem, rs, rr, ss, sr, xs, xr):
    rank, z, core = seat()
    right = 2 * lax.rem(z + 1, nz) + core
    left = 2 * lax.rem(z + nz - 1, nz) + core
    sib = rank + 1 - 2 * core
    par = lax.rem(z, 2)
    far = rank + 2 - 4 * par
    vrows = embed.shape[0]
    kn = wk_t.shape[0]
    half, sub_rows = vrows // 2, vrows // 4
    vocab = vrows * 2 * nz
    events = 2 * nz

    ld = [pltpu.make_async_copy(embed, table.at[pl.ds(pl.multiple_of(rank * vrows, vrows), vrows)], in_sem.at[0]),
          pltpu.make_async_copy(wq, wq_v, in_sem.at[1])]
    for i, w in enumerate((wk_t, wv_t, wk_t, wv_t)):
        ld.append(pltpu.make_async_copy(w, wkv_v.at[pl.ds(i * kn, kn)], in_sem.at[2 + i]))
    for c in ld:
        c.start()
    enter((right, left, sib))
    ld[0].wait()

    def row_of(d, e, c):
        s = e // 2
        zd = lax.rem(z + (nz - s if d == 0 else s), nz)
        return pl.multiple_of(vrows * (2 * zd + c) + half * d + sub_rows * lax.rem(e, 2), sub_rows)

    def chunk(d, e, c):
        return table.at[pl.ds(row_of(d, e, c), sub_rows)]

    def ring(d, e):
        a = chunk(d, e, core)
        return rdma(a, a, rs.at[d, e], rr.at[d, e + 2], right if d == 0 else left)

    def ring_in(d, e):
        a = chunk(d, e, core)
        return rdma(a, a, rs.at[d, e], rr.at[d, e], right if d == 0 else left)

    def side(d, e):
        a = chunk(d, e, core)
        return rdma(a, a, ss.at[d, e], sr.at[d, e], sib)

    def h_copy(slot, i, row):
        return pltpu.make_async_copy(hbuf.at[slot, pl.ds(i * sub_rows, sub_rows)], h_out.at[pl.ds(row, sub_rows)], h_sem.at[slot, i])

    own = 2 * par + core
    lane = lax.broadcasted_iota(jnp.int32, (sub_rows, 4 * kn), 1)

    def work(e):
        slot = lax.rem(e, 2)

        @pl.when(e >= 2)
        def _():
            for i in range(4):
                h_copy(slot, i, row_of(0, e, core)).wait()

        rows = [row_of(d, e, c) for d in (0, 1) for c in (0, 1)]
        for i, row in enumerate(rows):
            x = table[pl.ds(row, sub_rows), :].astype(F32)
            ids = row + lax.broadcasted_iota(jnp.int32, (sub_rows, tok_dev.shape[1]), 0)
            hit = jnp.zeros((sub_rows, tok_dev.shape[1]), F32)
            for j in range(tok_dev.shape[0]):
                hit = jnp.maximum(hit, jnp.where(tok_dev[j:j + 1, :] == ids, 1.0, 0.0))
            used = jnp.max(hit, axis=1, keepdims=True)
            h = jnp.where(used > 0.5, rms_f32(x, gain[...]), 0.0)
            hbuf[slot, pl.ds(i * sub_rows, sub_rows), :] = h.astype(BF)
            h_copy(slot, i, row).start()
        hb = hbuf[slot]
        q = dotf(hb, wq_v[...]).astype(BF)
        kv = dotf(hb, wkv_v[...], NT).astype(BF)
        for i, row in enumerate(rows):
            q_out[pl.ds(row, sub_rows), :] = q[i * sub_rows:(i + 1) * sub_rows]
            upper = row // (vocab // 2)
            r2 = pl.multiple_of(lax.rem(row, vocab // 2), sub_rows)
            new = kv[i * sub_rows:(i + 1) * sub_rows]
            old = kvx[own, pl.ds(r2, sub_rows), :]
            mine = (lane // (2 * kn)) == upper
            kvx[own, pl.ds(r2, sub_rows), :] = jnp.where(mine, new.astype(F32), old.astype(F32)).astype(BF)

    kvx[...] = jnp.zeros_like(kvx)

    def step(e, _):
        @pl.when(e >= 2)
        def _():
            for d in (0, 1):
                ring_in(d, e).wait_recv()

        @pl.when(e < events - 2)
        def _():
            for d in (0, 1):
                ring(d, e).start()
        for d in (0, 1):
            side(d, e).start()

        @pl.when(e == 1)
        def _():
            for c in ld[1:]:
                c.wait()

        @pl.when(e >= 1)
        def _():
            for d in (0, 1):
                side(d, e - 1).wait_recv()
            work(e - 1)
        return 0

    lax.fori_loop(0, events, step, 0)
    for d in (0, 1):
        side(d, events - 1).wait_recv()
    work(events - 1)

    opp = 2 * (1 - par) + core
    to_far = rdma(kvx.at[own], kvx.at[own], xs.at[0], xr.at[0], far)
    to_sib = rdma(kvx.at[own], kvx.at[own], xs.at[1], xr.at[1], sib)
    relay = rdma(kvx.at[opp], kvx.at[opp], xs.at[2], xr.at[2], sib)
    to_far.start()
    to_sib.start()
    mine = jnp.broadcast_to(tok_dev[pl.ds(rank, 1), :].astype(F32), (tok_dev.shape[1], tok_dev.shape[1]))
    col = mine.T.astype(jnp.int32)
    lanes = lax.broadcasted_iota(jnp.int32, col.shape, 1)
    hot = jnp.concatenate([jnp.where(col == lanes + j * col.shape[1], 1.0, 0.0).astype(BF) for j in range(vocab // col.shape[1])], axis=1)
    width = 512 if embed.shape[1] % 512 == 0 else embed.shape[1]

    def pick(j, _):
        cols = pl.ds(pl.multiple_of(j * width, width), width)
        x_out[:, cols] = dotf(hot, table[:, cols]).astype(BF)
        return 0

    lax.fori_loop(0, embed.shape[1] // width, pick, 0)
    to_far.wait_recv()
    relay.start()
    to_sib.wait_recv()
    relay.wait_recv()
    hd = kv_out.shape[1] // 2
    for up in (0, 1):
        acc = None
        for r in range(4):
            l_i = lax.broadcasted_iota(jnp.int32, (4 * kn, 2 * hd), 0) - 2 * kn * up
            m_i = lax.broadcasted_iota(jnp.int32, (4 * kn, 2 * hd), 1)
            is_k = (l_i >= 0) & (l_i < kn) & (m_i == l_i + kn * r)
            is_v = (l_i >= kn) & (l_i < 2 * kn) & (m_i == hd + kn * r + l_i - kn)
            place = jnp.where(is_k | is_v, 1.0, 0.0).astype(BF)
            t = dotf(kvx[r], place)
            acc = t if acc is None else acc + t
        kv_out[up * (vocab // 2):(up + 1) * (vocab // 2), :] = acc.astype(BF)
    for c in (to_far, to_sib, relay):
        c.wait_send()

    def drain(e, _):
        @pl.when(e < events - 2)
        def _():
            for d in (0, 1):
                ring(d, e).wait_send()
        for d in (0, 1):
            side(d, e).wait_send()
        return 0

    lax.fori_loop(0, events, drain, 0)
    for slot in (0, 1):
        for i in range(4):
            h_copy(slot, i, row_of(0, 0, core)).wait()


def gather_project(nz, embed, wq, wk_t, wv_t, gain, tok_dev):
    vrows, d = embed.shape
    vocab = vrows * 2 * nz
    qn = wq.shape[1]
    kn = wk_t.shape[0]
    hd = 4 * kn
    ev = 2 * nz
    dma = pltpu.SemaphoreType.DMA
    anym = pl.BlockSpec(memory_space=pl.ANY)
    vm = pl.BlockSpec(memory_space=pltpu.VMEM)
    return pl.pallas_call(
        functools.partial(k1_body, nz),
        name='gather_project',
        out_shape=(jax.ShapeDtypeStruct((vocab, d), BF), jax.ShapeDtypeStruct((vocab, qn), BF), jax.ShapeDtypeStruct((vocab, 2 * hd), BF), jax.ShapeDtypeStruct((vrows, d), BF)),
        in_specs=[anym, anym, anym, anym, vm, vm],
        out_specs=(anym, vm, vm, vm),
        scratch_shapes=[pltpu.VMEM((vocab, d), BF), pltpu.VMEM((2, vrows, d), BF), pltpu.VMEM((d, qn), BF), pltpu.VMEM((4 * kn, d), BF), pltpu.VMEM((4, vocab // 2, 4 * kn), BF),
                        dma((6,)), dma((2, 4)), dma((2, ev)), dma((2, ev)), dma((2, ev)), dma((2, ev)), dma((3,)), dma((3,))],
        compiler_params=pltpu.CompilerParams(collective_id=0, has_side_effects=True, vmem_limit_bytes=56 * 1024 * 1024),
        cost_estimate=pl.CostEstimate(flops=2 * vocab * d * (qn + 4 * kn), bytes_accessed=4 * vocab * d, transcendentals=0),
    )(embed, wq, wk_t, wv_t, gain, tok_dev)


def rope_tables(seq_len, head_dim):
    half_dim = head_dim // 2
    inv_freq = ROPE_BASE ** (-2.0 * jnp.arange(half_dim, dtype=F32) / head_dim)
    angles = jnp.arange(seq_len, dtype=F32)[:, None] * inv_freq[None, :]
    angles = jnp.concatenate([angles, angles], axis=-1)
    return jnp.cos(angles), jnp.sin(angles)


def rms_scale(wide_in, gain_vec):
    return wide_in * lax.rsqrt(jnp.mean(wide_in * wide_in, axis=-1, keepdims=True) + EPS) * gain_vec


def norm_rope(raw_heads, gain_vec, cos_tab, sin_tab):
    normed = rms_scale(raw_heads.astype(F32), gain_vec)
    half_dim = normed.shape[-1] // 2
    rotated = jnp.concatenate([-normed[..., half_dim:], normed[..., :half_dim]], axis=-1)
    return normed * cos_tab[:, None, :] + rotated * sin_tab[:, None, :]


def mm(spec, a, b):
    return jnp.einsum(spec, a, b, preferred_element_type=F32)


def attention_core(q_four, k_rot, v_three):
    seq_len = q_four.shape[1]
    scores = mm('bqgh,bsh->bgqs', q_four, k_rot) * q_four.shape[-1] ** -0.5
    causal = jnp.arange(seq_len)[:, None] >= jnp.arange(seq_len)[None, :]
    attn_prob = jax.nn.softmax(jnp.where(causal, scores, NEG_BIG), axis=-1)
    prob_bf = attn_prob.astype(BF)
    attn_out = mm('bgqs,bsh->bqgh', prob_bf, v_three).astype(BF)
    return attn_prob, prob_bf, attn_out


def attention_grad(attn_prob, prob_bf, q_four, k_rot, v_three, grad_four):
    attn_scale = q_four.shape[-1] ** -0.5
    grad_prob = mm('bqgh,bsh->bgqs', grad_four, v_three)
    grad_values = mm('bgqs,bqgh->bsh', prob_bf, grad_four).astype(BF)
    grad_scores = (attn_prob * (grad_prob - jnp.sum(attn_prob * grad_prob, axis=-1, keepdims=True)) * attn_scale).astype(BF)
    grad_q_rot = mm('bgqs,bsh->bqgh', grad_scores, k_rot)
    grad_k_rot = mm('bgqs,bqgh->bsh', grad_scores, q_four)
    return grad_q_rot, grad_k_rot, grad_values


def solution(mesh):
    tp = mesh.shape['tp']

    def local_step(tok_ids, embed_loc, norm_gain, q_gain, k_gain, wq, wk, wv, wo, gy_loc):
        rank = lax.axis_index('tp')
        vrows, d_model = embed_loc.shape
        batch, seq = tok_ids.shape
        seq_dev = seq // tp
        vocab = vrows * tp
        hd = q_gain.shape[0]
        qn = wq.shape[1]
        heads = qn // hd
        kn = wk.shape[1]
        share = hd // kn
        toks = batch * seq
        tok_flat = tok_ids.reshape(toks)

        dev_ids = tok_ids.reshape(batch, tp, seq_dev).transpose(1, 0, 2)
        hidden, q_rows, kv_rows, x_mine = gather_project(tp // 2, embed_loc, wq, wk.T, wv.T, norm_gain[None, :], dev_ids.reshape(tp, batch * seq_dev))
        gy_in, q_rows = lax.optimization_barrier((gy_loc, q_rows))
        gy_all = lax.all_gather(gy_in, 'tp', axis=0, tiled=False).reshape(toks, d_model)
        onehot = (tok_flat[:, None] == jnp.arange(vocab, dtype=tok_ids.dtype)[None, :]).astype(BF)
        q_tok = mm('tr,rn->tn', onehot, q_rows).astype(BF)
        kv_tok = mm('tr,rn->tn', onehot, kv_rows).astype(BF)
        w_all = jnp.concatenate([wq, wk, wv], axis=1)
        swap1 = [(i, i ^ 1) for i in range(tp)]
        swap2 = [(i, i ^ 2) for i in range(tp)]
        odd = (rank & 1) == 1
        far = (rank & 2) == 2
        cos_tab, sin_tab = rope_tables(seq, hd)
        rope_fn = functools.partial(norm_rope, cos_tab=cos_tab, sin_tab=sin_tab)
        q_wide, q_pull = jax.vjp(rope_fn, q_tok.reshape(batch, seq, heads, hd), q_gain)
        k_wide, k_pull = jax.vjp(rope_fn, kv_tok[:, :hd].reshape(batch, seq, 1, hd), k_gain)
        q_four = q_wide.astype(BF)
        k_rot = k_wide.astype(BF)[:, :, 0]
        v_three = kv_tok[:, hd:].reshape(batch, seq, hd)
        attn_prob, prob_bf, attn_out = attention_core(q_four, k_rot, v_three)
        attn_dev = attn_out.reshape(batch, tp, seq_dev, qn).transpose(1, 0, 2, 3).reshape(toks, qn)

        out_part = mm('tn,nd->td', attn_dev, wo).astype(BF)
        attn_sum = lax.psum_scatter(out_part, 'tp', scatter_dimension=0, tiled=True)
        y_loc = (x_mine.astype(F32) + attn_sum.astype(F32)).astype(BF).reshape(batch, seq_dev, d_model)

        gw_out = mm('tn,td->nd', attn_dev, gy_all)
        grad_attn = mm('td,nd->tn', gy_all, wo).astype(BF)
        grad_four = grad_attn.reshape(tp, batch, seq_dev, qn).transpose(1, 0, 2, 3).reshape(batch, seq, heads, hd)
        gq_rot, gk_rot, g_val = attention_grad(attn_prob, prob_bf, q_four, k_rot, v_three, grad_four)
        gq_raw, gq_gain = q_pull(gq_rot.astype(BF).astype(F32))
        gk_raw, gk_gain = k_pull(gk_rot.astype(BF).astype(F32)[:, :, None])
        gkv_tok = jnp.concatenate([gk_raw.reshape(toks, hd), g_val.reshape(toks, hd)], axis=1)
        gq_rows = mm('tr,tn->rn', onehot, gq_raw.reshape(toks, qn)).astype(BF)
        gkv_t = mm('tn,tr->nr', gkv_tok, onehot).reshape(2, share, kn, vocab).transpose(1, 0, 2, 3)
        gkv_t = gkv_t.reshape(2, 2, 2 * kn, vocab)
        mine1 = jnp.where(odd, gkv_t[:, 1], gkv_t[:, 0])
        send1 = jnp.where(odd, gkv_t[:, 0], gkv_t[:, 1]).astype(BF)
        half = mine1 + lax.ppermute(send1, 'tp', swap1).astype(F32)
        mine2 = jnp.where(far, half[1], half[0])
        send2 = jnp.where(far, half[0], half[1]).astype(BF)
        gkv_rows = (mine2 + lax.ppermute(send2, 'tp', swap2).astype(F32)).astype(BF).T
        g_rows = jnp.concatenate([gq_rows, gkv_rows], axis=1)
        gh_part = mm('rn,dn->rd', g_rows, w_all).astype(BF)
        gh = lax.psum_scatter(gh_part, 'tp', scatter_dimension=0, tiled=True)
        gw_query = mm('rd,rn->dn', hidden, gq_rows)
        gw_kv = mm('rd,rn->dn', hidden, gkv_rows)
        dev_ids = dev_ids.reshape(toks)
        my_rows = rank * vrows + jnp.arange(vrows, dtype=tok_ids.dtype)
        mine_hot = (my_rows[:, None] == dev_ids[None, :]).astype(BF)
        gy_rows = lax.optimization_barrier(mm('rt,td->rd', mine_hot, gy_all))
        _, norm_pull = jax.vjp(rms_scale, embed_loc.astype(F32), norm_gain)
        gx_norm, gn_gain = norm_pull(gh.astype(F32))
        g_embed = lax.optimization_barrier(gy_rows) + gx_norm
        gains = jnp.concatenate([gn_gain, gq_gain, gk_gain])
        gains = jnp.sum(lax.all_gather(gains, 'tp', axis=0, tiled=False), axis=0)
        return (y_loc, g_embed, gains[:d_model], gains[d_model:d_model + hd], gains[d_model + hd:], gw_query, gw_kv[:, :kn], gw_kv[:, kn:], gw_out)

    in_specs = (P('dp', None), P('tp', None), P(), P(), P(), P(None, 'tp'), P(None, 'tp'), P(None, 'tp'), P('tp', None), P('dp', 'tp', None))
    out_specs = (P('dp', 'tp', None), P(('dp', 'tp'), None), P('dp'), P('dp'), P('dp'), P('dp', 'tp'), P('dp', 'tp'), P('dp', 'tp'), P(('dp', 'tp'), None))
    return jax.shard_map(local_step, mesh=mesh, in_specs=in_specs, out_specs=out_specs, check_vma=False)
```

```python
import functools
import jax
import numpy as np
import jax.numpy as jnp
from jax import lax
from jax.experimental import pallas as pl
from jax.experimental.pallas import tpu as pltpu
from jax.sharding import PartitionSpec as P


BF = jnp.bfloat16
F32 = jnp.float32
EPS = 1.0e-6
ROPE_BASE = 1.0e6
NEG_BIG = -1.0e30
MESH = pl.DeviceIdType.MESH
ANY = pl.BlockSpec(memory_space=pl.ANY)
VM = pl.BlockSpec(memory_space=pltpu.VMEM)
NT = (((1,), (1,)), ((), ()))
NN = (((1,), (0,)), ((), ()))
TN = (((0,), (0,)), ((), ()))


def dotf(a, b, dims=NN):
    return lax.dot_general(a, b, dims, preferred_element_type=F32)


def rdma(src, dst, ssem, rsem, dev):
    return pltpu.make_async_remote_copy(src_ref=src, dst_ref=dst, send_sem=ssem, recv_sem=rsem, device_id={'tp': dev}, device_id_type=MESH)


def enter(devs):
    barrier = pltpu.get_barrier_semaphore()
    for dev in devs:
        pl.semaphore_signal(barrier, inc=1, device_id={'tp': dev}, device_id_type=MESH)
    pl.semaphore_wait(barrier, len(devs))


def rms_f32(x, gain):
    return x * lax.rsqrt(jnp.mean(x * x, axis=-1, keepdims=True) + EPS) * gain


def rope_f32(raw, gain, cos, sin_s):
    n = rms_f32(raw.astype(F32), gain)
    return n * cos + pltpu.roll(n, n.shape[1] // 2, 1) * sin_s


def masked(scores, first):
    r_i = lax.broadcasted_iota(jnp.int32, scores.shape, 0) + first
    c_i = lax.broadcasted_iota(jnp.int32, scores.shape, 1)
    return jnp.where(r_i >= c_i, scores, NEG_BIG)


def soft(scores):
    e = jnp.exp(scores - jnp.max(scores, axis=-1, keepdims=True))
    return e * (1.0 / jnp.sum(e, axis=-1, keepdims=True))


def ka_body(nz, embed, gy, wq, wk_t, wv_t, wo, gain, qg, kg, cos, sin_s, tok_dev, tok_seq,
            h_out, gy_out, q_tok, kv_tok, q_rot, k_rot, o_out, do_out, x_out,
            table, hbuf, wq_v, wkv_v, wo_v, idcol, kvacc, kvx, gown, gbuf,
            in_sem, h_sem, g_sem, rs, rr, ss, sr, rs2, rr2, ss2, sr2, xs, xr):
    rank = lax.axis_index('tp')
    z, core = rank // 2, lax.rem(rank, 2)
    right = 2 * lax.rem(z + 1, nz) + core
    left = 2 * lax.rem(z + nz - 1, nz) + core
    sib = rank + 1 - 2 * core
    par = lax.rem(z, 2)
    far = rank + 2 - 4 * par
    vrows = embed.shape[0]
    kn = wk_t.shape[0]
    half, sub_rows = vrows // 2, vrows // 4
    vocab = vrows * 2 * nz
    batch, seq = tok_seq.shape
    toks = batch * seq
    qn = wq.shape[1]
    hd = qg.shape[1]
    heads = qn // hd
    events = 2 * nz
    pos = seq // (2 * nz)

    ld = [pltpu.make_async_copy(embed, table.at[pl.ds(pl.multiple_of(rank * vrows, vrows), vrows)], in_sem.at[0]),
          pltpu.make_async_copy(gy, gown, in_sem.at[1]),
          pltpu.make_async_copy(wq, wq_v, in_sem.at[2]),
          pltpu.make_async_copy(wo, wo_v, in_sem.at[3])]
    for i, w in enumerate((wk_t, wv_t, wk_t, wv_t)):
        ld.append(pltpu.make_async_copy(w, wkv_v.at[pl.ds(i * kn, kn)], in_sem.at[4 + i]))
    for c in ld:
        c.start()
    enter((right, left, sib))
    ld[0].wait()

    def zd_of(d, e):
        s = e // 2
        return lax.rem(z + (nz - s if d == 0 else s), nz)

    def row_of(d, e, c):
        return pl.multiple_of(vrows * (2 * zd_of(d, e) + c) + half * d + sub_rows * lax.rem(e, 2), sub_rows)

    def ring(d, e, recv_e):
        a = table.at[pl.ds(row_of(d, e, core), sub_rows)]
        return rdma(a, a, rs.at[d, e], rr.at[d, recv_e], right if d == 0 else left)

    def side(d, e):
        a = table.at[pl.ds(row_of(d, e, core), sub_rows)]
        return rdma(a, a, ss.at[d, e], sr.at[d, e], sib)

    def h_copy(slot, i, row):
        return pltpu.make_async_copy(hbuf.at[slot, pl.ds(i * sub_rows, sub_rows)], h_out.at[pl.ds(row, sub_rows)], h_sem.at[slot, i])

    def g_row(d, e, c):
        return pl.multiple_of(seq * (2 * d + lax.rem(e, 2)) + pos * (2 * zd_of(d, e) + c), pos)

    def g_piece(d, e, c):
        return gy_out.at[pl.ds(g_row(d, e, c), pos)]

    def g_own(d, e):
        return gown.at[pl.ds(pl.multiple_of(pos * (2 * d + lax.rem(e, 2)), pos), pos)]

    def g_ring(d, e, recv_e, first):
        a = g_piece(d, e, core)
        return rdma(g_own(d, e) if first else a, a, rs2.at[d, e], rr2.at[d, recv_e], right if d == 0 else left)

    def g_side(d, e, first):
        a = g_piece(d, e, core)
        return rdma(g_own(d, e) if first else a, a, ss2.at[d, e], sr2.at[d, e], sib)

    def g_home(d, e):
        return pltpu.make_async_copy(g_own(d, e), g_piece(d, e, core), in_sem.at[8 + 2 * d + e])

    def g_load(slot, i, d, c, e):
        return pltpu.make_async_copy(g_piece(d, e, c), gbuf.at[slot, pl.ds(i * pos, pos)], g_sem.at[slot, i])

    for b in range(batch):
        wide = jnp.broadcast_to(tok_seq[b:b + 1, :].astype(F32), (idcol.shape[1], seq))
        idcol[b * seq:(b + 1) * seq, :] = wide.T.astype(jnp.int32)
    q_tok[...] = jnp.zeros_like(q_tok)
    kvacc[...] = jnp.zeros_like(kvacc)

    def work(e):
        slot = lax.rem(e, 2)

        @pl.when(e >= 2)
        def _():
            for i in range(4):
                h_copy(slot, i, row_of(0, e, core)).wait()

        rows = [row_of(d, e, c) for d in (0, 1) for c in (0, 1)]
        for i, row in enumerate(rows):
            x = table[pl.ds(row, sub_rows), :].astype(F32)
            ids = row + lax.broadcasted_iota(jnp.int32, (sub_rows, tok_dev.shape[1]), 0)
            hit = jnp.zeros((sub_rows, tok_dev.shape[1]), F32)
            for j in range(tok_dev.shape[0]):
                hit = jnp.maximum(hit, jnp.where(tok_dev[j:j + 1, :] == ids, 1.0, 0.0))
            used = jnp.max(hit, axis=1, keepdims=True)
            h = jnp.where(used > 0.5, rms_f32(x, gain[...]), 0.0)
            hbuf[slot, pl.ds(i * sub_rows, sub_rows), :] = h.astype(BF)
            h_copy(slot, i, row).start()
        hb = hbuf[slot]
        qkv = jnp.concatenate([dotf(hb, wq_v[...]).astype(BF), dotf(hb, wkv_v[...], NT).astype(BF)], axis=1)
        lane = lax.broadcasted_iota(jnp.int32, (1, vrows), 1)
        rowid = jnp.zeros((1, vrows), jnp.int32)
        for i, row in enumerate(rows):
            rowid = jnp.where(lane // sub_rows == i, row + lane - i * sub_rows, rowid)
        for b in range(batch):
            sl = slice(b * seq, (b + 1) * seq)
            hot = jnp.where(idcol[sl, :] == rowid, 1.0, 0.0).astype(BF)
            got = dotf(hot, qkv)
            q_tok[sl, :] = (q_tok[sl, :].astype(F32) + got[:, :qn]).astype(BF)
            kvacc[sl, :] = (kvacc[sl, :].astype(F32) + got[:, qn:]).astype(BF)

    def step_a(e, _):
        @pl.when((e >= 2) & (e < events))
        def _():
            for d in (0, 1):
                ring(d, e, e).wait_recv()

        @pl.when(e < events - 2)
        def _():
            for d in (0, 1):
                ring(d, e, e + 2).start()

        @pl.when(e < events)
        def _():
            for d in (0, 1):
                side(d, e).start()

        @pl.when(e == 1)
        def _():
            for c in ld[1:]:
                c.wait()
            for d in (0, 1):
                for k in (0, 1):
                    g_home(d, k).start()

        @pl.when(e == events - 2)
        def _():
            for d in (0, 1):
                g_ring(d, 0, 2, True).start()

        @pl.when(e >= 1)
        def _():
            for d in (0, 1):
                side(d, e - 1).wait_recv()
            work(e - 1)
        return 0

    lax.fori_loop(0, events + 1, step_a, 0)

    own = 2 * par + core
    opp = 2 * (1 - par) + core
    low = lax.broadcasted_iota(jnp.int32, (toks // 2, 4 * kn), 1) < 2 * kn
    kvx[own] = jnp.where(low, kvacc[:toks // 2, :].astype(F32), kvacc[toks // 2:, :].astype(F32)).astype(BF)
    to_far = rdma(kvx.at[own], kvx.at[own], xs.at[0], xr.at[0], far)
    to_sib = rdma(kvx.at[own], kvx.at[own], xs.at[1], xr.at[1], sib)
    relay = rdma(kvx.at[opp], kvx.at[opp], xs.at[2], xr.at[2], sib)
    mine = jnp.broadcast_to(tok_dev[pl.ds(rank, 1), :].astype(F32), (vrows, tok_dev.shape[1]))
    col = mine.T.astype(jnp.int32)
    lanes = lax.broadcasted_iota(jnp.int32, col.shape, 1)
    hot_mine = jnp.concatenate([jnp.where(col == lanes + j * vrows, 1.0, 0.0).astype(BF) for j in range(vocab // vrows)], axis=1)
    to_far.start()
    to_sib.start()
    for d in (0, 1):
        g_ring(d, 1, 3, True).start()
        for k in (0, 1):
            g_side(d, k, True).start()
            g_home(d, k).wait()
    width = min(512, embed.shape[1])

    def pick(j, _):
        cols = pl.ds(pl.multiple_of(j * width, width), width)
        x_out[:, cols] = dotf(hot_mine, table[:, cols]).astype(BF)
        return 0

    lax.fori_loop(0, embed.shape[1] // width, pick, 0)
    to_far.wait_recv()
    relay.start()
    to_sib.wait_recv()
    relay.wait_recv()
    for up in (0, 1):
        acc = None
        for r in range(4):
            l_i = lax.broadcasted_iota(jnp.int32, (4 * kn, 2 * hd), 0) - 2 * kn * up
            m_i = lax.broadcasted_iota(jnp.int32, (4 * kn, 2 * hd), 1)
            is_k = (l_i >= 0) & (l_i < kn) & (m_i == l_i + kn * r)
            is_v = (l_i >= kn) & (l_i < 2 * kn) & (m_i == hd + kn * r + l_i - kn)
            t = dotf(kvx[r], jnp.where(is_k | is_v, 1.0, 0.0).astype(BF))
            acc = t if acc is None else acc + t
        kv_tok[up * (toks // 2):(up + 1) * (toks // 2), :] = acc.astype(BF)
    for b in range(batch):
        sl = slice(b * seq, (b + 1) * seq)
        k_rot[sl, :] = rope_f32(kv_tok[sl, :hd], kg[...], cos[...], sin_s[...]).astype(BF)

    scale = hd ** -0.5
    blk = seq // 2

    def unit(u, _):
        rows = pl.ds(pl.multiple_of((u // heads) * seq, seq), seq)
        cols = pl.ds(pl.multiple_of(lax.rem(u, heads) * hd, hd), hd)
        qr = rope_f32(q_tok[rows, cols], qg[...], cos[...], sin_s[...]).astype(BF)
        q_rot[rows, cols] = qr
        kr = k_rot[rows, :]
        v = kv_tok[rows, hd:]
        for i in (0, 1):
            n = blk * (i + 1)
            s = masked(dotf(qr[i * blk:(i + 1) * blk], kr[:n], NT) * scale, i * blk)
            o = dotf(soft(s).astype(BF), v[:n]).astype(BF)
            o_out[pl.ds(pl.multiple_of((u // heads) * seq + i * blk, blk), blk), cols] = o
        return 0

    def do_work(e):
        slot = lax.rem(e, 2)
        places = [(d, c) for d in (0, 1) for c in (0, 1)]
        for i, (d, c) in enumerate(places):
            g_load(slot, i, d, c, e).wait()
        r = dotf(gbuf[slot], wo_v[...], NT).astype(BF)
        for i, (d, c) in enumerate(places):
            do_out[pl.ds(g_row(d, e, c), pos), :] = r[i * pos:(i + 1) * pos]

    units = batch * heads
    slots = events - 3

    def step_b(e, _):
        @pl.when((e >= 2) & (e < events))
        def _():
            for d in (0, 1):
                g_ring(d, e, e, False).wait_recv()

        @pl.when((e >= 2) & (e < events - 2))
        def _():
            for d in (0, 1):
                g_ring(d, e, e + 2, False).start()

        @pl.when((e >= 2) & (e < events))
        def _():
            for d in (0, 1):
                g_side(d, e, False).start()

        @pl.when((e >= 1) & (e <= events))
        def _():
            for d in (0, 1):
                g_side(d, e - 1, False).wait_recv()
            for i, (d, c) in enumerate([(d, c) for d in (0, 1) for c in (0, 1)]):
                g_load(lax.rem(e - 1, 2), i, d, c, e - 1).start()

        lax.fori_loop(jnp.minimum((e * units) // slots, units), jnp.minimum(((e + 1) * units) // slots, units), unit, 0)

        @pl.when(e >= 2)
        def _():
            do_work(e - 2)
        return 0

    lax.fori_loop(0, events + 2, step_b, 0)

    for c in (to_far, to_sib, relay):
        c.wait_send()

    def drain(e, _):
        @pl.when(e < events - 2)
        def _():
            for d in (0, 1):
                ring(d, e, e + 2).wait_send()
                g_ring(d, e, e + 2, False).wait_send()
        for d in (0, 1):
            side(d, e).wait_send()
            g_side(d, e, False).wait_send()
        return 0

    lax.fori_loop(0, events, drain, 0)
    for slot in (0, 1):
        for i in range(4):
            h_copy(slot, i, row_of(0, 0, core)).wait()


def forward_kernel(nz, embed, gy, wq, wk_t, wv_t, wo, gain, qg, kg, cos, sin_s, tok_dev, tok_seq):
    vrows, d = embed.shape
    vocab = vrows * 2 * nz
    qn, kn = wq.shape[1], wk_t.shape[0]
    hd = qg.shape[1]
    batch, seq = tok_seq.shape
    toks = batch * seq
    ev = 2 * nz
    dma = pltpu.SemaphoreType.DMA

    def arr(*shape):
        return jax.ShapeDtypeStruct(shape, BF)

    return pl.pallas_call(
        functools.partial(ka_body, nz),
        name='forward_kernel',
        out_shape=(arr(vocab, d), arr(toks, d), arr(toks, qn), arr(toks, 2 * hd), arr(toks, qn), arr(toks, hd), arr(toks, qn), arr(toks, qn), arr(vrows, d)),
        in_specs=[ANY] * 6 + [VM] * 7,
        out_specs=(ANY, ANY) + (VM,) * 7,
        scratch_shapes=[pltpu.VMEM((vocab, d), BF), pltpu.VMEM((2, vrows, d), BF), pltpu.VMEM((d, qn), BF), pltpu.VMEM((4 * kn, d), BF), pltpu.VMEM((qn, d), BF),
                        pltpu.VMEM((toks, vrows), jnp.int32), pltpu.VMEM((toks, 4 * kn), BF), pltpu.VMEM((4, toks // 2, 4 * kn), BF), pltpu.VMEM((vrows, d), BF), pltpu.VMEM((2, vrows, d), BF),
                        dma((12,)), dma((2, 4)), dma((2, 4))] + [dma((2, ev))] * 8 + [dma((3,)), dma((3,))],
        compiler_params=pltpu.CompilerParams(collective_id=0, has_side_effects=True, vmem_limit_bytes=62 * 1024 * 1024),
        cost_estimate=pl.CostEstimate(flops=2 * vocab * d * (2 * qn + 4 * kn), bytes_accessed=8 * vocab * d, transcendentals=0),
    )(embed, gy, wq, wk_t, wv_t, wo, gain, qg, kg, cos, sin_s, tok_dev, tok_seq)


def rope_consts(seq, hd):
    inv = np.float32(ROPE_BASE) ** (np.float32(-2.0) * np.arange(hd // 2, dtype=np.float32) / np.float32(hd))
    ang = np.arange(seq, dtype=np.float32)[:, None] * inv.astype(np.float32)[None, :]
    ang = np.concatenate([ang, ang], axis=-1)
    sign = np.where(np.arange(hd) < hd // 2, -1.0, 1.0).astype(np.float32)
    return np.cos(ang).astype(np.float32), (np.sin(ang) * sign).astype(np.float32)


def rope_tables(seq_len, head_dim):
    half_dim = head_dim // 2
    inv_freq = ROPE_BASE ** (-2.0 * jnp.arange(half_dim, dtype=F32) / head_dim)
    angles = jnp.arange(seq_len, dtype=F32)[:, None] * inv_freq[None, :]
    angles = jnp.concatenate([angles, angles], axis=-1)
    return jnp.cos(angles), jnp.sin(angles)


def rms_scale(wide_in, gain_vec):
    return wide_in * lax.rsqrt(jnp.mean(wide_in * wide_in, axis=-1, keepdims=True) + EPS) * gain_vec


def norm_rope(raw_heads, gain_vec, cos_tab, sin_tab):
    normed = rms_scale(raw_heads.astype(F32), gain_vec)
    half_dim = normed.shape[-1] // 2
    rotated = jnp.concatenate([-normed[..., half_dim:], normed[..., :half_dim]], axis=-1)
    return normed * cos_tab[:, None, :] + rotated * sin_tab[:, None, :]


def mm(spec, a, b):
    return jnp.einsum(spec, a, b, preferred_element_type=F32)


def attention_core(q_four, k_rot, v_three):
    seq_len = q_four.shape[1]
    scores = mm('bqgh,bsh->bgqs', q_four, k_rot) * q_four.shape[-1] ** -0.5
    causal = jnp.arange(seq_len)[:, None] >= jnp.arange(seq_len)[None, :]
    attn_prob = jax.nn.softmax(jnp.where(causal, scores, NEG_BIG), axis=-1)
    prob_bf = attn_prob.astype(BF)
    attn_out = mm('bgqs,bsh->bqgh', prob_bf, v_three).astype(BF)
    return attn_prob, prob_bf, attn_out


def attention_grad(attn_prob, prob_bf, q_four, k_rot, v_three, grad_four):
    attn_scale = q_four.shape[-1] ** -0.5
    grad_prob = mm('bqgh,bsh->bgqs', grad_four, v_three)
    grad_values = mm('bgqs,bqgh->bsh', prob_bf, grad_four).astype(BF)
    grad_scores = (attn_prob * (grad_prob - jnp.sum(attn_prob * grad_prob, axis=-1, keepdims=True)) * attn_scale).astype(BF)
    grad_q_rot = mm('bgqs,bsh->bqgh', grad_scores, k_rot)
    grad_k_rot = mm('bgqs,bqgh->bsh', grad_scores, q_four)
    return grad_q_rot, grad_k_rot, grad_values


def solution(mesh):
    tp = mesh.shape['tp']

    def local_step(tok_ids, embed_loc, norm_gain, q_gain, k_gain, wq, wk, wv, wo, gy_loc):
        rank = lax.axis_index('tp')
        vrows, d_model = embed_loc.shape
        batch, seq = tok_ids.shape
        seq_dev = seq // tp
        vocab = vrows * tp
        hd = q_gain.shape[0]
        qn = wq.shape[1]
        heads = qn // hd
        kn = wk.shape[1]
        share = hd // kn
        toks = batch * seq
        tok_flat = tok_ids.reshape(toks)

        cos_c, sin_c = rope_consts(seq, hd)
        dev_ids = tok_ids.reshape(batch, tp, seq_dev).transpose(1, 0, 2)
        hidden, gy_all, q_tok, kv_tok, q_rot, k_rot, attn_flat, grad_attn, x_mine = forward_kernel(
            tp // 2, embed_loc, gy_loc.reshape(batch * seq_dev, d_model), wq, wk.T, wv.T, wo, norm_gain[None, :], q_gain[None, :], k_gain[None, :],
            jnp.asarray(cos_c), jnp.asarray(sin_c), dev_ids.reshape(tp, batch * seq_dev), tok_ids)
        onehot = (tok_flat[:, None] == jnp.arange(vocab, dtype=tok_ids.dtype)[None, :]).astype(BF)
        w_all = jnp.concatenate([wq, wk, wv], axis=1)
        swap1 = [(i, i ^ 1) for i in range(tp)]
        swap2 = [(i, i ^ 2) for i in range(tp)]
        odd = (rank & 1) == 1
        far = (rank & 2) == 2
        cos_tab, sin_tab = rope_tables(seq, hd)
        rope_fn = functools.partial(norm_rope, cos_tab=cos_tab, sin_tab=sin_tab)
        _, q_pull = jax.vjp(rope_fn, q_tok.reshape(batch, seq, heads, hd), q_gain)
        _, k_pull = jax.vjp(rope_fn, kv_tok[:, :hd].reshape(batch, seq, 1, hd), k_gain)
        q_four = q_rot.reshape(batch, seq, heads, hd)
        k_rot = k_rot.reshape(batch, seq, hd)
        v_three = kv_tok[:, hd:].reshape(batch, seq, hd)
        attn_prob, prob_bf, _ = attention_core(q_four, k_rot, v_three)
        attn_dev = attn_flat.reshape(batch, tp, seq_dev, qn).transpose(1, 0, 2, 3).reshape(toks, qn)

        out_part = mm('tn,nd->td', attn_dev, wo).astype(BF)
        attn_sum = lax.psum_scatter(out_part, 'tp', scatter_dimension=0, tiled=True)
        y_loc = (x_mine.astype(F32) + attn_sum.astype(F32)).astype(BF).reshape(batch, seq_dev, d_model)

        gw_out = mm('tn,td->nd', attn_flat, gy_all)
        grad_four = grad_attn.reshape(batch, seq, heads, hd)
        gq_rot, gk_rot, g_val = attention_grad(attn_prob, prob_bf, q_four, k_rot, v_three, grad_four)
        gq_raw, gq_gain = q_pull(gq_rot.astype(BF).astype(F32))
        gk_raw, gk_gain = k_pull(gk_rot.astype(BF).astype(F32)[:, :, None])
        gkv_tok = jnp.concatenate([gk_raw.reshape(toks, hd), g_val.reshape(toks, hd)], axis=1)
        gq_rows = mm('tr,tn->rn', onehot, gq_raw.reshape(toks, qn)).astype(BF)
        gkv_t = mm('tn,tr->nr', gkv_tok, onehot).reshape(2, share, kn, vocab).transpose(1, 0, 2, 3)
        gkv_t = gkv_t.reshape(2, 2, 2 * kn, vocab)
        mine1 = jnp.where(odd, gkv_t[:, 1], gkv_t[:, 0])
        send1 = jnp.where(odd, gkv_t[:, 0], gkv_t[:, 1]).astype(BF)
        half = mine1 + lax.ppermute(send1, 'tp', swap1).astype(F32)
        mine2 = jnp.where(far, half[1], half[0])
        send2 = jnp.where(far, half[0], half[1]).astype(BF)
        gkv_rows = (mine2 + lax.ppermute(send2, 'tp', swap2).astype(F32)).astype(BF).T
        g_rows = jnp.concatenate([gq_rows, gkv_rows], axis=1)
        gh_part = mm('rn,dn->rd', g_rows, w_all).astype(BF)
        gh = lax.psum_scatter(gh_part, 'tp', scatter_dimension=0, tiled=True)
        gw_query = mm('rd,rn->dn', hidden, gq_rows)
        gw_kv = mm('rd,rn->dn', hidden, gkv_rows)
        my_rows = rank * vrows + jnp.arange(vrows, dtype=tok_ids.dtype)
        mine_hot = (my_rows[:, None] == tok_flat[None, :]).astype(BF)
        gy_rows = lax.optimization_barrier(mm('rt,td->rd', mine_hot, gy_all))
        _, norm_pull = jax.vjp(rms_scale, embed_loc.astype(F32), norm_gain)
        gx_norm, gn_gain = norm_pull(gh.astype(F32))
        g_embed = lax.optimization_barrier(gy_rows) + gx_norm
        gains = jnp.concatenate([gn_gain, gq_gain, gk_gain])
        gains = jnp.sum(lax.all_gather(gains, 'tp', axis=0, tiled=False), axis=0)
        return (y_loc, g_embed, gains[:d_model], gains[d_model:d_model + hd], gains[d_model + hd:], gw_query, gw_kv[:, :kn], gw_kv[:, kn:], gw_out)

    in_specs = (P('dp', None), P('tp', None), P(), P(), P(), P(None, 'tp'), P(None, 'tp'), P(None, 'tp'), P('tp', None), P('dp', 'tp', None))
    out_specs = (P('dp', 'tp', None), P(('dp', 'tp'), None), P('dp'), P('dp'), P('dp'), P('dp', 'tp'), P('dp', 'tp'), P('dp', 'tp'), P(('dp', 'tp'), None))
    return jax.shard_map(local_step, mesh=mesh, in_specs=in_specs, out_specs=out_specs, check_vma=False)
```

```python
import functools
import jax
import jax.numpy as jnp
import numpy as np
from jax import lax
from jax.experimental import pallas as pl
from jax.experimental.pallas import tpu as pltpu
from jax.sharding import PartitionSpec as P

BF = jnp.bfloat16
F32 = jnp.float32
EPS = 1.0e-6
ROPE_BASE = 1.0e6
NEG_BIG = -1.0e30
MESH = pl.DeviceIdType.MESH
ANY = pl.BlockSpec(memory_space=pl.ANY)
VM = pl.BlockSpec(memory_space=pltpu.VMEM)
NT = (((1,), (1,)), ((), ()))
NN = (((1,), (0,)), ((), ()))
TN = (((0,), (0,)), ((), ()))


def dotf(a, b, dims=NN):
    return lax.dot_general(a, b, dims, preferred_element_type=F32)


def rdma(src, dst, ssem, rsem, dev):
    return pltpu.make_async_remote_copy(src_ref=src, dst_ref=dst, send_sem=ssem, recv_sem=rsem, device_id={'tp': dev}, device_id_type=MESH)


def enter(devs):
    barrier = pltpu.get_barrier_semaphore()
    for dev in devs:
        pl.semaphore_signal(barrier, inc=1, device_id={'tp': dev}, device_id_type=MESH)
    pl.semaphore_wait(barrier, len(devs))


def rms_f32(x, gain):
    return x * lax.rsqrt(jnp.mean(x * x, axis=-1, keepdims=True) + EPS) * gain


def rope_f32(raw, gain, cos, sin_s):
    n = rms_f32(raw.astype(F32), gain)
    return n * cos + pltpu.roll(n, n.shape[1] // 2, 1) * sin_s


def masked(scores, first):
    r_i = lax.broadcasted_iota(jnp.int32, scores.shape, 0) + first
    c_i = lax.broadcasted_iota(jnp.int32, scores.shape, 1)
    return jnp.where(r_i >= c_i, scores, NEG_BIG)


def soft(scores):
    e = jnp.exp(scores - jnp.max(scores, axis=-1, keepdims=True))
    return e * (1.0 / jnp.sum(e, axis=-1, keepdims=True))


def ka_body(nz, embed, gy, wq, wk_t, wv_t, wo, gain, qg, kg, cos, sin_s, tok_dev, tok_seq,
            h_out, gy_out, osib_out, wosib_out, wqt_out, wqtsib_out, wkvsib_out, q_tok, kv_tok, q_rot, k_rot, o_out, do_out, x_out,
            table, hbuf, wq_v, wkv_v, wo_v, idcol, kvacc, kvx, gown, gbuf, tbuf,
            in_sem, h_sem, g_sem, rs, rr, ss, sr, rs2, rr2, ss2, sr2, xs, xr, ts, wos, wor, wqs, wqr, wks, wkr, os_, or_):
    rank = lax.axis_index('tp')
    z, core = rank // 2, lax.rem(rank, 2)
    right = 2 * lax.rem(z + 1, nz) + core
    left = 2 * lax.rem(z + nz - 1, nz) + core
    sib = rank + 1 - 2 * core
    par = lax.rem(z, 2)
    far = rank + 2 - 4 * par
    vrows = embed.shape[0]
    kn = wk_t.shape[0]
    half, sub_rows = vrows // 2, vrows // 4
    vocab = vrows * 2 * nz
    batch, seq = tok_seq.shape
    toks = batch * seq
    qn = wq.shape[1]
    hd = qg.shape[1]
    heads = qn // hd
    events = 2 * nz
    pos = seq // (2 * nz)

    ld = [pltpu.make_async_copy(embed, table.at[pl.ds(pl.multiple_of(rank * vrows, vrows), vrows)], in_sem.at[0]),
          pltpu.make_async_copy(gy, gown, in_sem.at[1]),
          pltpu.make_async_copy(wq, wq_v, in_sem.at[2]),
          pltpu.make_async_copy(wo, wo_v, in_sem.at[3])]
    for i, w in enumerate((wk_t, wv_t, wk_t, wv_t)):
        ld.append(pltpu.make_async_copy(w, wkv_v.at[pl.ds(i * kn, kn)], in_sem.at[4 + i]))
    for c in ld:
        c.start()
    enter((right, left, sib))
    ld[0].wait()

    def zd_of(d, e):
        s = e // 2
        return lax.rem(z + (nz - s if d == 0 else s), nz)

    def row_of(d, e, c):
        return pl.multiple_of(vrows * (2 * zd_of(d, e) + c) + half * d + sub_rows * lax.rem(e, 2), sub_rows)

    def ring(d, e, recv_e):
        a = table.at[pl.ds(row_of(d, e, core), sub_rows)]
        return rdma(a, a, rs.at[d, e], rr.at[d, recv_e], right if d == 0 else left)

    def side(d, e):
        a = table.at[pl.ds(row_of(d, e, core), sub_rows)]
        return rdma(a, a, ss.at[d, e], sr.at[d, e], sib)

    def h_copy(slot, i, row):
        return pltpu.make_async_copy(hbuf.at[slot, pl.ds(i * sub_rows, sub_rows)], h_out.at[pl.ds(row, sub_rows)], h_sem.at[slot, i])

    def g_row(d, e, c):
        return pl.multiple_of(seq * (2 * d + lax.rem(e, 2)) + pos * (2 * zd_of(d, e) + c), pos)

    def g_piece(d, e, c):
        return gy_out.at[pl.ds(g_row(d, e, c), pos)]

    def g_own(d, e):
        return gown.at[pl.ds(pl.multiple_of(pos * (2 * d + lax.rem(e, 2)), pos), pos)]

    def g_ring(d, e, recv_e, first):
        a = g_piece(d, e, core)
        return rdma(g_own(d, e) if first else a, a, rs2.at[d, e], rr2.at[d, recv_e], right if d == 0 else left)

    def g_side(d, e, first):
        a = g_piece(d, e, core)
        return rdma(g_own(d, e) if first else a, a, ss2.at[d, e], sr2.at[d, e], sib)

    def g_home(d, e):
        return pltpu.make_async_copy(g_own(d, e), g_piece(d, e, core), in_sem.at[8 + 2 * d + e])

    def g_load(slot, i, d, c, e):
        return pltpu.make_async_copy(g_piece(d, e, c), gbuf.at[slot, pl.ds(i * pos, pos)], g_sem.at[slot, i])

    parts = 8
    wo_p, wq_p = qn // parts, embed.shape[1] // parts

    def wo_push(k):
        rows = pl.ds(pl.multiple_of(k * wo_p, wo_p), wo_p)
        return rdma(wo.at[rows], wosib_out.at[rows], wos.at[k], wor.at[k], sib)

    def wq_push(k):
        cols = pl.ds(pl.multiple_of(k * wq_p, wq_p), wq_p)
        return rdma(tbuf.at[lax.rem(k, 2)], wqtsib_out.at[:, cols], wqs.at[k], wqr.at[k], sib)

    def wq_home(k):
        cols = pl.ds(pl.multiple_of(k * wq_p, wq_p), wq_p)
        return pltpu.make_async_copy(tbuf.at[lax.rem(k, 2)], wqt_out.at[:, cols], ts.at[k])

    def wk_push(k):
        return rdma((wk_t, wv_t)[k], wkvsib_out.at[pl.ds(k * kn, kn)], wks.at[k], wkr.at[k], sib)

    def o_push(b):
        rows = pl.ds(pl.multiple_of(b * seq, seq), seq)
        return rdma(o_out.at[rows], osib_out.at[rows], os_.at[b], or_.at[b], sib)

    for b in range(batch):
        wide = jnp.broadcast_to(tok_seq[b:b + 1, :].astype(F32), (idcol.shape[1], seq))
        idcol[b * seq:(b + 1) * seq, :] = wide.T.astype(jnp.int32)
    q_tok[...] = jnp.zeros_like(q_tok)
    kvacc[...] = jnp.zeros_like(kvacc)

    def work(e):
        slot = lax.rem(e, 2)

        @pl.when(e >= 2)
        def _():
            for i in range(4):
                h_copy(slot, i, row_of(0, e, core)).wait()

        rows = [row_of(d, e, c) for d in (0, 1) for c in (0, 1)]
        for i, row in enumerate(rows):
            x = table[pl.ds(row, sub_rows), :].astype(F32)
            ids = row + lax.broadcasted_iota(jnp.int32, (sub_rows, tok_dev.shape[1]), 0)
            hit = jnp.zeros((sub_rows, tok_dev.shape[1]), F32)
            for j in range(tok_dev.shape[0]):
                hit = jnp.maximum(hit, jnp.where(tok_dev[j:j + 1, :] == ids, 1.0, 0.0))
            used = jnp.max(hit, axis=1, keepdims=True)
            h = jnp.where(used > 0.5, rms_f32(x, gain[...]), 0.0)
            hbuf[slot, pl.ds(i * sub_rows, sub_rows), :] = h.astype(BF)
            h_copy(slot, i, row).start()
        hb = hbuf[slot]
        qkv = jnp.concatenate([dotf(hb, wq_v[...]).astype(BF), dotf(hb, wkv_v[...], NT).astype(BF)], axis=1)
        lane = lax.broadcasted_iota(jnp.int32, (1, vrows), 1)
        rowid = jnp.zeros((1, vrows), jnp.int32)
        for i, row in enumerate(rows):
            rowid = jnp.where(lane // sub_rows == i, row + lane - i * sub_rows, rowid)
        for b in range(batch):
            sl = slice(b * seq, (b + 1) * seq)
            hot = jnp.where(idcol[sl, :] == rowid, 1.0, 0.0).astype(BF)
            got = dotf(hot, qkv)
            q_tok[sl, :] = (q_tok[sl, :].astype(F32) + got[:, :qn]).astype(BF)
            kvacc[sl, :] = (kvacc[sl, :].astype(F32) + got[:, qn:]).astype(BF)

    def step_a(e, _):
        @pl.when((e >= 2) & (e < events))
        def _():
            for d in (0, 1):
                ring(d, e, e).wait_recv()

        @pl.when(e < events - 2)
        def _():
            for d in (0, 1):
                ring(d, e, e + 2).start()

        @pl.when(e < events)
        def _():
            for d in (0, 1):
                side(d, e).start()

        @pl.when(e == 1)
        def _():
            for c in ld[1:]:
                c.wait()
            for d in (0, 1):
                for k in (0, 1):
                    g_home(d, k).start()

        @pl.when(e == events - 2)
        def _():
            for d in (0, 1):
                g_ring(d, 0, 2, True).start()

        @pl.when((e >= 2) & (e < 2 + parts))
        def _():
            k = e - 2

            @pl.when(k >= 2)
            def _():
                wq_push(k - 2).wait_send()
                wq_home(k - 2).wait()
            block = wq_v[pl.ds(pl.multiple_of(k * wq_p, wq_p), wq_p), :]
            tbuf[lax.rem(k, 2)] = block.astype(F32).T.astype(BF)
            wo_push(k).start()
            wq_push(k).start()
            wq_home(k).start()

        @pl.when(e == 2 + parts)
        def _():
            for k in (0, 1):
                wk_push(k).start()

        @pl.when(e >= 1)
        def _():
            for d in (0, 1):
                side(d, e - 1).wait_recv()
            work(e - 1)
        return 0

    lax.fori_loop(0, events + 1, step_a, 0)

    own = 2 * par + core
    opp = 2 * (1 - par) + core
    low = lax.broadcasted_iota(jnp.int32, (toks // 2, 4 * kn), 1) < 2 * kn
    kvx[own] = jnp.where(low, kvacc[:toks // 2, :].astype(F32), kvacc[toks // 2:, :].astype(F32)).astype(BF)
    to_far = rdma(kvx.at[own], kvx.at[own], xs.at[0], xr.at[0], far)
    to_sib = rdma(kvx.at[own], kvx.at[own], xs.at[1], xr.at[1], sib)
    relay = rdma(kvx.at[opp], kvx.at[opp], xs.at[2], xr.at[2], sib)
    mine = jnp.broadcast_to(tok_dev[pl.ds(rank, 1), :].astype(F32), (vrows, tok_dev.shape[1]))
    col = mine.T.astype(jnp.int32)
    lanes = lax.broadcasted_iota(jnp.int32, col.shape, 1)
    hot_mine = jnp.concatenate([jnp.where(col == lanes + j * vrows, 1.0, 0.0).astype(BF) for j in range(vocab // vrows)], axis=1)
    to_far.start()
    to_sib.start()
    for d in (0, 1):
        g_ring(d, 1, 3, True).start()
        for k in (0, 1):
            g_side(d, k, True).start()
            g_home(d, k).wait()
    width = min(512, embed.shape[1])

    def pick(j, _):
        cols = pl.ds(pl.multiple_of(j * width, width), width)
        x_out[:, cols] = dotf(hot_mine, table[:, cols]).astype(BF)
        return 0

    lax.fori_loop(0, embed.shape[1] // width, pick, 0)
    to_far.wait_recv()
    relay.start()
    to_sib.wait_recv()
    relay.wait_recv()
    for up in (0, 1):
        acc = None
        for r in range(4):
            l_i = lax.broadcasted_iota(jnp.int32, (4 * kn, 2 * hd), 0) - 2 * kn * up
            m_i = lax.broadcasted_iota(jnp.int32, (4 * kn, 2 * hd), 1)
            is_k = (l_i >= 0) & (l_i < kn) & (m_i == l_i + kn * r)
            is_v = (l_i >= kn) & (l_i < 2 * kn) & (m_i == hd + kn * r + l_i - kn)
            t = dotf(kvx[r], jnp.where(is_k | is_v, 1.0, 0.0).astype(BF))
            acc = t if acc is None else acc + t
        kv_tok[up * (toks // 2):(up + 1) * (toks // 2), :] = acc.astype(BF)
    for b in range(batch):
        sl = slice(b * seq, (b + 1) * seq)
        k_rot[sl, :] = rope_f32(kv_tok[sl, :hd], kg[...], cos[...], sin_s[...]).astype(BF)

    scale = hd ** -0.5
    blk = seq // 2

    def unit(u, _):
        rows = pl.ds(pl.multiple_of((u // heads) * seq, seq), seq)
        cols = pl.ds(pl.multiple_of(lax.rem(u, heads) * hd, hd), hd)
        qr = rope_f32(q_tok[rows, cols], qg[...], cos[...], sin_s[...]).astype(BF)
        q_rot[rows, cols] = qr
        kr = k_rot[rows, :]
        v = kv_tok[rows, hd:]
        for i in (0, 1):
            n = blk * (i + 1)
            s = masked(dotf(qr[i * blk:(i + 1) * blk], kr[:n], NT) * scale, i * blk)
            o = dotf(soft(s).astype(BF), v[:n]).astype(BF)
            o_out[pl.ds(pl.multiple_of((u // heads) * seq + i * blk, blk), blk), cols] = o
        return 0

    def do_work(e):
        slot = lax.rem(e, 2)
        places = [(d, c) for d in (0, 1) for c in (0, 1)]
        for i, (d, c) in enumerate(places):
            g_load(slot, i, d, c, e).wait()
        r = dotf(gbuf[slot], wo_v[...], NT).astype(BF)
        for i, (d, c) in enumerate(places):
            do_out[pl.ds(g_row(d, e, c), pos), :] = r[i * pos:(i + 1) * pos]

    units = batch * heads
    slots = events - 3

    def step_b(e, _):
        @pl.when((e >= 2) & (e < events))
        def _():
            for d in (0, 1):
                g_ring(d, e, e, False).wait_recv()

        @pl.when((e >= 2) & (e < events - 2))
        def _():
            for d in (0, 1):
                g_ring(d, e, e + 2, False).start()

        @pl.when((e >= 2) & (e < events))
        def _():
            for d in (0, 1):
                g_side(d, e, False).start()

        @pl.when((e >= 1) & (e <= events))
        def _():
            for d in (0, 1):
                g_side(d, e - 1, False).wait_recv()
            for i, (d, c) in enumerate([(d, c) for d in (0, 1) for c in (0, 1)]):
                g_load(lax.rem(e - 1, 2), i, d, c, e - 1).start()

        def give(b, _):
            o_push(b).start()
            return 0

        lax.fori_loop(jnp.minimum((jnp.maximum(e - 1, 0) * units) // slots, units) // heads, jnp.minimum((e * units) // slots, units) // heads, give, 0)
        lax.fori_loop(jnp.minimum((e * units) // slots, units), jnp.minimum(((e + 1) * units) // slots, units), unit, 0)

        @pl.when(e >= 2)
        def _():
            do_work(e - 2)
        return 0

    lax.fori_loop(0, events + 2, step_b, 0)

    for c in (to_far, to_sib, relay):
        c.wait_send()
    for k in range(parts):
        if k >= parts - 2:
            wq_push(k).wait_send()
            wq_home(k).wait()
        wq_push(k).wait_recv()
        wo_push(k).wait()
    for k in (0, 1):
        wk_push(k).wait()
    for b in range(batch):
        o_push(b).wait()

    def drain(e, _):
        @pl.when(e < events - 2)
        def _():
            for d in (0, 1):
                ring(d, e, e + 2).wait_send()
                g_ring(d, e, e + 2, False).wait_send()
        for d in (0, 1):
            side(d, e).wait_send()
            g_side(d, e, False).wait_send()
        return 0

    lax.fori_loop(0, events, drain, 0)
    for slot in (0, 1):
        for i in range(4):
            h_copy(slot, i, row_of(0, 0, core)).wait()


def forward_kernel(nz, embed, gy, wq, wk_t, wv_t, wo, gain, qg, kg, cos, sin_s, tok_dev, tok_seq):
    vrows, d = embed.shape
    vocab = vrows * 2 * nz
    qn, kn = wq.shape[1], wk_t.shape[0]
    hd = qg.shape[1]
    batch, seq = tok_seq.shape
    toks = batch * seq
    ev = 2 * nz
    dma = pltpu.SemaphoreType.DMA

    def arr(*shape):
        return jax.ShapeDtypeStruct(shape, BF)

    return pl.pallas_call(
        functools.partial(ka_body, nz),
        name='forward_kernel',
        out_shape=(arr(vocab, d), arr(toks, d), arr(toks, qn), arr(qn, d), arr(qn, d), arr(qn, d), arr(2 * kn, d), arr(toks, qn), arr(toks, 2 * hd), arr(toks, qn), arr(toks, hd), arr(toks, qn), arr(toks, qn), arr(vrows, d)),
        in_specs=[ANY] * 6 + [VM] * 7,
        out_specs=(ANY,) * 7 + (VM,) * 7,
        scratch_shapes=[pltpu.VMEM((vocab, d), BF), pltpu.VMEM((2, vrows, d), BF), pltpu.VMEM((d, qn), BF), pltpu.VMEM((4 * kn, d), BF), pltpu.VMEM((qn, d), BF),
                        pltpu.VMEM((toks, vrows), jnp.int32), pltpu.VMEM((toks, 4 * kn), BF), pltpu.VMEM((4, toks // 2, 4 * kn), BF), pltpu.VMEM((vrows, d), BF), pltpu.VMEM((2, vrows, d), BF), pltpu.VMEM((2, qn, d // 8), BF),
                        dma((12,)), dma((2, 4)), dma((2, 4))] + [dma((2, ev))] * 8 + [dma((3,)), dma((3,))] + [dma((8,))] * 5 + [dma((2,)), dma((2,)), dma((batch,)), dma((batch,))],
        compiler_params=pltpu.CompilerParams(collective_id=0, has_side_effects=True, vmem_limit_bytes=62 * 1024 * 1024),
        cost_estimate=pl.CostEstimate(flops=2 * vocab * d * (2 * qn + 4 * kn), bytes_accessed=8 * vocab * d, transcendentals=0),
    )(embed, gy, wq, wk_t, wv_t, wo, gain, qg, kg, cos, sin_s, tok_dev, tok_seq)


def rope_consts(seq, hd):
    inv = np.float32(ROPE_BASE) ** (np.float32(-2.0) * np.arange(hd // 2, dtype=np.float32) / np.float32(hd))
    ang = np.arange(seq, dtype=np.float32)[:, None] * inv.astype(np.float32)[None, :]
    ang = np.concatenate([ang, ang], axis=-1)
    sign = np.where(np.arange(hd) < hd // 2, -1.0, 1.0).astype(np.float32)
    return np.cos(ang).astype(np.float32), (np.sin(ang) * sign).astype(np.float32)


def kb_body(nz, o_own, o_sib, wo, wo_sib, wqt, wqt_sib, wk_t, wv_t, wkv_sib, gy, hid, q_in, kv_tok, qr_in, k_rot, do_in, x_mine, embed,
            gain, qg, kg, cos, sin_s, tok_seq,
            y_out, ge_out, gq_out, gkv_out, gwo_out, gains_out,
            opair, wpair, qt, qr, gd, d_rows, kvrow, sq, skv, part, lhs, rbuf, sbuf, gblk, hblk, swo, swq, hotm, dk_acc, dv_acc, pk, rk1, fk, hk, rk2, kvt, gn, qga, kga, gall,
            in_sem, rs, rr, p1s, p1r, p2s, p2r, qs, qv, gls, hls, wos, wqs, gs, gr):
    rank = lax.axis_index('tp')
    z, core = rank // 2, lax.rem(rank, 2)
    right = 2 * lax.rem(z + 1, nz) + core
    left = 2 * lax.rem(z + nz - 1, nz) + core
    sib = rank + 1 - 2 * core
    par = lax.rem(z, 2)
    far = rank + 2 - 4 * par
    vrows, d = embed.shape
    kn = wk_t.shape[0]
    half, sub_rows = vrows // 2, vrows // 4
    vocab = vrows * 2 * nz
    batch, seq = tok_seq.shape
    toks = batch * seq
    qn = q_in.shape[1]
    hd = qg.shape[1]
    heads = qn // hd
    events = 2 * nz
    pos = seq // (2 * nz)
    blk = seq // 2
    scale = hd ** -0.5
    cw = min(512, d)
    bw = d // events

    ld = [pltpu.make_async_copy(s, t, in_sem.at[i]) for i, (s, t) in enumerate((
        (wo, wpair.at[pl.ds(0, qn)]), (wo_sib, wpair.at[pl.ds(qn, qn)]), (o_own, opair.at[0]), (o_sib, opair.at[1]),
        (q_in, qt), (qr_in, qr), (do_in, gd),
        (wk_t, wpair.at[pl.ds(2 * qn, kn)]), (wv_t, wpair.at[pl.ds(2 * qn + kn, kn)]), (wkv_sib, wpair.at[pl.ds(2 * qn + 2 * kn, 2 * kn)])))]
    ld2 = [pltpu.make_async_copy(s, t, in_sem.at[10 + i]) for i, (s, t) in enumerate((
        (wqt, wpair.at[pl.ds(0, qn)]), (wqt_sib, wpair.at[pl.ds(qn, qn)])))]
    for c in ld:
        c.start()
    barrier = pltpu.get_barrier_semaphore()
    for k in range(1, 2 * nz):
        pl.semaphore_signal(barrier, inc=1, device_id={'tp': lax.rem(rank + k, 2 * nz)}, device_id_type=MESH)
    pl.semaphore_wait(barrier, 2 * nz - 1)

    def zd_of(dr, s):
        return lax.rem(z + (2 * nz - 1 - s if dr == 0 else 1 + s), nz)

    def send(ph, dr, e):
        sl = sbuf.at[ph, lax.rem(e // 2, 2), dr, lax.rem(e, 2)]
        return rdma(sl, rbuf.at[dr, e], rs.at[ph, dr, e], rr.at[ph, dr, e], right if dr == 0 else left)

    pieces = [(dr, sub) for dr in (0, 1) for sub in (0, 1)]

    def times(k):
        def tile(j, _):
            cols = pl.ds(pl.multiple_of(j * cw, cw), cw)
            part[:, cols] = dotf(lhs[:, :k], wpair[:k, cols])
            return 0
        lax.fori_loop(0, d // cw, tile, 0)

    def part_y(s):
        for i, (dr, sub) in enumerate(pieces):
            row = pl.multiple_of(seq * (2 * dr + sub) + pos * (2 * zd_of(dr, s) + core), pos)
            lhs[i * pos:(i + 1) * pos, :qn] = opair[0, pl.ds(row, pos), :]
            lhs[i * pos:(i + 1) * pos, qn:2 * qn] = opair[1, pl.ds(row, pos), :]
        times(2 * qn)

    def part_h(s):
        for i, (dr, sub) in enumerate(pieces):
            zd = zd_of(dr, s)
            off = half * dr + sub_rows * sub
            row = pl.multiple_of(vrows * (2 * zd + core) + off, sub_rows)
            row2 = pl.multiple_of(vrows * zd + off, sub_rows)
            at = slice(i * sub_rows, (i + 1) * sub_rows)
            lhs[at, :qn] = qt[pl.ds(row, sub_rows), :]
            lhs[at, qn:2 * qn] = sq[pl.ds(row2, sub_rows), :]
            lhs[at, 2 * qn:] = (kvrow[pl.ds(row, sub_rows), :].astype(F32) + pltpu.roll(skv[pl.ds(row2, sub_rows), :].astype(F32), 2 * kn, 1)).astype(BF)
        times(2 * qn + 4 * kn)

    def serve(ph, e, final):
        s, sub = e // 2, lax.rem(e, 2)

        @pl.when(e >= 2)
        def _():
            for dr in (0, 1):
                send(ph, dr, e - 2).wait_recv()

        def mine(dr):
            return part[pl.ds(pl.multiple_of((2 * dr + sub) * sub_rows, sub_rows), sub_rows), :]

        @pl.when(e < 2)
        def _():
            for dr in (0, 1):
                sbuf[ph, lax.rem(s, 2), dr, sub] = mine(dr).astype(BF)

        @pl.when((e >= 2) & (e < events - 2))
        def _():
            @pl.when(e >= 4)
            def _():
                for dr in (0, 1):
                    send(ph, dr, e - 4).wait_send()
            for dr in (0, 1):
                sbuf[ph, lax.rem(s, 2), dr, sub] = (mine(dr) + rbuf[dr, e - 2].astype(F32)).astype(BF)

        @pl.when(e < events - 2)
        def _():
            for dr in (0, 1):
                send(ph, dr, e).start()

        @pl.when(e >= events - 2)
        def _():
            for dr in (0, 1):
                final(dr, sub, mine(dr) + rbuf[dr, e - 2].astype(F32))

    def final_y(dr, sub, acc):
        rows = pl.ds(pl.multiple_of((2 * dr + sub) * pos, pos), pos)
        y_out[rows, :] = (x_mine[rows, :].astype(F32) + acc).astype(BF)

    def final_h(dr, sub, gh):
        rows = pl.ds(pl.multiple_of(half * dr + sub_rows * sub, sub_rows), sub_rows)
        x = embed[rows, :].astype(F32)
        r = lax.rsqrt(jnp.mean(x * x, axis=-1, keepdims=True) + EPS)
        dxr = gh * gain[...]
        ge_out[rows, :] += r * dxr - x * (r * r * r * jnp.mean(x * dxr, axis=-1, keepdims=True))
        gn[...] += jnp.sum(gh * (x * r), axis=0, keepdims=True)

    def pull(raw, dout, g):
        x = raw.astype(F32)
        r = lax.rsqrt(jnp.mean(x * x, axis=-1, keepdims=True) + EPS)
        dn = dout * cos[...] + pltpu.roll(dout * sin_s[...], hd // 2, 1)
        dxr = dn * g
        dx = r * dxr - x * (r * r * r * jnp.mean(x * dxr, axis=-1, keepdims=True))
        return dx.astype(BF), jnp.sum(dn * (x * r), axis=0, keepdims=True)

    def unit(u):
        b, h = u // heads, lax.rem(u, heads)
        rows = pl.ds(pl.multiple_of(b * seq, seq), seq)
        cols = pl.ds(pl.multiple_of(h * hd, hd), hd)

        @pl.when(h == 0)
        def _():
            dk_acc[...] = jnp.zeros_like(dk_acc)
            dv_acc[...] = jnp.zeros_like(dv_acc)
        q, g = qr[rows, cols], gd[rows, cols]
        kr, v = k_rot[rows, :], kv_tok[rows, hd:]
        dqs = []
        for i in (0, 1):
            n = blk * (i + 1)
            qi, gi = q[i * blk:(i + 1) * blk], g[i * blk:(i + 1) * blk]
            p = soft(masked(dotf(qi, kr[:n], NT) * scale, i * blk))
            dp = dotf(gi, v[:n], NT)
            dv_acc[:n, :] += dotf(p.astype(BF), gi, TN)
            ds = (p * (dp - jnp.sum(p * dp, axis=-1, keepdims=True)) * scale).astype(BF)
            dqs.append(dotf(ds, kr[:n]))
            dk_acc[:n, :] += dotf(ds, qi, TN)
        dq = jnp.concatenate(dqs, axis=0).astype(BF).astype(F32)
        dx, dg = pull(qt[rows, cols], dq, qg[...])
        gd[rows, cols] = dx
        qga[...] += dg

    def pick(r, up):
        m_i = lax.broadcasted_iota(jnp.int32, (2 * hd, 4 * kn), 0)
        l_i = lax.broadcasted_iota(jnp.int32, (2 * hd, 4 * kn), 1) - 2 * kn * up
        is_k = (l_i >= 0) & (l_i < kn) & (m_i == l_i + kn * r)
        is_v = (l_i >= kn) & (l_i < 2 * kn) & (m_i == hd + kn * r + l_i - kn)
        return jnp.where(is_k | is_v, 1.0, 0.0).astype(BF)

    def to_side(b, p):
        return rdma(pk.at[b, 2 * p + 1 - core], rk1.at[b, p], p1s.at[b, p], p1r.at[b, p], sib)

    def to_far(b):
        return rdma(fk.at[b], rk2.at[b], p2s.at[b], p2r.at[b], far)

    def kv_one(b):
        rows = pl.ds(pl.multiple_of(b * seq, seq), seq)
        dk = dk_acc[...].astype(BF).astype(F32)
        dx, dg = pull(kv_tok[rows, :hd], dk, kg[...])
        kga[...] += dg
        gkv = jnp.concatenate([dx, dv_acc[...].astype(BF)], axis=1)
        for r in range(4):
            pk[b, r] = (dotf(gkv[:blk], pick(r, 0)) + dotf(gkv[blk:], pick(r, 1))).astype(BF)
        for p in (0, 1):
            to_side(b, p).start()

    def kv_two(b):
        for p in (0, 1):
            to_side(b, p).wait_recv()
        a = pk[b, 2 * (1 - par) + core].astype(F32) + rk1[b, 1 - par].astype(F32)
        fk[b] = a.astype(BF)
        hk[b] = pk[b, 2 * par + core].astype(F32) + rk1[b, par].astype(F32)
        to_far(b).start()

    def kv_three(b):
        to_far(b).wait_recv()
        t = hk[b] + rk2[b].astype(F32)
        low = lax.broadcasted_iota(jnp.int32, t.shape, 1) < 2 * kn
        kvt[b, :blk, :] = jnp.where(low, t, 0.0).astype(BF)
        kvt[b, blk:, :] = jnp.where(low, pltpu.roll(t, 2 * kn, 1), 0.0).astype(BF)

    def fold(b, tile):
        rows = pl.ds(pl.multiple_of(tile * seq, seq), seq)
        ids = tile * seq + lax.broadcasted_iota(jnp.int32, (seq, seq), 0)
        hot = jnp.where(ids == tok_seq[pl.ds(b, 1), :], 1.0, 0.0).astype(BF)
        d_rows[rows, :qn] += dotf(hot, gd[pl.ds(pl.multiple_of(b * seq, seq), seq), :])
        d_rows[rows, qn:] += dotf(hot, kvt[b])

    def g_load(j):
        return pltpu.make_async_copy(gy.at[:, pl.ds(pl.multiple_of(j * bw, bw), bw)], gblk.at[lax.rem(j, 2)], gls.at[lax.rem(j, 2)])

    def h_load(j):
        return pltpu.make_async_copy(hid.at[:, pl.ds(pl.multiple_of(j * bw, bw), bw)], hblk.at[lax.rem(j, 2)], hls.at[lax.rem(j, 2)])

    def wo_store(j):
        return pltpu.make_async_copy(swo.at[lax.rem(j, 2)], gwo_out.at[:, pl.ds(pl.multiple_of(j * bw, bw), bw)], wos.at[lax.rem(j, 2)])

    def wq_store(j):
        return pltpu.make_async_copy(swq.at[lax.rem(j, 2)], gq_out.at[pl.ds(pl.multiple_of(j * bw, bw), bw)], wqs.at[lax.rem(j, 2)])

    def wo_block(j):
        sl = lax.rem(j, 2)
        g_load(j).wait()

        @pl.when(j + 1 < events)
        def _():
            g_load(j + 1).start()

        @pl.when(j >= 2)
        def _():
            wo_store(j - 2).wait()
        swo[sl] = dotf(opair[0], gblk[sl], TN)
        ge_out[:, pl.ds(pl.multiple_of(j * bw, bw), bw)] = dotf(hotm[...], gblk[sl])
        wo_store(j).start()

    def wq_block(j):
        sl = lax.rem(j, 2)
        h_load(j).wait()

        @pl.when(j + 1 < events)
        def _():
            h_load(j + 1).start()

        @pl.when(j >= 2)
        def _():
            wq_store(j - 2).wait()
        swq[sl] = dotf(hblk[sl], qt[...], TN)
        gkv_out[:, pl.ds(pl.multiple_of(j * bw, bw), bw)] = dotf(kvrow[...], hblk[sl], TN)[:2 * kn]
        wq_store(j).start()

    for c in ld[:4]:
        c.wait()
    part_y(0)
    d_rows[...] = jnp.zeros_like(d_rows)
    for b in range(batch):
        ids = rank * vrows + lax.broadcasted_iota(jnp.int32, (vrows, seq), 0)
        hotm[:, b * seq:(b + 1) * seq] = jnp.where(ids == tok_seq[b:b + 1, :], 1.0, 0.0).astype(BF)
    gn[...] = jnp.zeros_like(gn)
    qga[...] = jnp.zeros_like(qga)
    kga[...] = jnp.zeros_like(kga)
    g_load(0).start()
    h_load(0).start()

    def phase_y(e, _):
        serve(0, e, final_y)

        @pl.when((lax.rem(e, 2) == 1) & (e < events - 2))
        def _():
            part_y(e // 2 + 1)

        @pl.when(e == events - 3)
        def _():
            for c in ld2:
                c.start()

        @pl.when(e == 0)
        def _():
            for c in ld[4:]:
                c.wait()
        unit(e)
        b, h = e // heads, lax.rem(e, heads)

        @pl.when(h == heads - 1)
        def _():
            kv_one(b)

        @pl.when(b >= 1)
        def _():
            @pl.when(h == 0)
            def _():
                kv_two(b - 1)

            @pl.when(h == 1)
            def _():
                kv_three(b - 1)

            @pl.when(h >= 2)
            def _():
                fold(b - 1, 2 * (h - 2))
                fold(b - 1, 2 * (h - 2) + 1)
        return 0

    lax.fori_loop(0, events, phase_y, 0)
    early = 3

    def blocks(lo, hi, f):
        def go(j, _):
            f(j)
            return 0
        lax.fori_loop(lo, hi, go, 0)

    blocks(0, 1, wo_block)
    kv_two(batch - 1)
    blocks(1, early, wo_block)
    kv_three(batch - 1)

    def last(t, _):
        fold(batch - 1, t)
        return 0

    lax.fori_loop(0, vocab // seq, last, 0)

    def settle(t, _):
        rows = pl.ds(pl.multiple_of(t * vrows, vrows), vrows)
        qt[rows, :] = d_rows[rows, :qn].astype(BF)
        kvrow[rows, :] = d_rows[rows, qn:].astype(BF)
        return 0

    lax.fori_loop(0, 2 * nz, settle, 0)

    def q_side(k, kk):
        src = pl.ds(pl.multiple_of(vrows * (2 * k + 1 - core), vrows), vrows)
        dst = pl.ds(pl.multiple_of(vrows * k, vrows), vrows)
        return rdma((qt, kvrow)[kk].at[src], (sq, skv)[kk].at[dst], qs.at[kk, k], qv.at[kk, k], sib)

    def swap(k, _):
        for kk in (0, 1):
            q_side(k, kk).start()
        return 0

    lax.fori_loop(0, nz, swap, 0)
    for c in ld2:
        c.wait()

    def swapped(k, _):
        for kk in (0, 1):
            q_side(k, kk).wait_recv()
        return 0

    lax.fori_loop(0, nz, swapped, 0)
    part_h(0)

    def phase_h(e, _):
        serve(1, e, final_h)

        @pl.when((lax.rem(e, 2) == 1) & (e < events - 2))
        def _():
            part_h(e // 2 + 1)

        @pl.when(e < events - 3)
        def _():
            @pl.when(e + early < events)
            def _():
                wo_block(e + early)

            @pl.when(e < events - 6)
            def _():
                wq_block(e)

            @pl.when(e >= events - 6)
            def _():
                wq_block(2 * e - events + 6)
                wq_block(2 * e - events + 7)
        return 0

    lax.fori_loop(0, events, phase_h, 0)

    wide = gains_out.shape[1]
    for j in range(d // wide):
        gall[rank, j:j + 1, :] = gn[:, j * wide:(j + 1) * wide]
    gall[rank, d // wide:d // wide + 1, :] = qga[...]
    gall[rank, d // wide + 1:d // wide + 2, :] = kga[...]
    for j in (events - 2, events - 1):
        wo_store(j).wait()
        wq_store(j).wait()

    def spread(k):
        return rdma(gall.at[rank], gall.at[rank], gs.at[k], gr.at[k], lax.rem(rank + k, 2 * nz))

    def spread_from(k):
        src = lax.rem(rank + 2 * nz - k, 2 * nz)
        return rdma(gall.at[src], gall.at[src], gs.at[k], gr.at[k], sib)

    for k in range(1, 2 * nz):
        spread(k).start()

    def drain(e, _):
        for dr in (0, 1):
            @pl.when(e >= events - 6)
            def _():
                send(0, dr, e).wait_send()
                send(1, dr, e).wait_send()
        return 0

    lax.fori_loop(0, events - 2, drain, 0)
    for b in range(batch):
        for p in (0, 1):
            to_side(b, p).wait_send()
        to_far(b).wait_send()

    def swept(k, _):
        for kk in (0, 1):
            q_side(k, kk).wait_send()
        return 0

    lax.fori_loop(0, nz, swept, 0)
    for k in range(1, 2 * nz):
        spread_from(k).wait_recv()
    gains_out[...] = jnp.sum(gall[...], axis=0)
    for k in range(1, 2 * nz):
        spread(k).wait_send()


def backward_kernel(nz, o_own, o_sib, wo, wo_sib, wqt, wqt_sib, wk_t, wv_t, wkv_sib, gy, hid, q_in, kv_tok, qr_in, k_rot, do_in, x_mine, embed, gain, qg, kg, cos, sin_s, tok_seq):
    vrows, d = embed.shape
    vocab = vrows * 2 * nz
    qn, kn = q_in.shape[1], wk_t.shape[0]
    hd = qg.shape[1]
    batch, seq = tok_seq.shape
    toks = batch * seq
    ev = 2 * nz
    bw = d // ev
    grow = (d // hd + 2 + 7) // 8 * 8
    dma = pltpu.SemaphoreType.DMA
    v = pltpu.VMEM

    def arr(*shape):
        return jax.ShapeDtypeStruct(shape, F32)

    return pl.pallas_call(
        functools.partial(kb_body, nz),
        name='backward_kernel',
        out_shape=(jax.ShapeDtypeStruct((vrows, d), BF), arr(vrows, d), arr(d, qn), arr(2 * kn, d), arr(qn, d), arr(grow, hd)),
        in_specs=[ANY] * 12 + [VM, ANY, VM, ANY] + [VM] * 8,
        out_specs=(VM, VM, ANY, VM, ANY, VM),
        scratch_shapes=[v((2, toks, qn), BF), v((2 * qn + 4 * kn, d), BF), v((vocab, qn), BF), v((toks, qn), BF), v((toks, qn), BF), v((vocab, qn + 4 * kn), F32),
                        v((vocab, 4 * kn), BF), v((vocab // 2, qn), BF), v((vocab // 2, 4 * kn), BF), v((vrows, d), F32), v((vrows, 2 * qn + 4 * kn), BF),
                        v((2, ev - 2, vrows // 4, d), BF), v((2, 2, 2, 2, vrows // 4, d), BF), v((2, toks, bw), BF), v((2, vocab, bw), BF), v((2, qn, bw), F32), v((2, bw, qn), F32),
                        v((vrows, toks), BF), v((seq, hd), F32), v((seq, hd), F32), v((batch, 4, seq // 2, 4 * kn), BF), v((batch, 2, seq // 2, 4 * kn), BF), v((batch, seq // 2, 4 * kn), BF),
                        v((batch, seq // 2, 4 * kn), F32), v((batch, seq // 2, 4 * kn), BF), v((batch, seq, 4 * kn), BF), v((1, d), F32), v((1, hd), F32), v((1, hd), F32), v((ev, grow, hd), F32),
                        dma((12,)), dma((2, 2, ev - 2)), dma((2, 2, ev - 2)), dma((batch, 2)), dma((batch, 2)), dma((batch,)), dma((batch,)), dma((2, nz)), dma((2, nz)),
                        dma((2,)), dma((2,)), dma((2,)), dma((2,)), dma((ev,)), dma((ev,))],
        compiler_params=pltpu.CompilerParams(collective_id=1, has_side_effects=True, vmem_limit_bytes=63 * 1024 * 1024),
        cost_estimate=pl.CostEstimate(flops=2 * vocab * d * (5 * qn), bytes_accessed=12 * vocab * d, transcendentals=0),
    )(o_own, o_sib, wo, wo_sib, wqt, wqt_sib, wk_t, wv_t, wkv_sib, gy, hid, q_in, kv_tok, qr_in, k_rot, do_in, x_mine, embed, gain, qg, kg, cos, sin_s, tok_seq)


def solution(mesh):
    tp = mesh.shape['tp']
    nz = tp // 2

    def local_step(tok_ids, embed_loc, norm_gain, q_gain, k_gain, wq, wk, wv, wo, gy_loc):
        vrows, d_model = embed_loc.shape
        batch, seq = tok_ids.shape
        seq_dev = seq // tp
        hd = q_gain.shape[0]
        kn = wk.shape[1]
        cos_c, sin_c = (jnp.asarray(t) for t in rope_consts(seq, hd))
        tok_dev = tok_ids.reshape(batch, tp, seq_dev).transpose(1, 0, 2).reshape(tp, batch * seq_dev)
        gains = (norm_gain[None, :], q_gain[None, :], k_gain[None, :])
        hid, gy, o_sib, wo_sib, wqt, wqt_sib, wkv_sib, q_tok, kv_tok, q_rot, k_rot, o_own, d_o, x_mine = forward_kernel(
            nz, embed_loc, gy_loc.reshape(batch * seq_dev, d_model), wq, wk.T, wv.T, wo, *gains, cos_c, sin_c, tok_dev, tok_ids)
        y, g_embed, g_wq, g_kv, g_wo, g_gain = backward_kernel(
            nz, o_own, o_sib, wo, wo_sib, wqt, wqt_sib, wk.T, wv.T, wkv_sib, gy, hid, q_tok, kv_tok, q_rot, k_rot, d_o, x_mine, embed_loc, *gains, cos_c, sin_c, tok_ids)
        n = d_model // hd
        return (y.reshape(batch, seq_dev, d_model), g_embed, g_gain[:n].reshape(d_model), g_gain[n], g_gain[n + 1], g_wq, g_kv[:kn].T, g_kv[kn:].T, g_wo)

    in_specs = (P('dp', None), P('tp', None), P(), P(), P(), P(None, 'tp'), P(None, 'tp'), P(None, 'tp'), P('tp', None), P('dp', 'tp', None))
    out_specs = (P('dp', 'tp', None), P(('dp', 'tp'), None), P('dp'), P('dp'), P('dp'), P('dp', 'tp'), P('dp', 'tp'), P('dp', 'tp'), P(('dp', 'tp'), None))
    return jax.shard_map(local_step, mesh=mesh, in_specs=in_specs, out_specs=out_specs, check_vma=False)
```

```python
import functools
import jax
import jax.numpy as jnp
import numpy as np
from jax import lax
from jax.experimental import pallas as pl
from jax.experimental.pallas import tpu as pltpu
from jax.sharding import PartitionSpec as P

BF = jnp.bfloat16
F32 = jnp.float32
EPS = 1.0e-6
ROPE_BASE = 1.0e6
NEG_BIG = -1.0e30
MESH = pl.DeviceIdType.MESH
ANY = pl.BlockSpec(memory_space=pl.ANY)
VM = pl.BlockSpec(memory_space=pltpu.VMEM)
NT = (((1,), (1,)), ((), ()))
NN = (((1,), (0,)), ((), ()))
TN = (((0,), (0,)), ((), ()))


def dotf(a, b, dims=NN):
    return lax.dot_general(a, b, dims, preferred_element_type=F32)


def rdma(src, dst, ssem, rsem, dev):
    return pltpu.make_async_remote_copy(src_ref=src, dst_ref=dst, send_sem=ssem, recv_sem=rsem, device_id={'tp': dev}, device_id_type=MESH)


def span(start, size):
    return pl.ds(pl.multiple_of(start, size), size)


def each(lo, hi, f):
    def go(j, _):
        f(j)
        return 0
    lax.fori_loop(lo, hi, go, 0)


def rms_f32(x, gain):
    return x * lax.rsqrt(jnp.mean(x * x, axis=-1, keepdims=True) + EPS) * gain


def rms_pull(x, dxr, r):
    return r * dxr - x * (r * r * r * jnp.mean(x * dxr, axis=-1, keepdims=True))


def masked(scores, first):
    r_i = lax.broadcasted_iota(jnp.int32, scores.shape, 0) + first
    c_i = lax.broadcasted_iota(jnp.int32, scores.shape, 1)
    return jnp.where(r_i >= c_i, scores, NEG_BIG)


def soft(scores):
    e = jnp.exp(scores - jnp.max(scores, axis=-1, keepdims=True))
    return e * (1.0 / jnp.sum(e, axis=-1, keepdims=True))


def body(nz, embed, gy, wq, wk_t, wv_t, wo, gain, qg, kg, cos, sin_s, tok_dev, tok_seq,
         y_hbm, ge_hbm, gq_hbm, gk_hbm, gv_hbm, gwo_hbm, gains_out, hid, gy_out, wqt_out, wqts_out, py_out, ph_out,
         table, wpair, wq_v, qt, o_own, o_sib, sq, kv_tok, k_rot, kvacc, farkv, kvrow, skv, kvc, d_rows, pbuf, hbuf, gown, hotm,
         dk_acc, dv_acc, pk, rk1, fk, hk, rk2, kvt, gn, qga, kga, gall, y_v, ge_v, gkv_v,
         in_sem, h_sem, g_sem, a_rs, a_rr, a_ss, a_sr, b_rs, b_rr, b_ss, b_sr, xs, xr, ts, wos, wor, wqs, wqr, wks, wkr, o_s, o_r,
         pt_sem, pl_sem, rs, rr, p1s, p1r, p2s, p2r, qs, qv, gls, hls, swos, swqs, gs, gr, out_sem):
    rank = lax.axis_index('tp')
    z, core = rank // 2, lax.rem(rank, 2)
    right = 2 * lax.rem(z + 1, nz) + core
    left = 2 * lax.rem(z + nz - 1, nz) + core
    sib = rank + 1 - 2 * core
    par = lax.rem(z, 2)
    far = rank + 2 - 4 * par
    vrows, d = embed.shape
    kn = wk_t.shape[0]
    sub_rows = vrows // 4
    vocab = vrows * 2 * nz
    vhalf = vocab // 2
    batch, seq = tok_seq.shape
    toks = batch * seq
    qn = wq.shape[1]
    hd = qg.shape[1]
    heads = qn // hd
    events = 2 * nz
    pos = seq // events
    blk = seq // 2
    bw = d // events
    scale = hd ** -0.5
    units = batch * heads
    parts = 8
    wo_p, wq_p = qn // parts, d // parts
    both = (0, 1)
    places = [(dr, c) for dr in both for c in both]
    qr = wq_v.at[pl.ds(0, toks)]
    gd = wq_v.at[pl.ds(toks, toks)]
    w_q = wq_v.at[pl.ds(0, d)]

    ld = [pltpu.make_async_copy(s, t, in_sem.at[i]) for i, (s, t) in enumerate((
        (embed, table.at[span(rank * vrows, vrows)]), (gy, gown), (wq, w_q), (wo, wpair.at[pl.ds(0, qn)]),
        (wk_t, wpair.at[pl.ds(2 * qn, kn)]), (wv_t, wpair.at[pl.ds(2 * qn + kn, kn)])))]
    ld2 = [pltpu.make_async_copy(s, t, in_sem.at[i]) for i, (s, t) in enumerate((
        (wqt_out, wpair.at[pl.ds(0, qn)]), (wqts_out, wpair.at[pl.ds(qn, qn)]), (embed, gown)))]
    for c in ld:
        c.start()
    barrier = pltpu.get_barrier_semaphore()
    for k in range(1, 2 * nz):
        pl.semaphore_signal(barrier, inc=1, device_id={'tp': lax.rem(rank + k, 2 * nz)}, device_id_type=MESH)
    pl.semaphore_wait(barrier, 2 * nz - 1)
    ld[0].wait()

    def nbr(dr):
        return right if dr == 0 else left

    def zd_of(dr, e):
        s = e // 2
        return lax.rem(z + (nz - s if dr == 0 else s), nz)

    def row_of(dr, e, c):
        return pl.multiple_of(vrows * (2 * zd_of(dr, e) + c) + sub_rows * (2 * dr + lax.rem(e, 2)), sub_rows)

    def ring(dr, e, recv_e):
        a = table.at[pl.ds(row_of(dr, e, core), sub_rows)]
        return rdma(a, a, a_rs.at[dr, e], a_rr.at[dr, recv_e], nbr(dr))

    def side(dr, e):
        a = table.at[pl.ds(row_of(dr, e, core), sub_rows)]
        return rdma(a, a, a_ss.at[dr, e], a_sr.at[dr, e], sib)

    def h_copy(slot, i, row):
        return pltpu.make_async_copy(hbuf.at[slot, pl.ds(i * sub_rows, sub_rows)], hid.at[pl.ds(row, sub_rows)], h_sem.at[slot, i])

    def g_row(dr, e, c):
        return pl.multiple_of(seq * (2 * dr + lax.rem(e, 2)) + pos * (2 * zd_of(dr, e) + c), pos)

    def g_piece(dr, e, c):
        return gy_out.at[pl.ds(g_row(dr, e, c), pos)]

    def g_own(dr, e):
        return gown.at[span(pos * (2 * dr + lax.rem(e, 2)), pos)]

    def g_ring(dr, e, recv_e, first):
        a = g_piece(dr, e, core)
        return rdma(g_own(dr, e) if first else a, a, b_rs.at[dr, e], b_rr.at[dr, recv_e], nbr(dr))

    def g_side(dr, e, first):
        a = g_piece(dr, e, core)
        return rdma(g_own(dr, e) if first else a, a, b_ss.at[dr, e], b_sr.at[dr, e], sib)

    def g_home(dr, e):
        return pltpu.make_async_copy(g_own(dr, e), g_piece(dr, e, core), in_sem.at[8 + 2 * dr + e])

    def g_fetch(slot, i, dr, c, e):
        return pltpu.make_async_copy(g_piece(dr, e, c), hbuf.at[slot, pl.ds(i * pos, pos)], g_sem.at[slot, i])

    def wo_push(k):
        return rdma(wpair.at[span(k * wo_p, wo_p)], wpair.at[pl.ds(pl.multiple_of(qn + k * wo_p, wo_p), wo_p)], wos.at[k], wor.at[k], sib)

    def tb(k):
        return o_own.at[span(lax.rem(k, 2) * qn, qn), pl.ds(0, wq_p)]

    def wq_push(k):
        return rdma(tb(k), wqts_out.at[:, span(k * wq_p, wq_p)], wqs.at[k], wqr.at[k], sib)

    def wq_home(k):
        return pltpu.make_async_copy(tb(k), wqt_out.at[:, span(k * wq_p, wq_p)], ts.at[k])

    def wk_push(k):
        return rdma((wk_t, wv_t)[k], wpair.at[pl.ds(2 * qn + (2 + k) * kn, kn)], wks.at[k], wkr.at[k], sib)

    def o_push(b, k):
        src = pl.multiple_of(b * seq + pos * (2 * k + 1 - core), pos)
        dst = pl.multiple_of(vrows * k + pos * b, pos)
        return rdma(o_own.at[pl.ds(src, pos)], o_sib.at[pl.ds(dst, pos)], o_s.at[b, k], o_r.at[b, k], sib)

    for k in both:
        wk_push(k).start()
    for b in range(batch):
        wide = jnp.broadcast_to(tok_seq[b:b + 1, :].astype(F32), (vrows, seq))
        d_rows[b * seq:(b + 1) * seq, :vrows] = wide.T
    qt[...] = jnp.zeros_like(qt)
    kvacc[...] = jnp.zeros_like(kvacc)

    def project(e):
        slot = lax.rem(e, 2)

        @pl.when(e >= 2)
        def _():
            for i in range(4):
                h_copy(slot, i, row_of(0, e, core)).wait()

        rows = [row_of(dr, e, c) for dr, c in places]
        for i, row in enumerate(rows):
            x = table[pl.ds(row, sub_rows), :].astype(F32)
            ids = row + lax.broadcasted_iota(jnp.int32, (sub_rows, tok_dev.shape[1]), 0)
            hit = jnp.zeros((sub_rows, tok_dev.shape[1]), F32)
            for j in range(tok_dev.shape[0]):
                hit = jnp.maximum(hit, jnp.where(tok_dev[j:j + 1, :] == ids, 1.0, 0.0))
            used = jnp.max(hit, axis=1, keepdims=True)
            h = jnp.where(used > 0.5, rms_f32(x, gain[...]), 0.0)
            hbuf[slot, pl.ds(i * sub_rows, sub_rows), :] = h.astype(BF)
            h_copy(slot, i, row).start()
        hb = hbuf[slot]
        qkv = jnp.concatenate([dotf(hb, w_q[...]).astype(BF), dotf(hb, wpair[2 * qn:2 * qn + 4 * kn, :], NT).astype(BF)], axis=1)
        lane = lax.broadcasted_iota(jnp.int32, (1, vrows), 1)
        rowid = jnp.zeros((1, vrows), jnp.int32)
        for i, row in enumerate(rows):
            rowid = jnp.where(lane // sub_rows == i, row + lane - i * sub_rows, rowid)
        rowid = rowid.astype(F32)
        for b in range(batch):
            sl = slice(b * seq, (b + 1) * seq)
            hot = jnp.where(d_rows[sl, :vrows] == rowid, 1.0, 0.0).astype(BF)
            got = dotf(hot, qkv)
            qt[sl, :] = (qt[sl, :].astype(F32) + got[:, :qn]).astype(BF)
            at = slice((b % 2) * seq, (b % 2 + 1) * seq)
            kvacc[b // 2, at, :] = (kvacc[b // 2, at, :].astype(F32) + got[:, qn:]).astype(BF)

    def step_a(e):
        @pl.when((e >= 2) & (e < events))
        def _():
            for dr in both:
                ring(dr, e, e).wait_recv()

        @pl.when(e < events - 2)
        def _():
            for dr in both:
                ring(dr, e, e + 2).start()

        @pl.when(e < events)
        def _():
            for dr in both:
                side(dr, e).start()

        @pl.when(e == 1)
        def _():
            for c in ld[1:]:
                c.wait()
            for k in both:
                wk_push(k).wait_recv()
            for dr in both:
                for k in both:
                    g_home(dr, k).start()

        @pl.when(e == events - 2)
        def _():
            for dr in both:
                g_ring(dr, 0, 2, True).start()

        @pl.when((e >= 2) & (e < 4 + parts))
        def _():
            @pl.when(e >= 4)
            def _():
                wq_push(e - 4).wait_send()
                wq_home(e - 4).wait()

            @pl.when(e < 2 + parts)
            def _():
                k = e - 2
                block = wq_v[span(k * wq_p, wq_p), :]
                tb(k)[...] = block.astype(F32).T.astype(BF)
                wo_push(k).start()
                wq_push(k).start()
                wq_home(k).start()

        @pl.when(e >= 1)
        def _():
            for dr in both:
                side(dr, e - 1).wait_recv()
            project(e - 1)

    each(0, events + 1, step_a)

    to_far = rdma(kvacc.at[core], farkv.at[core], xs.at[0], xr.at[0], far)
    relay = rdma(farkv.at[core], farkv.at[core], xs.at[1], xr.at[1], sib)
    mine = jnp.broadcast_to(tok_dev[pl.ds(rank, 1), :].astype(F32), (vrows, tok_dev.shape[1]))
    col = mine.T.astype(jnp.int32)
    lanes = lax.broadcasted_iota(jnp.int32, col.shape, 1)
    hot_mine = jnp.concatenate([jnp.where(col == lanes + j * vrows, 1.0, 0.0).astype(BF) for j in range(vocab // vrows)], axis=1)
    to_far.start()
    for dr in both:
        g_ring(dr, 1, 3, True).start()
        for k in both:
            g_side(dr, k, True).start()
            g_home(dr, k).wait()
    cw = min(512, d)

    def own_rows(j):
        y_v[:, span(j * cw, cw)] = dotf(hot_mine, table[:, span(j * cw, cw)]).astype(BF)

    each(0, d // cw, own_rows)
    for b in range(batch):
        ids = rank * vrows + lax.broadcasted_iota(jnp.int32, (vrows, seq), 0)
        hotm[:, b * seq:(b + 1) * seq] = jnp.where(ids == tok_seq[b:b + 1, :], 1.0, 0.0).astype(BF)
    to_far.wait_recv()
    relay.start()

    def place(p, first):
        l_i = lax.broadcasted_iota(jnp.int32, (4 * kn, 2 * hd), 0)
        m_i = lax.broadcasted_iota(jnp.int32, (4 * kn, 2 * hd), 1)
        upper = jnp.where(l_i >= 2 * kn, 1, 0)
        owner = jnp.where(upper == 1, 1 - first, first)
        l_i = l_i - 2 * kn * upper
        base = kn * (2 * p + owner)
        want = jnp.where(l_i < kn, base + l_i, hd + base + l_i - kn)
        return jnp.where(m_i == want, 1.0, 0.0).astype(BF)

    rdma(farkv.at[1 - core], farkv.at[1 - core], xs.at[1], xr.at[1], sib).wait_recv()
    for hf in both:
        kv_tok[hf * (toks // 2):(hf + 1) * (toks // 2), :] = (dotf(kvacc[hf], place(par, core)) + dotf(farkv[hf], place(1 - par, hf))).astype(BF)

    def rope(raw, g):
        n = rms_f32(raw.astype(F32), g)
        return (n * cos[...] + pltpu.roll(n, hd // 2, 1) * sin_s[...]).astype(BF)

    for b in range(batch):
        sl = slice(b * seq, (b + 1) * seq)
        k_rot[sl, :] = rope(kv_tok[sl, :hd], kg[...])

    def attend(u):
        base = (u // heads) * seq
        rows = span(base, seq)
        cols = span(lax.rem(u, heads) * hd, hd)
        q = rope(qt[rows, cols], qg[...])
        qr[rows, cols] = q
        kr = k_rot[rows, :]
        v = kv_tok[rows, hd:]
        for i in both:
            n = blk * (i + 1)
            s = masked(dotf(q[i * blk:(i + 1) * blk], kr[:n], NT) * scale, i * blk)
            o_own[pl.ds(pl.multiple_of(base + i * blk, blk), blk), cols] = dotf(soft(s).astype(BF), v[:n]).astype(BF)

    def grad_attend(e):
        slot = lax.rem(e, 2)
        for i, (dr, c) in enumerate(places):
            g_fetch(slot, i, dr, c, e).wait()
        r = dotf(hbuf[slot], wpair[:qn, :], NT).astype(BF)
        for i, (dr, c) in enumerate(places):
            gd[pl.ds(g_row(dr, e, c), pos), :] = r[i * pos:(i + 1) * pos]

    def pstage(j):
        return d_rows.at[span(lax.rem(j, 2) * vhalf, vhalf), pl.ds(0, bw)]

    def pstore(dst, j):
        return pltpu.make_async_copy(pstage(j), dst.at[:, span(j * bw, bw)], pt_sem.at[lax.rem(j, 2)])

    def pblock(dst, j, pairs):
        @pl.when(j >= 2)
        def _():
            pstore(dst, j - 2).wait()
        cols = span(j * bw, bw)
        acc = None
        for a, lo, n in pairs:
            t = dotf(a[...], wpair[lo:lo + n, cols])
            acc = t if acc is None else acc + t
        pstage(j)[...] = acc
        pstore(dst, j).start()

    y_pairs = [(sq, 0, qn), (o_sib, qn, qn)]
    h_pairs = [(o_sib, 0, qn), (sq, qn, qn), (kvc, 2 * qn, 4 * kn)]

    def pslot(ph, e, dr):
        return pbuf.at[2 * ph + lax.rem(e, 2), dr]

    def pfetch(ph, e, dr):
        s = e // 2
        zd = lax.rem(z + (2 * nz - 1 - s if dr == 0 else 1 + s), nz)
        row = pl.multiple_of(vrows * zd + sub_rows * (2 * dr + lax.rem(e, 2)), sub_rows)
        return pltpu.make_async_copy((py_out, ph_out)[ph].at[pl.ds(row, sub_rows)], pslot(ph, e, dr), pl_sem.at[ph, lax.rem(e, 2), dr])

    def rslot(dr, e):
        return table.at[span((dr * (events - 2) + e) * sub_rows, sub_rows)]

    def sslot(ph, dr, e):
        k = 2 * (events - 2) + 8 * ph + 4 * lax.rem(e // 2, 2) + 2 * dr + lax.rem(e, 2)
        return table.at[span(k * sub_rows, sub_rows)]

    def send(ph, dr, e):
        return rdma(sslot(ph, dr, e), rslot(dr, e), rs.at[ph, dr, e], rr.at[ph, dr, e], nbr(dr))

    def first_fetch(ph, dst):
        for j in (events - 2, events - 1):
            pstore(dst, j).wait()
        for e in both:
            for dr in both:
                pfetch(ph, e, dr).start()

    def first_sends(ph):
        for e in both:
            for dr in both:
                pfetch(ph, e, dr).wait()
                sslot(ph, dr, e)[...] = pslot(ph, e, dr)[...].astype(BF)
        for e in both:
            for dr in both:
                send(ph, dr, e).start()
                pfetch(ph, e + 2, dr).start()

    def serve(ph, e, final):
        for dr in both:
            send(ph, dr, e - 2).wait_recv()
            pfetch(ph, e, dr).wait()

        @pl.when(e < events - 2)
        def _():
            @pl.when(e >= 4)
            def _():
                for dr in both:
                    send(ph, dr, e - 4).wait_send()
            for dr in both:
                sslot(ph, dr, e)[...] = (pslot(ph, e, dr)[...] + rslot(dr, e - 2)[...].astype(F32)).astype(BF)
            for dr in both:
                send(ph, dr, e).start()
                pfetch(ph, e + 2, dr).start()

        @pl.when(e >= events - 2)
        def _():
            for dr in both:
                final(dr, lax.rem(e, 2), pslot(ph, e, dr)[...] + rslot(dr, e - 2)[...].astype(F32))

    slots = 9

    def gather_o(k):
        for b in range(batch):
            src = pl.multiple_of(b * seq + pos * (2 * k + core), pos)
            sq[pl.ds(pl.multiple_of(vrows * k + pos * b, pos), pos), :] = o_own[pl.ds(src, pos), :]

    def upto(e, n, over):
        return jnp.minimum((e * n) // over, n)

    def step_b(e):
        @pl.when(e == events - 2)
        def _():
            first_sends(0)

        @pl.when((e >= 2) & (e < events))
        def _():
            for dr in both:
                g_ring(dr, e, e, False).wait_recv()

        @pl.when((e >= 2) & (e < events - 2))
        def _():
            for dr in both:
                g_ring(dr, e, e + 2, False).start()

        @pl.when((e >= 2) & (e < events))
        def _():
            for dr in both:
                g_side(dr, e, False).start()

        @pl.when((e >= 1) & (e <= events))
        def _():
            for dr in both:
                g_side(dr, e - 1, False).wait_recv()
            for i, (dr, c) in enumerate(places):
                g_fetch(lax.rem(e - 1, 2), i, dr, c, e - 1).start()

        def give(b):
            each(0, nz, lambda k: o_push(b, k).start())

        each(upto(jnp.maximum(e - 1, 0), units, slots) // heads, upto(e, units, slots) // heads, give)
        each(upto(e, units, slots), upto(e + 1, units, slots), attend)

        @pl.when(e == 4)
        def _():
            def drain(k):
                @pl.when(k < events - 2)
                def _():
                    for dr in both:
                        ring(dr, k, k + 2).wait_send()
                for dr in both:
                    side(dr, k).wait_send()
            each(0, events, drain)

        @pl.when(e == slots + 1)
        def _():
            for k in range(parts):
                wo_push(k).wait_recv()
            for b in range(batch):
                each(0, nz, lambda k: o_push(b, k).wait_recv())
            each(0, nz, gather_o)

        @pl.when((e > slots) & (e <= slots + 4))
        def _():
            each(4 * (e - slots - 1), 4 * (e - slots), lambda j: pblock(py_out, j, y_pairs))

        @pl.when(e == slots + 4)
        def _():
            first_fetch(0, py_out)

        @pl.when(e >= 2)
        def _():
            grad_attend(e - 2)

    for slot in both:
        for i in range(4):
            h_copy(slot, i, row_of(0, 0, core)).wait()
    each(0, events + 2, step_b)

    def pull(raw, dout, g):
        x = raw.astype(F32)
        r = lax.rsqrt(jnp.mean(x * x, axis=-1, keepdims=True) + EPS)
        dn = dout * cos[...] + pltpu.roll(dout * sin_s[...], hd // 2, 1)
        return rms_pull(x, dn * g, r).astype(BF), jnp.sum(dn * (x * r), axis=0, keepdims=True)

    def unit(u):
        b, h = u // heads, lax.rem(u, heads)
        rows = span(b * seq, seq)
        cols = span(h * hd, hd)

        @pl.when(h == 0)
        def _():
            dk_acc[...] = jnp.zeros_like(dk_acc)
            dv_acc[...] = jnp.zeros_like(dv_acc)
        q, g = qr[rows, cols], gd[rows, cols]
        kr, v = k_rot[rows, :], kv_tok[rows, hd:]
        dqs = []
        for i in both:
            n = blk * (i + 1)
            qi, gi = q[i * blk:(i + 1) * blk], g[i * blk:(i + 1) * blk]
            p = soft(masked(dotf(qi, kr[:n], NT) * scale, i * blk))
            dp = dotf(gi, v[:n], NT)
            dv_acc[:n, :] += dotf(p.astype(BF), gi, TN)
            ds = (p * (dp - jnp.sum(p * dp, axis=-1, keepdims=True)) * scale).astype(BF)
            dqs.append(dotf(ds, kr[:n]))
            dk_acc[:n, :] += dotf(ds, qi, TN)
        dq = jnp.concatenate(dqs, axis=0).astype(BF).astype(F32)
        dx, dg = pull(qt[rows, cols], dq, qg[...])
        gd[rows, cols] = dx
        qga[...] += dg

    def pick(r, up):
        m_i = lax.broadcasted_iota(jnp.int32, (2 * hd, 4 * kn), 0)
        l_i = lax.broadcasted_iota(jnp.int32, (2 * hd, 4 * kn), 1) - 2 * kn * up
        is_k = (l_i >= 0) & (l_i < kn) & (m_i == l_i + kn * r)
        is_v = (l_i >= kn) & (l_i < 2 * kn) & (m_i == hd + kn * r + l_i - kn)
        return jnp.where(is_k | is_v, 1.0, 0.0).astype(BF)

    def to_side(b, p):
        return rdma(pk.at[b, 2 * p + 1 - core], rk1.at[b, p], p1s.at[b, p], p1r.at[b, p], sib)

    def to_far2(b):
        return rdma(fk.at[b], rk2.at[b], p2s.at[b], p2r.at[b], far)

    def kv_one(b):
        dk = dk_acc[...].astype(BF).astype(F32)
        dx, dg = pull(kv_tok[span(b * seq, seq), :hd], dk, kg[...])
        kga[...] += dg
        gkv = jnp.concatenate([dx, dv_acc[...].astype(BF)], axis=1)
        for r in range(4):
            pk[b, r] = (dotf(gkv[:blk], pick(r, 0)) + dotf(gkv[blk:], pick(r, 1))).astype(BF)
        for p in both:
            to_side(b, p).start()

    def kv_two(b):
        for p in both:
            to_side(b, p).wait_recv()
        fk[b] = (pk[b, 2 * (1 - par) + core].astype(F32) + rk1[b, 1 - par].astype(F32)).astype(BF)
        hk[b] = pk[b, 2 * par + core].astype(F32) + rk1[b, par].astype(F32)
        to_far2(b).start()

    def kv_three(b):
        to_far2(b).wait_recv()
        t = hk[b] + rk2[b].astype(F32)
        low = lax.broadcasted_iota(jnp.int32, t.shape, 1) < 2 * kn
        kvt[b, :blk, :] = jnp.where(low, t, 0.0).astype(BF)
        kvt[b, blk:, :] = jnp.where(low, pltpu.roll(t, 2 * kn, 1), 0.0).astype(BF)

    def fold(b, tile):
        rows = span(tile * seq, seq)
        ids = tile * seq + lax.broadcasted_iota(jnp.int32, (seq, seq), 0)
        hot = jnp.where(ids == tok_seq[pl.ds(b, 1), :], 1.0, 0.0).astype(BF)
        d_rows[rows, :qn] += dotf(hot, gd[span(b * seq, seq), :])
        d_rows[rows, qn:] += dotf(hot, kvt[b])

    tiles = vocab // seq // 2

    def job(k):
        @pl.when(k < units)
        def _():
            unit(k)

        @pl.when((k < units) & (lax.rem(k, heads) == heads - 1))
        def _():
            kv_one(k // heads)

        @pl.when(k >= heads)
        def _():
            b, h = k // heads - 1, lax.rem(k, heads)

            @pl.when(h == 0)
            def _():
                kv_two(b)

            @pl.when(h == 1)
            def _():
                kv_three(b)

            @pl.when(h >= 2)
            def _():
                each(tiles * (h - 2), tiles * (h - 1), lambda t: fold(b, t))

    def settle(t):
        rows = span(t * vrows, vrows)
        qt[rows, :] = d_rows[rows, :qn].astype(BF)
        kvrow[rows, :] = d_rows[rows, qn:].astype(BF)

    def swap(k, kk):
        src = pl.multiple_of(vrows * (2 * k + 1 - core), vrows)
        return rdma((qt, kvrow)[kk].at[pl.ds(src, vrows)], (sq, skv)[kk].at[span(vrows * k, vrows)], qs.at[kk, k], qv.at[kk, k], sib)

    def gather_h(k):
        src = pl.multiple_of(vrows * (2 * k + core), vrows)
        dst = span(vrows * k, vrows)
        o_sib[dst, :] = qt[pl.ds(src, vrows), :]
        kvc[dst, :] = (kvrow[pl.ds(src, vrows), :].astype(F32) + pltpu.roll(skv[dst, :].astype(F32), 2 * kn, 1)).astype(BF)

    def final_y(dr, sub, acc):
        rows = span((2 * dr + sub) * pos, pos)
        y_v[rows, :] = (y_v[rows, :].astype(F32) + acc).astype(BF)

    paced = 9

    def step_c(e):
        @pl.when(e == events - 2)
        def _():
            first_sends(1)

        @pl.when(e >= 2)
        def _():
            serve(0, e, final_y)

        @pl.when(e == 0)
        def _():
            for dr in both:
                for k in both:
                    g_ring(dr, k, k + 2, True).wait_send()
                    g_side(dr, k, True).wait_send()
            for k in range(parts):
                wq_push(k).wait_recv()
                wo_push(k).wait_send()
            for c in ld2:
                c.start()
            d_rows[...] = jnp.zeros_like(d_rows)
            gn[...] = jnp.zeros_like(gn)
            qga[...] = jnp.zeros_like(qga)
            kga[...] = jnp.zeros_like(kga)

        each(upto(e, units + heads, paced), upto(e + 1, units + heads, paced), job)

        @pl.when(e == paced)
        def _():
            each(0, 2 * nz, settle)
            each(0, nz, lambda k: [swap(k, kk).start() for kk in both])

        @pl.when(e == paced + 1)
        def _():
            for c in ld2:
                c.wait()
            each(0, nz, lambda k: [swap(k, kk).wait_recv() for kk in both])
            each(0, nz, gather_h)

        @pl.when((e > paced) & (e <= paced + 4))
        def _():
            each(4 * (e - paced - 1), 4 * (e - paced), lambda j: pblock(ph_out, j, h_pairs))

        @pl.when(e == paced + 4)
        def _():
            first_fetch(1, ph_out)

    each(0, events, step_c)

    def gblk(j):
        return qr.at[:, span(lax.rem(j, 2) * bw, bw)]

    def hblk(j):
        return gd.at[:, span(lax.rem(j, 2) * bw, bw)]

    def swo(j):
        return d_rows.at[pl.ds(0, qn), span(lax.rem(j, 2) * bw, bw)]

    def swq(j):
        return d_rows.at[pl.ds(pl.multiple_of(qn + lax.rem(j, 2) * bw, bw), bw), pl.ds(0, qn)]

    def g_load(j):
        return pltpu.make_async_copy(gy_out.at[:, span(j * bw, bw)], gblk(j), gls.at[lax.rem(j, 2)])

    def h_load(j):
        return pltpu.make_async_copy(hid.at[:, span(j * bw, bw)], hblk(j), hls.at[lax.rem(j, 2)])

    def wo_store(j):
        return pltpu.make_async_copy(swo(j), gwo_hbm.at[:, span(j * bw, bw)], swos.at[lax.rem(j, 2)])

    def wq_store(j):
        return pltpu.make_async_copy(swq(j), gq_hbm.at[span(j * bw, bw)], swqs.at[lax.rem(j, 2)])

    def block(j):
        g_load(j).wait()
        h_load(j).wait()

        @pl.when(j + 1 < events)
        def _():
            g_load(j + 1).start()
            h_load(j + 1).start()

        @pl.when(j >= 2)
        def _():
            wo_store(j - 2).wait()
            wq_store(j - 2).wait()
        cols = span(j * bw, bw)
        swo(j)[...] = dotf(o_own[...], gblk(j)[...], TN)
        ge_v[:, cols] = dotf(hotm[...], gblk(j)[...])
        wo_store(j).start()
        swq(j)[...] = dotf(hblk(j)[...], qt[...], TN)
        gkv_v[:, cols] = dotf(kvrow[...], hblk(j)[...], TN)[:2 * kn]
        wq_store(j).start()

    def final_h(dr, sub, gh):
        rows = span((2 * dr + sub) * sub_rows, sub_rows)
        x = gown[rows, :].astype(F32)
        r = lax.rsqrt(jnp.mean(x * x, axis=-1, keepdims=True) + EPS)
        ge_v[rows, :] += rms_pull(x, gh * gain[...], r)
        gn[...] += jnp.sum(gh * (x * r), axis=0, keepdims=True)

    outs = [pltpu.make_async_copy(s, t, out_sem.at[i]) for i, (s, t) in enumerate((
        (y_v, y_hbm), (gkv_v.at[pl.ds(0, kn)], gk_hbm), (gkv_v.at[pl.ds(kn, kn)], gv_hbm), (ge_v, ge_hbm)))]
    g_load(0).start()
    h_load(0).start()
    outs[0].start()
    work_d = events - 3

    def step_d(e):
        @pl.when(e >= 2)
        def _():
            serve(1, e, final_h)

        each(upto(e, events, work_d), upto(e + 1, events, work_d), block)

    each(0, events, step_d)

    outs[3].start()
    wide = gains_out.shape[1]
    for j in range(d // wide):
        gall[rank, j:j + 1, :] = gn[:, j * wide:(j + 1) * wide]
    gall[rank, d // wide:d // wide + 1, :] = qga[...]
    gall[rank, d // wide + 1:d // wide + 2, :] = kga[...]
    outs[1].start()
    outs[2].start()
    for j in (events - 2, events - 1):
        wo_store(j).wait()
        wq_store(j).wait()

    def spread(k, src):
        return rdma(gall.at[src], gall.at[src], gs.at[k], gr.at[k], lax.rem(rank + k, 2 * nz))

    for k in range(1, 2 * nz):
        spread(k, rank).start()

    def drain_c(e):
        for ph in both:
            for dr in both:
                send(ph, dr, e).wait_send()

    each(events - 6, events - 2, drain_c)

    def drain_b(e):
        @pl.when(e < events - 2)
        def _():
            for dr in both:
                g_ring(dr, e, e + 2, False).wait_send()
        for dr in both:
            g_side(dr, e, False).wait_send()

    each(2, events, drain_b)
    to_far.wait_send()
    relay.wait_send()
    for k in both:
        wk_push(k).wait_send()
    for b in range(batch):
        each(0, nz, lambda k: o_push(b, k).wait_send())
        for p in both:
            to_side(b, p).wait_send()
        to_far2(b).wait_send()
    each(0, nz, lambda k: [swap(k, kk).wait_send() for kk in both])
    for k in range(1, 2 * nz):
        spread(k, lax.rem(rank + 2 * nz - k, 2 * nz)).wait_recv()
    gains_out[...] = jnp.sum(gall[...], axis=0)
    for k in range(1, 2 * nz):
        spread(k, rank).wait_send()
    for c in outs:
        c.wait()


def step_kernel(nz, embed, gy, wq, wk_t, wv_t, wo, gain, qg, kg, cos, sin_s, tok_dev, tok_seq):
    vrows, d = embed.shape
    vocab = vrows * 2 * nz
    qn, kn = wq.shape[1], wk_t.shape[0]
    hd = qg.shape[1]
    batch, seq = tok_seq.shape
    toks = batch * seq
    ev = 2 * nz
    sr, hb, vh = vrows // 4, seq // 2, vocab // 2
    grow = (d // hd + 2 + 7) // 8 * 8
    dma = pltpu.SemaphoreType.DMA
    v = pltpu.VMEM

    def arr(dt, *shape):
        return jax.ShapeDtypeStruct(shape, dt)

    outs = (arr(BF, vrows, d), arr(F32, vrows, d), arr(F32, d, qn), arr(F32, kn, d), arr(F32, kn, d), arr(F32, qn, d), arr(F32, grow, hd),
            arr(BF, vocab, d), arr(BF, toks, d), arr(BF, qn, d), arr(BF, qn, d), arr(F32, vh, d), arr(F32, vh, d))
    return pl.pallas_call(
        functools.partial(body, nz),
        name='step_kernel',
        out_shape=outs,
        in_specs=[ANY] * 6 + [VM] * 7,
        out_specs=(ANY,) * 6 + (VM,) + (ANY,) * 6,
        scratch_shapes=[v((vocab, d), BF), v((2 * qn + 4 * kn, d), BF), v((max(d, 2 * toks), qn), BF), v((vocab, qn), BF), v((toks, qn), BF), v((vh, qn), BF), v((vh, qn), BF),
                        v((toks, 2 * hd), BF), v((toks, hd), BF), v((2, toks // 2, 4 * kn), BF), v((2, toks // 2, 4 * kn), BF), v((vocab, 4 * kn), BF), v((vh, 4 * kn), BF), v((vh, 4 * kn), BF),
                        v((vocab, qn + 4 * kn), F32), v((4, 2, sr, d), F32), v((2, vrows, d), BF), v((vrows, d), BF), v((vrows, toks), BF),
                        v((seq, hd), F32), v((seq, hd), F32), v((batch, 4, hb, 4 * kn), BF), v((batch, 2, hb, 4 * kn), BF), v((batch, hb, 4 * kn), BF), v((batch, hb, 4 * kn), F32),
                        v((batch, hb, 4 * kn), BF), v((batch, seq, 4 * kn), BF), v((1, d), F32), v((1, hd), F32), v((1, hd), F32), v((ev, grow, hd), F32), v((vrows, d), BF), v((vrows, d), F32), v((2 * kn, d), F32),
                        dma((12,)), dma((2, 4)), dma((2, 4))] + [dma((2, ev))] * 8 + [dma((2,)), dma((2,))] + [dma((8,))] * 5 + [dma((2,)), dma((2,)), dma((batch, nz)), dma((batch, nz)),
                        dma((2,)), dma((2, 2, 2)), dma((2, 2, ev - 2)), dma((2, 2, ev - 2)), dma((batch, 2)), dma((batch, 2)), dma((batch,)), dma((batch,)), dma((2, nz)), dma((2, nz)),
                        dma((2,)), dma((2,)), dma((2,)), dma((2,)), dma((ev,)), dma((ev,)), dma((4,))],
        compiler_params=pltpu.CompilerParams(collective_id=0, has_side_effects=True, vmem_limit_bytes=67043328),
        cost_estimate=pl.CostEstimate(flops=2 * vocab * d * 8 * qn, bytes_accessed=20 * vocab * d, transcendentals=0),
    )(embed, gy, wq, wk_t, wv_t, wo, gain, qg, kg, cos, sin_s, tok_dev, tok_seq)


def emit_body(cuts, *refs):
    n = len(cuts)
    src, dst = refs[:n], refs[n:2 * n]
    bufs, s_in, s_out = refs[2 * n:-2], refs[-2], refs[-1]
    ins, outs = [], []
    for i, c in enumerate(cuts):
        step = src[i].shape[0] // c
        for j in range(c):
            b = bufs[i].at[pl.ds(j * step, step)]
            ins.append(pltpu.make_async_copy(src[i].at[pl.ds(j * step, step)], b, s_in.at[len(ins)]))
            outs.append(pltpu.make_async_copy(b, dst[i].at[pl.ds(j * step, step)], s_out.at[len(outs)]))
    for c in ins:
        c.start()
    for a, b in zip(ins, outs):
        a.wait()
        b.start()
    for b in outs:
        b.wait()


def emit(*arrays):
    size = 1 << 21
    cuts = tuple(max(1, a.size * a.dtype.itemsize // size) for a in arrays)
    return pl.pallas_call(
        functools.partial(emit_body, cuts),
        name='emit',
        out_shape=tuple(jax.ShapeDtypeStruct(a.shape, a.dtype) for a in arrays),
        in_specs=[ANY] * len(arrays),
        out_specs=(ANY,) * len(arrays),
        scratch_shapes=[pltpu.VMEM(a.shape, a.dtype) for a in arrays] + [pltpu.SemaphoreType.DMA((sum(cuts),))] * 2,
        compiler_params=pltpu.CompilerParams(vmem_limit_bytes=60 * 1024 * 1024),
        cost_estimate=pl.CostEstimate(flops=0, bytes_accessed=2 * sum(a.size * a.dtype.itemsize for a in arrays), transcendentals=0),
    )(*arrays)


def rope_consts(seq, hd):
    inv = np.float32(ROPE_BASE) ** (np.float32(-2.0) * np.arange(hd // 2, dtype=np.float32) / np.float32(hd))
    ang = np.arange(seq, dtype=np.float32)[:, None] * inv.astype(np.float32)[None, :]
    ang = np.concatenate([ang, ang], axis=-1)
    sign = np.where(np.arange(hd) < hd // 2, -1.0, 1.0).astype(np.float32)
    return np.cos(ang).astype(np.float32), (np.sin(ang) * sign).astype(np.float32)


def solution(mesh):
    tp = mesh.shape['tp']
    nz = tp // 2

    def local_step(tok_ids, embed_loc, norm_gain, q_gain, k_gain, wq, wk, wv, wo, gy_loc):
        d_model = embed_loc.shape[1]
        batch, seq = tok_ids.shape
        seq_dev = seq // tp
        hd = q_gain.shape[0]
        cos_c, sin_c = (jnp.asarray(t) for t in rope_consts(seq, hd))
        tok_dev = tok_ids.reshape(batch, tp, seq_dev).transpose(1, 0, 2).reshape(tp, batch * seq_dev)
        r = step_kernel(nz, embed_loc, gy_loc.reshape(batch * seq_dev, d_model), wq, wk.T, wv.T, wo, norm_gain[None, :], q_gain[None, :], k_gain[None, :], cos_c, sin_c, tok_dev, tok_ids)
        y, g_embed, g_wq, g_wk, g_wv, g_wo = emit(*r[:6])
        g_gain = r[6]
        n = d_model // hd
        return (y.reshape(batch, seq_dev, d_model), g_embed, g_gain[:n].reshape(d_model), g_gain[n], g_gain[n + 1], g_wq, g_wk.T, g_wv.T, g_wo)

    in_specs = (P('dp', None), P('tp', None), P(), P(), P(), P(None, 'tp'), P(None, 'tp'), P(None, 'tp'), P('tp', None), P('dp', 'tp', None))
    out_specs = (P('dp', 'tp', None), P(('dp', 'tp'), None), P('dp'), P('dp'), P('dp'), P('dp', 'tp'), P('dp', 'tp'), P('dp', 'tp'), P(('dp', 'tp'), None))
    return jax.shard_map(local_step, mesh=mesh, in_specs=in_specs, out_specs=out_specs, check_vma=False)
```

```python
import functools
import jax
import jax.numpy as jnp
import numpy as np
from jax import lax
from jax.experimental import pallas as pl
from jax.experimental.pallas import tpu as pltpu
from jax.sharding import PartitionSpec as P

BF = jnp.bfloat16
F32 = jnp.float32
EPS = 1.0e-6
ROPE_BASE = 1.0e6
NEG_BIG = -1.0e30
MESH = pl.DeviceIdType.MESH
ANY = pl.BlockSpec(memory_space=pl.ANY)
VM = pl.BlockSpec(memory_space=pltpu.VMEM)
NT = (((1,), (1,)), ((), ()))
NN = (((1,), (0,)), ((), ()))
TN = (((0,), (0,)), ((), ()))


def dotf(a, b, dims=NN):
    return lax.dot_general(a, b, dims, preferred_element_type=F32)


def rdma(src, dst, ssem, rsem, dev):
    return pltpu.make_async_remote_copy(src_ref=src, dst_ref=dst, send_sem=ssem, recv_sem=rsem, device_id={'tp': dev}, device_id_type=MESH)


def span(start, size):
    return pl.ds(pl.multiple_of(start, size), size)


def each(lo, hi, f):
    def go(j, _):
        f(j)
        return 0
    lax.fori_loop(lo, hi, go, 0)


def rms_f32(x, gain):
    return x * lax.rsqrt(jnp.mean(x * x, axis=-1, keepdims=True) + EPS) * gain


def rms_pull(x, dxr, r):
    return r * dxr - x * (r * r * r * jnp.mean(x * dxr, axis=-1, keepdims=True))


def masked(scores, first):
    r_i = lax.broadcasted_iota(jnp.int32, scores.shape, 0) + first
    c_i = lax.broadcasted_iota(jnp.int32, scores.shape, 1)
    return jnp.where(r_i >= c_i, scores, NEG_BIG)


def soft(scores):
    e = jnp.exp(scores - jnp.max(scores, axis=-1, keepdims=True))
    return e * (1.0 / jnp.sum(e, axis=-1, keepdims=True))


def body(nz, embed, gy, wq, wk_t, wv_t, wo, gain, qg, kg, cos, sin_s, tok_dev, tok_seq,
         y_hbm, ge_hbm, gq_hbm, gk_hbm, gv_hbm, gwo_hbm, gains_out, hid, gy_out, wqt_out, wqts_out, py_out, ph_out,
         table, wpair, wq_v, qt, o_own, o_sib, sq, kv_tok, k_rot, kvacc, farkv, kvrow, skv, kvc, d_rows, pbuf, hbuf, gown, hotm,
         dk_acc, dv_acc, pk, rk1, fk, hk, rk2, kvt, gn, qga, kga, gall, qall, y_v, ge_v, gkv_v,
         in_sem, h_sem, g_sem, a_rs, a_rr, a_ss, a_sr, b_rs, b_rr, b_ss, b_sr, xs, xr, ts, wos, wor, wqs, wqr, wks, wkr, o_s, o_r,
         pt_sem, pl_sem, rs, rr, p1s, p1r, p2s, p2r, qs, qv, gls, hls, swos, swqs, gs, gr, out_sem):
    rank = lax.axis_index('tp')
    z, core = rank // 2, lax.rem(rank, 2)
    right = 2 * lax.rem(z + 1, nz) + core
    left = 2 * lax.rem(z + nz - 1, nz) + core
    sib = rank + 1 - 2 * core
    par = lax.rem(z, 2)
    far = rank + 2 - 4 * par
    vrows, d = embed.shape
    kn = wk_t.shape[0]
    sub_rows = vrows // 4
    vocab = vrows * 2 * nz
    vhalf = vocab // 2
    batch, seq = tok_seq.shape
    toks = batch * seq
    qn = wq.shape[1]
    hd = qg.shape[1]
    heads = qn // hd
    events = 2 * nz
    pos = seq // events
    blk = seq // 2
    bw = d // events
    scale = hd ** -0.5
    units = batch * heads
    parts = 8
    wo_p, wq_p = qn // parts, d // parts
    both = (0, 1)
    places = [(dr, c) for dr in both for c in both]
    qr = wq_v.at[pl.ds(0, toks)]
    gd = wq_v.at[pl.ds(toks, toks)]
    w_q = wq_v.at[pl.ds(0, d)]

    ld = [pltpu.make_async_copy(s, t, in_sem.at[i]) for i, (s, t) in enumerate((
        (embed, table.at[span(rank * vrows, vrows)]), (gy, gown), (wq, w_q), (wo, wpair.at[pl.ds(0, qn)]),
        (wk_t, wpair.at[pl.ds(2 * qn, kn)]), (wv_t, wpair.at[pl.ds(2 * qn + kn, kn)])))]
    ld2 = [pltpu.make_async_copy(s, t, in_sem.at[i]) for i, (s, t) in enumerate((
        (wqt_out, wpair.at[pl.ds(0, qn)]), (wqts_out, wpair.at[pl.ds(qn, qn)]), (embed, gown)))]
    for c in ld:
        c.start()
    barrier = pltpu.get_barrier_semaphore()
    for dev in (right, left, sib):
        pl.semaphore_signal(barrier, inc=1, device_id={'tp': dev}, device_id_type=MESH)
    with jax.named_scope('head'):
        pl.semaphore_wait(barrier, 3)
        ld[0].wait()

    def nbr(dr):
        return right if dr == 0 else left

    def zd_of(dr, e):
        s = e // 2
        return lax.rem(z + (nz - s if dr == 0 else s), nz)

    def row_of(dr, e, c):
        return pl.multiple_of(vrows * (2 * zd_of(dr, e) + c) + sub_rows * (2 * dr + lax.rem(e, 2)), sub_rows)

    def ring(dr, e, recv_e):
        a = table.at[pl.ds(row_of(dr, e, core), sub_rows)]
        return rdma(a, a, a_rs.at[dr, e], a_rr.at[dr, recv_e], nbr(dr))

    def side(dr, e):
        a = table.at[pl.ds(row_of(dr, e, core), sub_rows)]
        return rdma(a, a, a_ss.at[dr, e], a_sr.at[dr, e], sib)

    def h_copy(slot, i, row):
        return pltpu.make_async_copy(hbuf.at[slot, pl.ds(i * sub_rows, sub_rows)], hid.at[pl.ds(row, sub_rows)], h_sem.at[slot, i])

    def g_row(dr, e, c):
        return pl.multiple_of(seq * (2 * dr + lax.rem(e, 2)) + pos * (2 * zd_of(dr, e) + c), pos)

    def g_piece(dr, e, c):
        return gy_out.at[pl.ds(g_row(dr, e, c), pos)]

    def g_own(dr, e):
        return gown.at[span(pos * (2 * dr + lax.rem(e, 2)), pos)]

    def g_ring(dr, e, recv_e, first):
        a = g_piece(dr, e, core)
        return rdma(g_own(dr, e) if first else a, a, b_rs.at[dr, e], b_rr.at[dr, recv_e], nbr(dr))

    def g_side(dr, e, first):
        a = g_piece(dr, e, core)
        return rdma(g_own(dr, e) if first else a, a, b_ss.at[dr, e], b_sr.at[dr, e], sib)

    def g_home(dr, e):
        return pltpu.make_async_copy(g_own(dr, e), g_piece(dr, e, core), in_sem.at[8 + 2 * dr + e])

    def g_fetch(slot, i, dr, c, e):
        return pltpu.make_async_copy(g_piece(dr, e, c), hbuf.at[slot, pl.ds(i * pos, pos)], g_sem.at[slot, i])

    def wo_push(k):
        return rdma(wpair.at[span(k * wo_p, wo_p)], wpair.at[pl.ds(pl.multiple_of(qn + k * wo_p, wo_p), wo_p)], wos.at[k], wor.at[k], sib)

    def tb(k):
        return o_own.at[span(lax.rem(k, 2) * qn, qn), pl.ds(0, wq_p)]

    def wq_push(k):
        return rdma(tb(k), wqts_out.at[:, span(k * wq_p, wq_p)], wqs.at[k], wqr.at[k], sib)

    def wq_home(k):
        return pltpu.make_async_copy(tb(k), wqt_out.at[:, span(k * wq_p, wq_p)], ts.at[k])

    def wk_push(k):
        return rdma((wk_t, wv_t)[k], wpair.at[pl.ds(2 * qn + (2 + k) * kn, kn)], wks.at[k], wkr.at[k], sib)

    def o_push(b, k):
        src = pl.multiple_of(b * seq + pos * (2 * k + 1 - core), pos)
        dst = pl.multiple_of(vrows * k + pos * b, pos)
        return rdma(o_own.at[pl.ds(src, pos)], o_sib.at[pl.ds(dst, pos)], o_s.at[b, k], o_r.at[b, k], sib)

    def project(e):
        slot = lax.rem(e, 2)

        @pl.when(e >= 2)
        def _():
            for i in range(4):
                h_copy(slot, i, row_of(0, e, core)).wait()

        rows = [row_of(dr, e, c) for dr, c in places]
        for i, row in enumerate(rows):
            x = table[pl.ds(row, sub_rows), :].astype(F32)
            ids = row + lax.broadcasted_iota(jnp.int32, (sub_rows, tok_dev.shape[1]), 0)
            hit = jnp.zeros((sub_rows, tok_dev.shape[1]), F32)
            for j in range(tok_dev.shape[0]):
                hit = jnp.maximum(hit, jnp.where(tok_dev[j:j + 1, :] == ids, 1.0, 0.0))
            used = jnp.max(hit, axis=1, keepdims=True)
            h = jnp.where(used > 0.5, rms_f32(x, gain[...]), 0.0)
            hbuf[slot, pl.ds(i * sub_rows, sub_rows), :] = h.astype(BF)
            h_copy(slot, i, row).start()
        hb = hbuf[slot]
        qkv = jnp.concatenate([dotf(hb, w_q[...]).astype(BF), dotf(hb, wpair[2 * qn:2 * qn + 4 * kn, :], NT).astype(BF)], axis=1)
        lane = lax.broadcasted_iota(jnp.int32, (1, vrows), 1)
        rowid = jnp.zeros((1, vrows), jnp.int32)
        for i, row in enumerate(rows):
            rowid = jnp.where(lane // sub_rows == i, row + lane - i * sub_rows, rowid)
        rowid = rowid.astype(F32)
        for b in range(batch):
            sl = slice(b * seq, (b + 1) * seq)
            hot = jnp.where(d_rows[sl, :vrows] == rowid, 1.0, 0.0).astype(BF)
            got = dotf(hot, qkv)
            qt[sl, :] = (qt[sl, :].astype(F32) + got[:, :qn]).astype(BF)
            at = slice((b % 2) * seq, (b % 2 + 1) * seq)
            kvacc[b // 2, at, :] = (kvacc[b // 2, at, :].astype(F32) + got[:, qn:]).astype(BF)

    def step_a(e):
        with jax.named_scope('a_wait'):
            @pl.when((e >= 2) & (e < events))
            def _():
                for dr in both:
                    ring(dr, e, e).wait_recv()

        @pl.when(e < events - 2)
        def _():
            for dr in both:
                ring(dr, e, e + 2).start()

        @pl.when(e < events)
        def _():
            for dr in both:
                side(dr, e).start()

        @pl.when(e == 0)
        def _():
            for k in both:
                wk_push(k).start()
            for b in range(batch):
                wide = jnp.broadcast_to(tok_seq[b:b + 1, :].astype(F32), (vrows, seq))
                d_rows[b * seq:(b + 1) * seq, :vrows] = wide.T
            qt[...] = jnp.zeros_like(qt)
            kvacc[...] = jnp.zeros_like(kvacc)

        @pl.when(e == 1)
        def _():
            for c in ld[1:]:
                c.wait()
            for k in both:
                wk_push(k).wait_recv()
            for dr in both:
                for k in both:
                    g_home(dr, k).start()

        @pl.when(e == events - 2)
        def _():
            for dr in both:
                g_ring(dr, 0, 2, True).start()

        @pl.when((e >= 2) & (e < 4 + parts))
        def _():
            @pl.when(e >= 4)
            def _():
                wq_push(e - 4).wait_send()
                wq_home(e - 4).wait()

            @pl.when(e < 2 + parts)
            def _():
                k = e - 2
                block = wq_v[span(k * wq_p, wq_p), :]
                tb(k)[...] = block.astype(F32).T.astype(BF)
                wo_push(k).start()
                wq_push(k).start()
                wq_home(k).start()

        with jax.named_scope('a_proj'):
            @pl.when(e >= 1)
            def _():
                for dr in both:
                    side(dr, e - 1).wait_recv()
                project(e - 1)

    each(0, events + 1, step_a)

    to_far = rdma(kvacc.at[core], farkv.at[core], xs.at[0], xr.at[0], far)
    relay = rdma(farkv.at[core], farkv.at[core], xs.at[1], xr.at[1], sib)
    mine = jnp.broadcast_to(tok_dev[pl.ds(rank, 1), :].astype(F32), (vrows, tok_dev.shape[1]))
    col = mine.T.astype(jnp.int32)
    lanes = lax.broadcasted_iota(jnp.int32, col.shape, 1)
    hot_mine = jnp.concatenate([jnp.where(col == lanes + j * vrows, 1.0, 0.0).astype(BF) for j in range(vocab // vrows)], axis=1)
    to_far.start()
    for dr in both:
        g_ring(dr, 1, 3, True).start()
        for k in both:
            g_side(dr, k, True).start()
            g_home(dr, k).wait()
    cw = min(512, d)

    def own_rows(j):
        y_v[:, span(j * cw, cw)] = dotf(hot_mine, table[:, span(j * cw, cw)]).astype(BF)

    each(0, d // cw, own_rows)
    for b in range(batch):
        ids = rank * vrows + lax.broadcasted_iota(jnp.int32, (vrows, seq), 0)
        hotm[:, b * seq:(b + 1) * seq] = jnp.where(ids == tok_seq[b:b + 1, :], 1.0, 0.0).astype(BF)

    def place(p, first):
        l_i = lax.broadcasted_iota(jnp.int32, (4 * kn, 2 * hd), 0)
        m_i = lax.broadcasted_iota(jnp.int32, (4 * kn, 2 * hd), 1)
        upper = jnp.where(l_i >= 2 * kn, 1, 0)
        owner = jnp.where(upper == 1, 1 - first, first)
        l_i = l_i - 2 * kn * upper
        base = kn * (2 * p + owner)
        want = jnp.where(l_i < kn, base + l_i, hd + base + l_i - kn)
        return jnp.where(m_i == want, 1.0, 0.0).astype(BF)

    def rope(raw, g):
        n = rms_f32(raw.astype(F32), g)
        return (n * cos[...] + pltpu.roll(n, hd // 2, 1) * sin_s[...]).astype(BF)

    def attend(u):
        base = (u // heads) * seq
        rows = span(base, seq)
        cols = span(lax.rem(u, heads) * hd, hd)
        q = rope(qt[rows, cols], qg[...])
        qr[rows, cols] = q
        kr = k_rot[rows, :]
        v = kv_tok[rows, hd:]
        for i in both:
            n = blk * (i + 1)
            s = masked(dotf(q[i * blk:(i + 1) * blk], kr[:n], NT) * scale, i * blk)
            o_own[pl.ds(pl.multiple_of(base + i * blk, blk), blk), cols] = dotf(soft(s).astype(BF), v[:n]).astype(BF)

    def grad_attend(e):
        slot = lax.rem(e, 2)
        for i, (dr, c) in enumerate(places):
            g_fetch(slot, i, dr, c, e).wait()
        r = dotf(hbuf[slot], wpair[:qn, :], NT).astype(BF)
        for i, (dr, c) in enumerate(places):
            gd[pl.ds(g_row(dr, e, c), pos), :] = r[i * pos:(i + 1) * pos]

    def pstage(j):
        return d_rows.at[span(lax.rem(j, 2) * vhalf, vhalf), pl.ds(0, bw)]

    def pstore(dst, j):
        return pltpu.make_async_copy(pstage(j), dst.at[:, span(j * bw, bw)], pt_sem.at[lax.rem(j, 2)])

    def pblock(dst, j, pairs):
        @pl.when(j >= 2)
        def _():
            pstore(dst, j - 2).wait()
        cols = span(j * bw, bw)
        acc = None
        for a, lo, n in pairs:
            t = dotf(a[...], wpair[lo:lo + n, cols])
            acc = t if acc is None else acc + t
        pstage(j)[...] = acc
        pstore(dst, j).start()

    y_pairs = [(sq, 0, qn), (o_sib, qn, qn)]
    h_pairs = [(o_sib, 0, qn), (sq, qn, qn), (kvc, 2 * qn, 4 * kn)]

    def pslot(ph, e, dr):
        return pbuf.at[2 * ph + lax.rem(e, 2), dr]

    def pfetch(ph, e, dr):
        s = e // 2
        zd = lax.rem(z + (2 * nz - 1 - s if dr == 0 else 1 + s), nz)
        row = pl.multiple_of(vrows * zd + sub_rows * (2 * dr + lax.rem(e, 2)), sub_rows)
        return pltpu.make_async_copy((py_out, ph_out)[ph].at[pl.ds(row, sub_rows)], pslot(ph, e, dr), pl_sem.at[ph, lax.rem(e, 2), dr])

    def rslot(dr, e):
        return table.at[span((dr * (events - 2) + e) * sub_rows, sub_rows)]

    def sslot(ph, dr, e):
        k = 2 * (events - 2) + 8 * ph + 4 * lax.rem(e // 2, 2) + 2 * dr + lax.rem(e, 2)
        return table.at[span(k * sub_rows, sub_rows)]

    def send(ph, dr, e):
        return rdma(sslot(ph, dr, e), rslot(dr, e), rs.at[ph, dr, e], rr.at[ph, dr, e], nbr(dr))

    def first_fetch(ph, dst):
        for j in (events - 2, events - 1):
            pstore(dst, j).wait()
        for e in both:
            for dr in both:
                pfetch(ph, e, dr).start()

    def first_sends(ph):
        for e in both:
            for dr in both:
                pfetch(ph, e, dr).wait()
                sslot(ph, dr, e)[...] = pslot(ph, e, dr)[...].astype(BF)
        for e in both:
            for dr in both:
                send(ph, dr, e).start()
                pfetch(ph, e + 2, dr).start()

    def serve(ph, e, final):
        for dr in both:
            send(ph, dr, e - 2).wait_recv()
            pfetch(ph, e, dr).wait()

        @pl.when(e < events - 2)
        def _():
            @pl.when(e >= 4)
            def _():
                for dr in both:
                    send(ph, dr, e - 4).wait_send()
            for dr in both:
                sslot(ph, dr, e)[...] = (pslot(ph, e, dr)[...] + rslot(dr, e - 2)[...].astype(F32)).astype(BF)
            for dr in both:
                send(ph, dr, e).start()
                pfetch(ph, e + 2, dr).start()

        @pl.when(e >= events - 2)
        def _():
            for dr in both:
                final(dr, lax.rem(e, 2), pslot(ph, e, dr)[...] + rslot(dr, e - 2)[...].astype(F32))

    slots = 9

    def gather_o(k):
        for b in range(batch):
            src = pl.multiple_of(b * seq + pos * (2 * k + core), pos)
            sq[pl.ds(pl.multiple_of(vrows * k + pos * b, pos), pos), :] = o_own[pl.ds(src, pos), :]

    def upto(e, n, over):
        return jnp.minimum((e * n) // over, n)

    def step_b(e):
        with jax.named_scope('b_first'):
            @pl.when(e == events - 2)
            def _():
                first_sends(0)

        with jax.named_scope('b_wait'):
            @pl.when((e >= 2) & (e < events))
            def _():
                for dr in both:
                    g_ring(dr, e, e, False).wait_recv()

        @pl.when((e >= 2) & (e < events - 2))
        def _():
            for dr in both:
                g_ring(dr, e, e + 2, False).start()

        @pl.when((e >= 2) & (e < events))
        def _():
            for dr in both:
                g_side(dr, e, False).start()

        @pl.when((e >= 1) & (e <= events))
        def _():
            for dr in both:
                g_side(dr, e - 1, False).wait_recv()
            for i, (dr, c) in enumerate(places):
                g_fetch(lax.rem(e - 1, 2), i, dr, c, e - 1).start()

        with jax.named_scope('kv_far'):
            @pl.when(e == 2)
            def _():
                to_far.wait_recv()
                relay.start()

        with jax.named_scope('kv_tok'):
            @pl.when(e == 3)
            def _():
                rdma(farkv.at[1 - core], farkv.at[1 - core], xs.at[1], xr.at[1], sib).wait_recv()
                for hf in both:
                    kv_tok[hf * (toks // 2):(hf + 1) * (toks // 2), :] = (dotf(kvacc[hf], place(par, core)) + dotf(farkv[hf], place(1 - par, hf))).astype(BF)
                for b in range(batch):
                    sl = slice(b * seq, (b + 1) * seq)
                    k_rot[sl, :] = rope(kv_tok[sl, :hd], kg[...])

        def give(b):
            each(0, nz, lambda k: o_push(b, k).start())

        def seen(t):
            return jnp.minimum((jnp.maximum(t - 3, 0) * units) // (slots - 3), units)

        each(seen(e - 1) // heads, seen(e) // heads, give)
        with jax.named_scope('b_attend'):
            each(seen(e), seen(e + 1), attend)

        @pl.when(e == 4)
        def _():
            def drain(k):
                @pl.when(k < events - 2)
                def _():
                    for dr in both:
                        ring(dr, k, k + 2).wait_send()
                for dr in both:
                    side(dr, k).wait_send()
            each(0, events, drain)

        @pl.when(e == slots + 1)
        def _():
            for k in range(parts):
                wo_push(k).wait_recv()
            for b in range(batch):
                each(0, nz, lambda k: o_push(b, k).wait_recv())
            each(0, nz, gather_o)

        with jax.named_scope('b_part'):
            @pl.when((e > slots) & (e <= slots + 4))
            def _():
                each(4 * (e - slots - 1), 4 * (e - slots), lambda j: pblock(py_out, j, y_pairs))

        @pl.when(e == slots + 4)
        def _():
            first_fetch(0, py_out)

        with jax.named_scope('b_grad'):
            @pl.when(e >= 2)
            def _():
                grad_attend(e - 2)

    for slot in both:
        for i in range(4):
            h_copy(slot, i, row_of(0, 0, core)).wait()
    each(0, events + 2, step_b)

    def pull(raw, dout, g):
        x = raw.astype(F32)
        r = lax.rsqrt(jnp.mean(x * x, axis=-1, keepdims=True) + EPS)
        dn = dout * cos[...] + pltpu.roll(dout * sin_s[...], hd // 2, 1)
        return rms_pull(x, dn * g, r).astype(BF), jnp.sum(dn * (x * r), axis=0, keepdims=True)

    def unit(u):
        b, h = u // heads, lax.rem(u, heads)
        rows = span(b * seq, seq)
        cols = span(h * hd, hd)

        @pl.when(h == 0)
        def _():
            dk_acc[...] = jnp.zeros_like(dk_acc)
            dv_acc[...] = jnp.zeros_like(dv_acc)
        q, g = qr[rows, cols], gd[rows, cols]
        kr, v = k_rot[rows, :], kv_tok[rows, hd:]
        dqs = []
        for i in both:
            n = blk * (i + 1)
            qi, gi = q[i * blk:(i + 1) * blk], g[i * blk:(i + 1) * blk]
            p = soft(masked(dotf(qi, kr[:n], NT) * scale, i * blk))
            dp = dotf(gi, v[:n], NT)
            dv_acc[:n, :] += dotf(p.astype(BF), gi, TN)
            ds = (p * (dp - jnp.sum(p * dp, axis=-1, keepdims=True)) * scale).astype(BF)
            dqs.append(dotf(ds, kr[:n]))
            dk_acc[:n, :] += dotf(ds, qi, TN)
        dq = jnp.concatenate(dqs, axis=0).astype(BF).astype(F32)
        dx, dg = pull(qt[rows, cols], dq, qg[...])
        gd[rows, cols] = dx
        qga[...] += dg

    def pick(r, up):
        m_i = lax.broadcasted_iota(jnp.int32, (2 * hd, 4 * kn), 0)
        l_i = lax.broadcasted_iota(jnp.int32, (2 * hd, 4 * kn), 1) - 2 * kn * up
        is_k = (l_i >= 0) & (l_i < kn) & (m_i == l_i + kn * r)
        is_v = (l_i >= kn) & (l_i < 2 * kn) & (m_i == hd + kn * r + l_i - kn)
        return jnp.where(is_k | is_v, 1.0, 0.0).astype(BF)

    def to_side(b, p):
        return rdma(pk.at[b, 2 * p + 1 - core], rk1.at[b, p], p1s.at[b, p], p1r.at[b, p], sib)

    def to_far2(b):
        return rdma(fk.at[b], rk2.at[b], p2s.at[b], p2r.at[b], far)

    def kv_one(b):
        dk = dk_acc[...].astype(BF).astype(F32)
        dx, dg = pull(kv_tok[span(b * seq, seq), :hd], dk, kg[...])
        kga[...] += dg
        gkv = jnp.concatenate([dx, dv_acc[...].astype(BF)], axis=1)
        for r in range(4):
            pk[b, r] = (dotf(gkv[:blk], pick(r, 0)) + dotf(gkv[blk:], pick(r, 1))).astype(BF)
        for p in both:
            to_side(b, p).start()

    def kv_two(b):
        for p in both:
            to_side(b, p).wait_recv()
        fk[b] = (pk[b, 2 * (1 - par) + core].astype(F32) + rk1[b, 1 - par].astype(F32)).astype(BF)
        hk[b] = pk[b, 2 * par + core].astype(F32) + rk1[b, par].astype(F32)
        to_far2(b).start()

    def kv_three(b):
        to_far2(b).wait_recv()
        t = hk[b] + rk2[b].astype(F32)
        low = lax.broadcasted_iota(jnp.int32, t.shape, 1) < 2 * kn
        kvt[b, :blk, :] = jnp.where(low, t, 0.0).astype(BF)
        kvt[b, blk:, :] = jnp.where(low, pltpu.roll(t, 2 * kn, 1), 0.0).astype(BF)

    def fold(b, tile):
        rows = span(tile * seq, seq)
        ids = tile * seq + lax.broadcasted_iota(jnp.int32, (seq, seq), 0)
        hot = jnp.where(ids == tok_seq[pl.ds(b, 1), :], 1.0, 0.0).astype(BF)
        d_rows[rows, :qn] += dotf(hot, gd[span(b * seq, seq), :])
        d_rows[rows, qn:] += dotf(hot, kvt[b])

    tiles = vocab // seq

    def run_unit(u):
        unit(u)

        @pl.when(lax.rem(u, heads) == heads - 1)
        def _():
            kv_one(u // heads)

        @pl.when((u >= heads) & (lax.rem(u, heads) == 1))
        def _():
            kv_two(u // heads - 1)

    def run_fold(f):
        b, tile = f // tiles, lax.rem(f, tiles)

        @pl.when(tile == 0)
        def _():
            kv_three(b)
        fold(b, tile)

    def share(e, first, n, over):
        return jnp.minimum((jnp.maximum(e - first, 0) * n) // over, n)

    def paced(e, first, n, over, f):
        each(share(e, first, n, over), share(e + 1, first, n, over), f)

    def settle(t):
        rows = span(t * vrows, vrows)
        qt[rows, :] = d_rows[rows, :qn].astype(BF)
        kvrow[rows, :] = d_rows[rows, qn:].astype(BF)

    def swap(k, kk):
        src = pl.multiple_of(vrows * (2 * k + 1 - core), vrows)
        return rdma((qt, kvrow)[kk].at[pl.ds(src, vrows)], (sq, skv)[kk].at[span(vrows * k, vrows)], qs.at[kk, k], qv.at[kk, k], sib)

    def gather_h(k):
        src = pl.multiple_of(vrows * (2 * k + core), vrows)
        dst = span(vrows * k, vrows)
        o_sib[dst, :] = qt[pl.ds(src, vrows), :]
        kvc[dst, :] = (kvrow[pl.ds(src, vrows), :].astype(F32) + pltpu.roll(skv[dst, :].astype(F32), 2 * kn, 1)).astype(BF)

    def final_y(dr, sub, acc):
        rows = span((2 * dr + sub) * pos, pos)
        y_v[rows, :] = (y_v[rows, :].astype(F32) + acc).astype(BF)

    def step_c(e):
        with jax.named_scope('c_first'):
            @pl.when(e == events - 2)
            def _():
                first_sends(1)

        with jax.named_scope('c_serve'):
            @pl.when(e >= 2)
            def _():
                serve(0, e, final_y)

        @pl.when(e == 0)
        def _():
            for dr in both:
                for k in both:
                    g_ring(dr, k, k + 2, True).wait_send()
                    g_side(dr, k, True).wait_send()
            for k in range(parts):
                wq_push(k).wait_recv()
                wo_push(k).wait_send()
            for c in ld2:
                c.start()
            d_rows[...] = jnp.zeros_like(d_rows)
            gn[...] = jnp.zeros_like(gn)
            qga[...] = jnp.zeros_like(qga)
            kga[...] = jnp.zeros_like(kga)

        with jax.named_scope('c_unit'):
            paced(e, 2, units, 5, run_unit)

        with jax.named_scope('c_kv2'):
            @pl.when(e == 7)
            def _():
                kv_two(batch - 1)
        with jax.named_scope('c_fold'):
            paced(e, 7, batch * tiles, 3, run_fold)

        with jax.named_scope('c_settle'):
            @pl.when(e == 9)
            def _():
                each(0, 2 * nz, settle)
                each(0, nz, lambda k: [swap(k, kk).start() for kk in both])

        with jax.named_scope('c_swap'):
            @pl.when(e == 10)
            def _():
                for c in ld2:
                    c.wait()
                each(0, nz, lambda k: [swap(k, kk).wait_recv() for kk in both])
                each(0, nz, gather_h)
        with jax.named_scope('c_part'):
            paced(e, 10, events, 3, lambda j: pblock(ph_out, j, h_pairs))

        @pl.when(e == 12)
        def _():
            first_fetch(1, ph_out)

    each(0, events, step_c)

    def gblk(j):
        return qr.at[:, span(lax.rem(j, 2) * bw, bw)]

    def hblk(j):
        return gd.at[:, span(lax.rem(j, 2) * bw, bw)]

    def swo(j):
        return d_rows.at[pl.ds(0, qn), span(lax.rem(j, 2) * bw, bw)]

    def swq(j):
        return d_rows.at[pl.ds(pl.multiple_of(qn + lax.rem(j, 2) * bw, bw), bw), pl.ds(0, qn)]

    def g_load(j):
        return pltpu.make_async_copy(gy_out.at[:, span(j * bw, bw)], gblk(j), gls.at[lax.rem(j, 2)])

    def h_load(j):
        return pltpu.make_async_copy(hid.at[:, span(j * bw, bw)], hblk(j), hls.at[lax.rem(j, 2)])

    def wo_store(j):
        return pltpu.make_async_copy(swo(j), gwo_hbm.at[:, span(j * bw, bw)], swos.at[lax.rem(j, 2)])

    def wq_store(j):
        return pltpu.make_async_copy(swq(j), gq_hbm.at[span(j * bw, bw)], swqs.at[lax.rem(j, 2)])

    def block(j):
        g_load(j).wait()
        h_load(j).wait()

        @pl.when(j + 1 < events)
        def _():
            g_load(j + 1).start()
            h_load(j + 1).start()

        @pl.when(j >= 2)
        def _():
            wo_store(j - 2).wait()
            wq_store(j - 2).wait()
        cols = span(j * bw, bw)
        swo(j)[...] = dotf(o_own[...], gblk(j)[...], TN)
        ge_v[:, cols] = dotf(hotm[...], gblk(j)[...])
        wo_store(j).start()
        swq(j)[...] = dotf(hblk(j)[...], qt[...], TN)
        gkv_v[:, cols] = dotf(kvrow[...], hblk(j)[...], TN)[:2 * kn]
        wq_store(j).start()

    def final_h(dr, sub, gh):
        rows = span((2 * dr + sub) * sub_rows, sub_rows)
        x = gown[rows, :].astype(F32)
        r = lax.rsqrt(jnp.mean(x * x, axis=-1, keepdims=True) + EPS)
        ge_v[rows, :] += rms_pull(x, gh * gain[...], r)
        gn[...] += jnp.sum(gh * (x * r), axis=0, keepdims=True)

    outs = [pltpu.make_async_copy(s, t, out_sem.at[i]) for i, (s, t) in enumerate((
        (y_v, y_hbm), (gkv_v.at[pl.ds(0, kn)], gk_hbm), (gkv_v.at[pl.ds(kn, kn)], gv_hbm), (ge_v, ge_hbm)))]
    g_load(0).start()
    h_load(0).start()
    outs[0].start()
    work_d = events - 3

    wide = gains_out.shape[1]
    gtop = d // wide
    order = sorted(range(1, 2 * nz), key=lambda k: -min((k + 1) // 2, nz - k // 2))

    def spread(t, k, src):
        buf = (gall, qall)[t]
        return rdma(buf.at[src], buf.at[src], gs.at[t, k], gr.at[t, k], lax.rem(rank + k, 2 * nz))

    def step_d(e):
        with jax.named_scope('d_serve'):
            @pl.when(e >= 2)
            def _():
                serve(1, e, final_h)

        @pl.when(e == 1)
        def _():
            qall[rank, 0:1, :] = qga[...]
            qall[rank, 1:2, :] = kga[...]

        @pl.when(e == 2)
        def _():
            for k in order:
                spread(1, k, rank).start()

        with jax.named_scope('d_block'):
            paced(e, 0, events, work_d, block)

    each(0, events, step_d)

    for j in range(gtop):
        gall[rank, j:j + 1, :] = gn[:, j * wide:(j + 1) * wide].astype(gall.dtype)
    outs[3].start()
    outs[1].start()
    outs[2].start()
    with jax.named_scope('t_store'):
        for j in (events - 2, events - 1):
            wo_store(j).wait()
            wq_store(j).wait()
    for k in order:
        spread(0, k, rank).start()

    def drain_c(e):
        for ph in both:
            for dr in both:
                send(ph, dr, e).wait_send()

    each(events - 6, events - 2, drain_c)

    def drain_b(e):
        @pl.when(e < events - 2)
        def _():
            for dr in both:
                g_ring(dr, e, e + 2, False).wait_send()
        for dr in both:
            g_side(dr, e, False).wait_send()

    each(2, events, drain_b)
    to_far.wait_send()
    relay.wait_send()
    for k in both:
        wk_push(k).wait_send()
    for b in range(batch):
        each(0, nz, lambda k: o_push(b, k).wait_send())
        for p in both:
            to_side(b, p).wait_send()
        to_far2(b).wait_send()
    each(0, nz, lambda k: [swap(k, kk).wait_send() for kk in both])
    with jax.named_scope('gain_wait'):
        for k in reversed(order):
            spread(1, k, lax.rem(rank + 2 * nz - k, 2 * nz)).wait_recv()
            spread(0, k, lax.rem(rank + 2 * nz - k, 2 * nz)).wait_recv()
    with jax.named_scope('gain_sum'):
        total = gall[0].astype(F32)
        for r in range(1, 2 * nz):
            total = total + gall[r].astype(F32)
        gains_out[0:gtop, :] = total
        gains_out[gtop:, :] = jnp.sum(qall[...], axis=0)
        for k in order:
            spread(0, k, rank).wait_send()
            spread(1, k, rank).wait_send()
    with jax.named_scope('t_outs'):
        for c in outs:
            c.wait()


def step_kernel(nz, embed, gy, wq, wk_t, wv_t, wo, gain, qg, kg, cos, sin_s, tok_dev, tok_seq):
    vrows, d = embed.shape
    vocab = vrows * 2 * nz
    qn, kn = wq.shape[1], wk_t.shape[0]
    hd = qg.shape[1]
    batch, seq = tok_seq.shape
    toks = batch * seq
    ev = 2 * nz
    sr, hb, vh = vrows // 4, seq // 2, vocab // 2
    grow = d // hd + 8
    dma = pltpu.SemaphoreType.DMA
    v = pltpu.VMEM

    def arr(dt, *shape):
        return jax.ShapeDtypeStruct(shape, dt)

    outs = (arr(BF, vrows, d), arr(F32, vrows, d), arr(F32, d, qn), arr(F32, kn, d), arr(F32, kn, d), arr(F32, qn, d), arr(F32, grow, hd),
            arr(BF, vocab, d), arr(BF, toks, d), arr(BF, qn, d), arr(BF, qn, d), arr(F32, vh, d), arr(F32, vh, d))
    return pl.pallas_call(
        functools.partial(body, nz),
        name='step_kernel',
        out_shape=outs,
        in_specs=[ANY] * 6 + [VM] * 7,
        out_specs=(ANY,) * 6 + (VM,) + (ANY,) * 6,
        scratch_shapes=[v((vocab, d), BF), v((2 * qn + 4 * kn, d), BF), v((max(d, 2 * toks), qn), BF), v((vocab, qn), BF), v((toks, qn), BF), v((vh, qn), BF), v((vh, qn), BF),
                        v((toks, 2 * hd), BF), v((toks, hd), BF), v((2, toks // 2, 4 * kn), BF), v((2, toks // 2, 4 * kn), BF), v((vocab, 4 * kn), BF), v((vh, 4 * kn), BF), v((vh, 4 * kn), BF),
                        v((vocab, qn + 4 * kn), F32), v((4, 2, sr, d), F32), v((2, vrows, d), BF), v((vrows, d), BF), v((vrows, toks), BF),
                        v((seq, hd), F32), v((seq, hd), F32), v((batch, 4, hb, 4 * kn), BF), v((batch, 2, hb, 4 * kn), BF), v((batch, hb, 4 * kn), BF), v((batch, hb, 4 * kn), F32),
                        v((batch, hb, 4 * kn), BF), v((batch, seq, 4 * kn), BF), v((1, d), F32), v((1, hd), F32), v((1, hd), F32), v((ev, d // hd, hd), BF), v((ev, 8, hd), F32), v((vrows, d), BF), v((vrows, d), F32), v((2 * kn, d), F32),
                        dma((12,)), dma((2, 4)), dma((2, 4))] + [dma((2, ev))] * 8 + [dma((2,)), dma((2,))] + [dma((8,))] * 5 + [dma((2,)), dma((2,)), dma((batch, nz)), dma((batch, nz)),
                        dma((2,)), dma((2, 2, 2)), dma((2, 2, ev - 2)), dma((2, 2, ev - 2)), dma((batch, 2)), dma((batch, 2)), dma((batch,)), dma((batch,)), dma((2, nz)), dma((2, nz)),
                        dma((2,)), dma((2,)), dma((2,)), dma((2,)), dma((2, ev)), dma((2, ev)), dma((4,))],
        compiler_params=pltpu.CompilerParams(collective_id=0, has_side_effects=True, vmem_limit_bytes=67043328),
        cost_estimate=pl.CostEstimate(flops=2 * vocab * d * 8 * qn, bytes_accessed=20 * vocab * d, transcendentals=0),
    )(embed, gy, wq, wk_t, wv_t, wo, gain, qg, kg, cos, sin_s, tok_dev, tok_seq)


def emit_body(cuts, *refs):
    n = len(cuts)
    src, dst = refs[:n], refs[n:2 * n]
    bufs, s_in, s_out = refs[2 * n:-2], refs[-2], refs[-1]
    ins, outs = [], []
    for i, c in enumerate(cuts):
        step = src[i].shape[0] // c
        for j in range(c):
            b = bufs[i].at[pl.ds(j * step, step)]
            ins.append(pltpu.make_async_copy(src[i].at[pl.ds(j * step, step)], b, s_in.at[len(ins)]))
            outs.append(pltpu.make_async_copy(b, dst[i].at[pl.ds(j * step, step)], s_out.at[len(outs)]))
    for c in ins:
        c.start()
    for a, b in zip(ins, outs):
        a.wait()
        b.start()
    for b in outs:
        b.wait()


def emit(*arrays):
    size = 1 << 21
    cuts = tuple(max(1, a.size * a.dtype.itemsize // size) for a in arrays)
    return pl.pallas_call(
        functools.partial(emit_body, cuts),
        name='emit',
        out_shape=tuple(jax.ShapeDtypeStruct(a.shape, a.dtype) for a in arrays),
        in_specs=[ANY] * len(arrays),
        out_specs=(ANY,) * len(arrays),
        scratch_shapes=[pltpu.VMEM(a.shape, a.dtype) for a in arrays] + [pltpu.SemaphoreType.DMA((sum(cuts),))] * 2,
        compiler_params=pltpu.CompilerParams(vmem_limit_bytes=60 * 1024 * 1024),
        cost_estimate=pl.CostEstimate(flops=0, bytes_accessed=2 * sum(a.size * a.dtype.itemsize for a in arrays), transcendentals=0),
    )(*arrays)


def rope_consts(seq, hd):
    inv = np.float32(ROPE_BASE) ** (np.float32(-2.0) * np.arange(hd // 2, dtype=np.float32) / np.float32(hd))
    ang = np.arange(seq, dtype=np.float32)[:, None] * inv.astype(np.float32)[None, :]
    ang = np.concatenate([ang, ang], axis=-1)
    sign = np.where(np.arange(hd) < hd // 2, -1.0, 1.0).astype(np.float32)
    return np.cos(ang).astype(np.float32), (np.sin(ang) * sign).astype(np.float32)


def solution(mesh):
    tp = mesh.shape['tp']
    nz = tp // 2

    def local_step(tok_ids, embed_loc, norm_gain, q_gain, k_gain, wq, wk, wv, wo, gy_loc):
        d_model = embed_loc.shape[1]
        batch, seq = tok_ids.shape
        seq_dev = seq // tp
        hd = q_gain.shape[0]
        cos_c, sin_c = (jnp.asarray(t) for t in rope_consts(seq, hd))
        tok_dev = tok_ids.reshape(batch, tp, seq_dev).transpose(1, 0, 2).reshape(tp, batch * seq_dev)
        r = step_kernel(nz, embed_loc, gy_loc.reshape(batch * seq_dev, d_model), wq, wk.T, wv.T, wo, norm_gain[None, :], q_gain[None, :], k_gain[None, :], cos_c, sin_c, tok_dev, tok_ids)
        y, g_embed, g_wq, g_wk, g_wv, g_wo = emit(*r[:6])
        g_gain = r[6]
        n = d_model // hd
        return (y.reshape(batch, seq_dev, d_model), g_embed, g_gain[:n].reshape(d_model), g_gain[n], g_gain[n + 1], g_wq, g_wk.T, g_wv.T, g_wo)

    in_specs = (P('dp', None), P('tp', None), P(), P(), P(), P(None, 'tp'), P(None, 'tp'), P(None, 'tp'), P('tp', None), P('dp', 'tp', None))
    out_specs = (P('dp', 'tp', None), P(('dp', 'tp'), None), P('dp'), P('dp'), P('dp'), P('dp', 'tp'), P('dp', 'tp'), P('dp', 'tp'), P(('dp', 'tp'), None))
    return jax.shard_map(local_step, mesh=mesh, in_specs=in_specs, out_specs=out_specs, check_vma=False)
```

```python
import functools
import jax
import jax.numpy as jnp
import numpy as np
from jax import lax
from jax.experimental import pallas as pl
from jax.experimental.pallas import tpu as pltpu
from jax.sharding import PartitionSpec as P

BF = jnp.bfloat16
F32 = jnp.float32
EPS = 1.0e-6
ROPE_BASE = 1.0e6
NEG_BIG = -1.0e30
LOG2E = 1.4426950408889634
MESH = pl.DeviceIdType.MESH
ANY = pl.BlockSpec(memory_space=pl.ANY)
VM = pl.BlockSpec(memory_space=pltpu.VMEM)
NT = (((1,), (1,)), ((), ()))
NN = (((1,), (0,)), ((), ()))
TN = (((0,), (0,)), ((), ()))


def dotf(a, b, dims=NN):
    return lax.dot_general(a, b, dims, preferred_element_type=F32)


def rdma(src, dst, ssem, rsem, dev):
    return pltpu.make_async_remote_copy(src_ref=src, dst_ref=dst, send_sem=ssem, recv_sem=rsem, device_id={'tp': dev}, device_id_type=MESH)


def span(start, size):
    return pl.ds(pl.multiple_of(start, size), size)


def each(lo, hi, f):
    def go(j, _):
        f(j)
        return 0
    lax.fori_loop(lo, hi, go, 0)


def total(ref, sem):
    pltpu.make_async_copy(ref, ref, sem).wait()


def rms_f32(x, gain):
    return x * lax.rsqrt(jnp.mean(x * x, axis=-1, keepdims=True) + EPS) * gain


def rms_pull(x, dxr, r):
    return r * dxr - x * (r * r * r * jnp.mean(x * dxr, axis=-1, keepdims=True))


def causal_blocks(q, keys, i, blk):
    r_i = lax.broadcasted_iota(jnp.int32, (blk, blk), 0)
    c_i = lax.broadcasted_iota(jnp.int32, (blk, blk), 1)
    s = [dotf(q, keys[j * blk:(j + 1) * blk], NT) for j in range(i + 1)]
    s[i] = jnp.where(r_i >= c_i, s[i], NEG_BIG)
    top = functools.reduce(jnp.maximum, [jnp.max(t, axis=-1, keepdims=True) for t in s])
    c = q.shape[-1] ** -0.5 * LOG2E
    e = [jnp.exp2((t - top) * c) for t in s]
    inv = 1.0 / sum(jnp.sum(t, axis=-1, keepdims=True) for t in e)
    return [t * inv for t in e]


def body(nz, embed, gy, wq, wk_t, wv_t, wo, gain, qg, kg, cos, sin_s, tok_seq,
         y_hbm, ge_hbm, gq_hbm, gk_hbm, gv_hbm, gwo_hbm, gn_out, gqg_out, gkg_out, hid, gy_out, wqt_out, wqts_out, py_out, ph_out,
         table, wpair, wq_v, qt, o_own, o_sib, sq, kv_tok, k_rot, kvacc, farkv, kvrow, skv, kvc, d_rows, pbuf, hbuf, gown, hotm,
         dk_acc, dv_acc, pk, rk1, fk, hk, rk2, kvt, gn, qga, kga, gall, qall, y_v, ge_v, gkv_v,
         in_sem, h_sem, g_sem, r_sem, s_sem, a_s, b_s, xs, xr, wq_s, wq_r, w_s, o_s, pt_sem, pl_sem, rs, p1s, p1r, p2s, p2r, qs, gls, hls, swos, swqs, gs, out_sem):
    rank = lax.axis_index('tp')
    z, core = rank // 2, lax.rem(rank, 2)
    right = 2 * lax.rem(z + 1, nz) + core
    left = 2 * lax.rem(z + nz - 1, nz) + core
    sib = rank + 1 - 2 * core
    par = lax.rem(z, 2)
    far = rank + 2 - 4 * par
    vrows, d = embed.shape
    kn = wk_t.shape[0]
    sub_rows = vrows // 4
    vocab = vrows * 2 * nz
    vhalf = vocab // 2
    batch, seq = tok_seq.shape
    toks = batch * seq
    qn = wq.shape[1]
    hd = qg.shape[1]
    heads = qn // hd
    events = 2 * nz
    pos = seq // events
    blk = seq // 2
    bw = d // events
    scale = hd ** -0.5
    units = batch * heads
    parts = 8
    wo_p, wq_p = qn // parts, d // parts
    both = (0, 1)
    places = [(dr, c) for dr in both for c in both]
    qr = wq_v.at[pl.ds(0, toks)]
    gd = wq_v.at[pl.ds(toks, toks)]
    w_q = wq_v.at[pl.ds(0, d)]

    ld = [pltpu.make_async_copy(s, t, in_sem.at[i]) for i, (s, t) in enumerate((
        (embed, table.at[span(rank * vrows, vrows)]), (gy, gown), (wq, w_q), (wo, wpair.at[pl.ds(0, qn)]),
        (wk_t, wpair.at[pl.ds(2 * qn, kn)]), (wv_t, wpair.at[pl.ds(2 * qn + kn, kn)])))]
    ld2 = [pltpu.make_async_copy(s, t, in_sem.at[i]) for i, (s, t) in enumerate((
        (wqt_out, wpair.at[pl.ds(0, qn)]), (wqts_out, wpair.at[pl.ds(qn, qn)]), (embed, gown)))]
    for c in ld:
        c.start()
    barrier = pltpu.get_barrier_semaphore()
    for dev in (right, left, sib):
        pl.semaphore_signal(barrier, inc=1, device_id={'tp': dev}, device_id_type=MESH)
    with jax.named_scope('head'):
        pl.semaphore_wait(barrier, 3)
        ld[0].wait()

    def nbr(dr):
        return right if dr == 0 else left

    def zd_of(dr, e):
        s = e // 2
        return lax.rem(z + (nz - s if dr == 0 else s), nz)

    def row_of(dr, e, c):
        return pl.multiple_of(vrows * (2 * zd_of(dr, e) + c) + sub_rows * (2 * dr + lax.rem(e, 2)), sub_rows)

    def ring(dr, e, recv_e):
        a = table.at[pl.ds(row_of(dr, e, core), sub_rows)]
        return rdma(a, a, a_s.at[0], r_sem.at[dr, recv_e], nbr(dr))

    def side(dr, e):
        a = table.at[pl.ds(row_of(dr, e, core), sub_rows)]
        return rdma(a, a, a_s.at[1], s_sem.at[dr, e], sib)

    def h_copy(slot, i, row):
        return pltpu.make_async_copy(hbuf.at[slot, pl.ds(i * sub_rows, sub_rows)], hid.at[pl.ds(row, sub_rows)], h_sem.at[slot])

    def g_row(dr, e, c):
        return pl.multiple_of(seq * (2 * dr + lax.rem(e, 2)) + pos * (2 * zd_of(dr, e) + c), pos)

    def g_piece(dr, e, c):
        return gy_out.at[pl.ds(g_row(dr, e, c), pos)]

    def g_own(dr, e):
        return gown.at[span(pos * (2 * dr + lax.rem(e, 2)), pos)]

    def g_ring(dr, e, recv_e, first):
        a = g_piece(dr, e, core)
        return rdma(g_own(dr, e) if first else a, a, b_s.at[0 if first else 1], r_sem.at[dr, recv_e], nbr(dr))

    def g_side(dr, e, first):
        a = g_piece(dr, e, core)
        return rdma(g_own(dr, e) if first else a, a, b_s.at[2 if first else 3], s_sem.at[dr, e], sib)

    def g_home(dr, e):
        return pltpu.make_async_copy(g_own(dr, e), g_piece(dr, e, core), in_sem.at[8 + 2 * dr + e])

    def g_fetch(slot, i, dr, c, e):
        return pltpu.make_async_copy(g_piece(dr, e, c), hbuf.at[slot, pl.ds(i * pos, pos)], g_sem.at[0])

    def wo_push(k):
        return rdma(wpair.at[span(k * wo_p, wo_p)], wpair.at[pl.ds(pl.multiple_of(qn + k * wo_p, wo_p), wo_p)], w_s.at[0], w_s.at[1], sib)

    def tb(k):
        return o_own.at[span(lax.rem(k, 2) * qn, qn), pl.ds(0, wq_p)]

    def wq_push(k):
        return rdma(tb(k), wqts_out.at[:, span(k * wq_p, wq_p)], wq_s.at[0, lax.rem(k, 2)], wq_r.at[0], sib)

    def wq_home(k):
        return pltpu.make_async_copy(tb(k), wqt_out.at[:, span(k * wq_p, wq_p)], wq_s.at[1, lax.rem(k, 2)])

    def wk_push(k):
        return rdma((wk_t, wv_t)[k], wpair.at[pl.ds(2 * qn + (2 + k) * kn, kn)], w_s.at[2], w_s.at[3], sib)

    def o_push(b, k):
        src = pl.multiple_of(b * seq + pos * (2 * k + 1 - core), pos)
        dst = pl.multiple_of(vrows * k + pos * b, pos)
        return rdma(o_own.at[pl.ds(src, pos)], o_sib.at[pl.ds(dst, pos)], o_s.at[0], o_s.at[1], sib)

    def project(e):
        slot = lax.rem(e, 2)

        @pl.when(e >= 2)
        def _():
            total(hbuf.at[slot], h_sem.at[slot])

        rows = [row_of(dr, e, c) for dr, c in places]
        for i, row in enumerate(rows):
            x = table[pl.ds(row, sub_rows), :].astype(F32)
            ids = row + lax.broadcasted_iota(jnp.int32, (sub_rows, seq), 0)
            hit = jnp.zeros((sub_rows, seq), F32)
            for b in range(batch):
                hit = jnp.maximum(hit, jnp.where(tok_seq[b:b + 1, :] == ids, 1.0, 0.0))
            used = jnp.max(hit, axis=1, keepdims=True)
            h = jnp.where(used > 0.5, rms_f32(x, gain[...]), 0.0)
            hbuf[slot, pl.ds(i * sub_rows, sub_rows), :] = h.astype(BF)
            h_copy(slot, i, row).start()
        hb = hbuf[slot]
        qkv = jnp.concatenate([dotf(hb, w_q[...]).astype(BF), dotf(hb, wpair[2 * qn:2 * qn + 4 * kn, :], NT).astype(BF)], axis=1)
        lane = lax.broadcasted_iota(jnp.int32, (1, vrows), 1)
        rowid = jnp.zeros((1, vrows), jnp.int32)
        for i, row in enumerate(rows):
            rowid = jnp.where(lane // sub_rows == i, row + lane - i * sub_rows, rowid)
        rowid = rowid.astype(F32)
        for b in range(batch):
            sl = slice(b * seq, (b + 1) * seq)
            hot = jnp.where(d_rows[sl, :vrows] == rowid, 1.0, 0.0).astype(BF)
            got = dotf(hot, qkv)
            qt[sl, :] = (qt[sl, :].astype(F32) + got[:, :qn]).astype(BF)
            at = slice((b % 2) * seq, (b % 2 + 1) * seq)
            kvacc[b // 2, at, :] = (kvacc[b // 2, at, :].astype(F32) + got[:, qn:]).astype(BF)

    def step_a(e):
        with jax.named_scope('a_wait'):
            @pl.when((e >= 2) & (e < events))
            def _():
                for dr in both:
                    ring(dr, e, e).wait_recv()

        @pl.when(e < events - 2)
        def _():
            for dr in both:
                ring(dr, e, e + 2).start()

        @pl.when(e < events)
        def _():
            for dr in both:
                side(dr, e).start()

        @pl.when(e == 0)
        def _():
            for k in both:
                wk_push(k).start()
            for b in range(batch):
                wide = jnp.broadcast_to(tok_seq[b:b + 1, :].astype(F32), (vrows, seq))
                d_rows[b * seq:(b + 1) * seq, :vrows] = wide.T
            qt[...] = jnp.zeros_like(qt)
            kvacc[...] = jnp.zeros_like(kvacc)

        @pl.when(e == 1)
        def _():
            for c in ld[1:]:
                c.wait()
            total(wpair.at[pl.ds(2 * qn, 2 * kn)], w_s.at[3])
            for dr in both:
                for k in both:
                    g_home(dr, k).start()

        @pl.when(e == events - 2)
        def _():
            for dr in both:
                g_ring(dr, 0, 2, True).start()

        @pl.when((e >= 2) & (e < 4 + parts))
        def _():
            @pl.when(e >= 4)
            def _():
                wq_push(e - 4).wait_send()
                wq_home(e - 4).wait()

            @pl.when(e < 2 + parts)
            def _():
                k = e - 2
                block = wq_v[span(k * wq_p, wq_p), :]
                tb(k)[...] = block.astype(F32).T.astype(BF)
                wo_push(k).start()
                wq_push(k).start()
                wq_home(k).start()

        with jax.named_scope('a_proj'):
            @pl.when(e >= 1)
            def _():
                for dr in both:
                    side(dr, e - 1).wait_recv()
                project(e - 1)

    each(0, events + 1, step_a)

    to_far = rdma(kvacc.at[core], farkv.at[core], xs.at[0], xr.at[0], far)
    relay = rdma(farkv.at[core], farkv.at[core], xs.at[1], xr.at[1], sib)
    at_i = lax.broadcasted_iota(jnp.int32, (pos, seq), 1) - pos * rank
    own_i = lax.broadcasted_iota(jnp.int32, (pos, seq), 0)
    col = jnp.concatenate([jnp.sum(jnp.where(at_i == own_i, tok_seq[b:b + 1, :].astype(F32), 0.0), axis=1, keepdims=True) for b in range(batch)], axis=0).astype(jnp.int32)
    lanes = lax.broadcasted_iota(jnp.int32, (vrows, vrows), 1)
    hot_mine = jnp.concatenate([jnp.where(col == lanes + j * vrows, 1.0, 0.0).astype(BF) for j in range(vocab // vrows)], axis=1)
    to_far.start()
    for dr in both:
        g_ring(dr, 1, 3, True).start()
        for k in both:
            g_side(dr, k, True).start()
            g_home(dr, k).wait()
    cw = min(512, d)

    def own_rows(j):
        y_v[:, span(j * cw, cw)] = dotf(hot_mine, table[:, span(j * cw, cw)]).astype(BF)

    each(0, d // cw, own_rows)
    for b in range(batch):
        ids = rank * vrows + lax.broadcasted_iota(jnp.int32, (vrows, seq), 0)
        hotm[:, b * seq:(b + 1) * seq] = jnp.where(ids == tok_seq[b:b + 1, :], 1.0, 0.0).astype(BF)

    def place(p, first):
        l_i = lax.broadcasted_iota(jnp.int32, (4 * kn, 2 * hd), 0)
        m_i = lax.broadcasted_iota(jnp.int32, (4 * kn, 2 * hd), 1)
        upper = jnp.where(l_i >= 2 * kn, 1, 0)
        owner = jnp.where(upper == 1, 1 - first, first)
        l_i = l_i - 2 * kn * upper
        base = kn * (2 * p + owner)
        want = jnp.where(l_i < kn, base + l_i, hd + base + l_i - kn)
        return jnp.where(m_i == want, 1.0, 0.0).astype(BF)

    def rope(raw, g):
        n = rms_f32(raw.astype(F32), g)
        return (n * cos[...] + pltpu.roll(n, hd // 2, 1) * sin_s[...]).astype(BF)

    def attend(u):
        base = (u // heads) * seq
        rows = span(base, seq)
        cols = span(lax.rem(u, heads) * hd, hd)
        q = rope(qt[rows, cols], qg[...])
        qr[rows, cols] = q
        kr = k_rot[rows, :]
        v = kv_tok[rows, hd:]
        for i in both:
            p = causal_blocks(q[i * blk:(i + 1) * blk], kr, i, blk)
            o = sum(dotf(t.astype(BF), v[j * blk:(j + 1) * blk]) for j, t in enumerate(p))
            o_own[pl.ds(pl.multiple_of(base + i * blk, blk), blk), cols] = o.astype(BF)

    def grad_attend(e):
        total(hbuf, g_sem.at[0])
        r = dotf(hbuf[...].reshape(2 * vrows, d), wpair[:qn, :], NT).astype(BF)
        for k in both:
            for i, (dr, c) in enumerate(places):
                n = (4 * k + i) * pos
                gd[pl.ds(g_row(dr, e + k, c), pos), :] = r[n:n + pos]

    def pstage(j):
        return d_rows.at[span(lax.rem(j, 2) * vhalf, vhalf), pl.ds(0, bw)]

    def pstore(dst, j):
        return pltpu.make_async_copy(pstage(j), dst.at[:, span(j * bw, bw)], pt_sem.at[lax.rem(j, 2)])

    def pblock(dst, j, pairs):
        @pl.when(j >= 2)
        def _():
            pstore(dst, j - 2).wait()
        cols = span(j * bw, bw)
        acc = None
        for a, lo, n in pairs:
            t = dotf(a[...], wpair[lo:lo + n, cols])
            acc = t if acc is None else acc + t
        pstage(j)[...] = acc
        pstore(dst, j).start()

    y_pairs = [(sq, 0, qn), (o_sib, qn, qn)]
    h_pairs = [(o_sib, 0, qn), (sq, qn, qn), (kvc, 2 * qn, 4 * kn)]

    def pslot(ph, e, dr):
        return pbuf.at[2 * ph + lax.rem(e, 2), dr]

    def pfetch(ph, e, dr):
        s = e // 2
        zd = lax.rem(z + (2 * nz - 1 - s if dr == 0 else 1 + s), nz)
        row = pl.multiple_of(vrows * zd + sub_rows * (2 * dr + lax.rem(e, 2)), sub_rows)
        return pltpu.make_async_copy((py_out, ph_out)[ph].at[pl.ds(row, sub_rows)], pslot(ph, e, dr), pl_sem.at[ph, lax.rem(e, 2)])

    def rslot(dr, e):
        return table.at[span((dr * (events - 2) + e) * sub_rows, sub_rows)]

    def sslot(ph, dr, e):
        k = 2 * (events - 2) + 8 * ph + 4 * lax.rem(e // 2, 2) + 2 * dr + lax.rem(e, 2)
        return table.at[span(k * sub_rows, sub_rows)]

    def send(ph, dr, e):
        return rdma(sslot(ph, dr, e), rslot(dr, e), rs.at[ph, dr, lax.rem(e, 4)], r_sem.at[dr, e + 2], nbr(dr))

    def first_fetch(ph, dst):
        for j in (events - 2, events - 1):
            pstore(dst, j).wait()
        for e in both:
            for dr in both:
                pfetch(ph, e, dr).start()

    def first_sends(ph):
        for e in both:
            total(pbuf.at[2 * ph + e], pl_sem.at[ph, e])
            for dr in both:
                sslot(ph, dr, e)[...] = pslot(ph, e, dr)[...].astype(BF)
        for e in both:
            for dr in both:
                send(ph, dr, e).start()
                pfetch(ph, e + 2, dr).start()

    def serve(ph, e, final):
        for dr in both:
            send(ph, dr, e - 2).wait_recv()
        total(pbuf.at[2 * ph + lax.rem(e, 2)], pl_sem.at[ph, lax.rem(e, 2)])

        @pl.when(e < events - 2)
        def _():
            @pl.when(e >= 4)
            def _():
                for dr in both:
                    send(ph, dr, e - 4).wait_send()
            for dr in both:
                sslot(ph, dr, e)[...] = (pslot(ph, e, dr)[...] + rslot(dr, e - 2)[...].astype(F32)).astype(BF)
            for dr in both:
                send(ph, dr, e).start()
                pfetch(ph, e + 2, dr).start()

        @pl.when(e >= events - 2)
        def _():
            for dr in both:
                final(dr, lax.rem(e, 2), pslot(ph, e, dr)[...] + rslot(dr, e - 2)[...].astype(F32))

    slots = 9

    def gather_o(k):
        for b in range(batch):
            src = pl.multiple_of(b * seq + pos * (2 * k + core), pos)
            sq[pl.ds(pl.multiple_of(vrows * k + pos * b, pos), pos), :] = o_own[pl.ds(src, pos), :]

    def upto(e, n, over):
        return jnp.minimum((e * n) // over, n)

    def step_b(e):
        with jax.named_scope('b_first'):
            @pl.when(e == events - 2)
            def _():
                first_sends(0)

        with jax.named_scope('b_wait'):
            @pl.when((e >= 2) & (e < events))
            def _():
                for dr in both:
                    g_ring(dr, e, e, False).wait_recv()

        @pl.when((e >= 2) & (e < events - 2))
        def _():
            for dr in both:
                g_ring(dr, e, e + 2, False).start()

        @pl.when((e >= 2) & (e < events))
        def _():
            for dr in both:
                g_side(dr, e, False).start()

        @pl.when((e >= 1) & (e <= events))
        def _():
            for dr in both:
                g_side(dr, e - 1, False).wait_recv()

        with jax.named_scope('kv_far'):
            @pl.when(e == 2)
            def _():
                to_far.wait_recv()
                relay.start()

        with jax.named_scope('kv_tok'):
            @pl.when(e == 3)
            def _():
                rdma(farkv.at[1 - core], farkv.at[1 - core], xs.at[1], xr.at[1], sib).wait_recv()
                for hf in both:
                    kv_tok[hf * (toks // 2):(hf + 1) * (toks // 2), :] = (dotf(kvacc[hf], place(par, core)) + dotf(farkv[hf], place(1 - par, hf))).astype(BF)
                for b in range(batch):
                    sl = slice(b * seq, (b + 1) * seq)
                    k_rot[sl, :] = rope(kv_tok[sl, :hd], kg[...])

            @pl.when((e >= 2) & (lax.rem(e, 2) == 0))
            def _():
                for k in both:
                    for i, (dr, c) in enumerate(places):
                        g_fetch(k, i, dr, c, e - 2 + k).start()

        def give(b):
            each(0, nz, lambda k: o_push(b, k).start())

        def seen(t):
            return jnp.minimum((jnp.maximum(t - 3, 0) * units) // (slots - 3), units)

        each(seen(e - 1) // heads, seen(e) // heads, give)
        with jax.named_scope('b_attend'):
            each(seen(e), seen(e + 1), attend)

        @pl.when(e == 4)
        def _():
            total(table.at[pl.ds(0, 2 * (events - 2) * sub_rows)], a_s.at[0])
            total(table.at[pl.ds(0, 2 * events * sub_rows)], a_s.at[1])

        @pl.when(e == slots + 1)
        def _():
            total(wpair.at[pl.ds(0, qn)], w_s.at[1])
            total(o_sib, o_s.at[1])
            each(0, nz, gather_o)

        with jax.named_scope('b_part'):
            @pl.when((e > slots) & (e <= slots + 4))
            def _():
                each(4 * (e - slots - 1), 4 * (e - slots), lambda j: pblock(py_out, j, y_pairs))

        @pl.when(e == slots + 4)
        def _():
            first_fetch(0, py_out)

        with jax.named_scope('b_grad'):
            @pl.when((e >= 3) & (lax.rem(e, 2) == 1))
            def _():
                grad_attend(e - 3)

    for slot in both:
        total(hbuf.at[slot], h_sem.at[slot])
    each(0, events + 2, step_b)

    def pull(raw, dout, g):
        x = raw.astype(F32)
        r = lax.rsqrt(jnp.mean(x * x, axis=-1, keepdims=True) + EPS)
        dn = dout * cos[...] + pltpu.roll(dout * sin_s[...], hd // 2, 1)
        return rms_pull(x, dn * g, r).astype(BF), jnp.sum(dn * (x * r), axis=0, keepdims=True)

    def unit(u):
        b, h = u // heads, lax.rem(u, heads)
        rows = span(b * seq, seq)
        cols = span(h * hd, hd)

        @pl.when(h == 0)
        def _():
            dk_acc[...] = jnp.zeros_like(dk_acc)
            dv_acc[...] = jnp.zeros_like(dv_acc)
        q, g = qr[rows, cols], gd[rows, cols]
        kr, v = k_rot[rows, :], kv_tok[rows, hd:]
        dqs = []
        for i in both:
            qi, gi = q[i * blk:(i + 1) * blk], g[i * blk:(i + 1) * blk]
            p = causal_blocks(qi, kr, i, blk)
            dp = [dotf(gi, v[j * blk:(j + 1) * blk], NT) for j in range(i + 1)]
            tot = sum(jnp.sum(a * b, axis=-1, keepdims=True) for a, b in zip(p, dp))
            dq = None
            for j in range(i + 1):
                at = slice(j * blk, (j + 1) * blk)
                dv_acc[at, :] += dotf(p[j].astype(BF), gi, TN)
                ds = (p[j] * (dp[j] - tot)).astype(BF)
                t = dotf(ds, kr[at])
                dq = t if dq is None else dq + t
                dk_acc[at, :] += dotf(ds, qi, TN)
            dqs.append(dq * scale)
        dq = jnp.concatenate(dqs, axis=0).astype(BF).astype(F32)
        dx, dg = pull(qt[rows, cols], dq, qg[...])
        gd[rows, cols] = dx
        qga[...] += dg

    def pick(r, up):
        m_i = lax.broadcasted_iota(jnp.int32, (2 * hd, 4 * kn), 0)
        l_i = lax.broadcasted_iota(jnp.int32, (2 * hd, 4 * kn), 1) - 2 * kn * up
        is_k = (l_i >= 0) & (l_i < kn) & (m_i == l_i + kn * r)
        is_v = (l_i >= kn) & (l_i < 2 * kn) & (m_i == hd + kn * r + l_i - kn)
        return jnp.where(is_k | is_v, 1.0, 0.0).astype(BF)

    def to_side(b, p):
        return rdma(pk.at[b, 2 * p + 1 - core], rk1.at[b, p], p1s.at[0], p1r.at[b], sib)

    def to_far2(b):
        return rdma(fk.at[b], rk2.at[b], p2s.at[0], p2r.at[b], far)

    def kv_one(b):
        dk = (dk_acc[...] * scale).astype(BF).astype(F32)
        dx, dg = pull(kv_tok[span(b * seq, seq), :hd], dk, kg[...])
        kga[...] += dg
        gkv = jnp.concatenate([dx, dv_acc[...].astype(BF)], axis=1)
        for r in range(4):
            pk[b, r] = (dotf(gkv[:blk], pick(r, 0)) + dotf(gkv[blk:], pick(r, 1))).astype(BF)
        for p in both:
            to_side(b, p).start()

    def kv_two(b):
        total(rk1.at[b], p1r.at[b])
        fk[b] = (pk[b, 2 * (1 - par) + core].astype(F32) + rk1[b, 1 - par].astype(F32)).astype(BF)
        hk[b] = pk[b, 2 * par + core].astype(F32) + rk1[b, par].astype(F32)
        to_far2(b).start()

    def kv_three(b):
        to_far2(b).wait_recv()
        t = hk[b] + rk2[b].astype(F32)
        low = lax.broadcasted_iota(jnp.int32, t.shape, 1) < 2 * kn
        kvt[b, :blk, :] = jnp.where(low, t, 0.0).astype(BF)
        kvt[b, blk:, :] = jnp.where(low, pltpu.roll(t, 2 * kn, 1), 0.0).astype(BF)

    def fold(b, tile):
        rows = span(tile * seq, seq)
        ids = tile * seq + lax.broadcasted_iota(jnp.int32, (seq, seq), 0)
        hot = jnp.where(ids == tok_seq[pl.ds(b, 1), :], 1.0, 0.0).astype(BF)
        d_rows[rows, :qn] += dotf(hot, gd[span(b * seq, seq), :])
        d_rows[rows, qn:] += dotf(hot, kvt[b])

    tiles = vocab // seq

    def run_unit(u):
        unit(u)

        @pl.when(lax.rem(u, heads) == heads - 1)
        def _():
            kv_one(u // heads)

        @pl.when((u >= heads) & (lax.rem(u, heads) == 1))
        def _():
            kv_two(u // heads - 1)

    def run_fold(f):
        b, tile = f // tiles, lax.rem(f, tiles)

        @pl.when(tile == 0)
        def _():
            kv_three(b)
        fold(b, tile)

    def share(e, first, n, over):
        return jnp.minimum((jnp.maximum(e - first, 0) * n) // over, n)

    def paced(e, first, n, over, f):
        each(share(e, first, n, over), share(e + 1, first, n, over), f)

    def settle(t):
        rows = span(t * vrows, vrows)
        qt[rows, :] = d_rows[rows, :qn].astype(BF)
        kvrow[rows, :] = d_rows[rows, qn:].astype(BF)

    def swap(k, kk):
        src = pl.multiple_of(vrows * (2 * k + 1 - core), vrows)
        return rdma((qt, kvrow)[kk].at[pl.ds(src, vrows)], (sq, skv)[kk].at[span(vrows * k, vrows)], qs.at[0, kk], qs.at[1, kk], sib)

    def gather_h(k):
        src = pl.multiple_of(vrows * (2 * k + core), vrows)
        dst = span(vrows * k, vrows)
        o_sib[dst, :] = qt[pl.ds(src, vrows), :]
        kvc[dst, :] = (kvrow[pl.ds(src, vrows), :].astype(F32) + pltpu.roll(skv[dst, :].astype(F32), 2 * kn, 1)).astype(BF)

    def final_y(dr, sub, acc):
        rows = span((2 * dr + sub) * pos, pos)
        y_v[rows, :] = (y_v[rows, :].astype(F32) + acc).astype(BF)

    def step_c(e):
        with jax.named_scope('c_first'):
            @pl.when(e == events - 2)
            def _():
                first_sends(1)

        with jax.named_scope('c_serve'):
            @pl.when(e >= 2)
            def _():
                serve(0, e, final_y)

        @pl.when(e == 0)
        def _():
            total(gown, b_s.at[0])
            total(gown, b_s.at[2])
            total(wqts_out, wq_r.at[0])
            total(wpair.at[pl.ds(0, qn)], w_s.at[0])
            for c in ld2:
                c.start()
            d_rows[...] = jnp.zeros_like(d_rows)
            gn[...] = jnp.zeros_like(gn)
            qga[...] = jnp.zeros_like(qga)
            kga[...] = jnp.zeros_like(kga)

        with jax.named_scope('c_unit'):
            paced(e, 2, units, 6, run_unit)

        with jax.named_scope('c_kv2'):
            @pl.when(e == 8)
            def _():
                kv_two(batch - 1)
        with jax.named_scope('c_fold'):
            paced(e, 8, batch * tiles, 3, run_fold)

        with jax.named_scope('c_settle'):
            @pl.when(e == 10)
            def _():
                each(0, 2 * nz, settle)
                each(0, nz, lambda k: [swap(k, kk).start() for kk in both])

        with jax.named_scope('c_swap'):
            @pl.when(e == 11)
            def _():
                for c in ld2:
                    c.wait()
                total(sq, qs.at[1, 0])
                total(skv, qs.at[1, 1])
                each(0, nz, gather_h)
        with jax.named_scope('c_part'):
            paced(e, 11, events, 3, lambda j: pblock(ph_out, j, h_pairs))

        @pl.when(e == 13)
        def _():
            first_fetch(1, ph_out)

    each(0, events, step_c)

    def gblk(j):
        return qr.at[:, span(lax.rem(j, 2) * bw, bw)]

    def hblk(j):
        return gd.at[:, span(lax.rem(j, 2) * bw, bw)]

    def swo(j):
        return d_rows.at[pl.ds(0, qn), span(lax.rem(j, 2) * bw, bw)]

    def swq(j):
        return d_rows.at[pl.ds(pl.multiple_of(qn + lax.rem(j, 2) * bw, bw), bw), pl.ds(0, qn)]

    def g_load(j):
        return pltpu.make_async_copy(gy_out.at[:, span(j * bw, bw)], gblk(j), gls.at[lax.rem(j, 2)])

    def h_load(j):
        return pltpu.make_async_copy(hid.at[:, span(j * bw, bw)], hblk(j), hls.at[lax.rem(j, 2)])

    def wo_store(j):
        return pltpu.make_async_copy(swo(j), gwo_hbm.at[:, span(j * bw, bw)], swos.at[lax.rem(j, 2)])

    def wq_store(j):
        return pltpu.make_async_copy(swq(j), gq_hbm.at[span(j * bw, bw)], swqs.at[lax.rem(j, 2)])

    def block(j):
        g_load(j).wait()
        h_load(j).wait()

        @pl.when(j + 1 < events)
        def _():
            g_load(j + 1).start()
            h_load(j + 1).start()

        @pl.when(j >= 2)
        def _():
            wo_store(j - 2).wait()
            wq_store(j - 2).wait()
        cols = span(j * bw, bw)
        swo(j)[...] = dotf(o_own[...], gblk(j)[...], TN)
        ge_v[:, cols] = dotf(hotm[...], gblk(j)[...])
        wo_store(j).start()
        swq(j)[...] = dotf(hblk(j)[...], qt[...], TN)
        gkv_v[:, cols] = dotf(kvrow[...], hblk(j)[...], TN)[:2 * kn]
        wq_store(j).start()

    def final_h(dr, sub, gh):
        rows = span((2 * dr + sub) * sub_rows, sub_rows)
        x = gown[rows, :].astype(F32)
        r = lax.rsqrt(jnp.mean(x * x, axis=-1, keepdims=True) + EPS)
        ge_v[rows, :] += rms_pull(x, gh * gain[...], r)
        gn[...] += jnp.sum(gh * (x * r), axis=0, keepdims=True)

    outs = [pltpu.make_async_copy(s, t, out_sem.at[i]) for i, (s, t) in enumerate((
        (y_v, y_hbm), (gkv_v.at[pl.ds(0, kn)], gk_hbm), (gkv_v.at[pl.ds(kn, kn)], gv_hbm), (ge_v, ge_hbm)))]
    g_load(0).start()
    h_load(0).start()
    outs[0].start()
    work_d = events - 3

    wide = gn_out.shape[1]
    gtop = d // wide
    order = sorted(range(1, 2 * nz), key=lambda k: -min((k + 1) // 2, nz - k // 2))

    def spread(t, k, src):
        buf = (gall, qall)[t]
        return rdma(buf.at[src], buf.at[src], gs.at[0, t], gs.at[1, t], lax.rem(rank + k, 2 * nz))

    def step_d(e):
        with jax.named_scope('d_serve'):
            @pl.when(e >= 2)
            def _():
                serve(1, e, final_h)

        @pl.when(e == 1)
        def _():
            qall[rank, 0:1, :] = qga[...]
            qall[rank, 1:2, :] = kga[...]

        @pl.when(e == 2)
        def _():
            for k in order:
                spread(1, k, rank).start()

        with jax.named_scope('d_block'):
            paced(e, 0, events, work_d, block)

    each(0, events, step_d)

    for j in range(gtop):
        gall[rank, j:j + 1, :] = gn[:, j * wide:(j + 1) * wide].astype(gall.dtype)
    outs[3].start()
    outs[1].start()
    outs[2].start()
    with jax.named_scope('t_store'):
        for j in (events - 2, events - 1):
            wo_store(j).wait()
            wq_store(j).wait()
    for k in order:
        spread(0, k, rank).start()

    for ph in both:
        for dr in both:
            for e in range(events - 6, events - 2):
                send(ph, dr, e).wait_send()

    total(gy_out.at[pl.ds(0, 2 * (events - 4) * pos)], b_s.at[1])
    total(gy_out.at[pl.ds(0, 2 * (events - 2) * pos)], b_s.at[3])
    to_far.wait_send()
    relay.wait_send()
    total(wpair.at[pl.ds(2 * qn, 2 * kn)], w_s.at[2])
    total(o_sib, o_s.at[0])
    total(pk.at[pl.ds(0, batch // 2)], p1s.at[0])
    total(fk, p2s.at[0])
    total(sq, qs.at[0, 0])
    total(skv, qs.at[0, 1])
    with jax.named_scope('gain_wait'):
        peers = pl.ds(0, 2 * nz - 1)
        total(qall.at[peers], gs.at[1, 1])
        total(gall.at[peers], gs.at[1, 0])
    with jax.named_scope('gain_sum'):
        acc = gall[0].astype(F32)
        for r in range(1, 2 * nz):
            acc = acc + gall[r].astype(F32)
        gn_out[...] = acc
        qk = jnp.sum(qall[...], axis=0)
        gqg_out[...] = qk[0:1]
        gkg_out[...] = qk[1:2]
        total(gall.at[peers], gs.at[0, 0])
        total(qall.at[peers], gs.at[0, 1])
    with jax.named_scope('t_outs'):
        for c in outs:
            c.wait()


def step_kernel(nz, embed, gy, wq, wk_t, wv_t, wo, gain, qg, kg, cos, sin_s, tok_seq):
    vrows, d = embed.shape
    vocab = vrows * 2 * nz
    qn, kn = wq.shape[1], wk_t.shape[0]
    hd = qg.shape[1]
    batch, seq = tok_seq.shape
    toks = batch * seq
    ev = 2 * nz
    sr, hb, vh = vrows // 4, seq // 2, vocab // 2
    dma = pltpu.SemaphoreType.DMA
    v = pltpu.VMEM

    def arr(dt, *shape):
        return jax.ShapeDtypeStruct(shape, dt)

    outs = (arr(BF, vrows, d), arr(F32, vrows, d), arr(F32, d, qn), arr(F32, kn, d), arr(F32, kn, d), arr(F32, qn, d), arr(F32, d // hd, hd), arr(F32, 1, hd), arr(F32, 1, hd),
            arr(BF, vocab, d), arr(BF, toks, d), arr(BF, qn, d), arr(BF, qn, d), arr(F32, vh, d), arr(F32, vh, d))
    return pl.pallas_call(
        functools.partial(body, nz),
        name='step_kernel',
        out_shape=outs,
        in_specs=[ANY] * 6 + [VM] * 6,
        out_specs=(ANY,) * 6 + (VM,) * 3 + (ANY,) * 6,
        scratch_shapes=[v((vocab, d), BF), v((2 * qn + 4 * kn, d), BF), v((max(d, 2 * toks), qn), BF), v((vocab, qn), BF), v((toks, qn), BF), v((vh, qn), BF), v((vh, qn), BF),
                        v((toks, 2 * hd), BF), v((toks, hd), BF), v((2, toks // 2, 4 * kn), BF), v((2, toks // 2, 4 * kn), BF), v((vocab, 4 * kn), BF), v((vh, 4 * kn), BF), v((vh, 4 * kn), BF),
                        v((vocab, qn + 4 * kn), F32), v((4, 2, sr, d), F32), v((2, vrows, d), BF), v((vrows, d), BF), v((vrows, toks), BF),
                        v((seq, hd), F32), v((seq, hd), F32), v((batch, 4, hb, 4 * kn), BF), v((batch, 2, hb, 4 * kn), BF), v((batch, hb, 4 * kn), BF), v((batch, hb, 4 * kn), F32),
                        v((batch, hb, 4 * kn), BF), v((batch, seq, 4 * kn), BF), v((1, d), F32), v((1, hd), F32), v((1, hd), F32), v((ev, d // hd, hd), BF), v((ev, 8, hd), F32), v((vrows, d), BF), v((vrows, d), F32), v((2 * kn, d), F32),
                        dma((12,)), dma((2,)), dma((1,)), dma((2, ev)), dma((2, ev)), dma((2,)), dma((4,)), dma((2,)), dma((2,)), dma((2, 2)), dma((1,)), dma((4,)), dma((2,)),
                        dma((2,)), dma((2, 2)), dma((2, 2, 4)), dma((1,)), dma((batch,)), dma((1,)), dma((batch,)), dma((2, 2)),
                        dma((2,)), dma((2,)), dma((2,)), dma((2,)), dma((2, 2)), dma((4,))],
        compiler_params=pltpu.CompilerParams(collective_id=0, has_side_effects=True, vmem_limit_bytes=67043328),
        cost_estimate=pl.CostEstimate(flops=2 * vocab * d * 8 * qn, bytes_accessed=20 * vocab * d, transcendentals=0),
    )(embed, gy, wq, wk_t, wv_t, wo, gain, qg, kg, cos, sin_s, tok_seq)


def emit_body(cuts, *refs):
    n = len(cuts)
    src, dst = refs[:n], refs[n:2 * n]
    bufs, s_in, s_out = refs[2 * n:-2], refs[-2], refs[-1]
    ins, outs = [], []
    for i, c in enumerate(cuts):
        step = src[i].shape[0] // c
        for j in range(c):
            b = bufs[i].at[pl.ds(j * step, step)]
            ins.append(pltpu.make_async_copy(src[i].at[pl.ds(j * step, step)], b, s_in.at[len(ins)]))
            outs.append(pltpu.make_async_copy(b, dst[i].at[pl.ds(j * step, step)], s_out.at[len(outs)]))
    for c in ins:
        c.start()
    for a, b in zip(ins, outs):
        a.wait()
        b.start()
    for b in outs:
        b.wait()


def emit(*arrays):
    size = 1 << 21
    cuts = tuple(max(1, a.size * a.dtype.itemsize // size) for a in arrays)
    return pl.pallas_call(
        functools.partial(emit_body, cuts),
        name='emit',
        out_shape=tuple(jax.ShapeDtypeStruct(a.shape, a.dtype) for a in arrays),
        in_specs=[ANY] * len(arrays),
        out_specs=(ANY,) * len(arrays),
        scratch_shapes=[pltpu.VMEM(a.shape, a.dtype) for a in arrays] + [pltpu.SemaphoreType.DMA((sum(cuts),))] * 2,
        compiler_params=pltpu.CompilerParams(vmem_limit_bytes=60 * 1024 * 1024),
        cost_estimate=pl.CostEstimate(flops=0, bytes_accessed=2 * sum(a.size * a.dtype.itemsize for a in arrays), transcendentals=0),
    )(*arrays)


def rope_consts(seq, hd):
    inv = np.float32(ROPE_BASE) ** (np.float32(-2.0) * np.arange(hd // 2, dtype=np.float32) / np.float32(hd))
    ang = np.arange(seq, dtype=np.float32)[:, None] * inv.astype(np.float32)[None, :]
    ang = np.concatenate([ang, ang], axis=-1)
    sign = np.where(np.arange(hd) < hd // 2, -1.0, 1.0).astype(np.float32)
    return np.cos(ang).astype(np.float32), (np.sin(ang) * sign).astype(np.float32)


def solution(mesh):
    tp = mesh.shape['tp']
    nz = tp // 2

    def local_step(tok_ids, embed_loc, norm_gain, q_gain, k_gain, wq, wk, wv, wo, gy_loc):
        d_model = embed_loc.shape[1]
        batch, seq = tok_ids.shape
        seq_dev = seq // tp
        hd = q_gain.shape[0]
        cos_c, sin_c = (jnp.asarray(t) for t in rope_consts(seq, hd))
        r = step_kernel(nz, embed_loc, gy_loc.reshape(batch * seq_dev, d_model), wq, wk.T, wv.T, wo, norm_gain[None, :], q_gain[None, :], k_gain[None, :], cos_c, sin_c, tok_ids)
        y, g_embed, g_wq, g_wk, g_wv, g_wo, g_n, g_q, g_k = emit(*r[:9])
        return (y.reshape(batch, seq_dev, d_model), g_embed, g_n.reshape(d_model), g_q.reshape(hd), g_k.reshape(hd), g_wq, g_wk.T, g_wv.T, g_wo)

    in_specs = (P('dp', None), P('tp', None), P(), P(), P(), P(None, 'tp'), P(None, 'tp'), P(None, 'tp'), P('tp', None), P('dp', 'tp', None))
    out_specs = (P('dp', 'tp', None), P(('dp', 'tp'), None), P('dp'), P('dp'), P('dp'), P('dp', 'tp'), P('dp', 'tp'), P('dp', 'tp'), P(('dp', 'tp'), None))
    return jax.shard_map(local_step, mesh=mesh, in_specs=in_specs, out_specs=out_specs, check_vma=False)
```

```python
import functools
import jax
import jax.numpy as jnp
import numpy as np
from jax import lax
from jax.experimental import pallas as pl
from jax.experimental.pallas import tpu as pltpu
from jax.sharding import PartitionSpec as P

BF = jnp.bfloat16
F32 = jnp.float32
EPS = 1.0e-6
ROPE_BASE = 1.0e6
NEG_BIG = -1.0e30
LOG2E = 1.4426950408889634
MESH = pl.DeviceIdType.MESH
ANY = pl.BlockSpec(memory_space=pl.ANY)
VM = pl.BlockSpec(memory_space=pltpu.VMEM)
NT = (((1,), (1,)), ((), ()))
NN = (((1,), (0,)), ((), ()))
TN = (((0,), (0,)), ((), ()))


def dotf(a, b, dims=NN):
    return lax.dot_general(a, b, dims, preferred_element_type=F32)


def rdma(src, dst, ssem, rsem, dev):
    return pltpu.make_async_remote_copy(src_ref=src, dst_ref=dst, send_sem=ssem, recv_sem=rsem, device_id={'tp': dev}, device_id_type=MESH)


def span(start, size):
    return pl.ds(pl.multiple_of(start, size), size)


def each(lo, hi, f):
    def go(j, _):
        f(j)
        return 0
    lax.fori_loop(lo, hi, go, 0)


def total(ref, sem):
    pltpu.make_async_copy(ref, ref, sem).wait()


def rms_f32(x, gain):
    return x * lax.rsqrt(jnp.mean(x * x, axis=-1, keepdims=True) + EPS) * gain


def rms_pull(x, dxr, r):
    return r * dxr - x * (r * r * r * jnp.mean(x * dxr, axis=-1, keepdims=True))


def causal_blocks(q, keys, i, blk):
    r_i = lax.broadcasted_iota(jnp.int32, (blk, blk), 0)
    c_i = lax.broadcasted_iota(jnp.int32, (blk, blk), 1)
    s = [dotf(q, keys[j * blk:(j + 1) * blk], NT) for j in range(i + 1)]
    s[i] = jnp.where(r_i >= c_i, s[i], NEG_BIG)
    top = functools.reduce(jnp.maximum, [jnp.max(t, axis=-1, keepdims=True) for t in s])
    c = q.shape[-1] ** -0.5 * LOG2E
    e = [jnp.exp2((t - top) * c) for t in s]
    inv = 1.0 / sum(jnp.sum(t, axis=-1, keepdims=True) for t in e)
    return [t * inv for t in e]


def body(nz, embed, gy, wq, wk_t, wv_t, wo, gain, qg, kg, cos, sin_s, tok_seq,
         y_hbm, ge_hbm, gq_hbm, gk_hbm, gv_hbm, gwo_hbm, gn_out, gqg_out, gkg_out, hid, gy_out, wqt_out, wqts_out, py_out, ph_out,
         table, wpair, wq_v, qt, o_own, o_sib, sq, kv_tok, k_rot, kvacc, farkv, kvrow, skv, kvc, d_rows, pbuf, hbuf, gown, hotm,
         dk_acc, dv_acc, pk, rk1, fk, hk, rk2, kvt, gn, qga, kga, gall, qall, y_v, ge_v, gkv_v,
         in_sem, h_sem, g_sem, r_sem, s_sem, a_s, b_s, xs, xr, wq_s, wq_r, w_s, o_s, pt_sem, pl_sem, rs, p1s, p1r, p2s, p2r, qs, gls, hls, swos, swqs, gs, out_sem):
    rank = lax.axis_index('tp')
    z, core = rank // 2, lax.rem(rank, 2)
    right = 2 * lax.rem(z + 1, nz) + core
    left = 2 * lax.rem(z + nz - 1, nz) + core
    sib = rank + 1 - 2 * core
    par = lax.rem(z, 2)
    far = rank + 2 - 4 * par
    vrows, d = embed.shape
    kn = wk_t.shape[0]
    sub_rows = vrows // 4
    vocab = vrows * 2 * nz
    vhalf = vocab // 2
    batch, seq = tok_seq.shape
    toks = batch * seq
    qn = wq.shape[1]
    hd = qg.shape[1]
    heads = qn // hd
    events = 2 * nz
    pos = seq // events
    blk = seq // 2
    bw = d // events
    scale = hd ** -0.5
    units = batch * heads
    parts = 8
    wo_p, wq_p = qn // parts, d // parts
    both = (0, 1)
    places = [(dr, c) for dr in both for c in both]
    qr = wq_v.at[pl.ds(0, toks)]
    gd = wq_v.at[pl.ds(toks, toks)]
    w_q = wq_v.at[pl.ds(0, d)]

    ld = [pltpu.make_async_copy(s, t, in_sem.at[i]) for i, (s, t) in enumerate((
        (embed, table.at[span(rank * vrows, vrows)]), (gy, gown), (wq, w_q), (wo, wpair.at[pl.ds(0, qn)]),
        (wk_t, wpair.at[pl.ds(2 * qn, kn)]), (wv_t, wpair.at[pl.ds(2 * qn + kn, kn)])))]
    ld2 = [pltpu.make_async_copy(s, t, in_sem.at[i]) for i, (s, t) in enumerate((
        (wqt_out, wpair.at[pl.ds(0, qn)]), (wqts_out, wpair.at[pl.ds(qn, qn)]), (embed, gown)))]
    for c in ld:
        c.start()
    barrier = pltpu.get_barrier_semaphore()
    for dev in (right, left, sib):
        pl.semaphore_signal(barrier, inc=1, device_id={'tp': dev}, device_id_type=MESH)
    with jax.named_scope('head'):
        pl.semaphore_wait(barrier, 3)
        ld[0].wait()

    def nbr(dr):
        return right if dr == 0 else left

    def zd_of(dr, e):
        s = e // 2
        return lax.rem(z + (nz - s if dr == 0 else s), nz)

    def row_of(dr, e, c):
        return pl.multiple_of(vrows * (2 * zd_of(dr, e) + c) + sub_rows * (2 * dr + lax.rem(e, 2)), sub_rows)

    def ring(dr, e, recv_e):
        a = table.at[pl.ds(row_of(dr, e, core), sub_rows)]
        return rdma(a, a, a_s.at[0], r_sem.at[dr, recv_e], nbr(dr))

    def side(dr, e):
        a = table.at[pl.ds(row_of(dr, e, core), sub_rows)]
        return rdma(a, a, a_s.at[1], s_sem.at[dr, e], sib)

    def h_copy(slot, i, row):
        return pltpu.make_async_copy(hbuf.at[slot, pl.ds(i * sub_rows, sub_rows)], hid.at[pl.ds(row, sub_rows)], h_sem.at[slot])

    def g_row(dr, e, c):
        return pl.multiple_of(seq * (2 * dr + lax.rem(e, 2)) + pos * (2 * zd_of(dr, e) + c), pos)

    def g_piece(dr, e, c):
        return gy_out.at[pl.ds(g_row(dr, e, c), pos)]

    def g_own(dr, e):
        return gown.at[span(pos * (2 * dr + lax.rem(e, 2)), pos)]

    def g_ring(dr, e, recv_e, first):
        a = g_piece(dr, e, core)
        return rdma(g_own(dr, e) if first else a, a, b_s.at[0 if first else 1], r_sem.at[dr, recv_e], nbr(dr))

    def g_side(dr, e, first):
        a = g_piece(dr, e, core)
        return rdma(g_own(dr, e) if first else a, a, b_s.at[2 if first else 3], s_sem.at[dr, e], sib)

    def g_home(dr, e):
        return pltpu.make_async_copy(g_own(dr, e), g_piece(dr, e, core), in_sem.at[8 + 2 * dr + e])

    def g_fetch(slot, i, dr, c, e):
        return pltpu.make_async_copy(g_piece(dr, e, c), hbuf.at[slot, pl.ds(i * pos, pos)], g_sem.at[0])

    def wo_push(k):
        return rdma(wpair.at[span(k * wo_p, wo_p)], wpair.at[pl.ds(pl.multiple_of(qn + k * wo_p, wo_p), wo_p)], w_s.at[0], w_s.at[1], sib)

    def tb(k):
        return o_own.at[span(lax.rem(k, 2) * qn, qn), pl.ds(0, wq_p)]

    def wq_push(k):
        return rdma(tb(k), wqts_out.at[:, span(k * wq_p, wq_p)], wq_s.at[0, lax.rem(k, 2)], wq_r.at[0], sib)

    def wq_home(k):
        return pltpu.make_async_copy(tb(k), wqt_out.at[:, span(k * wq_p, wq_p)], wq_s.at[1, lax.rem(k, 2)])

    def wk_push(k):
        return rdma((wk_t, wv_t)[k], wpair.at[pl.ds(2 * qn + (2 + k) * kn, kn)], w_s.at[2], w_s.at[3], sib)

    def o_push(b, k):
        src = pl.multiple_of(b * seq + pos * (2 * k + 1 - core), pos)
        dst = pl.multiple_of(vrows * k + pos * b, pos)
        return rdma(o_own.at[pl.ds(src, pos)], o_sib.at[pl.ds(dst, pos)], o_s.at[0], o_s.at[1], sib)

    def project(e):
        slot = lax.rem(e, 2)

        @pl.when(e >= 2)
        def _():
            total(hbuf.at[slot], h_sem.at[slot])

        rows = [row_of(dr, e, c) for dr, c in places]
        for i, row in enumerate(rows):
            x = table[pl.ds(row, sub_rows), :].astype(F32)
            ids = row + lax.broadcasted_iota(jnp.int32, (sub_rows, seq), 0)
            hit = jnp.zeros((sub_rows, seq), F32)
            for b in range(batch):
                hit = jnp.maximum(hit, jnp.where(tok_seq[b:b + 1, :] == ids, 1.0, 0.0))
            used = jnp.max(hit, axis=1, keepdims=True)
            h = jnp.where(used > 0.5, rms_f32(x, gain[...]), 0.0)
            hbuf[slot, pl.ds(i * sub_rows, sub_rows), :] = h.astype(BF)
            h_copy(slot, i, row).start()
        hb = hbuf[slot]
        qkv = jnp.concatenate([dotf(hb, w_q[...]).astype(BF), dotf(hb, wpair[2 * qn:2 * qn + 4 * kn, :], NT).astype(BF)], axis=1)
        lane = lax.broadcasted_iota(jnp.int32, (1, vrows), 1)
        rowid = jnp.zeros((1, vrows), jnp.int32)
        for i, row in enumerate(rows):
            rowid = jnp.where(lane // sub_rows == i, row + lane - i * sub_rows, rowid)
        rowid = rowid.astype(F32)
        for b in range(batch):
            sl = slice(b * seq, (b + 1) * seq)
            hot = jnp.where(d_rows[sl, :vrows] == rowid, 1.0, 0.0).astype(BF)
            got = dotf(hot, qkv)
            qt[sl, :] = (qt[sl, :].astype(F32) + got[:, :qn]).astype(BF)
            at = slice((b % 2) * seq, (b % 2 + 1) * seq)
            kvacc[b // 2, at, :] = (kvacc[b // 2, at, :].astype(F32) + got[:, qn:]).astype(BF)

    def step_a(e):
        with jax.named_scope('a_wait'):
            @pl.when((e >= 2) & (e < events))
            def _():
                for dr in both:
                    ring(dr, e, e).wait_recv()

        @pl.when(e < events - 2)
        def _():
            for dr in both:
                ring(dr, e, e + 2).start()

        @pl.when(e < events)
        def _():
            for dr in both:
                side(dr, e).start()

        @pl.when(e == 0)
        def _():
            for k in both:
                wk_push(k).start()
            for b in range(batch):
                wide = jnp.broadcast_to(tok_seq[b:b + 1, :].astype(F32), (vrows, seq))
                d_rows[b * seq:(b + 1) * seq, :vrows] = wide.T
            qt[...] = jnp.zeros_like(qt)
            kvacc[...] = jnp.zeros_like(kvacc)

        @pl.when(e == 1)
        def _():
            for c in ld[1:]:
                c.wait()
            total(wpair.at[pl.ds(2 * qn, 2 * kn)], w_s.at[3])
            for dr in both:
                for k in both:
                    g_home(dr, k).start()

        @pl.when(e == events - 2)
        def _():
            for dr in both:
                g_ring(dr, 0, 2, True).start()

        @pl.when((e >= 2) & (e < 4 + parts))
        def _():
            @pl.when(e >= 4)
            def _():
                wq_push(e - 4).wait_send()
                wq_home(e - 4).wait()

            @pl.when(e < 2 + parts)
            def _():
                k = e - 2
                block = wq_v[span(k * wq_p, wq_p), :]
                tb(k)[...] = block.astype(F32).T.astype(BF)
                wo_push(k).start()
                wq_push(k).start()
                wq_home(k).start()

        with jax.named_scope('a_proj'):
            @pl.when(e >= 1)
            def _():
                for dr in both:
                    side(dr, e - 1).wait_recv()
                project(e - 1)

    each(0, events + 1, step_a)

    to_far = rdma(kvacc.at[core], farkv.at[core], xs.at[0], xr.at[0], far)
    relay = rdma(farkv.at[core], farkv.at[core], xs.at[1], xr.at[1], sib)
    at_i = lax.broadcasted_iota(jnp.int32, (pos, seq), 1) - pos * rank
    own_i = lax.broadcasted_iota(jnp.int32, (pos, seq), 0)
    col = jnp.concatenate([jnp.sum(jnp.where(at_i == own_i, tok_seq[b:b + 1, :].astype(F32), 0.0), axis=1, keepdims=True) for b in range(batch)], axis=0).astype(jnp.int32)
    lanes = lax.broadcasted_iota(jnp.int32, (vrows, vrows), 1)
    hot_mine = jnp.concatenate([jnp.where(col == lanes + j * vrows, 1.0, 0.0).astype(BF) for j in range(vocab // vrows)], axis=1)
    to_far.start()
    for dr in both:
        g_ring(dr, 1, 3, True).start()
        for k in both:
            g_side(dr, k, True).start()
            g_home(dr, k).wait()
    cw = min(512, d)

    def own_rows(j):
        y_v[:, span(j * cw, cw)] = dotf(hot_mine, table[:, span(j * cw, cw)]).astype(BF)

    each(0, d // cw, own_rows)
    for b in range(batch):
        ids = rank * vrows + lax.broadcasted_iota(jnp.int32, (vrows, seq), 0)
        hotm[:, b * seq:(b + 1) * seq] = jnp.where(ids == tok_seq[b:b + 1, :], 1.0, 0.0).astype(BF)

    def place(p, first):
        l_i = lax.broadcasted_iota(jnp.int32, (4 * kn, 2 * hd), 0)
        m_i = lax.broadcasted_iota(jnp.int32, (4 * kn, 2 * hd), 1)
        upper = jnp.where(l_i >= 2 * kn, 1, 0)
        owner = jnp.where(upper == 1, 1 - first, first)
        l_i = l_i - 2 * kn * upper
        base = kn * (2 * p + owner)
        want = jnp.where(l_i < kn, base + l_i, hd + base + l_i - kn)
        return jnp.where(m_i == want, 1.0, 0.0).astype(BF)

    def rope(raw, g):
        n = rms_f32(raw.astype(F32), g)
        return (n * cos[...] + pltpu.roll(n, hd // 2, 1) * sin_s[...]).astype(BF)

    def attend(u):
        base = (u // heads) * seq
        rows = span(base, seq)
        cols = span(lax.rem(u, heads) * hd, hd)
        q = rope(qt[rows, cols], qg[...])
        qr[rows, cols] = q
        kr = k_rot[rows, :]
        v = kv_tok[rows, hd:]
        for i in both:
            p = causal_blocks(q[i * blk:(i + 1) * blk], kr, i, blk)
            o = sum(dotf(t.astype(BF), v[j * blk:(j + 1) * blk]) for j, t in enumerate(p))
            o_own[pl.ds(pl.multiple_of(base + i * blk, blk), blk), cols] = o.astype(BF)

    def grad_attend(e):
        total(hbuf, g_sem.at[0])
        r = dotf(hbuf[...].reshape(2 * vrows, d), wpair[:qn, :], NT).astype(BF)
        for k in both:
            for i, (dr, c) in enumerate(places):
                n = (4 * k + i) * pos
                gd[pl.ds(g_row(dr, e + k, c), pos), :] = r[n:n + pos]

    def pstage(j):
        return d_rows.at[span(lax.rem(j, 2) * vhalf, vhalf), pl.ds(0, bw)]

    def pstore(dst, j):
        return pltpu.make_async_copy(pstage(j), dst.at[:, span(j * bw, bw)], pt_sem.at[lax.rem(j, 2)])

    def pblock(dst, j, pairs):
        @pl.when(j >= 2)
        def _():
            pstore(dst, j - 2).wait()
        cols = span(j * bw, bw)
        acc = None
        for a, lo, n in pairs:
            t = dotf(a[...], wpair[lo:lo + n, cols])
            acc = t if acc is None else acc + t
        pstage(j)[...] = acc
        pstore(dst, j).start()

    y_pairs = [(sq, 0, qn), (o_sib, qn, qn)]

    def pslot(ph, e, dr):
        return pbuf.at[2 * ph + lax.rem(e, 2), dr]

    def pfetch(ph, e, dr):
        s = e // 2
        step = s if ph else lax.rem(z + (2 * nz - 1 - s if dr == 0 else 1 + s), nz)
        row = pl.multiple_of(vrows * step + sub_rows * (2 * dr + lax.rem(e, 2)), sub_rows)
        return pltpu.make_async_copy((py_out, ph_out)[ph].at[pl.ds(row, sub_rows)], pslot(ph, e, dr), pl_sem.at[ph, lax.rem(e, 2)])

    def rslot(dr, e):
        return table.at[span((dr * (events - 2) + e) * sub_rows, sub_rows)]

    def sslot(ph, dr, e):
        k = 2 * (events - 2) + 8 * ph + 4 * lax.rem(e // 2, 2) + 2 * dr + lax.rem(e, 2)
        return table.at[span(k * sub_rows, sub_rows)]

    def send(ph, dr, e):
        return rdma(sslot(ph, dr, e), rslot(dr, e), rs.at[ph, dr, lax.rem(e, 4)], r_sem.at[dr, e + 2], nbr(dr))

    def first_fetch(ph):
        for e in both:
            for dr in both:
                pfetch(ph, e, dr).start()

    def first_sends(ph):
        for e in both:
            total(pbuf.at[2 * ph + e], pl_sem.at[ph, e])
            for dr in both:
                sslot(ph, dr, e)[...] = pslot(ph, e, dr)[...].astype(BF)
        for e in both:
            for dr in both:
                send(ph, dr, e).start()
                pfetch(ph, e + 2, dr).start()

    def serve(ph, e, final):
        for dr in both:
            send(ph, dr, e - 2).wait_recv()
        total(pbuf.at[2 * ph + lax.rem(e, 2)], pl_sem.at[ph, lax.rem(e, 2)])

        @pl.when(e < events - 2)
        def _():
            @pl.when(e >= 4)
            def _():
                for dr in both:
                    send(ph, dr, e - 4).wait_send()
            for dr in both:
                sslot(ph, dr, e)[...] = (pslot(ph, e, dr)[...] + rslot(dr, e - 2)[...].astype(F32)).astype(BF)
            for dr in both:
                send(ph, dr, e).start()
                pfetch(ph, e + 2, dr).start()

        @pl.when(e >= events - 2)
        def _():
            for dr in both:
                final(dr, lax.rem(e, 2), pslot(ph, e, dr)[...] + rslot(dr, e - 2)[...].astype(F32))

    slots = 9

    def gather_o(k):
        for b in range(batch):
            src = pl.multiple_of(b * seq + pos * (2 * k + core), pos)
            sq[pl.ds(pl.multiple_of(vrows * k + pos * b, pos), pos), :] = o_own[pl.ds(src, pos), :]

    def upto(e, n, over):
        return jnp.minimum((e * n) // over, n)

    def step_b(e):
        with jax.named_scope('b_first'):
            @pl.when(e == events - 2)
            def _():
                first_sends(0)

        with jax.named_scope('b_wait'):
            @pl.when((e >= 2) & (e < events))
            def _():
                for dr in both:
                    g_ring(dr, e, e, False).wait_recv()

        @pl.when((e >= 2) & (e < events - 2))
        def _():
            for dr in both:
                g_ring(dr, e, e + 2, False).start()

        @pl.when((e >= 2) & (e < events))
        def _():
            for dr in both:
                g_side(dr, e, False).start()

        @pl.when((e >= 1) & (e <= events))
        def _():
            for dr in both:
                g_side(dr, e - 1, False).wait_recv()

        with jax.named_scope('kv_far'):
            @pl.when(e == 2)
            def _():
                to_far.wait_recv()
                relay.start()

        with jax.named_scope('kv_tok'):
            @pl.when(e == 3)
            def _():
                rdma(farkv.at[1 - core], farkv.at[1 - core], xs.at[1], xr.at[1], sib).wait_recv()
                for hf in both:
                    kv_tok[hf * (toks // 2):(hf + 1) * (toks // 2), :] = (dotf(kvacc[hf], place(par, core)) + dotf(farkv[hf], place(1 - par, hf))).astype(BF)
                for b in range(batch):
                    sl = slice(b * seq, (b + 1) * seq)
                    k_rot[sl, :] = rope(kv_tok[sl, :hd], kg[...])

            @pl.when((e >= 2) & (lax.rem(e, 2) == 0))
            def _():
                for k in both:
                    for i, (dr, c) in enumerate(places):
                        g_fetch(k, i, dr, c, e - 2 + k).start()

        def give(b):
            each(0, nz, lambda k: o_push(b, k).start())

        def seen(t):
            return jnp.minimum((jnp.maximum(t - 3, 0) * units) // (slots - 3), units)

        each(seen(e - 1) // heads, seen(e) // heads, give)
        with jax.named_scope('b_attend'):
            each(seen(e), seen(e + 1), attend)

        @pl.when(e == 4)
        def _():
            total(table.at[pl.ds(0, 2 * (events - 2) * sub_rows)], a_s.at[0])
            total(table.at[pl.ds(0, 2 * events * sub_rows)], a_s.at[1])

        @pl.when(e == slots + 1)
        def _():
            total(wpair.at[pl.ds(0, qn)], w_s.at[1])
            total(o_sib, o_s.at[1])
            each(0, nz, gather_o)

        with jax.named_scope('b_part'):
            @pl.when((e > slots) & (e <= slots + 4))
            def _():
                each(4 * (e - slots - 1), 4 * (e - slots), lambda j: pblock(py_out, j, y_pairs))

        @pl.when(e == slots + 4)
        def _():
            for j in (events - 2, events - 1):
                pstore(py_out, j).wait()
            first_fetch(0)

        with jax.named_scope('b_grad'):
            @pl.when((e >= 3) & (lax.rem(e, 2) == 1))
            def _():
                grad_attend(e - 3)

    for slot in both:
        total(hbuf.at[slot], h_sem.at[slot])
    each(0, events + 2, step_b)

    def pull(raw, dout, g):
        x = raw.astype(F32)
        r = lax.rsqrt(jnp.mean(x * x, axis=-1, keepdims=True) + EPS)
        dn = dout * cos[...] + pltpu.roll(dout * sin_s[...], hd // 2, 1)
        return rms_pull(x, dn * g, r).astype(BF), jnp.sum(dn * (x * r), axis=0, keepdims=True)

    def unit(u):
        b, h = u // heads, lax.rem(u, heads)
        rows = span(b * seq, seq)
        cols = span(h * hd, hd)

        @pl.when(h == 0)
        def _():
            dk_acc[...] = jnp.zeros_like(dk_acc)
            dv_acc[...] = jnp.zeros_like(dv_acc)
        q, g = qr[rows, cols], gd[rows, cols]
        kr, v = k_rot[rows, :], kv_tok[rows, hd:]
        dqs = []
        for i in both:
            qi, gi = q[i * blk:(i + 1) * blk], g[i * blk:(i + 1) * blk]
            p = causal_blocks(qi, kr, i, blk)
            dp = [dotf(gi, v[j * blk:(j + 1) * blk], NT) for j in range(i + 1)]
            tot = sum(jnp.sum(a * b, axis=-1, keepdims=True) for a, b in zip(p, dp))
            dq = None
            for j in range(i + 1):
                at = slice(j * blk, (j + 1) * blk)
                dv_acc[at, :] += dotf(p[j].astype(BF), gi, TN)
                ds = (p[j] * (dp[j] - tot)).astype(BF)
                t = dotf(ds, kr[at])
                dq = t if dq is None else dq + t
                dk_acc[at, :] += dotf(ds, qi, TN)
            dqs.append(dq * scale)
        dq = jnp.concatenate(dqs, axis=0).astype(BF).astype(F32)
        dx, dg = pull(qt[rows, cols], dq, qg[...])
        gd[rows, cols] = dx
        qga[...] += dg

    def pick(r, up):
        m_i = lax.broadcasted_iota(jnp.int32, (2 * hd, 4 * kn), 0)
        l_i = lax.broadcasted_iota(jnp.int32, (2 * hd, 4 * kn), 1) - 2 * kn * up
        is_k = (l_i >= 0) & (l_i < kn) & (m_i == l_i + kn * r)
        is_v = (l_i >= kn) & (l_i < 2 * kn) & (m_i == hd + kn * r + l_i - kn)
        return jnp.where(is_k | is_v, 1.0, 0.0).astype(BF)

    def to_side(b, p):
        return rdma(pk.at[b, 2 * p + 1 - core], rk1.at[b, p], p1s.at[0], p1r.at[b], sib)

    def to_far2(b):
        return rdma(fk.at[b], rk2.at[b], p2s.at[0], p2r.at[b], far)

    def kv_one(b):
        dk = (dk_acc[...] * scale).astype(BF).astype(F32)
        dx, dg = pull(kv_tok[span(b * seq, seq), :hd], dk, kg[...])
        kga[...] += dg
        gkv = jnp.concatenate([dx, dv_acc[...].astype(BF)], axis=1)
        for r in range(4):
            pk[b, r] = (dotf(gkv[:blk], pick(r, 0)) + dotf(gkv[blk:], pick(r, 1))).astype(BF)
        for p in both:
            to_side(b, p).start()

    def kv_two(b):
        total(rk1.at[b], p1r.at[b])
        fk[b] = (pk[b, 2 * (1 - par) + core].astype(F32) + rk1[b, 1 - par].astype(F32)).astype(BF)
        hk[b] = pk[b, 2 * par + core].astype(F32) + rk1[b, par].astype(F32)
        to_far2(b).start()

    def kv_three(b):
        to_far2(b).wait_recv()
        t = hk[b] + rk2[b].astype(F32)
        low = lax.broadcasted_iota(jnp.int32, t.shape, 1) < 2 * kn
        kvt[b, :blk, :] = jnp.where(low, t, 0.0).astype(BF)
        kvt[b, blk:, :] = jnp.where(low, pltpu.roll(t, 2 * kn, 1), 0.0).astype(BF)

    def fold(b, tile):
        rows = span(tile * seq, seq)
        ids = tile * seq + lax.broadcasted_iota(jnp.int32, (seq, seq), 0)
        hot = jnp.where(ids == tok_seq[pl.ds(b, 1), :], 1.0, 0.0).astype(BF)
        d_rows[rows, :qn] += dotf(hot, gd[span(b * seq, seq), :])
        d_rows[rows, qn:] += dotf(hot, kvt[b])

    tiles = vocab // seq

    def run_unit(u):
        unit(u)

        @pl.when(lax.rem(u, heads) == heads - 1)
        def _():
            kv_one(u // heads)

        @pl.when((u >= heads) & (lax.rem(u, heads) == 1))
        def _():
            kv_two(u // heads - 1)

    def run_fold(f):
        b, tile = f // tiles, lax.rem(f, tiles)

        @pl.when(tile == 0)
        def _():
            kv_three(b)
        fold(b, tile)

    def share(e, first, n, over):
        return jnp.minimum((jnp.maximum(e - first, 0) * n) // over, n)

    def paced(e, first, n, over, f):
        each(share(e, first, n, over), share(e + 1, first, n, over), f)

    def settle(t):
        rows = span(t * vrows, vrows)
        qt[rows, :] = d_rows[rows, :qn].astype(BF)
        kvrow[rows, :] = d_rows[rows, qn:].astype(BF)

    def step_row(k, dr):
        return pl.multiple_of(vrows * lax.rem(z + nz - 1 - k if dr == 0 else k + nz - 1 - z, nz) + 2 * sub_rows * dr, 2 * sub_rows)

    def swap(k, dr, kk):
        src = pl.multiple_of(vrows * (2 * k + 1 - core) + 2 * sub_rows * dr, 2 * sub_rows)
        return rdma((qt, kvrow)[kk].at[pl.ds(src, 2 * sub_rows)], (sq, skv)[kk].at[pl.ds(step_row(k, dr), 2 * sub_rows)], qs.at[0, kk], qs.at[1, kk], sib)

    def gather_h(k):
        for dr in both:
            src = pl.multiple_of(vrows * (2 * k + core) + 2 * sub_rows * dr, 2 * sub_rows)
            dst = pl.ds(step_row(k, dr), 2 * sub_rows)
            o_sib[dst, :] = qt[pl.ds(src, 2 * sub_rows), :]
            kvc[dst, :] = (kvrow[pl.ds(src, 2 * sub_rows), :].astype(F32) + pltpu.roll(skv[dst, :].astype(F32), 2 * kn, 1)).astype(BF)

    hrows = vhalf // 2

    def hstage(j):
        return d_rows.at[pl.ds(pl.multiple_of(vhalf + lax.rem(j, 2) * hrows, hrows), hrows), pl.ds(0, bw)]

    def hstore(j):
        return pltpu.make_async_copy(hstage(j), ph_out.at[span((j // events) * hrows, hrows), span(lax.rem(j, events) * bw, bw)], pt_sem.at[lax.rem(j, 2)])

    def hblock(j):
        @pl.when(lax.rem(j, events) >= 2)
        def _():
            hstore(j - 2).wait()
        rows = span((j // events) * hrows, hrows)
        cols = span(lax.rem(j, events) * bw, bw)
        hstage(j)[...] = dotf(o_sib[rows, :], wpair[:qn, cols]) + dotf(sq[rows, :], wpair[qn:2 * qn, cols]) + dotf(kvc[rows, :], wpair[2 * qn:2 * qn + 4 * kn, cols])
        hstore(j).start()

    def final_y(dr, sub, acc):
        rows = span((2 * dr + sub) * pos, pos)
        y_v[rows, :] = (y_v[rows, :].astype(F32) + acc).astype(BF)

    def step_c(e):
        with jax.named_scope('c_first'):
            @pl.when(e == events - 2)
            def _():
                first_sends(1)

        with jax.named_scope('c_serve'):
            @pl.when(e >= 2)
            def _():
                serve(0, e, final_y)

        @pl.when(e == 0)
        def _():
            total(gown, b_s.at[0])
            total(gown, b_s.at[2])
            total(wqts_out, wq_r.at[0])
            total(wpair.at[pl.ds(0, qn)], w_s.at[0])
            for c in ld2:
                c.start()
            d_rows[...] = jnp.zeros_like(d_rows)
            gn[...] = jnp.zeros_like(gn)
            qga[...] = jnp.zeros_like(qga)
            kga[...] = jnp.zeros_like(kga)

        with jax.named_scope('c_unit'):
            paced(e, 2, units, 6, run_unit)

        with jax.named_scope('c_kv2'):
            @pl.when(e == 8)
            def _():
                kv_two(batch - 1)
        with jax.named_scope('c_fold'):
            paced(e, 8, batch * tiles, 3, run_fold)

        with jax.named_scope('c_settle'):
            @pl.when(e == 10)
            def _():
                each(0, 2 * nz, settle)
                each(0, nz, lambda k: [swap(k, dr, kk).start() for dr in both for kk in both])

        with jax.named_scope('c_swap'):
            @pl.when(e == 11)
            def _():
                for c in ld2:
                    c.wait()
                total(sq, qs.at[1, 0])
                total(skv, qs.at[1, 1])
                each(0, nz, gather_h)
        with jax.named_scope('c_part'):
            paced(e, 11, events, 2, hblock)

        @pl.when(e == 12)
        def _():
            for j in (events - 2, events - 1):
                hstore(j).wait()
            first_fetch(1)

    each(0, events, step_c)

    def gblk(j):
        return qr.at[:, span(lax.rem(j, 2) * bw, bw)]

    def hblk(j):
        return gd.at[:, span(lax.rem(j, 2) * bw, bw)]

    def swo(j):
        return d_rows.at[pl.ds(0, qn), span(lax.rem(j, 2) * bw, bw)]

    def swq(j):
        return d_rows.at[pl.ds(pl.multiple_of(qn + lax.rem(j, 2) * bw, bw), bw), pl.ds(0, qn)]

    def g_load(j):
        return pltpu.make_async_copy(gy_out.at[:, span(j * bw, bw)], gblk(j), gls.at[lax.rem(j, 2)])

    def h_load(j):
        return pltpu.make_async_copy(hid.at[:, span(j * bw, bw)], hblk(j), hls.at[lax.rem(j, 2)])

    def wo_store(j):
        return pltpu.make_async_copy(swo(j), gwo_hbm.at[:, span(j * bw, bw)], swos.at[lax.rem(j, 2)])

    def wq_store(j):
        return pltpu.make_async_copy(swq(j), gq_hbm.at[span(j * bw, bw)], swqs.at[lax.rem(j, 2)])

    def block(j):
        g_load(j).wait()
        h_load(j).wait()

        @pl.when(j + 1 < events)
        def _():
            g_load(j + 1).start()
            h_load(j + 1).start()

        @pl.when(j >= 2)
        def _():
            wo_store(j - 2).wait()
            wq_store(j - 2).wait()
        cols = span(j * bw, bw)
        swo(j)[...] = dotf(o_own[...], gblk(j)[...], TN)
        ge_v[:, cols] = dotf(hotm[...], gblk(j)[...])
        wo_store(j).start()
        swq(j)[...] = dotf(hblk(j)[...], qt[...], TN)
        gkv_v[:, cols] = dotf(kvrow[...], hblk(j)[...], TN)[:2 * kn]
        wq_store(j).start()

    def final_h(dr, sub, gh):
        rows = span((2 * dr + sub) * sub_rows, sub_rows)
        x = gown[rows, :].astype(F32)
        r = lax.rsqrt(jnp.mean(x * x, axis=-1, keepdims=True) + EPS)
        ge_v[rows, :] += rms_pull(x, gh * gain[...], r)
        gn[...] += jnp.sum(gh * (x * r), axis=0, keepdims=True)

    outs = [pltpu.make_async_copy(s, t, out_sem.at[i]) for i, (s, t) in enumerate((
        (y_v, y_hbm), (gkv_v.at[pl.ds(0, kn)], gk_hbm), (gkv_v.at[pl.ds(kn, kn)], gv_hbm), (ge_v, ge_hbm)))]
    g_load(0).start()
    h_load(0).start()
    outs[0].start()
    work_d = events - 3

    wide = gn_out.shape[1]
    gtop = d // wide
    order = sorted(range(1, 2 * nz), key=lambda k: -min((k + 1) // 2, nz - k // 2))

    def spread(t, k, src):
        buf = (gall, qall)[t]
        return rdma(buf.at[src], buf.at[src], gs.at[0, t], gs.at[1, t], lax.rem(rank + k, 2 * nz))

    def step_d(e):
        with jax.named_scope('d_serve'):
            @pl.when(e >= 2)
            def _():
                serve(1, e, final_h)

        @pl.when(e == 1)
        def _():
            qall[rank, 0:1, :] = qga[...]
            qall[rank, 1:2, :] = kga[...]

        @pl.when(e == 2)
        def _():
            for k in order:
                spread(1, k, rank).start()

        with jax.named_scope('d_part'):
            paced(e, 0, events, 5, lambda j: hblock(j + events))

        @pl.when(e == 5)
        def _():
            for j in (events - 2, events - 1):
                hstore(j + events).wait()
        with jax.named_scope('d_block'):
            paced(e, 1, events, work_d - 1, block)

    each(0, events, step_d)

    for j in range(gtop):
        gall[rank, j:j + 1, :] = gn[:, j * wide:(j + 1) * wide].astype(gall.dtype)
    outs[3].start()
    outs[1].start()
    outs[2].start()
    with jax.named_scope('t_store'):
        for j in (events - 2, events - 1):
            wo_store(j).wait()
            wq_store(j).wait()
    for k in order:
        spread(0, k, rank).start()

    for ph in both:
        for dr in both:
            for e in range(events - 6, events - 2):
                send(ph, dr, e).wait_send()

    total(gy_out.at[pl.ds(0, 2 * (events - 4) * pos)], b_s.at[1])
    total(gy_out.at[pl.ds(0, 2 * (events - 2) * pos)], b_s.at[3])
    to_far.wait_send()
    relay.wait_send()
    total(wpair.at[pl.ds(2 * qn, 2 * kn)], w_s.at[2])
    total(o_sib, o_s.at[0])
    total(pk.at[pl.ds(0, batch // 2)], p1s.at[0])
    total(fk, p2s.at[0])
    total(sq, qs.at[0, 0])
    total(skv, qs.at[0, 1])
    with jax.named_scope('gain_wait'):
        peers = pl.ds(0, 2 * nz - 1)
        total(qall.at[peers], gs.at[1, 1])
        total(gall.at[peers], gs.at[1, 0])
    with jax.named_scope('gain_sum'):
        acc = gall[0].astype(F32)
        for r in range(1, 2 * nz):
            acc = acc + gall[r].astype(F32)
        gn_out[...] = acc
        qk = jnp.sum(qall[...], axis=0)
        gqg_out[...] = qk[0:1]
        gkg_out[...] = qk[1:2]
        total(gall.at[peers], gs.at[0, 0])
        total(qall.at[peers], gs.at[0, 1])
    with jax.named_scope('t_outs'):
        for c in outs:
            c.wait()


def step_kernel(nz, embed, gy, wq, wk_t, wv_t, wo, gain, qg, kg, cos, sin_s, tok_seq):
    vrows, d = embed.shape
    vocab = vrows * 2 * nz
    qn, kn = wq.shape[1], wk_t.shape[0]
    hd = qg.shape[1]
    batch, seq = tok_seq.shape
    toks = batch * seq
    ev = 2 * nz
    sr, hb, vh = vrows // 4, seq // 2, vocab // 2
    dma = pltpu.SemaphoreType.DMA
    v = pltpu.VMEM

    def arr(dt, *shape):
        return jax.ShapeDtypeStruct(shape, dt)

    outs = (arr(BF, vrows, d), arr(F32, vrows, d), arr(F32, d, qn), arr(F32, kn, d), arr(F32, kn, d), arr(F32, qn, d), arr(F32, d // hd, hd), arr(F32, 1, hd), arr(F32, 1, hd),
            arr(BF, vocab, d), arr(BF, toks, d), arr(BF, qn, d), arr(BF, qn, d), arr(F32, vh, d), arr(F32, vh, d))
    return pl.pallas_call(
        functools.partial(body, nz),
        name='step_kernel',
        out_shape=outs,
        in_specs=[ANY] * 6 + [VM] * 6,
        out_specs=(ANY,) * 6 + (VM,) * 3 + (ANY,) * 6,
        scratch_shapes=[v((vocab, d), BF), v((2 * qn + 4 * kn, d), BF), v((max(d, 2 * toks), qn), BF), v((vocab, qn), BF), v((toks, qn), BF), v((vh, qn), BF), v((vh, qn), BF),
                        v((toks, 2 * hd), BF), v((toks, hd), BF), v((2, toks // 2, 4 * kn), BF), v((2, toks // 2, 4 * kn), BF), v((vocab, 4 * kn), BF), v((vh, 4 * kn), BF), v((vh, 4 * kn), BF),
                        v((vocab, qn + 4 * kn), F32), v((4, 2, sr, d), F32), v((2, vrows, d), BF), v((vrows, d), BF), v((vrows, toks), BF),
                        v((seq, hd), F32), v((seq, hd), F32), v((batch, 4, hb, 4 * kn), BF), v((batch, 2, hb, 4 * kn), BF), v((batch, hb, 4 * kn), BF), v((batch, hb, 4 * kn), F32),
                        v((batch, hb, 4 * kn), BF), v((batch, seq, 4 * kn), BF), v((1, d), F32), v((1, hd), F32), v((1, hd), F32), v((ev, d // hd, hd), BF), v((ev, 8, hd), F32), v((vrows, d), BF), v((vrows, d), F32), v((2 * kn, d), F32),
                        dma((12,)), dma((2,)), dma((1,)), dma((2, ev)), dma((2, ev)), dma((2,)), dma((4,)), dma((2,)), dma((2,)), dma((2, 2)), dma((1,)), dma((4,)), dma((2,)),
                        dma((2,)), dma((2, 2)), dma((2, 2, 4)), dma((1,)), dma((batch,)), dma((1,)), dma((batch,)), dma((2, 2)),
                        dma((2,)), dma((2,)), dma((2,)), dma((2,)), dma((2, 2)), dma((4,))],
        compiler_params=pltpu.CompilerParams(collective_id=0, has_side_effects=True, vmem_limit_bytes=67043328),
        cost_estimate=pl.CostEstimate(flops=2 * vocab * d * 8 * qn, bytes_accessed=20 * vocab * d, transcendentals=0),
    )(embed, gy, wq, wk_t, wv_t, wo, gain, qg, kg, cos, sin_s, tok_seq)


def emit_body(cuts, *refs):
    n = len(cuts)
    src, dst = refs[:n], refs[n:2 * n]
    bufs, s_in, s_out = refs[2 * n:-2], refs[-2], refs[-1]
    ins, outs = [], []
    for i, c in enumerate(cuts):
        step = src[i].shape[0] // c
        for j in range(c):
            b = bufs[i].at[pl.ds(j * step, step)]
            ins.append(pltpu.make_async_copy(src[i].at[pl.ds(j * step, step)], b, s_in.at[len(ins)]))
            outs.append(pltpu.make_async_copy(b, dst[i].at[pl.ds(j * step, step)], s_out.at[len(outs)]))
    for c in ins:
        c.start()
    for a, b in zip(ins, outs):
        a.wait()
        b.start()
    for b in outs:
        b.wait()


def emit(*arrays):
    size = 1 << 20
    cuts = tuple(max(1, a.size * a.dtype.itemsize // size) for a in arrays)
    return pl.pallas_call(
        functools.partial(emit_body, cuts),
        name='emit',
        out_shape=tuple(jax.ShapeDtypeStruct(a.shape, a.dtype) for a in arrays),
        in_specs=[ANY] * len(arrays),
        out_specs=(ANY,) * len(arrays),
        scratch_shapes=[pltpu.VMEM(a.shape, a.dtype) for a in arrays] + [pltpu.SemaphoreType.DMA((sum(cuts),))] * 2,
        compiler_params=pltpu.CompilerParams(vmem_limit_bytes=60 * 1024 * 1024),
        cost_estimate=pl.CostEstimate(flops=0, bytes_accessed=2 * sum(a.size * a.dtype.itemsize for a in arrays), transcendentals=0),
    )(*arrays)


def rope_consts(seq, hd):
    inv = np.float32(ROPE_BASE) ** (np.float32(-2.0) * np.arange(hd // 2, dtype=np.float32) / np.float32(hd))
    ang = np.arange(seq, dtype=np.float32)[:, None] * inv.astype(np.float32)[None, :]
    ang = np.concatenate([ang, ang], axis=-1)
    sign = np.where(np.arange(hd) < hd // 2, -1.0, 1.0).astype(np.float32)
    return np.cos(ang).astype(np.float32), (np.sin(ang) * sign).astype(np.float32)


def solution(mesh):
    tp = mesh.shape['tp']
    nz = tp // 2

    def local_step(tok_ids, embed_loc, norm_gain, q_gain, k_gain, wq, wk, wv, wo, gy_loc):
        d_model = embed_loc.shape[1]
        batch, seq = tok_ids.shape
        seq_dev = seq // tp
        hd = q_gain.shape[0]
        cos_c, sin_c = (jnp.asarray(t) for t in rope_consts(seq, hd))
        r = step_kernel(nz, embed_loc, gy_loc.reshape(batch * seq_dev, d_model), wq, wk.T, wv.T, wo, norm_gain[None, :], q_gain[None, :], k_gain[None, :], cos_c, sin_c, tok_ids)
        y, g_embed, g_wq, g_wk, g_wv, g_wo, g_n, g_q, g_k = emit(*r[:9])
        return (y.reshape(batch, seq_dev, d_model), g_embed, g_n.reshape(d_model), g_q.reshape(hd), g_k.reshape(hd), g_wq, g_wk.T, g_wv.T, g_wo)

    in_specs = (P('dp', None), P('tp', None), P(), P(), P(), P(None, 'tp'), P(None, 'tp'), P(None, 'tp'), P('tp', None), P('dp', 'tp', None))
    out_specs = (P('dp', 'tp', None), P(('dp', 'tp'), None), P('dp'), P('dp'), P('dp'), P('dp', 'tp'), P('dp', 'tp'), P('dp', 'tp'), P(('dp', 'tp'), None))
    return jax.shard_map(local_step, mesh=mesh, in_specs=in_specs, out_specs=out_specs, check_vma=False)
```

```python
import functools
import jax
import jax.numpy as jnp
import numpy as np
from jax import lax
from jax.experimental import pallas as pl
from jax.experimental.pallas import tpu as pltpu
from jax.sharding import PartitionSpec as P

BF = jnp.bfloat16
F32 = jnp.float32
EPS = 1.0e-6
ROPE_BASE = 1.0e6
NEG_BIG = -1.0e30
LOG2E = 1.4426950408889634
MESH = pl.DeviceIdType.MESH
ANY = pl.BlockSpec(memory_space=pl.ANY)
VM = pl.BlockSpec(memory_space=pltpu.VMEM)
NT = (((1,), (1,)), ((), ()))
NN = (((1,), (0,)), ((), ()))
TN = (((0,), (0,)), ((), ()))


def dotf(a, b, dims=NN):
    return lax.dot_general(a, b, dims, preferred_element_type=F32)


def rdma(src, dst, ssem, rsem, dev):
    return pltpu.make_async_remote_copy(src_ref=src, dst_ref=dst, send_sem=ssem, recv_sem=rsem, device_id={'tp': dev}, device_id_type=MESH)


def span(start, size):
    return pl.ds(pl.multiple_of(start, size), size)


def each(lo, hi, f):
    def go(j, _):
        f(j)
        return 0
    lax.fori_loop(lo, hi, go, 0)


def total(ref, sem):
    pltpu.make_async_copy(ref, ref, sem).wait()


def rms_f32(x, gain):
    return x * lax.rsqrt(jnp.mean(x * x, axis=-1, keepdims=True) + EPS) * gain


def rms_pull(x, dxr, r):
    return r * dxr - x * (r * r * r * jnp.mean(x * dxr, axis=-1, keepdims=True))


def causal_blocks(q, keys, i, blk):
    r_i = lax.broadcasted_iota(jnp.int32, (blk, blk), 0)
    c_i = lax.broadcasted_iota(jnp.int32, (blk, blk), 1)
    s = [dotf(q, keys[j * blk:(j + 1) * blk], NT) for j in range(i + 1)]
    s[i] = jnp.where(r_i >= c_i, s[i], NEG_BIG)
    top = functools.reduce(jnp.maximum, [jnp.max(t, axis=-1, keepdims=True) for t in s])
    c = q.shape[-1] ** -0.5 * LOG2E
    e = [jnp.exp2((t - top) * c) for t in s]
    inv = 1.0 / sum(jnp.sum(t, axis=-1, keepdims=True) for t in e)
    return [t * inv for t in e]


def body(nz, embed, gy, wq, wk_t, wv_t, wo, gain, qg, kg, cos, sin_s, tok_seq,
         y_hbm, ge_hbm, gq_hbm, gk_hbm, gv_hbm, gwo_hbm, gn_out, gqg_out, gkg_out, erows, hid, gy_out, wqt_out, wqts_out, py_out, ph_out,
         table, wpair, wq_v, qt, o_own, o_sib, sq, kv_tok, k_rot, kvacc, farkv, kvrow, skv, kvc, d_rows, pbuf, hbuf, gown, hotm,
         dk_acc, dv_acc, pk, rk1, fk, hk, rk2, kvt, gn, qga, kga, gall, qall, y_v, ge_v, gkv_v,
         in_sem, h_sem, g_sem, r_sem, s_sem, a_s, b_s, xs, xr, wq_s, wq_r, w_s, o_s, pt_sem, pl_sem, rs, p1s, p1r, p2s, p2r, qs, gls, hls, swos, swqs, gs, out_sem, e_sem):
    rank = lax.axis_index('tp')
    z, core = rank // 2, lax.rem(rank, 2)
    right = 2 * lax.rem(z + 1, nz) + core
    left = 2 * lax.rem(z + nz - 1, nz) + core
    sib = rank + 1 - 2 * core
    par = lax.rem(z, 2)
    far = rank + 2 - 4 * par
    vrows, d = embed.shape
    kn = wk_t.shape[0]
    sub_rows = vrows // 4
    vocab = vrows * 2 * nz
    vhalf = vocab // 2
    batch, seq = tok_seq.shape
    toks = batch * seq
    qn = wq.shape[1]
    hd = qg.shape[1]
    heads = qn // hd
    events = 2 * nz
    pos = seq // events
    blk = seq // 2
    bw = d // events
    scale = hd ** -0.5
    units = batch * heads
    parts = 8
    wo_p, wq_p = qn // parts, d // parts
    both = (0, 1)
    places = [(dr, c) for dr in both for c in both]
    qr = wq_v.at[pl.ds(0, toks)]
    gd = wq_v.at[pl.ds(toks, toks)]
    w_q = wq_v.at[pl.ds(0, d)]

    ld = [pltpu.make_async_copy(s, t, in_sem.at[i]) for i, (s, t) in enumerate((
        (embed, table.at[span(rank * vrows, vrows)]), (gy, gown), (wq, w_q), (wo, wpair.at[pl.ds(0, qn)]),
        (wk_t, wpair.at[pl.ds(2 * qn, kn)]), (wv_t, wpair.at[pl.ds(2 * qn + kn, kn)])))]
    ld2 = [pltpu.make_async_copy(s, t, in_sem.at[i]) for i, (s, t) in enumerate((
        (wqt_out, wpair.at[pl.ds(0, qn)]), (wqts_out, wpair.at[pl.ds(qn, qn)]), (embed, gown)))]
    ld[0].start()
    barrier = pltpu.get_barrier_semaphore()
    for dev in (right, left, sib):
        pl.semaphore_signal(barrier, inc=1, device_id={'tp': dev}, device_id_type=MESH)
    with jax.named_scope('head'):
        pl.semaphore_wait(barrier, 3)
        ld[0].wait()

    def nbr(dr):
        return right if dr == 0 else left

    def zd_of(dr, e):
        s = e // 2
        return lax.rem(z + (nz - s if dr == 0 else s), nz)

    def row_of(dr, e, c):
        return pl.multiple_of(vrows * (2 * zd_of(dr, e) + c) + sub_rows * (2 * dr + lax.rem(e, 2)), sub_rows)

    def ring(dr, e, recv_e):
        a = table.at[pl.ds(row_of(dr, e, core), sub_rows)]
        return rdma(a, a, a_s.at[0], r_sem.at[dr, recv_e], nbr(dr))

    def side(dr, e):
        a = table.at[pl.ds(row_of(dr, e, core), sub_rows)]
        return rdma(a, a, a_s.at[1], s_sem.at[dr, e], sib)

    def e_keep(dr, e):
        dst = pl.multiple_of(vrows * lax.rem(e // 2 + nz - 1, nz) + sub_rows * (2 * dr + lax.rem(e, 2)), sub_rows)
        return pltpu.make_async_copy(table.at[pl.ds(row_of(dr, e, core), sub_rows)], erows.at[pl.ds(dst, sub_rows)], e_sem.at[0])

    def h_copy(slot, i, row):
        return pltpu.make_async_copy(hbuf.at[slot, pl.ds(i * sub_rows, sub_rows)], hid.at[pl.ds(row, sub_rows)], h_sem.at[slot])

    def g_row(dr, e, c):
        return pl.multiple_of(seq * (2 * dr + lax.rem(e, 2)) + pos * (2 * zd_of(dr, e) + c), pos)

    def g_piece(dr, e, c):
        return gy_out.at[pl.ds(g_row(dr, e, c), pos)]

    def g_own(dr, e):
        return gown.at[span(pos * (2 * dr + lax.rem(e, 2)), pos)]

    def g_ring(dr, e, recv_e, first):
        a = g_piece(dr, e, core)
        return rdma(g_own(dr, e) if first else a, a, b_s.at[0 if first else 1], r_sem.at[dr, recv_e], nbr(dr))

    def g_side(dr, e, first):
        a = g_piece(dr, e, core)
        return rdma(g_own(dr, e) if first else a, a, b_s.at[2 if first else 3], s_sem.at[dr, e], sib)

    def g_home(dr, e):
        return pltpu.make_async_copy(g_own(dr, e), g_piece(dr, e, core), in_sem.at[8 + 2 * dr + e])

    def g_fetch(slot, i, dr, c, e):
        return pltpu.make_async_copy(g_piece(dr, e, c), hbuf.at[slot, pl.ds(i * pos, pos)], g_sem.at[0])

    def wo_push(k):
        return rdma(wpair.at[span(k * wo_p, wo_p)], wpair.at[pl.ds(pl.multiple_of(qn + k * wo_p, wo_p), wo_p)], w_s.at[0], w_s.at[1], sib)

    def tb(k):
        return o_own.at[span(lax.rem(k, 2) * qn, qn), pl.ds(0, wq_p)]

    def wq_push(k):
        return rdma(tb(k), wqts_out.at[:, span(k * wq_p, wq_p)], wq_s.at[0, lax.rem(k, 2)], wq_r.at[0], sib)

    def wq_home(k):
        return pltpu.make_async_copy(tb(k), wqt_out.at[:, span(k * wq_p, wq_p)], wq_s.at[1, lax.rem(k, 2)])

    def wk_push(k):
        return rdma((wk_t, wv_t)[k], wpair.at[pl.ds(2 * qn + (2 + k) * kn, kn)], w_s.at[2], w_s.at[3], sib)

    def o_push(b, k):
        src = pl.multiple_of(b * seq + pos * (2 * k + 1 - core), pos)
        dst = pl.multiple_of(vrows * k + pos * b, pos)
        return rdma(o_own.at[pl.ds(src, pos)], o_sib.at[pl.ds(dst, pos)], o_s.at[0], o_s.at[1], sib)

    def project(e):
        slot = lax.rem(e, 2)

        @pl.when(e >= 2)
        def _():
            total(hbuf.at[slot], h_sem.at[slot])

        rows = [row_of(dr, e, c) for dr, c in places]
        for i, row in enumerate(rows):
            x = table[pl.ds(row, sub_rows), :].astype(F32)
            ids = row + lax.broadcasted_iota(jnp.int32, (sub_rows, seq), 0)
            hit = jnp.zeros((sub_rows, seq), F32)
            for b in range(batch):
                hit = jnp.maximum(hit, jnp.where(tok_seq[b:b + 1, :] == ids, 1.0, 0.0))
            used = jnp.max(hit, axis=1, keepdims=True)
            h = jnp.where(used > 0.5, rms_f32(x, gain[...]), 0.0)
            hbuf[slot, pl.ds(i * sub_rows, sub_rows), :] = h.astype(BF)
            h_copy(slot, i, row).start()
        hb = hbuf[slot]
        qkv = jnp.concatenate([dotf(hb, w_q[...]).astype(BF), dotf(hb, wpair[2 * qn:2 * qn + 4 * kn, :], NT).astype(BF)], axis=1)
        lane = lax.broadcasted_iota(jnp.int32, (1, vrows), 1)
        rowid = jnp.zeros((1, vrows), jnp.int32)
        for i, row in enumerate(rows):
            rowid = jnp.where(lane // sub_rows == i, row + lane - i * sub_rows, rowid)
        rowid = rowid.astype(F32)
        for b in range(batch):
            sl = slice(b * seq, (b + 1) * seq)
            hot = jnp.where(d_rows[sl, :vrows] == rowid, 1.0, 0.0).astype(BF)
            got = dotf(hot, qkv)
            qt[sl, :] = (qt[sl, :].astype(F32) + got[:, :qn]).astype(BF)
            at = slice((b % 2) * seq, (b % 2 + 1) * seq)
            kvacc[b // 2, at, :] = (kvacc[b // 2, at, :].astype(F32) + got[:, qn:]).astype(BF)

    def step_a(e):
        with jax.named_scope('a_wait'):
            @pl.when((e >= 2) & (e < events))
            def _():
                for dr in both:
                    ring(dr, e, e).wait_recv()

        @pl.when(e < events - 2)
        def _():
            for dr in both:
                ring(dr, e, e + 2).start()

        @pl.when(e < events)
        def _():
            for dr in both:
                side(dr, e).start()
                e_keep(dr, e).start()

        @pl.when(e == 0)
        def _():
            for c in ld[1:]:
                c.start()
            for k in both:
                wk_push(k).start()
            for b in range(batch):
                wide = jnp.broadcast_to(tok_seq[b:b + 1, :].astype(F32), (vrows, seq))
                d_rows[b * seq:(b + 1) * seq, :vrows] = wide.T
            qt[...] = jnp.zeros_like(qt)
            kvacc[...] = jnp.zeros_like(kvacc)

        @pl.when(e == 1)
        def _():
            for c in ld[1:]:
                c.wait()
            total(wpair.at[pl.ds(2 * qn, 2 * kn)], w_s.at[3])
            for dr in both:
                for k in both:
                    g_home(dr, k).start()

        @pl.when(e == events - 2)
        def _():
            for dr in both:
                g_ring(dr, 0, 2, True).start()

        @pl.when((e >= 2) & (e < 4 + parts))
        def _():
            @pl.when(e >= 4)
            def _():
                wq_push(e - 4).wait_send()
                wq_home(e - 4).wait()

            @pl.when(e < 2 + parts)
            def _():
                k = e - 2
                block = wq_v[span(k * wq_p, wq_p), :]
                tb(k)[...] = block.astype(F32).T.astype(BF)
                wo_push(k).start()
                wq_push(k).start()
                wq_home(k).start()

        with jax.named_scope('a_proj'):
            @pl.when(e >= 1)
            def _():
                for dr in both:
                    side(dr, e - 1).wait_recv()
                project(e - 1)

    each(0, events + 1, step_a)

    to_far = rdma(kvacc.at[core], farkv.at[core], xs.at[0], xr.at[0], far)
    relay = rdma(farkv.at[core], farkv.at[core], xs.at[1], xr.at[1], sib)
    at_i = lax.broadcasted_iota(jnp.int32, (pos, seq), 1) - pos * rank
    own_i = lax.broadcasted_iota(jnp.int32, (pos, seq), 0)
    col = jnp.concatenate([jnp.sum(jnp.where(at_i == own_i, tok_seq[b:b + 1, :].astype(F32), 0.0), axis=1, keepdims=True) for b in range(batch)], axis=0).astype(jnp.int32)
    lanes = lax.broadcasted_iota(jnp.int32, (vrows, vrows), 1)
    hot_mine = jnp.concatenate([jnp.where(col == lanes + j * vrows, 1.0, 0.0).astype(BF) for j in range(vocab // vrows)], axis=1)
    to_far.start()
    for dr in both:
        g_ring(dr, 1, 3, True).start()
        for k in both:
            g_side(dr, k, True).start()
            g_home(dr, k).wait()
    cw = min(512, d)

    def own_rows(j):
        y_v[:, span(j * cw, cw)] = dotf(hot_mine, table[:, span(j * cw, cw)]).astype(BF)

    each(0, d // cw, own_rows)
    for b in range(batch):
        ids = rank * vrows + lax.broadcasted_iota(jnp.int32, (vrows, seq), 0)
        hotm[:, b * seq:(b + 1) * seq] = jnp.where(ids == tok_seq[b:b + 1, :], 1.0, 0.0).astype(BF)

    def place(p, first):
        l_i = lax.broadcasted_iota(jnp.int32, (4 * kn, 2 * hd), 0)
        m_i = lax.broadcasted_iota(jnp.int32, (4 * kn, 2 * hd), 1)
        upper = jnp.where(l_i >= 2 * kn, 1, 0)
        owner = jnp.where(upper == 1, 1 - first, first)
        l_i = l_i - 2 * kn * upper
        base = kn * (2 * p + owner)
        want = jnp.where(l_i < kn, base + l_i, hd + base + l_i - kn)
        return jnp.where(m_i == want, 1.0, 0.0).astype(BF)

    def rope(raw, g):
        n = rms_f32(raw.astype(F32), g)
        return (n * cos[...] + pltpu.roll(n, hd // 2, 1) * sin_s[...]).astype(BF)

    def attend(u):
        base = (u // heads) * seq
        rows = span(base, seq)
        cols = span(lax.rem(u, heads) * hd, hd)
        q = rope(qt[rows, cols], qg[...])
        qr[rows, cols] = q
        kr = k_rot[rows, :]
        v = kv_tok[rows, hd:]
        for i in both:
            p = causal_blocks(q[i * blk:(i + 1) * blk], kr, i, blk)
            o = sum(dotf(t.astype(BF), v[j * blk:(j + 1) * blk]) for j, t in enumerate(p))
            o_own[pl.ds(pl.multiple_of(base + i * blk, blk), blk), cols] = o.astype(BF)

    def grad_attend(e):
        total(hbuf, g_sem.at[0])
        r = dotf(hbuf[...].reshape(2 * vrows, d), wpair[:qn, :], NT).astype(BF)
        for k in both:
            for i, (dr, c) in enumerate(places):
                n = (4 * k + i) * pos
                gd[pl.ds(g_row(dr, e + k, c), pos), :] = r[n:n + pos]

    def pstage(j):
        return d_rows.at[span(lax.rem(j, 2) * vhalf, vhalf), pl.ds(0, bw)]

    def pstore(dst, j):
        return pltpu.make_async_copy(pstage(j), dst.at[:, span(j * bw, bw)], pt_sem.at[lax.rem(j, 2)])

    def pblock(dst, j, pairs):
        @pl.when(j >= 2)
        def _():
            pstore(dst, j - 2).wait()
        cols = span(j * bw, bw)
        acc = None
        for a, lo, n in pairs:
            t = dotf(a[...], wpair[lo:lo + n, cols])
            acc = t if acc is None else acc + t
        pstage(j)[...] = acc
        pstore(dst, j).start()

    y_pairs = [(sq, 0, qn), (o_sib, qn, qn)]

    def pslot(ph, e, dr):
        return pbuf.at[2 * ph + lax.rem(e, 2), dr]

    def pfetch(ph, e, dr):
        s = e // 2
        step = s if ph else lax.rem(z + (2 * nz - 1 - s if dr == 0 else 1 + s), nz)
        row = pl.multiple_of(vrows * step + sub_rows * (2 * dr + lax.rem(e, 2)), sub_rows)
        return pltpu.make_async_copy((py_out, ph_out)[ph].at[pl.ds(row, sub_rows)], pslot(ph, e, dr), pl_sem.at[ph, lax.rem(e, 2)])

    def eslot(e, dr):
        return hbuf.at[lax.rem(e, 2), pl.ds(dr * sub_rows, sub_rows)]

    def efetch(e, dr):
        row = pl.multiple_of(vrows * (e // 2) + sub_rows * (2 * dr + lax.rem(e, 2)), sub_rows)
        return pltpu.make_async_copy(erows.at[pl.ds(row, sub_rows)], eslot(e, dr), e_sem.at[1 + lax.rem(e, 2)])

    def fetch(ph, e, dr):
        pfetch(ph, e, dr).start()
        if ph:
            efetch(e, dr).start()

    def fetched(ph, e):
        total(pbuf.at[2 * ph + lax.rem(e, 2)], pl_sem.at[ph, lax.rem(e, 2)])
        if ph:
            total(hbuf.at[lax.rem(e, 2), pl.ds(0, 2 * sub_rows)], e_sem.at[1 + lax.rem(e, 2)])

    def gain_part(ph, e):
        if ph:
            for dr in both:
                x = eslot(e, dr)[...].astype(F32)
                t = pslot(ph, e, dr)[...] * (x * lax.rsqrt(jnp.mean(x * x, axis=-1, keepdims=True) + EPS))
                gn[...] += sum(t[i:i + 8] for i in range(0, sub_rows, 8))

    def rslot(dr, e):
        return table.at[span((dr * (events - 2) + e) * sub_rows, sub_rows)]

    def sslot(ph, dr, e):
        k = 2 * (events - 2) + 8 * ph + 4 * lax.rem(e // 2, 2) + 2 * dr + lax.rem(e, 2)
        return table.at[span(k * sub_rows, sub_rows)]

    def send(ph, dr, e):
        return rdma(sslot(ph, dr, e), rslot(dr, e), rs.at[ph, dr, lax.rem(e, 4)], r_sem.at[dr, e + 2], nbr(dr))

    def first_fetch(ph):
        for e in both:
            for dr in both:
                fetch(ph, e, dr)

    def first_sends(ph):
        for e in both:
            fetched(ph, e)
            for dr in both:
                sslot(ph, dr, e)[...] = pslot(ph, e, dr)[...].astype(BF)
        for e in both:
            for dr in both:
                send(ph, dr, e).start()
        for e in both:
            gain_part(ph, e)
            for dr in both:
                fetch(ph, e + 2, dr)

    def serve(ph, e, final):
        for dr in both:
            send(ph, dr, e - 2).wait_recv()
        if ph == 0:
            fetched(ph, e)

        @pl.when(e < events - 2)
        def _():
            if ph:
                fetched(ph, e)

            @pl.when(e >= 4)
            def _():
                for dr in both:
                    send(ph, dr, e - 4).wait_send()
            for dr in both:
                sslot(ph, dr, e)[...] = (pslot(ph, e, dr)[...] + rslot(dr, e - 2)[...].astype(F32)).astype(BF)
            for dr in both:
                send(ph, dr, e).start()
            gain_part(ph, e)
            for dr in both:
                fetch(ph, e + 2, dr)

        @pl.when(e >= events - 2)
        def _():
            for dr in both:
                final(dr, lax.rem(e, 2), pslot(ph, e, dr)[...] + rslot(dr, e - 2)[...].astype(F32))

    slots = 9

    def gather_o(k):
        for b in range(batch):
            src = pl.multiple_of(b * seq + pos * (2 * k + core), pos)
            sq[pl.ds(pl.multiple_of(vrows * k + pos * b, pos), pos), :] = o_own[pl.ds(src, pos), :]

    def upto(e, n, over):
        return jnp.minimum((e * n) // over, n)

    def step_b(e):
        with jax.named_scope('b_first'):
            @pl.when(e == events - 2)
            def _():
                first_sends(0)

        with jax.named_scope('b_wait'):
            @pl.when((e >= 2) & (e < events))
            def _():
                for dr in both:
                    g_ring(dr, e, e, False).wait_recv()

        @pl.when((e >= 2) & (e < events - 2))
        def _():
            for dr in both:
                g_ring(dr, e, e + 2, False).start()

        @pl.when((e >= 2) & (e < events))
        def _():
            for dr in both:
                g_side(dr, e, False).start()

        @pl.when((e >= 1) & (e <= events))
        def _():
            for dr in both:
                g_side(dr, e - 1, False).wait_recv()

        with jax.named_scope('kv_far'):
            @pl.when(e == 2)
            def _():
                to_far.wait_recv()
                relay.start()

        with jax.named_scope('kv_tok'):
            @pl.when(e == 3)
            def _():
                rdma(farkv.at[1 - core], farkv.at[1 - core], xs.at[1], xr.at[1], sib).wait_recv()
                for hf in both:
                    kv_tok[hf * (toks // 2):(hf + 1) * (toks // 2), :] = (dotf(kvacc[hf], place(par, core)) + dotf(farkv[hf], place(1 - par, hf))).astype(BF)
                for b in range(batch):
                    sl = slice(b * seq, (b + 1) * seq)
                    k_rot[sl, :] = rope(kv_tok[sl, :hd], kg[...])

            @pl.when((e >= 2) & (lax.rem(e, 2) == 0))
            def _():
                for k in both:
                    for i, (dr, c) in enumerate(places):
                        g_fetch(k, i, dr, c, e - 2 + k).start()

        def give(b):
            each(0, nz, lambda k: o_push(b, k).start())

        def seen(t):
            return jnp.minimum((jnp.maximum(t - 3, 0) * units) // (slots - 3), units)

        each(seen(e - 1) // heads, seen(e) // heads, give)
        with jax.named_scope('b_attend'):
            each(seen(e), seen(e + 1), attend)

        @pl.when(e == 4)
        def _():
            total(table.at[pl.ds(0, 2 * (events - 2) * sub_rows)], a_s.at[0])
            total(table.at[pl.ds(0, 2 * events * sub_rows)], a_s.at[1])
            total(erows, e_sem.at[0])

        @pl.when(e == slots + 1)
        def _():
            total(wpair.at[pl.ds(0, qn)], w_s.at[1])
            total(o_sib, o_s.at[1])
            each(0, nz, gather_o)

        with jax.named_scope('b_part'):
            @pl.when((e > slots) & (e <= slots + 4))
            def _():
                each(4 * (e - slots - 1), 4 * (e - slots), lambda j: pblock(py_out, j, y_pairs))

        @pl.when(e == slots + 4)
        def _():
            for j in (events - 2, events - 1):
                pstore(py_out, j).wait()
            first_fetch(0)

        with jax.named_scope('b_grad'):
            @pl.when((e >= 3) & (lax.rem(e, 2) == 1))
            def _():
                grad_attend(e - 3)

    for slot in both:
        total(hbuf.at[slot], h_sem.at[slot])
    each(0, events + 2, step_b)

    def pull(raw, dout, g):
        x = raw.astype(F32)
        r = lax.rsqrt(jnp.mean(x * x, axis=-1, keepdims=True) + EPS)
        dn = dout * cos[...] + pltpu.roll(dout * sin_s[...], hd // 2, 1)
        return rms_pull(x, dn * g, r).astype(BF), jnp.sum(dn * (x * r), axis=0, keepdims=True)

    def unit(u):
        b, h = u // heads, lax.rem(u, heads)
        rows = span(b * seq, seq)
        cols = span(h * hd, hd)

        @pl.when(h == 0)
        def _():
            dk_acc[...] = jnp.zeros_like(dk_acc)
            dv_acc[...] = jnp.zeros_like(dv_acc)
        q, g = qr[rows, cols], gd[rows, cols]
        kr, v = k_rot[rows, :], kv_tok[rows, hd:]
        dqs = []
        for i in both:
            qi, gi = q[i * blk:(i + 1) * blk], g[i * blk:(i + 1) * blk]
            p = causal_blocks(qi, kr, i, blk)
            dp = [dotf(gi, v[j * blk:(j + 1) * blk], NT) for j in range(i + 1)]
            tot = sum(jnp.sum(a * b, axis=-1, keepdims=True) for a, b in zip(p, dp))
            dq = None
            for j in range(i + 1):
                at = slice(j * blk, (j + 1) * blk)
                dv_acc[at, :] += dotf(p[j].astype(BF), gi, TN)
                ds = (p[j] * (dp[j] - tot)).astype(BF)
                t = dotf(ds, kr[at])
                dq = t if dq is None else dq + t
                dk_acc[at, :] += dotf(ds, qi, TN)
            dqs.append(dq * scale)
        dq = jnp.concatenate(dqs, axis=0).astype(BF).astype(F32)
        dx, dg = pull(qt[rows, cols], dq, qg[...])
        gd[rows, cols] = dx
        qga[...] += dg

    def pick(r, up):
        m_i = lax.broadcasted_iota(jnp.int32, (2 * hd, 4 * kn), 0)
        l_i = lax.broadcasted_iota(jnp.int32, (2 * hd, 4 * kn), 1) - 2 * kn * up
        is_k = (l_i >= 0) & (l_i < kn) & (m_i == l_i + kn * r)
        is_v = (l_i >= kn) & (l_i < 2 * kn) & (m_i == hd + kn * r + l_i - kn)
        return jnp.where(is_k | is_v, 1.0, 0.0).astype(BF)

    def to_side(b, p):
        return rdma(pk.at[b, 2 * p + 1 - core], rk1.at[b, p], p1s.at[0], p1r.at[b], sib)

    def to_far2(b):
        return rdma(fk.at[b], rk2.at[b], p2s.at[0], p2r.at[b], far)

    def kv_one(b):
        dk = (dk_acc[...] * scale).astype(BF).astype(F32)
        dx, dg = pull(kv_tok[span(b * seq, seq), :hd], dk, kg[...])
        kga[...] += dg
        gkv = jnp.concatenate([dx, dv_acc[...].astype(BF)], axis=1)
        for r in range(4):
            pk[b, r] = (dotf(gkv[:blk], pick(r, 0)) + dotf(gkv[blk:], pick(r, 1))).astype(BF)
        for p in both:
            to_side(b, p).start()

    def kv_two(b):
        total(rk1.at[b], p1r.at[b])
        fk[b] = (pk[b, 2 * (1 - par) + core].astype(F32) + rk1[b, 1 - par].astype(F32)).astype(BF)
        hk[b] = pk[b, 2 * par + core].astype(F32) + rk1[b, par].astype(F32)
        to_far2(b).start()

    def kv_three(b):
        to_far2(b).wait_recv()
        t = hk[b] + rk2[b].astype(F32)
        low = lax.broadcasted_iota(jnp.int32, t.shape, 1) < 2 * kn
        kvt[b, :blk, :] = jnp.where(low, t, 0.0).astype(BF)
        kvt[b, blk:, :] = jnp.where(low, pltpu.roll(t, 2 * kn, 1), 0.0).astype(BF)

    def fold(b, tile):
        rows = span(tile * seq, seq)
        ids = tile * seq + lax.broadcasted_iota(jnp.int32, (seq, seq), 0)
        hot = jnp.where(ids == tok_seq[pl.ds(b, 1), :], 1.0, 0.0).astype(BF)
        d_rows[rows, :qn] += dotf(hot, gd[span(b * seq, seq), :])
        d_rows[rows, qn:] += dotf(hot, kvt[b])

    tiles = vocab // seq

    def run_unit(u):
        unit(u)

        @pl.when(lax.rem(u, heads) == heads - 1)
        def _():
            kv_one(u // heads)

        @pl.when((u >= heads) & (lax.rem(u, heads) == 1))
        def _():
            kv_two(u // heads - 1)

    def run_fold(f):
        b, tile = f // tiles, lax.rem(f, tiles)

        @pl.when(tile == 0)
        def _():
            kv_three(b)
        fold(b, tile)

    def share(e, first, n, over):
        return jnp.minimum((jnp.maximum(e - first, 0) * n) // over, n)

    def paced(e, first, n, over, f):
        each(share(e, first, n, over), share(e + 1, first, n, over), f)

    def settle(t):
        rows = span(t * vrows, vrows)
        qt[rows, :] = d_rows[rows, :qn].astype(BF)
        kvrow[rows, :] = d_rows[rows, qn:].astype(BF)

    def step_row(k, dr):
        return pl.multiple_of(vrows * lax.rem(z + nz - 1 - k if dr == 0 else k + nz - 1 - z, nz) + 2 * sub_rows * dr, 2 * sub_rows)

    def swap(k, dr, kk):
        src = pl.multiple_of(vrows * (2 * k + 1 - core) + 2 * sub_rows * dr, 2 * sub_rows)
        return rdma((qt, kvrow)[kk].at[pl.ds(src, 2 * sub_rows)], (sq, skv)[kk].at[pl.ds(step_row(k, dr), 2 * sub_rows)], qs.at[0, kk], qs.at[1, kk], sib)

    def gather_h(k):
        for dr in both:
            src = pl.multiple_of(vrows * (2 * k + core) + 2 * sub_rows * dr, 2 * sub_rows)
            dst = pl.ds(step_row(k, dr), 2 * sub_rows)
            o_sib[dst, :] = qt[pl.ds(src, 2 * sub_rows), :]
            kvc[dst, :] = (kvrow[pl.ds(src, 2 * sub_rows), :].astype(F32) + pltpu.roll(skv[dst, :].astype(F32), 2 * kn, 1)).astype(BF)

    hrows = vhalf // 2

    def hstage(j):
        return d_rows.at[pl.ds(pl.multiple_of(vhalf + lax.rem(j, 2) * hrows, hrows), hrows), pl.ds(0, bw)]

    def hstore(j):
        return pltpu.make_async_copy(hstage(j), ph_out.at[span((j // events) * hrows, hrows), span(lax.rem(j, events) * bw, bw)], pt_sem.at[lax.rem(j, 2)])

    def hblock(j):
        @pl.when(lax.rem(j, events) >= 2)
        def _():
            hstore(j - 2).wait()
        rows = span((j // events) * hrows, hrows)
        cols = span(lax.rem(j, events) * bw, bw)
        hstage(j)[...] = dotf(o_sib[rows, :], wpair[:qn, cols]) + dotf(sq[rows, :], wpair[qn:2 * qn, cols]) + dotf(kvc[rows, :], wpair[2 * qn:2 * qn + 4 * kn, cols])
        hstore(j).start()

    def final_y(dr, sub, acc):
        rows = span((2 * dr + sub) * pos, pos)
        y_v[rows, :] = (y_v[rows, :].astype(F32) + acc).astype(BF)

    def step_c(e):
        with jax.named_scope('c_first'):
            @pl.when(e == events - 2)
            def _():
                first_sends(1)

        with jax.named_scope('c_serve'):
            @pl.when(e >= 2)
            def _():
                serve(0, e, final_y)

        @pl.when(e == 0)
        def _():
            total(gown, b_s.at[0])
            total(gown, b_s.at[2])
            total(wqts_out, wq_r.at[0])
            total(wpair.at[pl.ds(0, qn)], w_s.at[0])
            for c in ld2:
                c.start()
            d_rows[...] = jnp.zeros_like(d_rows)
            gn[...] = jnp.zeros_like(gn)
            qga[...] = jnp.zeros_like(qga)
            kga[...] = jnp.zeros_like(kga)

        with jax.named_scope('c_unit'):
            paced(e, 2, units, 6, run_unit)

        with jax.named_scope('c_kv2'):
            @pl.when(e == 8)
            def _():
                kv_two(batch - 1)
        with jax.named_scope('c_fold'):
            paced(e, 8, batch * tiles, 3, run_fold)

        with jax.named_scope('c_settle'):
            @pl.when(e == 10)
            def _():
                each(0, 2 * nz, settle)
                each(0, nz, lambda k: [swap(k, dr, kk).start() for dr in both for kk in both])

        with jax.named_scope('c_swap'):
            @pl.when(e == 11)
            def _():
                for c in ld2:
                    c.wait()
                total(sq, qs.at[1, 0])
                total(skv, qs.at[1, 1])
                each(0, nz, gather_h)
        with jax.named_scope('c_part'):
            paced(e, 11, events, 2, hblock)

        @pl.when(e == 12)
        def _():
            for j in (events - 2, events - 1):
                hstore(j).wait()
            first_fetch(1)

    each(0, events, step_c)

    def gblk(j):
        return qr.at[:, span(lax.rem(j, 2) * bw, bw)]

    def hblk(j):
        return gd.at[:, span(lax.rem(j, 2) * bw, bw)]

    def swo(j):
        return d_rows.at[pl.ds(0, qn), span(lax.rem(j, 2) * bw, bw)]

    def swq(j):
        return d_rows.at[pl.ds(pl.multiple_of(qn + lax.rem(j, 2) * bw, bw), bw), pl.ds(0, qn)]

    def g_load(j):
        return pltpu.make_async_copy(gy_out.at[:, span(j * bw, bw)], gblk(j), gls.at[lax.rem(j, 2)])

    def h_load(j):
        return pltpu.make_async_copy(hid.at[:, span(j * bw, bw)], hblk(j), hls.at[lax.rem(j, 2)])

    def wo_store(j):
        return pltpu.make_async_copy(swo(j), gwo_hbm.at[:, span(j * bw, bw)], swos.at[lax.rem(j, 2)])

    def wq_store(j):
        return pltpu.make_async_copy(swq(j), gq_hbm.at[span(j * bw, bw)], swqs.at[lax.rem(j, 2)])

    def block(j):
        g_load(j).wait()
        h_load(j).wait()

        @pl.when(j + 1 < events)
        def _():
            g_load(j + 1).start()
            h_load(j + 1).start()

        @pl.when(j >= 2)
        def _():
            wo_store(j - 2).wait()
            wq_store(j - 2).wait()
        cols = span(j * bw, bw)
        swo(j)[...] = dotf(o_own[...], gblk(j)[...], TN)
        ge_v[:, cols] = dotf(hotm[...], gblk(j)[...])
        wo_store(j).start()
        swq(j)[...] = dotf(hblk(j)[...], qt[...], TN)
        gkv_v[:, cols] = dotf(kvrow[...], hblk(j)[...], TN)[:2 * kn]
        wq_store(j).start()

    def final_h(dr, sub, gh):
        rows = span((2 * dr + sub) * sub_rows, sub_rows)
        x = gown[rows, :].astype(F32)
        r = lax.rsqrt(jnp.mean(x * x, axis=-1, keepdims=True) + EPS)
        ge_v[rows, :] += rms_pull(x, gh * gain[...], r)

    outs = [pltpu.make_async_copy(s, t, out_sem.at[i]) for i, (s, t) in enumerate((
        (y_v, y_hbm), (gkv_v.at[pl.ds(0, kn)], gk_hbm), (gkv_v.at[pl.ds(kn, kn)], gv_hbm), (ge_v, ge_hbm)))]
    g_load(0).start()
    h_load(0).start()
    outs[0].start()
    work_d = events - 3

    wide = gn_out.shape[1]
    gtop = d // wide
    order = sorted(range(1, 2 * nz), key=lambda k: -min((k + 1) // 2, nz - k // 2))

    def spread(t, k, src):
        buf = (gall, qall)[t]
        return rdma(buf.at[src], buf.at[src], gs.at[0, t], gs.at[1, t], lax.rem(rank + k, 2 * nz))

    def step_d(e):
        @pl.when(e == events - 2)
        def _():
            for k in both:
                fetched(1, events - 2 + k)
                gain_part(1, events - 2 + k)
            whole = jnp.sum(gn[...], axis=0, keepdims=True)
            for j in range(gtop):
                gall[rank, j:j + 1, :] = whole[:, j * wide:(j + 1) * wide].astype(gall.dtype)
            for j in (events - 2, events - 1):
                wo_store(j).wait()
                wq_store(j).wait()
            for k in order:
                spread(0, k, rank).start()

        with jax.named_scope('d_serve'):
            @pl.when(e >= 2)
            def _():
                serve(1, e, final_h)

        @pl.when(e == 1)
        def _():
            qall[rank, 0:1, :] = qga[...]
            qall[rank, 1:2, :] = kga[...]

        @pl.when(e == 2)
        def _():
            for k in order:
                spread(1, k, rank).start()

        with jax.named_scope('d_part'):
            paced(e, 0, events, 5, lambda j: hblock(j + events))

        @pl.when(e == 5)
        def _():
            for j in (events - 2, events - 1):
                hstore(j + events).wait()
        with jax.named_scope('d_block'):
            paced(e, 1, events, work_d - 1, block)

        @pl.when(e == events - 3)
        def _():
            outs[1].start()
            outs[2].start()

    each(0, events, step_d)

    outs[3].start()
    for ph in both:
        for dr in both:
            for e in range(events - 6, events - 2):
                send(ph, dr, e).wait_send()

    total(gy_out.at[pl.ds(0, 2 * (events - 4) * pos)], b_s.at[1])
    total(gy_out.at[pl.ds(0, 2 * (events - 2) * pos)], b_s.at[3])
    to_far.wait_send()
    relay.wait_send()
    total(wpair.at[pl.ds(2 * qn, 2 * kn)], w_s.at[2])
    total(o_sib, o_s.at[0])
    total(pk.at[pl.ds(0, batch // 2)], p1s.at[0])
    total(fk, p2s.at[0])
    total(sq, qs.at[0, 0])
    total(skv, qs.at[0, 1])
    with jax.named_scope('gain_wait'):
        peers = pl.ds(0, 2 * nz - 1)
        total(qall.at[peers], gs.at[1, 1])
        total(gall.at[peers], gs.at[1, 0])
    with jax.named_scope('gain_sum'):
        acc = gall[0].astype(F32)
        for r in range(1, 2 * nz):
            acc = acc + gall[r].astype(F32)
        gn_out[...] = acc
        qk = jnp.sum(qall[...], axis=0)
        gqg_out[...] = qk[0:1]
        gkg_out[...] = qk[1:2]
        total(gall.at[peers], gs.at[0, 0])
        total(qall.at[peers], gs.at[0, 1])
    with jax.named_scope('t_outs'):
        for c in outs:
            c.wait()


def step_kernel(nz, embed, gy, wq, wk_t, wv_t, wo, gain, qg, kg, cos, sin_s, tok_seq):
    vrows, d = embed.shape
    vocab = vrows * 2 * nz
    qn, kn = wq.shape[1], wk_t.shape[0]
    hd = qg.shape[1]
    batch, seq = tok_seq.shape
    toks = batch * seq
    ev = 2 * nz
    sr, hb, vh = vrows // 4, seq // 2, vocab // 2
    dma = pltpu.SemaphoreType.DMA
    v = pltpu.VMEM

    def arr(dt, *shape):
        return jax.ShapeDtypeStruct(shape, dt)

    outs = (arr(BF, vrows, d), arr(F32, vrows, d), arr(F32, d, qn), arr(F32, kn, d), arr(F32, kn, d), arr(F32, qn, d), arr(F32, d // hd, hd), arr(F32, 1, hd), arr(F32, 1, hd), arr(BF, vh, d),
            arr(BF, vocab, d), arr(BF, toks, d), arr(BF, qn, d), arr(BF, qn, d), arr(F32, vh, d), arr(F32, vh, d))
    return pl.pallas_call(
        functools.partial(body, nz),
        name='step_kernel',
        out_shape=outs,
        in_specs=[ANY] * 6 + [VM] * 6,
        out_specs=(ANY,) * 6 + (VM,) * 3 + (ANY,) * 7,
        scratch_shapes=[v((vocab, d), BF), v((2 * qn + 4 * kn, d), BF), v((max(d, 2 * toks), qn), BF), v((vocab, qn), BF), v((toks, qn), BF), v((vh, qn), BF), v((vh, qn), BF),
                        v((toks, 2 * hd), BF), v((toks, hd), BF), v((2, toks // 2, 4 * kn), BF), v((2, toks // 2, 4 * kn), BF), v((vocab, 4 * kn), BF), v((vh, 4 * kn), BF), v((vh, 4 * kn), BF),
                        v((vocab, qn + 4 * kn), F32), v((4, 2, sr, d), F32), v((2, vrows, d), BF), v((vrows, d), BF), v((vrows, toks), BF),
                        v((seq, hd), F32), v((seq, hd), F32), v((batch, 4, hb, 4 * kn), BF), v((batch, 2, hb, 4 * kn), BF), v((batch, hb, 4 * kn), BF), v((batch, hb, 4 * kn), F32),
                        v((batch, hb, 4 * kn), BF), v((batch, seq, 4 * kn), BF), v((8, d), F32), v((1, hd), F32), v((1, hd), F32), v((ev, d // hd, hd), BF), v((ev, 8, hd), F32), v((vrows, d), BF), v((vrows, d), F32), v((2 * kn, d), F32),
                        dma((12,)), dma((2,)), dma((1,)), dma((2, ev)), dma((2, ev)), dma((2,)), dma((4,)), dma((2,)), dma((2,)), dma((2, 2)), dma((1,)), dma((4,)), dma((2,)),
                        dma((2,)), dma((2, 2)), dma((2, 2, 4)), dma((1,)), dma((batch,)), dma((1,)), dma((batch,)), dma((2, 2)),
                        dma((2,)), dma((2,)), dma((2,)), dma((2,)), dma((2, 2)), dma((4,)), dma((3,))],
        compiler_params=pltpu.CompilerParams(collective_id=0, has_side_effects=True, vmem_limit_bytes=67043328),
        cost_estimate=pl.CostEstimate(flops=2 * vocab * d * 8 * qn, bytes_accessed=20 * vocab * d, transcendentals=0),
    )(embed, gy, wq, wk_t, wv_t, wo, gain, qg, kg, cos, sin_s, tok_seq)


def emit_body(cuts, *refs):
    n = len(cuts)
    src, dst = refs[:n], refs[n:2 * n]
    bufs, s_in, s_out = refs[2 * n:-2], refs[-2], refs[-1]
    ins, outs = [], []
    for i, c in enumerate(cuts):
        step = src[i].shape[0] // c
        for j in range(c):
            b = bufs[i].at[pl.ds(j * step, step)]
            ins.append(pltpu.make_async_copy(src[i].at[pl.ds(j * step, step)], b, s_in.at[len(ins)]))
            outs.append(pltpu.make_async_copy(b, dst[i].at[pl.ds(j * step, step)], s_out.at[len(outs)]))
    for c in ins:
        c.start()
    for a, b in zip(ins, outs):
        a.wait()
        b.start()
    for b in outs:
        b.wait()


def emit(*arrays):
    size = 1 << 20
    cuts = tuple(max(1, a.size * a.dtype.itemsize // size) for a in arrays)
    return pl.pallas_call(
        functools.partial(emit_body, cuts),
        name='emit',
        out_shape=tuple(jax.ShapeDtypeStruct(a.shape, a.dtype) for a in arrays),
        in_specs=[ANY] * len(arrays),
        out_specs=(ANY,) * len(arrays),
        scratch_shapes=[pltpu.VMEM(a.shape, a.dtype) for a in arrays] + [pltpu.SemaphoreType.DMA((sum(cuts),))] * 2,
        compiler_params=pltpu.CompilerParams(vmem_limit_bytes=60 * 1024 * 1024),
        cost_estimate=pl.CostEstimate(flops=0, bytes_accessed=2 * sum(a.size * a.dtype.itemsize for a in arrays), transcendentals=0),
    )(*arrays)


def rope_consts(seq, hd):
    inv = np.float32(ROPE_BASE) ** (np.float32(-2.0) * np.arange(hd // 2, dtype=np.float32) / np.float32(hd))
    ang = np.arange(seq, dtype=np.float32)[:, None] * inv.astype(np.float32)[None, :]
    ang = np.concatenate([ang, ang], axis=-1)
    sign = np.where(np.arange(hd) < hd // 2, -1.0, 1.0).astype(np.float32)
    return np.cos(ang).astype(np.float32), (np.sin(ang) * sign).astype(np.float32)


def solution(mesh):
    tp = mesh.shape['tp']
    nz = tp // 2

    def local_step(tok_ids, embed_loc, norm_gain, q_gain, k_gain, wq, wk, wv, wo, gy_loc):
        d_model = embed_loc.shape[1]
        batch, seq = tok_ids.shape
        seq_dev = seq // tp
        hd = q_gain.shape[0]
        cos_c, sin_c = (jnp.asarray(t) for t in rope_consts(seq, hd))
        r = step_kernel(nz, embed_loc, gy_loc.reshape(batch * seq_dev, d_model), wq, wk.T, wv.T, wo, norm_gain[None, :], q_gain[None, :], k_gain[None, :], cos_c, sin_c, tok_ids)
        y, g_embed, g_wq, g_wk, g_wv, g_wo, g_n, g_q, g_k = emit(*r[:9])
        return (y.reshape(batch, seq_dev, d_model), g_embed, g_n.reshape(d_model), g_q.reshape(hd), g_k.reshape(hd), g_wq, g_wk.T, g_wv.T, g_wo)

    in_specs = (P('dp', None), P('tp', None), P(), P(), P(), P(None, 'tp'), P(None, 'tp'), P(None, 'tp'), P('tp', None), P('dp', 'tp', None))
    out_specs = (P('dp', 'tp', None), P(('dp', 'tp'), None), P('dp'), P('dp'), P('dp'), P('dp', 'tp'), P('dp', 'tp'), P('dp', 'tp'), P(('dp', 'tp'), None))
    return jax.shard_map(local_step, mesh=mesh, in_specs=in_specs, out_specs=out_specs, check_vma=False)
```

```python
import functools
import jax
import jax.numpy as jnp
import numpy as np
from jax import lax
from jax.experimental import pallas as pl
from jax.experimental.pallas import tpu as pltpu
from jax.sharding import PartitionSpec as P

BF = jnp.bfloat16
F32 = jnp.float32
EPS = 1.0e-6
ROPE_BASE = 1.0e6
NEG_BIG = -1.0e30
LOG2E = 1.4426950408889634
MESH = pl.DeviceIdType.MESH
ANY = pl.BlockSpec(memory_space=pl.ANY)
VM = pl.BlockSpec(memory_space=pltpu.VMEM)
NT = (((1,), (1,)), ((), ()))
NN = (((1,), (0,)), ((), ()))
TN = (((0,), (0,)), ((), ()))


def dotf(a, b, dims=NN):
    return lax.dot_general(a, b, dims, preferred_element_type=F32)


def rdma(src, dst, ssem, rsem, dev):
    return pltpu.make_async_remote_copy(src_ref=src, dst_ref=dst, send_sem=ssem, recv_sem=rsem, device_id={'tp': dev}, device_id_type=MESH)


def span(start, size):
    return pl.ds(pl.multiple_of(start, size), size)


def each(lo, hi, f):
    def go(j, _):
        f(j)
        return 0
    lax.fori_loop(lo, hi, go, 0)


def total(ref, sem):
    pltpu.make_async_copy(ref, ref, sem).wait()


def rms_f32(x, gain):
    return x * lax.rsqrt(jnp.mean(x * x, axis=-1, keepdims=True) + EPS) * gain


def rms_pull(x, dxr, r):
    return r * dxr - x * (r * r * r * jnp.mean(x * dxr, axis=-1, keepdims=True))


def causal_blocks(q, keys, i, blk):
    r_i = lax.broadcasted_iota(jnp.int32, (blk, blk), 0)
    c_i = lax.broadcasted_iota(jnp.int32, (blk, blk), 1)
    s = [dotf(q, keys[j * blk:(j + 1) * blk], NT) for j in range(i + 1)]
    s[i] = jnp.where(r_i >= c_i, s[i], NEG_BIG)
    top = functools.reduce(jnp.maximum, [jnp.max(t, axis=-1, keepdims=True) for t in s])
    c = q.shape[-1] ** -0.5 * LOG2E
    e = [jnp.exp2((t - top) * c) for t in s]
    inv = 1.0 / sum(jnp.sum(t, axis=-1, keepdims=True) for t in e)
    return [t * inv for t in e]


def body(nz, embed, gy, wq, wk_t, wv_t, wo, gain, qg, kg, cos, sin_s, tok_seq,
         y_hbm, ge_hbm, gq_hbm, gk_hbm, gv_hbm, gwo_hbm, gn_out, gqg_out, gkg_out, erows, hid, gy_out, wqt_out, wqts_out, py_out, ph_out,
         table, wpair, wq_v, qt, o_own, o_sib, sq, kv_tok, k_rot, kvacc, farkv, kvrow, skv, kvc, d_rows, pbuf, hbuf, gown, hotm,
         dk_acc, dv_acc, pk, rk1, fk, hk, rk2, kvt, gn, qga, kga, gmine, gsib, gcol, gfin, y_v, ge_v, gkv_v,
         in_sem, h_sem, g_sem, r_sem, s_sem, a_s, b_s, xs, xr, wq_s, wq_r, w_s, o_s, pt_sem, pl_sem, rs, p1s, p1r, p2s, p2r, qs, gls, hls, swos, swqs, gs, out_sem, e_sem):
    rank = lax.axis_index('tp')
    z, core = rank // 2, lax.rem(rank, 2)
    right = 2 * lax.rem(z + 1, nz) + core
    left = 2 * lax.rem(z + nz - 1, nz) + core
    sib = rank + 1 - 2 * core
    par = lax.rem(z, 2)
    far = rank + 2 - 4 * par
    vrows, d = embed.shape
    kn = wk_t.shape[0]
    sub_rows = vrows // 4
    vocab = vrows * 2 * nz
    vhalf = vocab // 2
    batch, seq = tok_seq.shape
    toks = batch * seq
    qn = wq.shape[1]
    hd = qg.shape[1]
    heads = qn // hd
    events = 2 * nz
    pos = seq // events
    blk = seq // 2
    bw = d // events
    scale = hd ** -0.5
    units = batch * heads
    parts = 8
    wo_p, wq_p = qn // parts, d // parts
    both = (0, 1)
    places = [(dr, c) for dr in both for c in both]
    qr = wq_v.at[pl.ds(0, toks)]
    gd = wq_v.at[pl.ds(toks, toks)]
    w_q = wq_v.at[pl.ds(0, d)]

    ld = [pltpu.make_async_copy(s, t, in_sem.at[i]) for i, (s, t) in enumerate((
        (embed, table.at[span(rank * vrows, vrows)]), (gy, gown), (wq, w_q), (wo, wpair.at[pl.ds(0, qn)]),
        (wk_t, wpair.at[pl.ds(2 * qn, kn)]), (wv_t, wpair.at[pl.ds(2 * qn + kn, kn)])))]
    ld2 = [pltpu.make_async_copy(s, t, in_sem.at[i]) for i, (s, t) in enumerate((
        (wqt_out, wpair.at[pl.ds(0, qn)]), (wqts_out, wpair.at[pl.ds(qn, qn)]), (embed, gown)))]
    ld[0].start()
    barrier = pltpu.get_barrier_semaphore()
    for dev in (right, left, sib):
        pl.semaphore_signal(barrier, inc=1, device_id={'tp': dev}, device_id_type=MESH)
    with jax.named_scope('hbar'):
        pl.semaphore_wait(barrier, 3)
    with jax.named_scope('hload'):
        ld[0].wait()

    def nbr(dr):
        return right if dr == 0 else left

    def arrived(sem):
        total(table.at[pl.ds(0, 2 * sub_rows)], sem)

    def zd_of(dr, e):
        s = e // 2
        return lax.rem(z + (nz - s if dr == 0 else s), nz)

    def row_of(dr, e, c):
        return pl.multiple_of(vrows * (2 * zd_of(dr, e) + c) + sub_rows * (2 * dr + lax.rem(e, 2)), sub_rows)

    def ring(dr, e, recv_e):
        a = table.at[pl.ds(row_of(dr, e, core), sub_rows)]
        return rdma(a, a, a_s.at[0], r_sem.at[recv_e], nbr(dr))

    def side(dr, e):
        a = table.at[pl.ds(row_of(dr, e, core), sub_rows)]
        return rdma(a, a, a_s.at[1], s_sem.at[e], sib)

    def e_keep(dr, e):
        dst = pl.multiple_of(vrows * lax.rem(e // 2 + nz - 1, nz) + sub_rows * (2 * dr + lax.rem(e, 2)), sub_rows)
        return pltpu.make_async_copy(table.at[pl.ds(row_of(dr, e, core), sub_rows)], erows.at[pl.ds(dst, sub_rows)], e_sem.at[0])

    def h_copy(slot, i, row):
        return pltpu.make_async_copy(hbuf.at[slot, pl.ds(i * sub_rows, sub_rows)], hid.at[pl.ds(row, sub_rows)], h_sem.at[slot])

    def g_row(dr, e, c):
        return pl.multiple_of(seq * (2 * dr + lax.rem(e, 2)) + pos * (2 * zd_of(dr, e) + c), pos)

    def g_piece(dr, e, c):
        return gy_out.at[pl.ds(g_row(dr, e, c), pos)]

    def g_own(dr, e):
        return gown.at[span(pos * (2 * dr + lax.rem(e, 2)), pos)]

    def g_ring(dr, e, recv_e, first):
        a = g_piece(dr, e, core)
        return rdma(g_own(dr, e) if first else a, a, b_s.at[0 if first else 1], r_sem.at[recv_e], nbr(dr))

    def g_side(dr, e, first):
        a = g_piece(dr, e, core)
        return rdma(g_own(dr, e) if first else a, a, b_s.at[2 if first else 3], s_sem.at[e], sib)

    def g_home(dr, e):
        return pltpu.make_async_copy(g_own(dr, e), g_piece(dr, e, core), in_sem.at[8 + 2 * dr + e])

    def g_fetch(slot, i, dr, c, e):
        return pltpu.make_async_copy(g_piece(dr, e, c), hbuf.at[slot, pl.ds(i * pos, pos)], g_sem.at[0])

    def wo_push(k):
        return rdma(wpair.at[span(k * wo_p, wo_p)], wpair.at[pl.ds(pl.multiple_of(qn + k * wo_p, wo_p), wo_p)], w_s.at[0], w_s.at[1], sib)

    def tb(k):
        return o_own.at[span(lax.rem(k, 2) * qn, qn), pl.ds(0, wq_p)]

    def wq_push(k):
        return rdma(tb(k), wqts_out.at[:, span(k * wq_p, wq_p)], wq_s.at[0, lax.rem(k, 2)], wq_r.at[0], sib)

    def wq_home(k):
        return pltpu.make_async_copy(tb(k), wqt_out.at[:, span(k * wq_p, wq_p)], wq_s.at[1, lax.rem(k, 2)])

    def wk_push(k):
        return rdma((wk_t, wv_t)[k], wpair.at[pl.ds(2 * qn + (2 + k) * kn, kn)], w_s.at[2], w_s.at[3], sib)

    def o_push(b, k):
        src = pl.multiple_of(b * seq + pos * (2 * k + 1 - core), pos)
        dst = pl.multiple_of(vrows * k + pos * b, pos)
        return rdma(o_own.at[pl.ds(src, pos)], o_sib.at[pl.ds(dst, pos)], o_s.at[0], o_s.at[1], sib)

    def project(e):
        slot = lax.rem(e, 2)

        @pl.when(e >= 2)
        def _():
            total(hbuf.at[slot], h_sem.at[slot])

        rows = [row_of(dr, e, c) for dr, c in places]
        for i, row in enumerate(rows):
            x = table[pl.ds(row, sub_rows), :].astype(F32)
            ids = row + lax.broadcasted_iota(jnp.int32, (sub_rows, seq), 0)
            hit = jnp.zeros((sub_rows, seq), F32)
            for b in range(batch):
                hit = jnp.maximum(hit, jnp.where(tok_seq[b:b + 1, :] == ids, 1.0, 0.0))
            used = jnp.max(hit, axis=1, keepdims=True)
            h = jnp.where(used > 0.5, rms_f32(x, gain[...]), 0.0)
            hbuf[slot, pl.ds(i * sub_rows, sub_rows), :] = h.astype(BF)
            h_copy(slot, i, row).start()
        hb = hbuf[slot]
        qkv = jnp.concatenate([dotf(hb, w_q[...]).astype(BF), dotf(hb, wpair[2 * qn:2 * qn + 4 * kn, :], NT).astype(BF)], axis=1)
        lane = lax.broadcasted_iota(jnp.int32, (1, vrows), 1)
        rowid = jnp.zeros((1, vrows), jnp.int32)
        for i, row in enumerate(rows):
            rowid = jnp.where(lane // sub_rows == i, row + lane - i * sub_rows, rowid)
        rowid = rowid.astype(F32)
        for b in range(batch):
            sl = slice(b * seq, (b + 1) * seq)
            hot = jnp.where(d_rows[sl, :vrows] == rowid, 1.0, 0.0).astype(BF)
            got = dotf(hot, qkv)
            qt[sl, :] = (qt[sl, :].astype(F32) + got[:, :qn]).astype(BF)
            at = slice((b % 2) * seq, (b % 2 + 1) * seq)
            kvacc[b // 2, at, :] = (kvacc[b // 2, at, :].astype(F32) + got[:, qn:]).astype(BF)

    def step_a(e):
        with jax.named_scope('a_wait'):
            @pl.when((e >= 2) & (e < events))
            def _():
                arrived(r_sem.at[e])

            @pl.when(e < events - 2)
            def _():
                for dr in both:
                    ring(dr, e, e + 2).start()

        @pl.when(e < events)
        def _():
            for dr in both:
                side(dr, e).start()
                e_keep(dr, e).start()

        @pl.when(e == 0)
        def _():
            for c in ld[1:]:
                c.start()
            for k in both:
                wk_push(k).start()
            for b in range(batch):
                wide = jnp.broadcast_to(tok_seq[b:b + 1, :].astype(F32), (vrows, seq))
                d_rows[b * seq:(b + 1) * seq, :vrows] = wide.T
            qt[...] = jnp.zeros_like(qt)
            kvacc[...] = jnp.zeros_like(kvacc)

        @pl.when(e == 1)
        def _():
            for c in ld[1:]:
                c.wait()
            total(wpair.at[pl.ds(2 * qn, 2 * kn)], w_s.at[3])
            for dr in both:
                for k in both:
                    g_home(dr, k).start()

        @pl.when(e == events - 2)
        def _():
            for dr in both:
                g_ring(dr, 0, 2, True).start()

        @pl.when((e >= 2) & (e < 4 + parts))
        def _():
            @pl.when(e >= 4)
            def _():
                wq_push(e - 4).wait_send()
                wq_home(e - 4).wait()

            @pl.when(e < 2 + parts)
            def _():
                k = e - 2
                block = wq_v[span(k * wq_p, wq_p), :]
                tb(k)[...] = block.astype(F32).T.astype(BF)
                wo_push(k).start()
                wq_push(k).start()
                wq_home(k).start()

        with jax.named_scope('a_proj'):
            @pl.when(e >= 1)
            def _():
                arrived(s_sem.at[e - 1])
                project(e - 1)

    each(0, events + 1, step_a)

    to_far = rdma(kvacc.at[core], farkv.at[core], xs.at[0], xr.at[0], far)
    relay = rdma(farkv.at[core], farkv.at[core], xs.at[1], xr.at[1], sib)
    at_i = lax.broadcasted_iota(jnp.int32, (pos, seq), 1) - pos * rank
    own_i = lax.broadcasted_iota(jnp.int32, (pos, seq), 0)
    col = jnp.concatenate([jnp.sum(jnp.where(at_i == own_i, tok_seq[b:b + 1, :].astype(F32), 0.0), axis=1, keepdims=True) for b in range(batch)], axis=0).astype(jnp.int32)
    lanes = lax.broadcasted_iota(jnp.int32, (vrows, vrows), 1)
    hot_mine = jnp.concatenate([jnp.where(col == lanes + j * vrows, 1.0, 0.0).astype(BF) for j in range(vocab // vrows)], axis=1)
    to_far.start()
    for dr in both:
        g_ring(dr, 1, 3, True).start()
        for k in both:
            g_side(dr, k, True).start()
            g_home(dr, k).wait()
    cw = min(512, d)

    def own_rows(j):
        y_v[:, span(j * cw, cw)] = dotf(hot_mine, table[:, span(j * cw, cw)]).astype(BF)

    each(0, d // cw, own_rows)
    for b in range(batch):
        ids = rank * vrows + lax.broadcasted_iota(jnp.int32, (vrows, seq), 0)
        hotm[:, b * seq:(b + 1) * seq] = jnp.where(ids == tok_seq[b:b + 1, :], 1.0, 0.0).astype(BF)

    def place(p, first):
        l_i = lax.broadcasted_iota(jnp.int32, (4 * kn, 2 * hd), 0)
        m_i = lax.broadcasted_iota(jnp.int32, (4 * kn, 2 * hd), 1)
        upper = jnp.where(l_i >= 2 * kn, 1, 0)
        owner = jnp.where(upper == 1, 1 - first, first)
        l_i = l_i - 2 * kn * upper
        base = kn * (2 * p + owner)
        want = jnp.where(l_i < kn, base + l_i, hd + base + l_i - kn)
        return jnp.where(m_i == want, 1.0, 0.0).astype(BF)

    def rope(raw, g):
        n = rms_f32(raw.astype(F32), g)
        return (n * cos[...] + pltpu.roll(n, hd // 2, 1) * sin_s[...]).astype(BF)

    def attend(u):
        base = (u // heads) * seq
        rows = span(base, seq)
        cols = span(lax.rem(u, heads) * hd, hd)
        q = rope(qt[rows, cols], qg[...])
        qr[rows, cols] = q
        kr = k_rot[rows, :]
        v = kv_tok[rows, hd:]
        for i in both:
            p = causal_blocks(q[i * blk:(i + 1) * blk], kr, i, blk)
            o = sum(dotf(t.astype(BF), v[j * blk:(j + 1) * blk]) for j, t in enumerate(p))
            o_own[pl.ds(pl.multiple_of(base + i * blk, blk), blk), cols] = o.astype(BF)

    def grad_attend(e):
        total(hbuf, g_sem.at[0])
        r = dotf(hbuf[...].reshape(2 * vrows, d), wpair[:qn, :], NT).astype(BF)
        for k in both:
            for i, (dr, c) in enumerate(places):
                n = (4 * k + i) * pos
                gd[pl.ds(g_row(dr, e + k, c), pos), :] = r[n:n + pos]

    def pstage(j):
        return d_rows.at[span(lax.rem(j, 2) * vhalf, vhalf), pl.ds(0, bw)]

    def pstore(dst, j):
        return pltpu.make_async_copy(pstage(j), dst.at[:, span(j * bw, bw)], pt_sem.at[lax.rem(j, 2)])

    def pblock(dst, j, pairs):
        @pl.when(j >= 2)
        def _():
            pstore(dst, j - 2).wait()
        cols = span(j * bw, bw)
        acc = None
        for a, lo, n in pairs:
            t = dotf(a[...], wpair[lo:lo + n, cols])
            acc = t if acc is None else acc + t
        pstage(j)[...] = acc
        pstore(dst, j).start()

    y_pairs = [(sq, 0, qn), (o_sib, qn, qn)]

    def pslot(ph, e, dr):
        return pbuf.at[2 * ph + lax.rem(e, 2), dr]

    def pfetch(ph, e, dr):
        s = e // 2
        step = s if ph else lax.rem(z + (2 * nz - 1 - s if dr == 0 else 1 + s), nz)
        row = pl.multiple_of(vrows * step + sub_rows * (2 * dr + lax.rem(e, 2)), sub_rows)
        return pltpu.make_async_copy((py_out, ph_out)[ph].at[pl.ds(row, sub_rows)], pslot(ph, e, dr), pl_sem.at[ph, lax.rem(e, 2)])

    def item(i):
        row = vrows * (i // 2)
        cps = []
        for dr in both:
            at = pl.ds(pl.multiple_of(row + sub_rows * (2 * dr + lax.rem(i, 2)), sub_rows), sub_rows)
            cps.append(pltpu.make_async_copy(ph_out.at[at], pbuf.at[lax.rem(i, 2), dr], pl_sem.at[0, lax.rem(i, 2)]))
            cps.append(pltpu.make_async_copy(erows.at[at], hbuf.at[lax.rem(i, 2), pl.ds(dr * sub_rows, sub_rows)], e_sem.at[1 + lax.rem(i, 2)]))
        return cps

    def gain_part(i):
        total(pbuf.at[lax.rem(i, 2)], pl_sem.at[0, lax.rem(i, 2)])
        total(hbuf.at[lax.rem(i, 2), pl.ds(0, 2 * sub_rows)], e_sem.at[1 + lax.rem(i, 2)])
        for dr in both:
            x = hbuf[lax.rem(i, 2), dr * sub_rows:(dr + 1) * sub_rows, :].astype(F32)
            t = pbuf[lax.rem(i, 2), dr] * (x * lax.rsqrt(jnp.mean(x * x, axis=-1, keepdims=True) + EPS))
            gn[...] += sum(t[k:k + 8] for k in range(0, sub_rows, 8))

        @pl.when(i + 2 < events)
        def _():
            for c in item(i + 2):
                c.start()

    def fetched(ph, e):
        total(pbuf.at[2 * ph + lax.rem(e, 2)], pl_sem.at[ph, lax.rem(e, 2)])

    def rslot(dr, e):
        return table.at[span((dr * (events - 2) + e) * sub_rows, sub_rows)]

    def sslot(ph, dr, e):
        k = 2 * (events - 2) + 8 * ph + 4 * lax.rem(e // 2, 2) + 2 * dr + lax.rem(e, 2)
        return table.at[span(k * sub_rows, sub_rows)]

    def send(ph, dr, e):
        return rdma(sslot(ph, dr, e), rslot(dr, e), rs.at[ph, lax.rem(e, 4)], r_sem.at[e + 2], nbr(dr))

    def first_fetch(ph):
        for e in both:
            for dr in both:
                pfetch(ph, e, dr).start()

    def first_sends(ph):
        for e in both:
            fetched(ph, e)
            for dr in both:
                sslot(ph, dr, e)[...] = pslot(ph, e, dr)[...].astype(BF)
        for e in both:
            for dr in both:
                send(ph, dr, e).start()
                pfetch(ph, e + 2, dr).start()

    def serve(ph, e, final):
        arrived(r_sem.at[e])
        fetched(ph, e)

        @pl.when(e < events - 2)
        def _():
            @pl.when(e >= 4)
            def _():
                arrived(rs.at[ph, lax.rem(e, 4)])
            for dr in both:
                sslot(ph, dr, e)[...] = (pslot(ph, e, dr)[...] + rslot(dr, e - 2)[...].astype(F32)).astype(BF)
            for dr in both:
                send(ph, dr, e).start()
                pfetch(ph, e + 2, dr).start()

        @pl.when(e >= events - 2)
        def _():
            for dr in both:
                final(dr, lax.rem(e, 2), pslot(ph, e, dr)[...] + rslot(dr, e - 2)[...].astype(F32))

    slots = 9

    def gather_o(k):
        for b in range(batch):
            src = pl.multiple_of(b * seq + pos * (2 * k + core), pos)
            sq[pl.ds(pl.multiple_of(vrows * k + pos * b, pos), pos), :] = o_own[pl.ds(src, pos), :]

    def upto(e, n, over):
        return jnp.minimum((e * n) // over, n)

    def step_b(e):
        with jax.named_scope('b_first'):
            @pl.when(e == events - 2)
            def _():
                first_sends(0)

        with jax.named_scope('b_wait'):
            @pl.when((e >= 2) & (e < events))
            def _():
                arrived(r_sem.at[e])

            @pl.when((e >= 2) & (e < events - 2))
            def _():
                for dr in both:
                    g_ring(dr, e, e + 2, False).start()

        @pl.when((e >= 2) & (e < events))
        def _():
            for dr in both:
                g_side(dr, e, False).start()

        @pl.when((e >= 1) & (e <= events))
        def _():
            arrived(s_sem.at[e - 1])

        with jax.named_scope('kv_far'):
            @pl.when(e == 2)
            def _():
                to_far.wait_recv()
                relay.start()

        with jax.named_scope('kv_tok'):
            @pl.when(e == 3)
            def _():
                rdma(farkv.at[1 - core], farkv.at[1 - core], xs.at[1], xr.at[1], sib).wait_recv()
                for hf in both:
                    kv_tok[hf * (toks // 2):(hf + 1) * (toks // 2), :] = (dotf(kvacc[hf], place(par, core)) + dotf(farkv[hf], place(1 - par, hf))).astype(BF)
                for b in range(batch):
                    sl = slice(b * seq, (b + 1) * seq)
                    k_rot[sl, :] = rope(kv_tok[sl, :hd], kg[...])

            @pl.when((e >= 2) & (lax.rem(e, 2) == 0))
            def _():
                for k in both:
                    for i, (dr, c) in enumerate(places):
                        g_fetch(k, i, dr, c, e - 2 + k).start()

        def give(b):
            each(0, nz, lambda k: o_push(b, k).start())

        def seen(t):
            return jnp.minimum((jnp.maximum(t - 3, 0) * units) // (slots - 3), units)

        each(seen(e - 1) // heads, seen(e) // heads, give)
        with jax.named_scope('b_attend'):
            each(seen(e), seen(e + 1), attend)

        @pl.when(e == 4)
        def _():
            total(table.at[pl.ds(0, 2 * (events - 2) * sub_rows)], a_s.at[0])
            total(table.at[pl.ds(0, 2 * events * sub_rows)], a_s.at[1])
            total(erows, e_sem.at[0])

        @pl.when(e == slots + 1)
        def _():
            total(wpair.at[pl.ds(0, qn)], w_s.at[1])
            total(o_sib, o_s.at[1])
            each(0, nz, gather_o)

        with jax.named_scope('b_part'):
            @pl.when((e > slots) & (e <= slots + 4))
            def _():
                each(4 * (e - slots - 1), 4 * (e - slots), lambda j: pblock(py_out, j, y_pairs))

        @pl.when(e == slots + 4)
        def _():
            for j in (events - 2, events - 1):
                pstore(py_out, j).wait()
            first_fetch(0)

        with jax.named_scope('b_grad'):
            @pl.when((e >= 3) & (lax.rem(e, 2) == 1))
            def _():
                grad_attend(e - 3)

    for slot in both:
        total(hbuf.at[slot], h_sem.at[slot])
    each(0, events + 2, step_b)

    def pull(raw, dout, g):
        x = raw.astype(F32)
        r = lax.rsqrt(jnp.mean(x * x, axis=-1, keepdims=True) + EPS)
        dn = dout * cos[...] + pltpu.roll(dout * sin_s[...], hd // 2, 1)
        return rms_pull(x, dn * g, r).astype(BF), jnp.sum(dn * (x * r), axis=0, keepdims=True)

    def unit(u):
        b, h = u // heads, lax.rem(u, heads)
        rows = span(b * seq, seq)
        cols = span(h * hd, hd)

        @pl.when(h == 0)
        def _():
            dk_acc[...] = jnp.zeros_like(dk_acc)
            dv_acc[...] = jnp.zeros_like(dv_acc)
        q, g = qr[rows, cols], gd[rows, cols]
        kr, v = k_rot[rows, :], kv_tok[rows, hd:]
        dqs = []
        for i in both:
            qi, gi = q[i * blk:(i + 1) * blk], g[i * blk:(i + 1) * blk]
            p = causal_blocks(qi, kr, i, blk)
            dp = [dotf(gi, v[j * blk:(j + 1) * blk], NT) for j in range(i + 1)]
            tot = sum(jnp.sum(a * b, axis=-1, keepdims=True) for a, b in zip(p, dp))
            dq = None
            for j in range(i + 1):
                at = slice(j * blk, (j + 1) * blk)
                dv_acc[at, :] += dotf(p[j].astype(BF), gi, TN)
                ds = (p[j] * (dp[j] - tot)).astype(BF)
                t = dotf(ds, kr[at])
                dq = t if dq is None else dq + t
                dk_acc[at, :] += dotf(ds, qi, TN)
            dqs.append(dq * scale)
        dq = jnp.concatenate(dqs, axis=0).astype(BF).astype(F32)
        dx, dg = pull(qt[rows, cols], dq, qg[...])
        gd[rows, cols] = dx
        qga[...] += dg

    def pick(r, up):
        m_i = lax.broadcasted_iota(jnp.int32, (2 * hd, 4 * kn), 0)
        l_i = lax.broadcasted_iota(jnp.int32, (2 * hd, 4 * kn), 1) - 2 * kn * up
        is_k = (l_i >= 0) & (l_i < kn) & (m_i == l_i + kn * r)
        is_v = (l_i >= kn) & (l_i < 2 * kn) & (m_i == hd + kn * r + l_i - kn)
        return jnp.where(is_k | is_v, 1.0, 0.0).astype(BF)

    def to_side(b, p):
        return rdma(pk.at[b, 2 * p + 1 - core], rk1.at[b, p], p1s.at[0], p1r.at[b], sib)

    def to_far2(b):
        return rdma(fk.at[b], rk2.at[b], p2s.at[0], p2r.at[b], far)

    def kv_one(b):
        dk = (dk_acc[...] * scale).astype(BF).astype(F32)
        dx, dg = pull(kv_tok[span(b * seq, seq), :hd], dk, kg[...])
        kga[...] += dg
        gkv = jnp.concatenate([dx, dv_acc[...].astype(BF)], axis=1)
        for r in range(4):
            pk[b, r] = (dotf(gkv[:blk], pick(r, 0)) + dotf(gkv[blk:], pick(r, 1))).astype(BF)
        for p in both:
            to_side(b, p).start()

    def kv_two(b):
        total(rk1.at[b], p1r.at[b])
        fk[b] = (pk[b, 2 * (1 - par) + core].astype(F32) + rk1[b, 1 - par].astype(F32)).astype(BF)
        hk[b] = pk[b, 2 * par + core].astype(F32) + rk1[b, par].astype(F32)
        to_far2(b).start()

    def kv_three(b):
        to_far2(b).wait_recv()
        t = hk[b] + rk2[b].astype(F32)
        low = lax.broadcasted_iota(jnp.int32, t.shape, 1) < 2 * kn
        kvt[b, :blk, :] = jnp.where(low, t, 0.0).astype(BF)
        kvt[b, blk:, :] = jnp.where(low, pltpu.roll(t, 2 * kn, 1), 0.0).astype(BF)

    def fold(b, tile):
        rows = span(tile * seq, seq)
        ids = tile * seq + lax.broadcasted_iota(jnp.int32, (seq, seq), 0)
        hot = jnp.where(ids == tok_seq[pl.ds(b, 1), :], 1.0, 0.0).astype(BF)
        d_rows[rows, :qn] += dotf(hot, gd[span(b * seq, seq), :])
        d_rows[rows, qn:] += dotf(hot, kvt[b])

    tiles = vocab // seq

    def run_unit(u):
        unit(u)

        @pl.when(lax.rem(u, heads) == heads - 1)
        def _():
            kv_one(u // heads)

        @pl.when((u >= heads) & (lax.rem(u, heads) == 1))
        def _():
            kv_two(u // heads - 1)

    def run_fold(f):
        b, tile = f // tiles, lax.rem(f, tiles)

        @pl.when(tile == 0)
        def _():
            kv_three(b)
        fold(b, tile)

    def share(e, first, n, over):
        return jnp.minimum((jnp.maximum(e - first, 0) * n) // over, n)

    def paced(e, first, n, over, f):
        each(share(e, first, n, over), share(e + 1, first, n, over), f)

    def settle(t):
        rows = span(t * vrows, vrows)
        qt[rows, :] = d_rows[rows, :qn].astype(BF)
        kvrow[rows, :] = d_rows[rows, qn:].astype(BF)

    def step_row(k, dr):
        return pl.multiple_of(vrows * lax.rem(z + nz - 1 - k if dr == 0 else k + nz - 1 - z, nz) + 2 * sub_rows * dr, 2 * sub_rows)

    def swap(k, dr, kk):
        src = pl.multiple_of(vrows * (2 * k + 1 - core) + 2 * sub_rows * dr, 2 * sub_rows)
        return rdma((qt, kvrow)[kk].at[pl.ds(src, 2 * sub_rows)], (sq, skv)[kk].at[pl.ds(step_row(k, dr), 2 * sub_rows)], qs.at[0, kk], qs.at[1, kk], sib)

    def gather_h(k):
        for dr in both:
            src = pl.multiple_of(vrows * (2 * k + core) + 2 * sub_rows * dr, 2 * sub_rows)
            dst = pl.ds(step_row(k, dr), 2 * sub_rows)
            o_sib[dst, :] = qt[pl.ds(src, 2 * sub_rows), :]
            kvc[dst, :] = (kvrow[pl.ds(src, 2 * sub_rows), :].astype(F32) + pltpu.roll(skv[dst, :].astype(F32), 2 * kn, 1)).astype(BF)

    hrows = vhalf // 2

    def hstage(j):
        return d_rows.at[pl.ds(pl.multiple_of(vhalf + lax.rem(j, 2) * hrows, hrows), hrows), pl.ds(0, bw)]

    def hstore(j):
        return pltpu.make_async_copy(hstage(j), ph_out.at[span((j // events) * hrows, hrows), span(lax.rem(j, events) * bw, bw)], pt_sem.at[lax.rem(j, 2)])

    def hblock(j):
        @pl.when(lax.rem(j, events) >= 2)
        def _():
            hstore(j - 2).wait()
        rows = span((j // events) * hrows, hrows)
        cols = span(lax.rem(j, events) * bw, bw)
        hstage(j)[...] = dotf(o_sib[rows, :], wpair[:qn, cols]) + dotf(sq[rows, :], wpair[qn:2 * qn, cols]) + dotf(kvc[rows, :], wpair[2 * qn:2 * qn + 4 * kn, cols])
        hstore(j).start()

    def final_y(dr, sub, acc):
        rows = span((2 * dr + sub) * pos, pos)
        y_v[rows, :] = (y_v[rows, :].astype(F32) + acc).astype(BF)

    def step_c(e):
        with jax.named_scope('c_first'):
            @pl.when(e == events - 2)
            def _():
                first_sends(1)

        with jax.named_scope('c_serve'):
            @pl.when(e >= 2)
            def _():
                serve(0, e, final_y)

        @pl.when(e == 0)
        def _():
            total(gown, b_s.at[0])
            total(gown, b_s.at[2])
            total(wqts_out, wq_r.at[0])
            total(wpair.at[pl.ds(0, qn)], w_s.at[0])
            for c in ld2:
                c.start()
            d_rows[...] = jnp.zeros_like(d_rows)
            gn[...] = jnp.zeros_like(gn)
            qga[...] = jnp.zeros_like(qga)
            kga[...] = jnp.zeros_like(kga)

        with jax.named_scope('c_unit'):
            paced(e, 2, units, 6, run_unit)

        with jax.named_scope('c_kv2'):
            @pl.when(e == 8)
            def _():
                kv_two(batch - 1)
        with jax.named_scope('c_fold'):
            paced(e, 8, batch * tiles, 3, run_fold)

        with jax.named_scope('c_settle'):
            @pl.when(e == 10)
            def _():
                each(0, 2 * nz, settle)
                each(0, nz, lambda k: [swap(k, dr, kk).start() for dr in both for kk in both])

        with jax.named_scope('c_swap'):
            @pl.when(e == 11)
            def _():
                for c in ld2:
                    c.wait()
                total(sq, qs.at[1, 0])
                total(skv, qs.at[1, 1])
                each(0, nz, gather_h)
        with jax.named_scope('c_part'):
            paced(e, 11, events, 2, hblock)

        @pl.when(e == 12)
        def _():
            for j in (events - 2, events - 1):
                hstore(j).wait()
            first_fetch(1)

    each(0, events, step_c)

    def gblk(j):
        return qr.at[:, span(lax.rem(j, 2) * bw, bw)]

    def hblk(j):
        return gd.at[:, span(lax.rem(j, 2) * bw, bw)]

    def swo(j):
        return d_rows.at[pl.ds(0, qn), span(lax.rem(j, 2) * bw, bw)]

    def swq(j):
        return d_rows.at[pl.ds(pl.multiple_of(qn + lax.rem(j, 2) * bw, bw), bw), pl.ds(0, qn)]

    def g_load(j):
        return pltpu.make_async_copy(gy_out.at[:, span(j * bw, bw)], gblk(j), gls.at[lax.rem(j, 2)])

    def h_load(j):
        return pltpu.make_async_copy(hid.at[:, span(j * bw, bw)], hblk(j), hls.at[lax.rem(j, 2)])

    def wo_store(j):
        return pltpu.make_async_copy(swo(j), gwo_hbm.at[:, span(j * bw, bw)], swos.at[lax.rem(j, 2)])

    def wq_store(j):
        return pltpu.make_async_copy(swq(j), gq_hbm.at[span(j * bw, bw)], swqs.at[lax.rem(j, 2)])

    def block(j):
        g_load(j).wait()
        h_load(j).wait()

        @pl.when(j + 1 < events)
        def _():
            g_load(j + 1).start()
            h_load(j + 1).start()

        @pl.when(j >= 2)
        def _():
            wo_store(j - 2).wait()
            wq_store(j - 2).wait()
        cols = span(j * bw, bw)
        swo(j)[...] = dotf(o_own[...], gblk(j)[...], TN)
        ge_v[:, cols] = dotf(hotm[...], gblk(j)[...])
        wo_store(j).start()
        swq(j)[...] = dotf(hblk(j)[...], qt[...], TN)
        gkv_v[:, cols] = dotf(kvrow[...], hblk(j)[...], TN)[:2 * kn]
        wq_store(j).start()

    def final_h(dr, sub, gh):
        rows = span((2 * dr + sub) * sub_rows, sub_rows)
        x = gown[rows, :].astype(F32)
        r = lax.rsqrt(jnp.mean(x * x, axis=-1, keepdims=True) + EPS)
        ge_v[rows, :] += rms_pull(x, gh * gain[...], r)

    outs = [pltpu.make_async_copy(s, t, out_sem.at[i]) for i, (s, t) in enumerate((
        (y_v, y_hbm), (gkv_v.at[pl.ds(0, kn)], gk_hbm), (gkv_v.at[pl.ds(kn, kn)], gv_hbm), (ge_v, ge_hbm)))]
    g_load(0).start()
    h_load(0).start()
    outs[0].start()
    work_d = events - 3

    wide = gn_out.shape[1]
    gtop = d // wide
    mrow = gtop // 2

    def to_sib(t):
        if t:
            return rdma(gfin.at[core], gfin.at[core], gs.at[4], gs.at[5], sib)
        return rdma(gmine.at[1 - core], gsib, gs.at[0], gs.at[1], sib)

    def to_col(k):
        return rdma(gcol.at[z], gcol.at[z], gs.at[2], gs.at[3], 2 * lax.rem(z + k, nz) + core)

    def step_d(e):
        with jax.named_scope('d_serve'):
            @pl.when(e >= 2)
            def _():
                serve(1, e, final_h)

        @pl.when(e == 0)
        def _():
            for k in both:
                for c in item(k):
                    c.start()

        with jax.named_scope('d_part'):
            paced(e, 0, events, 5, lambda j: hblock(j + events))

        @pl.when(e == 5)
        def _():
            for j in (events - 2, events - 1):
                hstore(j + events).wait()
        with jax.named_scope('d_gain'):
            paced(e, 2, events, 8, gain_part)
        with jax.named_scope('d_block'):
            paced(e, 1, events, work_d - 1, block)

        @pl.when(e == 10)
        def _():
            whole = jnp.sum(gn[...], axis=0, keepdims=True)
            for k, extra in ((0, qga), (1, kga)):
                for j in range(mrow):
                    c0 = (k * mrow + j) * wide
                    gmine[k, j:j + 1, :] = whole[:, c0:c0 + wide].astype(BF)
                gmine[k, mrow:mrow + 1, :] = extra[...].astype(BF)
            to_sib(0).start()

        @pl.when(e == 11)
        def _():
            total(gsib, gs.at[1])
            gcol[z] = (gmine[core].astype(F32) + gsib[...].astype(F32)).astype(BF)
            for k in range(1, nz):
                to_col(k).start()

        @pl.when(e == 13)
        def _():
            total(gcol.at[pl.ds(0, nz - 1)], gs.at[3])
            gfin[core] = sum(gcol[k].astype(F32) for k in range(nz))
            to_sib(1).start()

        @pl.when(e == events - 3)
        def _():
            outs[1].start()
            outs[2].start()

    each(0, events, step_d)

    outs[3].start()
    for ph in both:
        for k in range(4):
            arrived(rs.at[ph, k])

    total(gy_out.at[pl.ds(0, 2 * (events - 4) * pos)], b_s.at[1])
    total(gy_out.at[pl.ds(0, 2 * (events - 2) * pos)], b_s.at[3])
    to_far.wait_send()
    relay.wait_send()
    total(wpair.at[pl.ds(2 * qn, 2 * kn)], w_s.at[2])
    total(o_sib, o_s.at[0])
    total(pk.at[pl.ds(0, batch // 2)], p1s.at[0])
    total(fk, p2s.at[0])
    total(sq, qs.at[0, 0])
    total(skv, qs.at[0, 1])
    with jax.named_scope('gain_wait'):
        total(gfin.at[0], gs.at[5])
    gn_out[0:mrow, :] = gfin[0, 0:mrow, :]
    gn_out[mrow:, :] = gfin[1, 0:mrow, :]
    gqg_out[...] = gfin[0, mrow:mrow + 1, :]
    gkg_out[...] = gfin[1, mrow:mrow + 1, :]
    total(gsib, gs.at[0])
    total(gcol.at[pl.ds(0, nz - 1)], gs.at[2])
    total(gfin.at[0], gs.at[4])
    for j in (events - 2, events - 1):
        wo_store(j).wait()
        wq_store(j).wait()
    with jax.named_scope('t_outs'):
        for c in outs:
            c.wait()


def step_kernel(nz, embed, gy, wq, wk_t, wv_t, wo, gain, qg, kg, cos, sin_s, tok_seq):
    vrows, d = embed.shape
    vocab = vrows * 2 * nz
    qn, kn = wq.shape[1], wk_t.shape[0]
    hd = qg.shape[1]
    batch, seq = tok_seq.shape
    toks = batch * seq
    ev = 2 * nz
    sr, hb, vh = vrows // 4, seq // 2, vocab // 2
    mr = (d // hd // 2 + 1 + 15) // 16 * 16
    dma = pltpu.SemaphoreType.DMA
    v = pltpu.VMEM

    def arr(dt, *shape):
        return jax.ShapeDtypeStruct(shape, dt)

    outs = (arr(BF, vrows, d), arr(F32, vrows, d), arr(F32, d, qn), arr(F32, kn, d), arr(F32, kn, d), arr(F32, qn, d), arr(F32, d // hd, hd), arr(F32, 1, hd), arr(F32, 1, hd), arr(BF, vh, d),
            arr(BF, vocab, d), arr(BF, toks, d), arr(BF, qn, d), arr(BF, qn, d), arr(F32, vh, d), arr(F32, vh, d))
    return pl.pallas_call(
        functools.partial(body, nz),
        name='step_kernel',
        out_shape=outs,
        in_specs=[ANY] * 6 + [VM] * 6,
        out_specs=(ANY,) * 6 + (VM,) * 3 + (ANY,) * 7,
        scratch_shapes=[v((vocab, d), BF), v((2 * qn + 4 * kn, d), BF), v((max(d, 2 * toks), qn), BF), v((vocab, qn), BF), v((toks, qn), BF), v((vh, qn), BF), v((vh, qn), BF),
                        v((toks, 2 * hd), BF), v((toks, hd), BF), v((2, toks // 2, 4 * kn), BF), v((2, toks // 2, 4 * kn), BF), v((vocab, 4 * kn), BF), v((vh, 4 * kn), BF), v((vh, 4 * kn), BF),
                        v((vocab, qn + 4 * kn), F32), v((4, 2, sr, d), F32), v((2, vrows, d), BF), v((vrows, d), BF), v((vrows, toks), BF),
                        v((seq, hd), F32), v((seq, hd), F32), v((batch, 4, hb, 4 * kn), BF), v((batch, 2, hb, 4 * kn), BF), v((batch, hb, 4 * kn), BF), v((batch, hb, 4 * kn), F32),
                        v((batch, hb, 4 * kn), BF), v((batch, seq, 4 * kn), BF), v((8, d), F32), v((1, hd), F32), v((1, hd), F32), v((2, mr, hd), BF), v((mr, hd), BF), v((nz, mr, hd), BF), v((2, mr, hd), F32), v((vrows, d), BF), v((vrows, d), F32), v((2 * kn, d), F32),
                        dma((12,)), dma((2,)), dma((1,)), dma((ev,)), dma((ev,)), dma((2,)), dma((4,)), dma((2,)), dma((2,)), dma((2, 2)), dma((1,)), dma((4,)), dma((2,)),
                        dma((2,)), dma((2, 2)), dma((2, 4)), dma((1,)), dma((batch,)), dma((1,)), dma((batch,)), dma((2, 2)),
                        dma((2,)), dma((2,)), dma((2,)), dma((2,)), dma((6,)), dma((4,)), dma((3,))],
        compiler_params=pltpu.CompilerParams(collective_id=0, has_side_effects=True, vmem_limit_bytes=67043328),
        cost_estimate=pl.CostEstimate(flops=2 * vocab * d * 8 * qn, bytes_accessed=20 * vocab * d, transcendentals=0),
    )(embed, gy, wq, wk_t, wv_t, wo, gain, qg, kg, cos, sin_s, tok_seq)


def emit_body(cuts, *refs):
    n = len(cuts)
    src, dst = refs[:n], refs[n:2 * n]
    bufs, s_in, s_out = refs[2 * n:-2], refs[-2], refs[-1]
    ins, outs = [], []
    for i, c in enumerate(cuts):
        step = src[i].shape[0] // c
        for j in range(c):
            b = bufs[i].at[pl.ds(j * step, step)]
            ins.append(pltpu.make_async_copy(src[i].at[pl.ds(j * step, step)], b, s_in.at[len(ins)]))
            outs.append(pltpu.make_async_copy(b, dst[i].at[pl.ds(j * step, step)], s_out.at[len(outs)]))
    for c in ins:
        c.start()
    for a, b in zip(ins, outs):
        a.wait()
        b.start()
    for b in outs:
        b.wait()


def emit(*arrays):
    size = 1 << 20
    cuts = tuple(max(1, a.size * a.dtype.itemsize // size) for a in arrays)
    return pl.pallas_call(
        functools.partial(emit_body, cuts),
        name='emit',
        out_shape=tuple(jax.ShapeDtypeStruct(a.shape, a.dtype) for a in arrays),
        in_specs=[ANY] * len(arrays),
        out_specs=(ANY,) * len(arrays),
        scratch_shapes=[pltpu.VMEM(a.shape, a.dtype) for a in arrays] + [pltpu.SemaphoreType.DMA((sum(cuts),))] * 2,
        compiler_params=pltpu.CompilerParams(vmem_limit_bytes=60 * 1024 * 1024),
        cost_estimate=pl.CostEstimate(flops=0, bytes_accessed=2 * sum(a.size * a.dtype.itemsize for a in arrays), transcendentals=0),
    )(*arrays)


def rope_consts(seq, hd):
    inv = np.float32(ROPE_BASE) ** (np.float32(-2.0) * np.arange(hd // 2, dtype=np.float32) / np.float32(hd))
    ang = np.arange(seq, dtype=np.float32)[:, None] * inv.astype(np.float32)[None, :]
    ang = np.concatenate([ang, ang], axis=-1)
    sign = np.where(np.arange(hd) < hd // 2, -1.0, 1.0).astype(np.float32)
    return np.cos(ang).astype(np.float32), (np.sin(ang) * sign).astype(np.float32)


def solution(mesh):
    tp = mesh.shape['tp']
    nz = tp // 2

    def local_step(tok_ids, embed_loc, norm_gain, q_gain, k_gain, wq, wk, wv, wo, gy_loc):
        d_model = embed_loc.shape[1]
        batch, seq = tok_ids.shape
        seq_dev = seq // tp
        hd = q_gain.shape[0]
        cos_c, sin_c = (jnp.asarray(t) for t in rope_consts(seq, hd))
        r = step_kernel(nz, embed_loc, gy_loc.reshape(batch * seq_dev, d_model), wq, wk.T, wv.T, wo, norm_gain[None, :], q_gain[None, :], k_gain[None, :], cos_c, sin_c, tok_ids)
        y, g_embed, g_wq, g_wk, g_wv, g_wo, g_n, g_q, g_k = emit(*r[:9])
        return (y.reshape(batch, seq_dev, d_model), g_embed, g_n.reshape(d_model), g_q.reshape(hd), g_k.reshape(hd), g_wq, g_wk.T, g_wv.T, g_wo)

    in_specs = (P('dp', None), P('tp', None), P(), P(), P(), P(None, 'tp'), P(None, 'tp'), P(None, 'tp'), P('tp', None), P('dp', 'tp', None))
    out_specs = (P('dp', 'tp', None), P(('dp', 'tp'), None), P('dp'), P('dp'), P('dp'), P('dp', 'tp'), P('dp', 'tp'), P('dp', 'tp'), P(('dp', 'tp'), None))
    return jax.shard_map(local_step, mesh=mesh, in_specs=in_specs, out_specs=out_specs, check_vma=False)
```

```python
import functools
import jax
import jax.numpy as jnp
import numpy as np
from jax import lax
from jax.experimental import pallas as pl
from jax.experimental.pallas import tpu as pltpu
from jax.sharding import PartitionSpec as P

BF = jnp.bfloat16
F32 = jnp.float32
EPS = 1.0e-6
ROPE_BASE = 1.0e6
NEG_BIG = -1.0e30
LOG2E = 1.4426950408889634
MESH = pl.DeviceIdType.MESH
ANY = pl.BlockSpec(memory_space=pl.ANY)
VM = pl.BlockSpec(memory_space=pltpu.VMEM)
NT = (((1,), (1,)), ((), ()))
NN = (((1,), (0,)), ((), ()))
TN = (((0,), (0,)), ((), ()))


def dotf(a, b, dims=NN):
    return lax.dot_general(a, b, dims, preferred_element_type=F32)


def rdma(src, dst, ssem, rsem, dev):
    return pltpu.make_async_remote_copy(src_ref=src, dst_ref=dst, send_sem=ssem, recv_sem=rsem, device_id={'tp': dev}, device_id_type=MESH)


def span(start, size):
    return pl.ds(pl.multiple_of(start, size), size)


def each(lo, hi, f):
    def go(j, _):
        f(j)
        return 0
    lax.fori_loop(lo, hi, go, 0)


def total(ref, sem):
    pltpu.make_async_copy(ref, ref, sem).wait()


def rms_f32(x, gain):
    return x * lax.rsqrt(jnp.mean(x * x, axis=-1, keepdims=True) + EPS) * gain


def rms_pull(x, dxr, r):
    return r * dxr - x * (r * r * r * jnp.mean(x * dxr, axis=-1, keepdims=True))


def causal_blocks(q, keys, i, blk):
    r_i = lax.broadcasted_iota(jnp.int32, (blk, blk), 0)
    c_i = lax.broadcasted_iota(jnp.int32, (blk, blk), 1)
    s = [dotf(q, keys[j * blk:(j + 1) * blk], NT) for j in range(i + 1)]
    s[i] = jnp.where(r_i >= c_i, s[i], NEG_BIG)
    top = functools.reduce(jnp.maximum, [jnp.max(t, axis=-1, keepdims=True) for t in s])
    c = q.shape[-1] ** -0.5 * LOG2E
    e = [jnp.exp2((t - top) * c) for t in s]
    inv = 1.0 / sum(jnp.sum(t, axis=-1, keepdims=True) for t in e)
    return [t * inv for t in e]


def body(nz, embed, gy, wq, wk_t, wv_t, wo, gain, qg, kg, cos, sin_s, tok_seq,
         y_hbm, ge_hbm, gq_hbm, gk_hbm, gv_hbm, gwo_hbm, gn_out, gqg_out, gkg_out, erows, hid, gy_out, wqt_out, wqts_out, py_out, ph_out,
         table, wpair, wq_v, qt, o_own, o_sib, sq, kv_tok, k_rot, kvacc, farkv, kvrow, skv, kvc, d_rows, pbuf, hbuf, gown, hotm,
         dk_acc, dv_acc, pk, rk1, fk, hk, rk2, kvt, gn, qga, kga, gmine, gsib, gcol, gfin, y_v, ge_v, gkv_v,
         in_sem, h_sem, g_sem, r_sem, s_sem, a_s, b_s, xs, xr, wq_s, wq_r, w_s, o_s, pt_sem, pl_sem, rs, p1s, p1r, p2s, p2r, qs, gls, hls, swos, swqs, gs, out_sem, e_sem):
    rank = lax.axis_index('tp')
    z, core = rank // 2, lax.rem(rank, 2)
    right = 2 * lax.rem(z + 1, nz) + core
    left = 2 * lax.rem(z + nz - 1, nz) + core
    sib = rank + 1 - 2 * core
    par = lax.rem(z, 2)
    far = rank + 2 - 4 * par
    vrows, d = embed.shape
    kn = wk_t.shape[0]
    sub_rows = vrows // 4
    vocab = vrows * 2 * nz
    vhalf = vocab // 2
    batch, seq = tok_seq.shape
    toks = batch * seq
    qn = wq.shape[1]
    hd = qg.shape[1]
    heads = qn // hd
    events = 2 * nz
    pos = seq // events
    blk = seq // 2
    bw = d // events
    scale = hd ** -0.5
    units = batch * heads
    parts = 8
    wo_p, wq_p = qn // parts, d // parts
    both = (0, 1)
    places = [(dr, c) for dr in both for c in both]
    qr = wq_v.at[pl.ds(0, toks)]
    gd = wq_v.at[pl.ds(toks, toks)]
    w_q = wq_v.at[pl.ds(0, d)]

    ld = [pltpu.make_async_copy(s, t, in_sem.at[i]) for i, (s, t) in enumerate((
        (embed, table.at[span(rank * vrows, vrows)]), (gy, gown), (wq, w_q), (wo, wpair.at[pl.ds(0, qn)]),
        (wk_t, wpair.at[pl.ds(2 * qn, kn)]), (wv_t, wpair.at[pl.ds(2 * qn + kn, kn)])))]
    ld2 = [pltpu.make_async_copy(s, t, in_sem.at[i]) for i, (s, t) in enumerate((
        (wqt_out, wpair.at[pl.ds(0, qn)]), (wqts_out, wpair.at[pl.ds(qn, qn)]), (embed, gown)))]
    ld[0].start()
    barrier = pltpu.get_barrier_semaphore()
    for dev in (right, left, sib):
        pl.semaphore_signal(barrier, inc=1, device_id={'tp': dev}, device_id_type=MESH)
    with jax.named_scope('hbar'):
        pl.semaphore_wait(barrier, 3)
    with jax.named_scope('hload'):
        ld[0].wait()

    def nbr(dr):
        return right if dr == 0 else left

    def arrived(sem):
        total(table.at[pl.ds(0, 2 * sub_rows)], sem)

    def zd_of(dr, e):
        s = e // 2
        return lax.rem(z + (nz - s if dr == 0 else s), nz)

    def row_of(dr, e, c):
        return pl.multiple_of(vrows * (2 * zd_of(dr, e) + c) + sub_rows * (2 * dr + lax.rem(e, 2)), sub_rows)

    def ring(dr, e, recv_e):
        a = table.at[pl.ds(row_of(dr, e, core), sub_rows)]
        return rdma(a, a, a_s.at[0], r_sem.at[recv_e], nbr(dr))

    def side(dr, e):
        a = table.at[pl.ds(row_of(dr, e, core), sub_rows)]
        return rdma(a, a, a_s.at[1], s_sem.at[e], sib)

    def e_keep(dr, e):
        dst = pl.multiple_of(vrows * lax.rem(e // 2 + nz - 1, nz) + sub_rows * (2 * dr + lax.rem(e, 2)), sub_rows)
        return pltpu.make_async_copy(table.at[pl.ds(row_of(dr, e, core), sub_rows)], erows.at[pl.ds(dst, sub_rows)], e_sem.at[0])

    def h_copy(slot, i, row):
        return pltpu.make_async_copy(hbuf.at[slot, pl.ds(i * sub_rows, sub_rows)], hid.at[pl.ds(row, sub_rows)], h_sem.at[slot])

    quarters = range(4)
    hp = pos // 2

    def way(k, sub, flip):
        if k == 1:
            return sub * flip
        if k == 3:
            return 1 - sub * (1 - flip)
        return k // 2

    def toward(turn):
        return right + turn * (left - right)

    def g_way(k, e):
        return way(k, lax.rem(e, 2), 1 - lax.rem(z + e // 2, 2))

    def g_row(k, e, c):
        turn, sub, s = g_way(k, e), lax.rem(e, 2), e // 2
        zd = lax.rem(z + turn * s + (1 - turn) * (nz - s), nz)
        return pl.multiple_of(seq * (2 * (k // 2) + sub) + pos * (2 * zd + c) + hp * (k % 2), hp)

    def g_piece(k, e, c):
        return gy_out.at[pl.ds(g_row(k, e, c), hp)]

    def g_own(k, e):
        return gown.at[pl.ds(pl.multiple_of(pos * (2 * (k // 2) + lax.rem(e, 2)) + hp * (k % 2), hp), hp)]

    def g_ring(k, e, recv_e, first):
        a = g_piece(k, e, core)
        return rdma(g_own(k, e) if first else a, a, b_s.at[0 if first else 1], r_sem.at[recv_e], toward(g_way(k, e)))

    def g_side(k, e, first):
        a = g_piece(k, e, core)
        return rdma(g_own(k, e) if first else a, a, b_s.at[2 if first else 3], s_sem.at[e], sib)

    def g_home(dr, e):
        dst = pl.multiple_of(seq * (2 * dr + e) + pos * rank, pos)
        return pltpu.make_async_copy(gown.at[pl.ds(pos * (2 * dr + e), pos)], gy_out.at[pl.ds(dst, pos)], in_sem.at[8 + 2 * dr + e])

    def g_fetch(slot, k, c, e):
        return pltpu.make_async_copy(g_piece(k, e, c), hbuf.at[slot, pl.ds((2 * k + c) * hp, hp)], g_sem.at[0])

    def wo_push(k):
        return rdma(wpair.at[span(k * wo_p, wo_p)], wpair.at[pl.ds(pl.multiple_of(qn + k * wo_p, wo_p), wo_p)], w_s.at[0], w_s.at[1], sib)

    def tb(k):
        return o_own.at[span(lax.rem(k, 2) * qn, qn), pl.ds(0, wq_p)]

    def wq_push(k):
        return rdma(tb(k), wqts_out.at[:, span(k * wq_p, wq_p)], wq_s.at[0, lax.rem(k, 2)], wq_r.at[0], sib)

    def wq_home(k):
        return pltpu.make_async_copy(tb(k), wqt_out.at[:, span(k * wq_p, wq_p)], wq_s.at[1, lax.rem(k, 2)])

    def wk_push(k):
        return rdma((wk_t, wv_t)[k], wpair.at[pl.ds(2 * qn + (2 + k) * kn, kn)], w_s.at[2], w_s.at[3], sib)

    def o_push(b, k):
        src = pl.multiple_of(b * seq + pos * (2 * k + 1 - core), pos)
        dst = pl.multiple_of(vrows * k + pos * b, pos)
        return rdma(o_own.at[pl.ds(src, pos)], o_sib.at[pl.ds(dst, pos)], o_s.at[0], o_s.at[1], sib)

    def project(e):
        slot = lax.rem(e, 2)

        @pl.when(e >= 2)
        def _():
            total(hbuf.at[slot], h_sem.at[slot])

        rows = [row_of(dr, e, c) for dr, c in places]
        for i, row in enumerate(rows):
            x = table[pl.ds(row, sub_rows), :].astype(F32)
            ids = row + lax.broadcasted_iota(jnp.int32, (sub_rows, seq), 0)
            hit = jnp.zeros((sub_rows, seq), F32)
            for b in range(batch):
                hit = jnp.maximum(hit, jnp.where(tok_seq[b:b + 1, :] == ids, 1.0, 0.0))
            used = jnp.max(hit, axis=1, keepdims=True)
            h = jnp.where(used > 0.5, rms_f32(x, gain[...]), 0.0)
            hbuf[slot, pl.ds(i * sub_rows, sub_rows), :] = h.astype(BF)
            h_copy(slot, i, row).start()
        hb = hbuf[slot]
        qkv = jnp.concatenate([dotf(hb, w_q[...]).astype(BF), dotf(hb, wpair[2 * qn:2 * qn + 4 * kn, :], NT).astype(BF)], axis=1)
        lane = lax.broadcasted_iota(jnp.int32, (1, vrows), 1)
        rowid = jnp.zeros((1, vrows), jnp.int32)
        for i, row in enumerate(rows):
            rowid = jnp.where(lane // sub_rows == i, row + lane - i * sub_rows, rowid)
        rowid = rowid.astype(F32)
        for b in range(batch):
            sl = slice(b * seq, (b + 1) * seq)
            hot = jnp.where(d_rows[sl, :vrows] == rowid, 1.0, 0.0).astype(BF)
            got = dotf(hot, qkv)
            qt[sl, :] = (qt[sl, :].astype(F32) + got[:, :qn]).astype(BF)
            at = slice((b % 2) * seq, (b % 2 + 1) * seq)
            kvacc[b // 2, at, :] = (kvacc[b // 2, at, :].astype(F32) + got[:, qn:]).astype(BF)

    def step_a(e):
        with jax.named_scope('a_wait'):
            @pl.when((e >= 2) & (e < events))
            def _():
                arrived(r_sem.at[e])

            @pl.when(e < events - 2)
            def _():
                for dr in both:
                    ring(dr, e, e + 2).start()

        @pl.when(e < events)
        def _():
            for dr in both:
                side(dr, e).start()
                e_keep(dr, e).start()

        @pl.when(e == 0)
        def _():
            for c in ld[1:]:
                c.start()
            for k in both:
                wk_push(k).start()
            for b in range(batch):
                wide = jnp.broadcast_to(tok_seq[b:b + 1, :].astype(F32), (vrows, seq))
                d_rows[b * seq:(b + 1) * seq, :vrows] = wide.T
            qt[...] = jnp.zeros_like(qt)
            kvacc[...] = jnp.zeros_like(kvacc)

        @pl.when(e == 1)
        def _():
            for c in ld[1:]:
                c.wait()
            total(wpair.at[pl.ds(2 * qn, 2 * kn)], w_s.at[3])
            for dr in both:
                for k in both:
                    g_home(dr, k).start()

        @pl.when(e == events - 2)
        def _():
            for k in quarters:
                g_ring(k, 0, 2, True).start()

        @pl.when((e >= 2) & (e < 4 + parts))
        def _():
            @pl.when(e >= 4)
            def _():
                wq_push(e - 4).wait_send()
                wq_home(e - 4).wait()

            @pl.when(e < 2 + parts)
            def _():
                k = e - 2
                block = wq_v[span(k * wq_p, wq_p), :]
                tb(k)[...] = block.astype(F32).T.astype(BF)
                wo_push(k).start()
                wq_push(k).start()
                wq_home(k).start()

        with jax.named_scope('a_proj'):
            @pl.when(e >= 1)
            def _():
                arrived(s_sem.at[e - 1])
                project(e - 1)

    each(0, events + 1, step_a)

    to_far = rdma(kvacc.at[core], farkv.at[core], xs.at[0], xr.at[0], far)
    relay = rdma(farkv.at[core], farkv.at[core], xs.at[1], xr.at[1], sib)
    at_i = lax.broadcasted_iota(jnp.int32, (pos, seq), 1) - pos * rank
    own_i = lax.broadcasted_iota(jnp.int32, (pos, seq), 0)
    col = jnp.concatenate([jnp.sum(jnp.where(at_i == own_i, tok_seq[b:b + 1, :].astype(F32), 0.0), axis=1, keepdims=True) for b in range(batch)], axis=0).astype(jnp.int32)
    lanes = lax.broadcasted_iota(jnp.int32, (vrows, vrows), 1)
    hot_mine = jnp.concatenate([jnp.where(col == lanes + j * vrows, 1.0, 0.0).astype(BF) for j in range(vocab // vrows)], axis=1)
    to_far.start()
    for k in quarters:
        g_ring(k, 1, 3, True).start()
    for k in quarters:
        for e in both:
            g_side(k, e, True).start()
    for dr in both:
        for e in both:
            g_home(dr, e).wait()
    cw = min(512, d)

    def own_rows(j):
        y_v[:, span(j * cw, cw)] = dotf(hot_mine, table[:, span(j * cw, cw)]).astype(BF)

    each(0, d // cw, own_rows)
    for b in range(batch):
        ids = rank * vrows + lax.broadcasted_iota(jnp.int32, (vrows, seq), 0)
        hotm[:, b * seq:(b + 1) * seq] = jnp.where(ids == tok_seq[b:b + 1, :], 1.0, 0.0).astype(BF)

    def place(p, first):
        l_i = lax.broadcasted_iota(jnp.int32, (4 * kn, 2 * hd), 0)
        m_i = lax.broadcasted_iota(jnp.int32, (4 * kn, 2 * hd), 1)
        upper = jnp.where(l_i >= 2 * kn, 1, 0)
        owner = jnp.where(upper == 1, 1 - first, first)
        l_i = l_i - 2 * kn * upper
        base = kn * (2 * p + owner)
        want = jnp.where(l_i < kn, base + l_i, hd + base + l_i - kn)
        return jnp.where(m_i == want, 1.0, 0.0).astype(BF)

    def rope(raw, g):
        n = rms_f32(raw.astype(F32), g)
        return (n * cos[...] + pltpu.roll(n, hd // 2, 1) * sin_s[...]).astype(BF)

    def attend(u):
        base = (u // heads) * seq
        rows = span(base, seq)
        cols = span(lax.rem(u, heads) * hd, hd)
        q = rope(qt[rows, cols], qg[...])
        qr[rows, cols] = q
        kr = k_rot[rows, :]
        v = kv_tok[rows, hd:]
        for i in both:
            p = causal_blocks(q[i * blk:(i + 1) * blk], kr, i, blk)
            o = sum(dotf(t.astype(BF), v[j * blk:(j + 1) * blk]) for j, t in enumerate(p))
            o_own[pl.ds(pl.multiple_of(base + i * blk, blk), blk), cols] = o.astype(BF)

    def grad_attend(e):
        total(hbuf, g_sem.at[0])
        r = dotf(hbuf[...].reshape(2 * vrows, d), wpair[:qn, :], NT).astype(BF)
        for i in both:
            for k in quarters:
                for c in both:
                    n = (8 * i + 2 * k + c) * hp
                    gd[pl.ds(g_row(k, e + i, c), hp), :] = r[n:n + hp]

    def pstage(j):
        return d_rows.at[span(lax.rem(j, 2) * vhalf, vhalf), pl.ds(0, bw)]

    def pstore(dst, j):
        return pltpu.make_async_copy(pstage(j), dst.at[:, span(j * bw, bw)], pt_sem.at[lax.rem(j, 2)])

    def pblock(dst, j, pairs):
        @pl.when(j >= 2)
        def _():
            pstore(dst, j - 2).wait()
        cols = span(j * bw, bw)
        acc = None
        for a, lo, n in pairs:
            t = dotf(a[...], wpair[lo:lo + n, cols])
            acc = t if acc is None else acc + t
        pstage(j)[...] = acc
        pstore(dst, j).start()

    y_pairs = [(sq, 0, qn), (o_sib, qn, qn)]

    def pslot(ph, e, dr):
        return pbuf.at[2 * ph + lax.rem(e, 2), dr]

    hs = sub_rows // 2

    def c_way(k, e):
        return way(k, lax.rem(e, 2), lax.rem(z + 1 + e // 2, 2))

    def pfetch(ph, e, dr):
        s, sub = e // 2, lax.rem(e, 2)
        sem = pl_sem.at[ph, sub]
        if ph:
            row = pl.multiple_of(vrows * s + sub_rows * (2 * dr + sub), sub_rows)
            pltpu.make_async_copy(ph_out.at[pl.ds(row, sub_rows)], pslot(ph, e, dr), sem).start()
            return
        for k in (2 * dr, 2 * dr + 1):
            turn = c_way(k, e)
            zd = lax.rem(z + turn * (1 + s) + (1 - turn) * (2 * nz - 1 - s), nz)
            row = pl.multiple_of(vrows * zd + sub_rows * (2 * dr + sub) + hs * (k % 2), hs)
            pltpu.make_async_copy(py_out.at[pl.ds(row, hs)], pbuf.at[2 * ph + sub, dr, pl.ds(hs * (k % 2), hs)], sem).start()

    def item(i):
        row = vrows * (i // 2)
        cps = []
        for dr in both:
            at = pl.ds(pl.multiple_of(row + sub_rows * (2 * dr + lax.rem(i, 2)), sub_rows), sub_rows)
            cps.append(pltpu.make_async_copy(ph_out.at[at], pbuf.at[lax.rem(i, 2), dr], pl_sem.at[0, lax.rem(i, 2)]))
            cps.append(pltpu.make_async_copy(erows.at[at], hbuf.at[lax.rem(i, 2), pl.ds(dr * sub_rows, sub_rows)], e_sem.at[1 + lax.rem(i, 2)]))
        return cps

    def gain_part(i):
        total(pbuf.at[lax.rem(i, 2)], pl_sem.at[0, lax.rem(i, 2)])
        total(hbuf.at[lax.rem(i, 2), pl.ds(0, 2 * sub_rows)], e_sem.at[1 + lax.rem(i, 2)])
        for dr in both:
            x = hbuf[lax.rem(i, 2), dr * sub_rows:(dr + 1) * sub_rows, :].astype(F32)
            t = pbuf[lax.rem(i, 2), dr] * (x * lax.rsqrt(jnp.mean(x * x, axis=-1, keepdims=True) + EPS))
            gn[...] += sum(t[k:k + 8] for k in range(0, sub_rows, 8))

        @pl.when(i + 2 < events)
        def _():
            for c in item(i + 2):
                c.start()

    def fetched(ph, e):
        total(pbuf.at[2 * ph + lax.rem(e, 2)], pl_sem.at[ph, lax.rem(e, 2)])

    def rslot(dr, e):
        return table.at[span((dr * (events - 2) + e) * sub_rows, sub_rows)]

    def s_row(ph, dr, e):
        return (2 * (events - 2) + 8 * ph + 4 * lax.rem(e // 2, 2) + 2 * dr + lax.rem(e, 2)) * sub_rows

    def sslot(ph, dr, e):
        return table.at[pl.ds(pl.multiple_of(s_row(ph, dr, e), sub_rows), sub_rows)]

    def send(ph, dr, e):
        sems = rs.at[ph, lax.rem(e, 4)], r_sem.at[e + 2]
        if ph:
            rdma(sslot(ph, dr, e), rslot(dr, e), *sems, nbr(dr)).start()
            return
        for k in (2 * dr, 2 * dr + 1):
            a = pl.multiple_of(s_row(ph, dr, e) + hs * (k % 2), hs)
            b = pl.multiple_of((dr * (events - 2) + e) * sub_rows + hs * (k % 2), hs)
            rdma(table.at[pl.ds(a, hs)], table.at[pl.ds(b, hs)], *sems, toward(c_way(k, e))).start()

    def first_fetch(ph):
        for e in both:
            for dr in both:
                pfetch(ph, e, dr)

    def first_sends(ph):
        for e in both:
            fetched(ph, e)
            for dr in both:
                sslot(ph, dr, e)[...] = pslot(ph, e, dr)[...].astype(BF)
        for e in both:
            for dr in both:
                send(ph, dr, e)
                pfetch(ph, e + 2, dr)

    def serve(ph, e, final):
        arrived(r_sem.at[e])
        fetched(ph, e)

        @pl.when(e < events - 2)
        def _():
            @pl.when(e >= 4)
            def _():
                arrived(rs.at[ph, lax.rem(e, 4)])
            for dr in both:
                sslot(ph, dr, e)[...] = (pslot(ph, e, dr)[...] + rslot(dr, e - 2)[...].astype(F32)).astype(BF)
            for dr in both:
                send(ph, dr, e)
                pfetch(ph, e + 2, dr)

        @pl.when(e >= events - 2)
        def _():
            for dr in both:
                final(dr, lax.rem(e, 2), pslot(ph, e, dr)[...] + rslot(dr, e - 2)[...].astype(F32))

    slots = 9

    def gather_o(k):
        for b in range(batch):
            src = pl.multiple_of(b * seq + pos * (2 * k + core), pos)
            sq[pl.ds(pl.multiple_of(vrows * k + pos * b, pos), pos), :] = o_own[pl.ds(src, pos), :]

    def upto(e, n, over):
        return jnp.minimum((e * n) // over, n)

    def step_b(e):
        with jax.named_scope('b_first'):
            @pl.when(e == events - 2)
            def _():
                first_sends(0)

        @pl.when((e >= 2) & (e < events))
        def _():
            arrived(r_sem.at[e])

        @pl.when((e >= 2) & (e < events - 2))
        def _():
            for k in quarters:
                g_ring(k, e, e + 2, False).start()

        @pl.when((e >= 2) & (e < events))
        def _():
            for k in quarters:
                g_side(k, e, False).start()

        @pl.when((e >= 1) & (e <= events))
        def _():
            arrived(s_sem.at[e - 1])

        with jax.named_scope('kv_far'):
            @pl.when(e == 2)
            def _():
                to_far.wait_recv()
                relay.start()

        with jax.named_scope('kv_tok'):
            @pl.when(e == 3)
            def _():
                rdma(farkv.at[1 - core], farkv.at[1 - core], xs.at[1], xr.at[1], sib).wait_recv()
                for hf in both:
                    kv_tok[hf * (toks // 2):(hf + 1) * (toks // 2), :] = (dotf(kvacc[hf], place(par, core)) + dotf(farkv[hf], place(1 - par, hf))).astype(BF)
                for b in range(batch):
                    sl = slice(b * seq, (b + 1) * seq)
                    k_rot[sl, :] = rope(kv_tok[sl, :hd], kg[...])

            @pl.when((e >= 2) & (lax.rem(e, 2) == 0))
            def _():
                for i in both:
                    for k in quarters:
                        for c in both:
                            g_fetch(i, k, c, e - 2 + i).start()

        def give(b):
            each(0, nz, lambda k: o_push(b, k).start())

        def seen(t):
            return jnp.minimum((jnp.maximum(t - 3, 0) * units) // (slots - 3), units)

        each(seen(e - 1) // heads, seen(e) // heads, give)
        with jax.named_scope('b_attend'):
            each(seen(e), seen(e + 1), attend)

        @pl.when(e == 4)
        def _():
            total(table.at[pl.ds(0, 2 * (events - 2) * sub_rows)], a_s.at[0])
            total(table.at[pl.ds(0, 2 * events * sub_rows)], a_s.at[1])
            total(erows, e_sem.at[0])

        @pl.when(e == slots + 1)
        def _():
            total(wpair.at[pl.ds(0, qn)], w_s.at[1])
            total(o_sib, o_s.at[1])
            each(0, nz, gather_o)

        with jax.named_scope('b_part'):
            @pl.when((e > slots) & (e <= slots + 4))
            def _():
                each(4 * (e - slots - 1), 4 * (e - slots), lambda j: pblock(py_out, j, y_pairs))

        @pl.when(e == slots + 4)
        def _():
            for j in (events - 2, events - 1):
                pstore(py_out, j).wait()
            first_fetch(0)

        with jax.named_scope('b_grad'):
            @pl.when((e >= 3) & (lax.rem(e, 2) == 1))
            def _():
                grad_attend(e - 3)

    for slot in both:
        total(hbuf.at[slot], h_sem.at[slot])
    each(0, events + 2, step_b)

    def pull(raw, dout, g):
        x = raw.astype(F32)
        r = lax.rsqrt(jnp.mean(x * x, axis=-1, keepdims=True) + EPS)
        dn = dout * cos[...] + pltpu.roll(dout * sin_s[...], hd // 2, 1)
        return rms_pull(x, dn * g, r).astype(BF), jnp.sum(dn * (x * r), axis=0, keepdims=True)

    def unit(u):
        b, h = u // heads, lax.rem(u, heads)
        rows = span(b * seq, seq)
        cols = span(h * hd, hd)

        @pl.when(h == 0)
        def _():
            dk_acc[...] = jnp.zeros_like(dk_acc)
            dv_acc[...] = jnp.zeros_like(dv_acc)
        q, g = qr[rows, cols], gd[rows, cols]
        kr, v = k_rot[rows, :], kv_tok[rows, hd:]
        dqs = []
        for i in both:
            qi, gi = q[i * blk:(i + 1) * blk], g[i * blk:(i + 1) * blk]
            p = causal_blocks(qi, kr, i, blk)
            dp = [dotf(gi, v[j * blk:(j + 1) * blk], NT) for j in range(i + 1)]
            tot = sum(jnp.sum(a * b, axis=-1, keepdims=True) for a, b in zip(p, dp))
            dq = None
            for j in range(i + 1):
                at = slice(j * blk, (j + 1) * blk)
                dv_acc[at, :] += dotf(p[j].astype(BF), gi, TN)
                ds = (p[j] * (dp[j] - tot)).astype(BF)
                t = dotf(ds, kr[at])
                dq = t if dq is None else dq + t
                dk_acc[at, :] += dotf(ds, qi, TN)
            dqs.append(dq * scale)
        dq = jnp.concatenate(dqs, axis=0).astype(BF).astype(F32)
        dx, dg = pull(qt[rows, cols], dq, qg[...])
        gd[rows, cols] = dx
        qga[...] += dg

    def pick(r, up):
        m_i = lax.broadcasted_iota(jnp.int32, (2 * hd, 4 * kn), 0)
        l_i = lax.broadcasted_iota(jnp.int32, (2 * hd, 4 * kn), 1) - 2 * kn * up
        is_k = (l_i >= 0) & (l_i < kn) & (m_i == l_i + kn * r)
        is_v = (l_i >= kn) & (l_i < 2 * kn) & (m_i == hd + kn * r + l_i - kn)
        return jnp.where(is_k | is_v, 1.0, 0.0).astype(BF)

    def to_side(b, p):
        return rdma(pk.at[b, 2 * p + 1 - core], rk1.at[b, p], p1s.at[0], p1r.at[b], sib)

    def to_far2(b):
        return rdma(fk.at[b], rk2.at[b], p2s.at[0], p2r.at[b], far)

    def kv_one(b):
        dk = (dk_acc[...] * scale).astype(BF).astype(F32)
        dx, dg = pull(kv_tok[span(b * seq, seq), :hd], dk, kg[...])
        kga[...] += dg
        gkv = jnp.concatenate([dx, dv_acc[...].astype(BF)], axis=1)
        for r in range(4):
            pk[b, r] = (dotf(gkv[:blk], pick(r, 0)) + dotf(gkv[blk:], pick(r, 1))).astype(BF)
        for p in both:
            to_side(b, p).start()

    def kv_two(b):
        total(rk1.at[b], p1r.at[b])
        fk[b] = (pk[b, 2 * (1 - par) + core].astype(F32) + rk1[b, 1 - par].astype(F32)).astype(BF)
        hk[b] = pk[b, 2 * par + core].astype(F32) + rk1[b, par].astype(F32)
        to_far2(b).start()

    def kv_three(b):
        to_far2(b).wait_recv()
        t = hk[b] + rk2[b].astype(F32)
        low = lax.broadcasted_iota(jnp.int32, t.shape, 1) < 2 * kn
        kvt[b, :blk, :] = jnp.where(low, t, 0.0).astype(BF)
        kvt[b, blk:, :] = jnp.where(low, pltpu.roll(t, 2 * kn, 1), 0.0).astype(BF)

    def fold(b, tile):
        rows = span(tile * seq, seq)
        ids = tile * seq + lax.broadcasted_iota(jnp.int32, (seq, seq), 0)
        hot = jnp.where(ids == tok_seq[pl.ds(b, 1), :], 1.0, 0.0).astype(BF)
        d_rows[rows, :qn] += dotf(hot, gd[span(b * seq, seq), :])
        d_rows[rows, qn:] += dotf(hot, kvt[b])

    tiles = vocab // seq

    def run_unit(u):
        unit(u)

        @pl.when(lax.rem(u, heads) == heads - 1)
        def _():
            kv_one(u // heads)

        @pl.when((u >= heads) & (lax.rem(u, heads) == 1))
        def _():
            kv_two(u // heads - 1)

    def run_fold(f):
        b, tile = f // tiles, lax.rem(f, tiles)

        @pl.when(tile == 0)
        def _():
            kv_three(b)
        fold(b, tile)

    def share(e, first, n, over):
        return jnp.minimum((jnp.maximum(e - first, 0) * n) // over, n)

    def paced(e, first, n, over, f):
        each(share(e, first, n, over), share(e + 1, first, n, over), f)

    def settle(t):
        rows = span(t * vrows, vrows)
        qt[rows, :] = d_rows[rows, :qn].astype(BF)
        kvrow[rows, :] = d_rows[rows, qn:].astype(BF)

    def step_row(k, dr):
        return pl.multiple_of(vrows * lax.rem(z + nz - 1 - k if dr == 0 else k + nz - 1 - z, nz) + 2 * sub_rows * dr, 2 * sub_rows)

    def swap(k, dr, kk):
        src = pl.multiple_of(vrows * (2 * k + 1 - core) + 2 * sub_rows * dr, 2 * sub_rows)
        return rdma((qt, kvrow)[kk].at[pl.ds(src, 2 * sub_rows)], (sq, skv)[kk].at[pl.ds(step_row(k, dr), 2 * sub_rows)], qs.at[0, kk], qs.at[1, kk], sib)

    def gather_h(k):
        for dr in both:
            src = pl.multiple_of(vrows * (2 * k + core) + 2 * sub_rows * dr, 2 * sub_rows)
            dst = pl.ds(step_row(k, dr), 2 * sub_rows)
            o_sib[dst, :] = qt[pl.ds(src, 2 * sub_rows), :]
            kvc[dst, :] = (kvrow[pl.ds(src, 2 * sub_rows), :].astype(F32) + pltpu.roll(skv[dst, :].astype(F32), 2 * kn, 1)).astype(BF)

    hrows = vhalf // 2

    def hstage(j):
        return d_rows.at[pl.ds(pl.multiple_of(vhalf + lax.rem(j, 2) * hrows, hrows), hrows), pl.ds(0, bw)]

    def hstore(j):
        return pltpu.make_async_copy(hstage(j), ph_out.at[span((j // events) * hrows, hrows), span(lax.rem(j, events) * bw, bw)], pt_sem.at[lax.rem(j, 2)])

    def hblock(j):
        @pl.when(lax.rem(j, events) >= 2)
        def _():
            hstore(j - 2).wait()
        rows = span((j // events) * hrows, hrows)
        cols = span(lax.rem(j, events) * bw, bw)
        hstage(j)[...] = dotf(o_sib[rows, :], wpair[:qn, cols]) + dotf(sq[rows, :], wpair[qn:2 * qn, cols]) + dotf(kvc[rows, :], wpair[2 * qn:2 * qn + 4 * kn, cols])
        hstore(j).start()

    def final_y(dr, sub, acc):
        rows = span((2 * dr + sub) * pos, pos)
        y_v[rows, :] = (y_v[rows, :].astype(F32) + acc).astype(BF)

    def step_c(e):
        with jax.named_scope('c_first'):
            @pl.when(e == events - 2)
            def _():
                first_sends(1)

        with jax.named_scope('c_serve'):
            @pl.when(e >= 2)
            def _():
                serve(0, e, final_y)

        @pl.when(e == 0)
        def _():
            total(gown, b_s.at[0])
            total(gown, b_s.at[2])
            total(wqts_out, wq_r.at[0])
            total(wpair.at[pl.ds(0, qn)], w_s.at[0])
            for c in ld2:
                c.start()
            d_rows[...] = jnp.zeros_like(d_rows)
            gn[...] = jnp.zeros_like(gn)
            qga[...] = jnp.zeros_like(qga)
            kga[...] = jnp.zeros_like(kga)

        with jax.named_scope('c_unit'):
            paced(e, 2, units, 6, run_unit)

        with jax.named_scope('c_kv2'):
            @pl.when(e == 8)
            def _():
                kv_two(batch - 1)
        with jax.named_scope('c_fold'):
            paced(e, 8, batch * tiles, 3, run_fold)

        with jax.named_scope('c_settle'):
            @pl.when(e == 10)
            def _():
                each(0, 2 * nz, settle)
                each(0, nz, lambda k: [swap(k, dr, kk).start() for dr in both for kk in both])

        with jax.named_scope('c_swap'):
            @pl.when(e == 11)
            def _():
                for c in ld2:
                    c.wait()
                total(sq, qs.at[1, 0])
                total(skv, qs.at[1, 1])
                each(0, nz, gather_h)
        with jax.named_scope('c_part'):
            paced(e, 11, events, 2, hblock)

        @pl.when(e == 12)
        def _():
            for j in (events - 2, events - 1):
                hstore(j).wait()
            first_fetch(1)

    each(0, events, step_c)

    def gblk(j):
        return qr.at[:, span(lax.rem(j, 2) * bw, bw)]

    def hblk(j):
        return gd.at[:, span(lax.rem(j, 2) * bw, bw)]

    def swo(j):
        return d_rows.at[pl.ds(0, qn), span(lax.rem(j, 2) * bw, bw)]

    def swq(j):
        return d_rows.at[pl.ds(pl.multiple_of(qn + lax.rem(j, 2) * bw, bw), bw), pl.ds(0, qn)]

    def g_load(j):
        return pltpu.make_async_copy(gy_out.at[:, span(j * bw, bw)], gblk(j), gls.at[lax.rem(j, 2)])

    def h_load(j):
        return pltpu.make_async_copy(hid.at[:, span(j * bw, bw)], hblk(j), hls.at[lax.rem(j, 2)])

    def wo_store(j):
        return pltpu.make_async_copy(swo(j), gwo_hbm.at[:, span(j * bw, bw)], swos.at[lax.rem(j, 2)])

    def wq_store(j):
        return pltpu.make_async_copy(swq(j), gq_hbm.at[span(j * bw, bw)], swqs.at[lax.rem(j, 2)])

    def block(j):
        g_load(j).wait()
        h_load(j).wait()

        @pl.when(j + 1 < events)
        def _():
            g_load(j + 1).start()
            h_load(j + 1).start()

        @pl.when(j >= 2)
        def _():
            wo_store(j - 2).wait()
            wq_store(j - 2).wait()
        cols = span(j * bw, bw)
        swo(j)[...] = dotf(o_own[...], gblk(j)[...], TN)
        ge_v[:, cols] = dotf(hotm[...], gblk(j)[...])
        wo_store(j).start()
        swq(j)[...] = dotf(hblk(j)[...], qt[...], TN)
        gkv_v[:, cols] = dotf(kvrow[...], hblk(j)[...], TN)[:2 * kn]
        wq_store(j).start()

    def final_h(dr, sub, gh):
        rows = span((2 * dr + sub) * sub_rows, sub_rows)
        x = gown[rows, :].astype(F32)
        r = lax.rsqrt(jnp.mean(x * x, axis=-1, keepdims=True) + EPS)
        ge_v[rows, :] += rms_pull(x, gh * gain[...], r)

    outs = [pltpu.make_async_copy(s, t, out_sem.at[i]) for i, (s, t) in enumerate((
        (y_v, y_hbm), (gkv_v.at[pl.ds(0, kn)], gk_hbm), (gkv_v.at[pl.ds(kn, kn)], gv_hbm), (ge_v, ge_hbm)))]
    g_load(0).start()
    h_load(0).start()
    outs[0].start()
    work_d = events - 3

    wide = gn_out.shape[1]
    gtop = d // wide
    mrow = gtop // 2

    def to_sib(t):
        if t:
            return rdma(gfin.at[core], gfin.at[core], gs.at[4], gs.at[5], sib)
        return rdma(gmine.at[1 - core], gsib, gs.at[0], gs.at[1], sib)

    def to_col(k):
        return rdma(gcol.at[z], gcol.at[z], gs.at[2], gs.at[3], 2 * lax.rem(z + k, nz) + core)

    def step_d(e):
        with jax.named_scope('d_serve'):
            @pl.when(e >= 2)
            def _():
                serve(1, e, final_h)

        @pl.when(e == 0)
        def _():
            for k in both:
                for c in item(k):
                    c.start()

        with jax.named_scope('d_part'):
            paced(e, 0, events, 5, lambda j: hblock(j + events))

        @pl.when(e == 5)
        def _():
            for j in (events - 2, events - 1):
                hstore(j + events).wait()
        with jax.named_scope('d_gain'):
            paced(e, 2, events, 8, gain_part)
        with jax.named_scope('d_block'):
            paced(e, 1, events, work_d - 1, block)

        @pl.when(e == 10)
        def _():
            whole = jnp.sum(gn[...], axis=0, keepdims=True)
            for k, extra in ((0, qga), (1, kga)):
                for j in range(mrow):
                    c0 = (k * mrow + j) * wide
                    gmine[k, j:j + 1, :] = whole[:, c0:c0 + wide].astype(BF)
                gmine[k, mrow:mrow + 1, :] = extra[...].astype(BF)
            to_sib(0).start()

        @pl.when(e == 11)
        def _():
            total(gsib, gs.at[1])
            gcol[z] = (gmine[core].astype(F32) + gsib[...].astype(F32)).astype(BF)
            for k in range(1, nz):
                to_col(k).start()

        @pl.when(e == 13)
        def _():
            total(gcol.at[pl.ds(0, nz - 1)], gs.at[3])
            gfin[core] = sum(gcol[k].astype(F32) for k in range(nz))
            to_sib(1).start()

        @pl.when(e == events - 3)
        def _():
            outs[1].start()
            outs[2].start()

    each(0, events, step_d)

    outs[3].start()
    for ph in both:
        for k in range(4):
            arrived(rs.at[ph, k])

    total(gy_out.at[pl.ds(0, 2 * (events - 4) * pos)], b_s.at[1])
    total(gy_out.at[pl.ds(0, 2 * (events - 2) * pos)], b_s.at[3])
    to_far.wait_send()
    relay.wait_send()
    total(wpair.at[pl.ds(2 * qn, 2 * kn)], w_s.at[2])
    total(o_sib, o_s.at[0])
    total(pk.at[pl.ds(0, batch // 2)], p1s.at[0])
    total(fk, p2s.at[0])
    total(sq, qs.at[0, 0])
    total(skv, qs.at[0, 1])
    with jax.named_scope('gain_wait'):
        total(gfin.at[0], gs.at[5])
    gn_out[0:mrow, :] = gfin[0, 0:mrow, :]
    gn_out[mrow:, :] = gfin[1, 0:mrow, :]
    gqg_out[...] = gfin[0, mrow:mrow + 1, :]
    gkg_out[...] = gfin[1, mrow:mrow + 1, :]
    total(gsib, gs.at[0])
    total(gcol.at[pl.ds(0, nz - 1)], gs.at[2])
    total(gfin.at[0], gs.at[4])
    for j in (events - 2, events - 1):
        wo_store(j).wait()
        wq_store(j).wait()
    with jax.named_scope('t_outs'):
        for c in outs:
            c.wait()


def step_kernel(nz, embed, gy, wq, wk_t, wv_t, wo, gain, qg, kg, cos, sin_s, tok_seq):
    vrows, d = embed.shape
    vocab = vrows * 2 * nz
    qn, kn = wq.shape[1], wk_t.shape[0]
    hd = qg.shape[1]
    batch, seq = tok_seq.shape
    toks = batch * seq
    ev = 2 * nz
    sr, hb, vh = vrows // 4, seq // 2, vocab // 2
    mr = (d // hd // 2 + 1 + 15) // 16 * 16
    dma = pltpu.SemaphoreType.DMA
    v = pltpu.VMEM

    def arr(dt, *shape):
        return jax.ShapeDtypeStruct(shape, dt)

    outs = (arr(BF, vrows, d), arr(F32, vrows, d), arr(F32, d, qn), arr(F32, kn, d), arr(F32, kn, d), arr(F32, qn, d), arr(F32, d // hd, hd), arr(F32, 1, hd), arr(F32, 1, hd), arr(BF, vh, d),
            arr(BF, vocab, d), arr(BF, toks, d), arr(BF, qn, d), arr(BF, qn, d), arr(F32, vh, d), arr(F32, vh, d))
    return pl.pallas_call(
        functools.partial(body, nz),
        name='step_kernel',
        out_shape=outs,
        in_specs=[ANY] * 6 + [VM] * 6,
        out_specs=(ANY,) * 6 + (VM,) * 3 + (ANY,) * 7,
        scratch_shapes=[v((vocab, d), BF), v((2 * qn + 4 * kn, d), BF), v((max(d, 2 * toks), qn), BF), v((vocab, qn), BF), v((toks, qn), BF), v((vh, qn), BF), v((vh, qn), BF),
                        v((toks, 2 * hd), BF), v((toks, hd), BF), v((2, toks // 2, 4 * kn), BF), v((2, toks // 2, 4 * kn), BF), v((vocab, 4 * kn), BF), v((vh, 4 * kn), BF), v((vh, 4 * kn), BF),
                        v((vocab, qn + 4 * kn), F32), v((4, 2, sr, d), F32), v((2, vrows, d), BF), v((vrows, d), BF), v((vrows, toks), BF),
                        v((seq, hd), F32), v((seq, hd), F32), v((batch, 4, hb, 4 * kn), BF), v((batch, 2, hb, 4 * kn), BF), v((batch, hb, 4 * kn), BF), v((batch, hb, 4 * kn), F32),
                        v((batch, hb, 4 * kn), BF), v((batch, seq, 4 * kn), BF), v((8, d), F32), v((1, hd), F32), v((1, hd), F32), v((2, mr, hd), BF), v((mr, hd), BF), v((nz, mr, hd), BF), v((2, mr, hd), F32), v((vrows, d), BF), v((vrows, d), F32), v((2 * kn, d), F32),
                        dma((12,)), dma((2,)), dma((1,)), dma((ev,)), dma((ev,)), dma((2,)), dma((4,)), dma((2,)), dma((2,)), dma((2, 2)), dma((1,)), dma((4,)), dma((2,)),
                        dma((2,)), dma((2, 2)), dma((2, 4)), dma((1,)), dma((batch,)), dma((1,)), dma((batch,)), dma((2, 2)),
                        dma((2,)), dma((2,)), dma((2,)), dma((2,)), dma((6,)), dma((4,)), dma((3,))],
        compiler_params=pltpu.CompilerParams(collective_id=0, has_side_effects=True, vmem_limit_bytes=67043328),
        cost_estimate=pl.CostEstimate(flops=2 * vocab * d * 8 * qn, bytes_accessed=20 * vocab * d, transcendentals=0),
    )(embed, gy, wq, wk_t, wv_t, wo, gain, qg, kg, cos, sin_s, tok_seq)


def emit_body(cuts, *refs):
    n = len(cuts)
    src, dst = refs[:n], refs[n:2 * n]
    bufs, s_in, s_out = refs[2 * n:-2], refs[-2], refs[-1]
    ins, outs = [], []
    for i, c in enumerate(cuts):
        step = src[i].shape[0] // c
        for j in range(c):
            b = bufs[i].at[pl.ds(j * step, step)]
            ins.append(pltpu.make_async_copy(src[i].at[pl.ds(j * step, step)], b, s_in.at[len(ins)]))
            outs.append(pltpu.make_async_copy(b, dst[i].at[pl.ds(j * step, step)], s_out.at[len(outs)]))
    for c in ins:
        c.start()
    for a, b in zip(ins, outs):
        a.wait()
        b.start()
    for b in outs:
        b.wait()


def emit(*arrays):
    size = 1 << 20
    cuts = tuple(max(1, a.size * a.dtype.itemsize // size) for a in arrays)
    return pl.pallas_call(
        functools.partial(emit_body, cuts),
        name='emit',
        out_shape=tuple(jax.ShapeDtypeStruct(a.shape, a.dtype) for a in arrays),
        in_specs=[ANY] * len(arrays),
        out_specs=(ANY,) * len(arrays),
        scratch_shapes=[pltpu.VMEM(a.shape, a.dtype) for a in arrays] + [pltpu.SemaphoreType.DMA((sum(cuts),))] * 2,
        compiler_params=pltpu.CompilerParams(vmem_limit_bytes=60 * 1024 * 1024),
        cost_estimate=pl.CostEstimate(flops=0, bytes_accessed=2 * sum(a.size * a.dtype.itemsize for a in arrays), transcendentals=0),
    )(*arrays)


def rope_consts(seq, hd):
    inv = np.float32(ROPE_BASE) ** (np.float32(-2.0) * np.arange(hd // 2, dtype=np.float32) / np.float32(hd))
    ang = np.arange(seq, dtype=np.float32)[:, None] * inv.astype(np.float32)[None, :]
    ang = np.concatenate([ang, ang], axis=-1)
    sign = np.where(np.arange(hd) < hd // 2, -1.0, 1.0).astype(np.float32)
    return np.cos(ang).astype(np.float32), (np.sin(ang) * sign).astype(np.float32)


def solution(mesh):
    tp = mesh.shape['tp']
    nz = tp // 2

    def local_step(tok_ids, embed_loc, norm_gain, q_gain, k_gain, wq, wk, wv, wo, gy_loc):
        d_model = embed_loc.shape[1]
        batch, seq = tok_ids.shape
        seq_dev = seq // tp
        hd = q_gain.shape[0]
        cos_c, sin_c = (jnp.asarray(t) for t in rope_consts(seq, hd))
        r = step_kernel(nz, embed_loc, gy_loc.reshape(batch * seq_dev, d_model), wq, wk.T, wv.T, wo, norm_gain[None, :], q_gain[None, :], k_gain[None, :], cos_c, sin_c, tok_ids)
        y, g_embed, g_wq, g_wk, g_wv, g_wo, g_n, g_q, g_k = emit(*r[:9])
        return (y.reshape(batch, seq_dev, d_model), g_embed, g_n.reshape(d_model), g_q.reshape(hd), g_k.reshape(hd), g_wq, g_wk.T, g_wv.T, g_wo)

    in_specs = (P('dp', None), P('tp', None), P(), P(), P(), P(None, 'tp'), P(None, 'tp'), P(None, 'tp'), P('tp', None), P('dp', 'tp', None))
    out_specs = (P('dp', 'tp', None), P(('dp', 'tp'), None), P('dp'), P('dp'), P('dp'), P('dp', 'tp'), P('dp', 'tp'), P('dp', 'tp'), P(('dp', 'tp'), None))
    return jax.shard_map(local_step, mesh=mesh, in_specs=in_specs, out_specs=out_specs, check_vma=False)
```

```python
import functools
import jax
import jax.numpy as jnp
import numpy as np
from jax import lax
from jax.experimental import pallas as pl
from jax.experimental.pallas import tpu as pltpu
from jax.sharding import PartitionSpec as P

BF = jnp.bfloat16
F32 = jnp.float32
EPS = 1.0e-6
ROPE_BASE = 1.0e6
NEG_BIG = -1.0e30
LOG2E = 1.4426950408889634
MESH = pl.DeviceIdType.MESH
ANY = pl.BlockSpec(memory_space=pl.ANY)
VM = pl.BlockSpec(memory_space=pltpu.VMEM)
NT = (((1,), (1,)), ((), ()))
NN = (((1,), (0,)), ((), ()))
TN = (((0,), (0,)), ((), ()))


def dotf(a, b, dims=NN):
    return lax.dot_general(a, b, dims, preferred_element_type=F32)


def rdma(src, dst, ssem, rsem, dev):
    return pltpu.make_async_remote_copy(src_ref=src, dst_ref=dst, send_sem=ssem, recv_sem=rsem, device_id={'tp': dev}, device_id_type=MESH)


def span(start, size):
    return pl.ds(pl.multiple_of(start, size), size)


def each(lo, hi, f):
    def go(j, _):
        f(j)
        return 0
    lax.fori_loop(lo, hi, go, 0)


def total(ref, sem):
    pltpu.make_async_copy(ref, ref, sem).wait()


def rms_f32(x, gain):
    return x * lax.rsqrt(jnp.mean(x * x, axis=-1, keepdims=True) + EPS) * gain


def rms_pull(x, dxr, r):
    return r * dxr - x * (r * r * r * jnp.mean(x * dxr, axis=-1, keepdims=True))


def causal_blocks(q, keys, i, blk):
    r_i = lax.broadcasted_iota(jnp.int32, (blk, blk), 0)
    c_i = lax.broadcasted_iota(jnp.int32, (blk, blk), 1)
    s = [dotf(q, keys[j * blk:(j + 1) * blk], NT) for j in range(i + 1)]
    s[i] = jnp.where(r_i >= c_i, s[i], NEG_BIG)
    top = functools.reduce(jnp.maximum, [jnp.max(t, axis=-1, keepdims=True) for t in s])
    c = q.shape[-1] ** -0.5 * LOG2E
    e = [jnp.exp2((t - top) * c) for t in s]
    inv = 1.0 / sum(jnp.sum(t, axis=-1, keepdims=True) for t in e)
    return [t * inv for t in e]


def body(nz, embed, gy, wq, wk_t, wv_t, wo, gain, qg, kg, cos, sin_s, tok_seq,
         y_hbm, ge_hbm, gq_hbm, gk_hbm, gv_hbm, gwo_hbm, gn_out, gqg_out, gkg_out, erows, hid, gy_out, wqt_out, wqts_out, py_out, ph_out,
         table, wpair, wq_v, qt, o_own, o_sib, sq, kv_tok, k_rot, kvacc, farkv, kvrow, skv, kvc, d_rows, pbuf, hbuf, gown, hotm,
         dk_acc, dv_acc, pk, rk1, fk, hk, rk2, kvt, gn, qga, kga, gmine, gsib, gcol, gfin, y_v, ge_v, gkv_v,
         in_sem, h_sem, g_sem, r_sem, s_sem, a_s, b_s, xs, xr, wq_s, wq_r, w_s, o_s, pt_sem, pl_sem, rs, p1s, p1r, p2s, p2r, qs, gls, hls, swos, swqs, gs, out_sem, e_sem):
    rank = lax.axis_index('tp')
    z, core = rank // 2, lax.rem(rank, 2)
    right = 2 * lax.rem(z + 1, nz) + core
    left = 2 * lax.rem(z + nz - 1, nz) + core
    sib = rank + 1 - 2 * core
    par = lax.rem(z, 2)
    far = rank + 2 - 4 * par
    vrows, d = embed.shape
    kn = wk_t.shape[0]
    sub_rows = vrows // 4
    vocab = vrows * 2 * nz
    vhalf = vocab // 2
    batch, seq = tok_seq.shape
    toks = batch * seq
    qn = wq.shape[1]
    hd = qg.shape[1]
    heads = qn // hd
    events = 2 * nz
    pos = seq // events
    blk = seq // 2
    bw = d // events
    scale = hd ** -0.5
    units = batch * heads
    parts = 8
    wo_p, wq_p = qn // parts, d // parts
    both = (0, 1)
    places = [(dr, c) for dr in both for c in both]
    qr = wq_v.at[pl.ds(0, toks)]
    gd = wq_v.at[pl.ds(toks, toks)]
    w_q = wq_v.at[pl.ds(0, d)]

    ld = [pltpu.make_async_copy(s, t, in_sem.at[i]) for i, (s, t) in enumerate((
        (embed, table.at[span(rank * vrows, vrows)]), (gy, gown), (wq, w_q), (wo, wpair.at[pl.ds(0, qn)]),
        (wk_t, wpair.at[pl.ds(2 * qn, kn)]), (wv_t, wpair.at[pl.ds(2 * qn + kn, kn)])))]
    ld2 = [pltpu.make_async_copy(s, t, in_sem.at[i]) for i, (s, t) in enumerate((
        (wqt_out, wpair.at[pl.ds(0, qn)]), (wqts_out, wpair.at[pl.ds(qn, qn)]), (embed, gown)))]
    ld[0].start()
    barrier = pltpu.get_barrier_semaphore()
    for dev in (right, left, sib):
        pl.semaphore_signal(barrier, inc=1, device_id={'tp': dev}, device_id_type=MESH)
    with jax.named_scope('hbar'):
        pl.semaphore_wait(barrier, 3)
    with jax.named_scope('hload'):
        ld[0].wait()

    def nbr(dr):
        return right if dr == 0 else left

    def arrived(sem):
        total(table.at[pl.ds(0, 2 * sub_rows)], sem)

    def zd_of(dr, e):
        s = e // 2
        return lax.rem(z + (nz - s if dr == 0 else s), nz)

    def row_of(dr, e, c):
        return pl.multiple_of(vrows * (2 * zd_of(dr, e) + c) + sub_rows * (2 * dr + lax.rem(e, 2)), sub_rows)

    def ring(dr, e, recv_e):
        a = table.at[pl.ds(row_of(dr, e, core), sub_rows)]
        return rdma(a, a, a_s.at[0], r_sem.at[recv_e], nbr(dr))

    def side(dr, e):
        a = table.at[pl.ds(row_of(dr, e, core), sub_rows)]
        return rdma(a, a, a_s.at[1], s_sem.at[e], sib)

    def e_keep(dr, e):
        dst = pl.multiple_of(vrows * lax.rem(e // 2 + nz - 1, nz) + sub_rows * (2 * dr + lax.rem(e, 2)), sub_rows)
        return pltpu.make_async_copy(table.at[pl.ds(row_of(dr, e, core), sub_rows)], erows.at[pl.ds(dst, sub_rows)], e_sem.at[0])

    def h_copy(slot, i, row):
        return pltpu.make_async_copy(hbuf.at[slot, pl.ds(i * sub_rows, sub_rows)], hid.at[pl.ds(row, sub_rows)], h_sem.at[slot])

    def g_row(dr, e, c):
        return pl.multiple_of(seq * (2 * dr + lax.rem(e, 2)) + pos * (2 * zd_of(dr, e) + c), pos)

    def g_piece(dr, e, c):
        return gy_out.at[pl.ds(g_row(dr, e, c), pos)]

    def g_own(dr, e):
        return gown.at[span(pos * (2 * dr + lax.rem(e, 2)), pos)]

    def g_ring(dr, e, recv_e, first):
        a = g_piece(dr, e, core)
        return rdma(g_own(dr, e) if first else a, a, b_s.at[0 if first else 1], r_sem.at[recv_e], nbr(dr))

    def g_side(dr, e, first):
        a = g_piece(dr, e, core)
        return rdma(g_own(dr, e) if first else a, a, b_s.at[2 if first else 3], s_sem.at[e], sib)

    def g_home(dr, e):
        return pltpu.make_async_copy(g_own(dr, e), g_piece(dr, e, core), in_sem.at[8 + 2 * dr + e])

    def g_fetch(slot, i, dr, c, e):
        return pltpu.make_async_copy(g_piece(dr, e, c), hbuf.at[slot, pl.ds(i * pos, pos)], g_sem.at[0])

    def wo_push(k):
        return rdma(wpair.at[span(k * wo_p, wo_p)], wpair.at[pl.ds(pl.multiple_of(qn + k * wo_p, wo_p), wo_p)], w_s.at[0], w_s.at[1], sib)

    def tb(k):
        return o_own.at[span(lax.rem(k, 2) * qn, qn), pl.ds(0, wq_p)]

    def wq_push(k):
        return rdma(tb(k), wqts_out.at[:, span(k * wq_p, wq_p)], wq_s.at[0, lax.rem(k, 2)], wq_r.at[0], sib)

    def wq_home(k):
        return pltpu.make_async_copy(tb(k), wqt_out.at[:, span(k * wq_p, wq_p)], wq_s.at[1, lax.rem(k, 2)])

    def wk_push(k):
        return rdma((wk_t, wv_t)[k], wpair.at[pl.ds(2 * qn + (2 + k) * kn, kn)], w_s.at[2], w_s.at[3], sib)

    def o_push(b, k):
        src = pl.multiple_of(b * seq + pos * (2 * k + 1 - core), pos)
        dst = pl.multiple_of(vrows * k + pos * b, pos)
        return rdma(o_own.at[pl.ds(src, pos)], o_sib.at[pl.ds(dst, pos)], o_s.at[0], o_s.at[1], sib)

    def project(e):
        slot = lax.rem(e, 2)

        @pl.when(e >= 2)
        def _():
            total(hbuf.at[slot], h_sem.at[slot])

        rows = [row_of(dr, e, c) for dr, c in places]
        for i, row in enumerate(rows):
            x = table[pl.ds(row, sub_rows), :].astype(F32)
            ids = row + lax.broadcasted_iota(jnp.int32, (sub_rows, seq), 0)
            hit = jnp.zeros((sub_rows, seq), F32)
            for b in range(batch):
                hit = jnp.maximum(hit, jnp.where(tok_seq[b:b + 1, :] == ids, 1.0, 0.0))
            used = jnp.max(hit, axis=1, keepdims=True)
            h = jnp.where(used > 0.5, rms_f32(x, gain[...]), 0.0)
            hbuf[slot, pl.ds(i * sub_rows, sub_rows), :] = h.astype(BF)
            h_copy(slot, i, row).start()
        hb = hbuf[slot]
        qkv = jnp.concatenate([dotf(hb, w_q[...]).astype(BF), dotf(hb, wpair[2 * qn:2 * qn + 4 * kn, :], NT).astype(BF)], axis=1)
        lane = lax.broadcasted_iota(jnp.int32, (1, vrows), 1)
        rowid = jnp.zeros((1, vrows), jnp.int32)
        for i, row in enumerate(rows):
            rowid = jnp.where(lane // sub_rows == i, row + lane - i * sub_rows, rowid)
        rowid = rowid.astype(F32)
        for b in range(batch):
            sl = slice(b * seq, (b + 1) * seq)
            hot = jnp.where(d_rows[sl, :vrows] == rowid, 1.0, 0.0).astype(BF)
            got = dotf(hot, qkv)
            qt[sl, :] = (qt[sl, :].astype(F32) + got[:, :qn]).astype(BF)
            at = slice((b % 2) * seq, (b % 2 + 1) * seq)
            kvacc[b // 2, at, :] = (kvacc[b // 2, at, :].astype(F32) + got[:, qn:]).astype(BF)

    def step_a(e):
        with jax.named_scope('a_wait'):
            @pl.when((e >= 2) & (e < events))
            def _():
                arrived(r_sem.at[e])

            @pl.when(e < events - 2)
            def _():
                for dr in both:
                    ring(dr, e, e + 2).start()

        @pl.when(e < events)
        def _():
            for dr in both:
                side(dr, e).start()
                e_keep(dr, e).start()

        @pl.when(e == 0)
        def _():
            for c in ld[1:]:
                c.start()
            for k in both:
                wk_push(k).start()
            for b in range(batch):
                wide = jnp.broadcast_to(tok_seq[b:b + 1, :].astype(F32), (vrows, seq))
                d_rows[b * seq:(b + 1) * seq, :vrows] = wide.T
            qt[...] = jnp.zeros_like(qt)
            kvacc[...] = jnp.zeros_like(kvacc)

        @pl.when(e == 1)
        def _():
            for c in ld[1:]:
                c.wait()
            total(wpair.at[pl.ds(2 * qn, 2 * kn)], w_s.at[3])
            for dr in both:
                for k in both:
                    g_home(dr, k).start()

        @pl.when((e >= events - 2) & (e < events))
        def _():
            for dr in both:
                g_ring(dr, e - events + 2, e - events + 4, True).start()

        @pl.when((e >= 2) & (e < 4 + parts))
        def _():
            @pl.when(e >= 4)
            def _():
                wq_push(e - 4).wait_send()
                wq_home(e - 4).wait()

            @pl.when(e < 2 + parts)
            def _():
                k = e - 2
                block = wq_v[span(k * wq_p, wq_p), :]
                tb(k)[...] = block.astype(F32).T.astype(BF)
                wo_push(k).start()
                wq_push(k).start()
                wq_home(k).start()

        with jax.named_scope('a_proj'):
            @pl.when(e >= 1)
            def _():
                arrived(s_sem.at[e - 1])
                project(e - 1)

    each(0, events + 1, step_a)

    to_far = rdma(kvacc.at[core], farkv.at[core], xs.at[0], xr.at[0], far)
    relay = rdma(farkv.at[core], farkv.at[core], xs.at[1], xr.at[1], sib)
    at_i = lax.broadcasted_iota(jnp.int32, (pos, seq), 1) - pos * rank
    own_i = lax.broadcasted_iota(jnp.int32, (pos, seq), 0)
    col = jnp.concatenate([jnp.sum(jnp.where(at_i == own_i, tok_seq[b:b + 1, :].astype(F32), 0.0), axis=1, keepdims=True) for b in range(batch)], axis=0).astype(jnp.int32)
    lanes = lax.broadcasted_iota(jnp.int32, (vrows, vrows), 1)
    hot_mine = jnp.concatenate([jnp.where(col == lanes + j * vrows, 1.0, 0.0).astype(BF) for j in range(vocab // vrows)], axis=1)
    to_far.start()
    for dr in both:
        for k in both:
            g_side(dr, k, True).start()
            g_home(dr, k).wait()
    cw = min(512, d)

    def own_rows(j):
        y_v[:, span(j * cw, cw)] = dotf(hot_mine, table[:, span(j * cw, cw)]).astype(BF)

    each(0, d // cw, own_rows)
    for b in range(batch):
        ids = rank * vrows + lax.broadcasted_iota(jnp.int32, (vrows, seq), 0)
        hotm[:, b * seq:(b + 1) * seq] = jnp.where(ids == tok_seq[b:b + 1, :], 1.0, 0.0).astype(BF)

    def place(p, first):
        l_i = lax.broadcasted_iota(jnp.int32, (4 * kn, 2 * hd), 0)
        m_i = lax.broadcasted_iota(jnp.int32, (4 * kn, 2 * hd), 1)
        upper = jnp.where(l_i >= 2 * kn, 1, 0)
        owner = jnp.where(upper == 1, 1 - first, first)
        l_i = l_i - 2 * kn * upper
        base = kn * (2 * p + owner)
        want = jnp.where(l_i < kn, base + l_i, hd + base + l_i - kn)
        return jnp.where(m_i == want, 1.0, 0.0).astype(BF)

    def rope(raw, g):
        n = rms_f32(raw.astype(F32), g)
        return (n * cos[...] + pltpu.roll(n, hd // 2, 1) * sin_s[...]).astype(BF)

    def attend(u):
        base = (u // heads) * seq
        rows = span(base, seq)
        cols = span(lax.rem(u, heads) * hd, hd)
        q = rope(qt[rows, cols], qg[...])
        qr[rows, cols] = q
        kr = k_rot[rows, :]
        v = kv_tok[rows, hd:]
        for i in both:
            p = causal_blocks(q[i * blk:(i + 1) * blk], kr, i, blk)
            o = sum(dotf(t.astype(BF), v[j * blk:(j + 1) * blk]) for j, t in enumerate(p))
            o_own[pl.ds(pl.multiple_of(base + i * blk, blk), blk), cols] = o.astype(BF)

    def grad_attend(e):
        total(hbuf, g_sem.at[0])
        r = dotf(hbuf[...].reshape(2 * vrows, d), wpair[:qn, :], NT).astype(BF)
        for k in both:
            for i, (dr, c) in enumerate(places):
                n = (4 * k + i) * pos
                gd[pl.ds(g_row(dr, e + k, c), pos), :] = r[n:n + pos]

    def pstage(j):
        return d_rows.at[span(lax.rem(j, 2) * vhalf, vhalf), pl.ds(0, bw)]

    def pstore(dst, j):
        return pltpu.make_async_copy(pstage(j), dst.at[:, span(j * bw, bw)], pt_sem.at[lax.rem(j, 2)])

    def pblock(dst, j, pairs):
        @pl.when(j >= 2)
        def _():
            pstore(dst, j - 2).wait()
        cols = span(j * bw, bw)
        acc = None
        for a, lo, n in pairs:
            t = dotf(a[...], wpair[lo:lo + n, cols])
            acc = t if acc is None else acc + t
        pstage(j)[...] = acc
        pstore(dst, j).start()

    y_pairs = [(sq, 0, qn), (o_sib, qn, qn)]

    def pslot(ph, e, dr):
        return pbuf.at[2 * ph + lax.rem(e, 2), dr]

    def pfetch(ph, e, dr):
        s = e // 2
        step = s if ph else lax.rem(z + (2 * nz - 1 - s if dr == 0 else 1 + s), nz)
        row = pl.multiple_of(vrows * step + sub_rows * (2 * dr + lax.rem(e, 2)), sub_rows)
        return pltpu.make_async_copy((py_out, ph_out)[ph].at[pl.ds(row, sub_rows)], pslot(ph, e, dr), pl_sem.at[ph, lax.rem(e, 2)])

    def item(i):
        row = vrows * (i // 2)
        cps = []
        for dr in both:
            at = pl.ds(pl.multiple_of(row + sub_rows * (2 * dr + lax.rem(i, 2)), sub_rows), sub_rows)
            cps.append(pltpu.make_async_copy(ph_out.at[at], pbuf.at[lax.rem(i, 2), dr], pl_sem.at[0, lax.rem(i, 2)]))
            cps.append(pltpu.make_async_copy(erows.at[at], hbuf.at[lax.rem(i, 2), pl.ds(dr * sub_rows, sub_rows)], e_sem.at[1 + lax.rem(i, 2)]))
        return cps

    def gain_part(i):
        total(pbuf.at[lax.rem(i, 2)], pl_sem.at[0, lax.rem(i, 2)])
        total(hbuf.at[lax.rem(i, 2), pl.ds(0, 2 * sub_rows)], e_sem.at[1 + lax.rem(i, 2)])
        for dr in both:
            x = hbuf[lax.rem(i, 2), dr * sub_rows:(dr + 1) * sub_rows, :].astype(F32)
            t = pbuf[lax.rem(i, 2), dr] * (x * lax.rsqrt(jnp.mean(x * x, axis=-1, keepdims=True) + EPS))
            gn[...] += sum(t[k:k + 8] for k in range(0, sub_rows, 8))

        @pl.when(i + 2 < events)
        def _():
            for c in item(i + 2):
                c.start()

    def fetched(ph, e):
        total(pbuf.at[2 * ph + lax.rem(e, 2)], pl_sem.at[ph, lax.rem(e, 2)])

    def rslot(dr, e):
        return table.at[span((dr * (events - 2) + e) * sub_rows, sub_rows)]

    def sslot(ph, dr, e):
        k = 2 * (events - 2) + 8 * ph + 4 * lax.rem(e // 2, 2) + 2 * dr + lax.rem(e, 2)
        return table.at[span(k * sub_rows, sub_rows)]

    def send(ph, dr, e):
        return rdma(sslot(ph, dr, e), rslot(dr, e), rs.at[ph, lax.rem(e, 4)], r_sem.at[e + 2], nbr(dr))

    def first_fetch(ph):
        for e in both:
            for dr in both:
                pfetch(ph, e, dr).start()

    def first_sends(ph):
        for e in both:
            fetched(ph, e)
            for dr in both:
                sslot(ph, dr, e)[...] = pslot(ph, e, dr)[...].astype(BF)
        for e in both:
            for dr in both:
                send(ph, dr, e).start()
                pfetch(ph, e + 2, dr).start()

    def serve(ph, e, final):
        arrived(r_sem.at[e])
        fetched(ph, e)

        @pl.when(e < events - 2)
        def _():
            @pl.when(e >= 4)
            def _():
                arrived(rs.at[ph, lax.rem(e, 4)])
            for dr in both:
                sslot(ph, dr, e)[...] = (pslot(ph, e, dr)[...] + rslot(dr, e - 2)[...].astype(F32)).astype(BF)
            for dr in both:
                send(ph, dr, e).start()
                pfetch(ph, e + 2, dr).start()

        @pl.when(e >= events - 2)
        def _():
            for dr in both:
                final(dr, lax.rem(e, 2), pslot(ph, e, dr)[...] + rslot(dr, e - 2)[...].astype(F32))

    slots = 9

    def gather_o(k):
        for b in range(batch):
            src = pl.multiple_of(b * seq + pos * (2 * k + core), pos)
            sq[pl.ds(pl.multiple_of(vrows * k + pos * b, pos), pos), :] = o_own[pl.ds(src, pos), :]

    def upto(e, n, over):
        return jnp.minimum((e * n) // over, n)

    def step_b(e):
        with jax.named_scope('b_first'):
            @pl.when(e == events - 2)
            def _():
                first_sends(0)

        with jax.named_scope('b_wait'):
            @pl.when((e >= 2) & (e < events))
            def _():
                arrived(r_sem.at[e])

            @pl.when((e >= 2) & (e < events - 2))
            def _():
                for dr in both:
                    g_ring(dr, e, e + 2, False).start()

        @pl.when((e >= 2) & (e < events))
        def _():
            for dr in both:
                g_side(dr, e, False).start()

        @pl.when((e >= 1) & (e <= events))
        def _():
            arrived(s_sem.at[e - 1])

        with jax.named_scope('kv_far'):
            @pl.when(e == 2)
            def _():
                to_far.wait_recv()
                relay.start()

        with jax.named_scope('kv_tok'):
            @pl.when(e == 3)
            def _():
                rdma(farkv.at[1 - core], farkv.at[1 - core], xs.at[1], xr.at[1], sib).wait_recv()
                for hf in both:
                    kv_tok[hf * (toks // 2):(hf + 1) * (toks // 2), :] = (dotf(kvacc[hf], place(par, core)) + dotf(farkv[hf], place(1 - par, hf))).astype(BF)
                for b in range(batch):
                    sl = slice(b * seq, (b + 1) * seq)
                    k_rot[sl, :] = rope(kv_tok[sl, :hd], kg[...])

            @pl.when((e >= 2) & (lax.rem(e, 2) == 0))
            def _():
                for k in both:
                    for i, (dr, c) in enumerate(places):
                        g_fetch(k, i, dr, c, e - 2 + k).start()

        def give(b):
            each(0, nz, lambda k: o_push(b, k).start())

        def seen(t):
            return jnp.minimum((jnp.maximum(t - 3, 0) * units) // (slots - 3), units)

        each(seen(e - 1) // heads, seen(e) // heads, give)
        with jax.named_scope('b_attend'):
            each(seen(e), seen(e + 1), attend)

        @pl.when(e == 4)
        def _():
            total(table.at[pl.ds(0, 2 * (events - 2) * sub_rows)], a_s.at[0])
            total(table.at[pl.ds(0, 2 * events * sub_rows)], a_s.at[1])
            total(erows, e_sem.at[0])

        @pl.when(e == slots + 1)
        def _():
            total(wpair.at[pl.ds(0, qn)], w_s.at[1])
            total(o_sib, o_s.at[1])
            each(0, nz, gather_o)

        with jax.named_scope('b_part'):
            @pl.when((e > slots) & (e <= slots + 4))
            def _():
                each(4 * (e - slots - 1), 4 * (e - slots), lambda j: pblock(py_out, j, y_pairs))

        @pl.when(e == slots + 4)
        def _():
            for j in (events - 2, events - 1):
                pstore(py_out, j).wait()
            first_fetch(0)

        with jax.named_scope('b_grad'):
            @pl.when((e >= 3) & (lax.rem(e, 2) == 1))
            def _():
                grad_attend(e - 3)

    for slot in both:
        total(hbuf.at[slot], h_sem.at[slot])
    each(0, events + 2, step_b)

    def pull(raw, dout, g):
        x = raw.astype(F32)
        r = lax.rsqrt(jnp.mean(x * x, axis=-1, keepdims=True) + EPS)
        dn = dout * cos[...] + pltpu.roll(dout * sin_s[...], hd // 2, 1)
        return rms_pull(x, dn * g, r).astype(BF), jnp.sum(dn * (x * r), axis=0, keepdims=True)

    def unit(u):
        b, h = u // heads, lax.rem(u, heads)
        rows = span(b * seq, seq)
        cols = span(h * hd, hd)

        @pl.when(h == 0)
        def _():
            dk_acc[...] = jnp.zeros_like(dk_acc)
            dv_acc[...] = jnp.zeros_like(dv_acc)
        q, g = qr[rows, cols], gd[rows, cols]
        kr, v = k_rot[rows, :], kv_tok[rows, hd:]
        dqs = []
        for i in both:
            qi, gi = q[i * blk:(i + 1) * blk], g[i * blk:(i + 1) * blk]
            p = causal_blocks(qi, kr, i, blk)
            dp = [dotf(gi, v[j * blk:(j + 1) * blk], NT) for j in range(i + 1)]
            tot = sum(jnp.sum(a * b, axis=-1, keepdims=True) for a, b in zip(p, dp))
            dq = None
            for j in range(i + 1):
                at = slice(j * blk, (j + 1) * blk)
                dv_acc[at, :] += dotf(p[j].astype(BF), gi, TN)
                ds = (p[j] * (dp[j] - tot)).astype(BF)
                t = dotf(ds, kr[at])
                dq = t if dq is None else dq + t
                dk_acc[at, :] += dotf(ds, qi, TN)
            dqs.append(dq * scale)
        dq = jnp.concatenate(dqs, axis=0).astype(BF).astype(F32)
        dx, dg = pull(qt[rows, cols], dq, qg[...])
        gd[rows, cols] = dx
        qga[...] += dg

    def pick(r, up):
        m_i = lax.broadcasted_iota(jnp.int32, (2 * hd, 4 * kn), 0)
        l_i = lax.broadcasted_iota(jnp.int32, (2 * hd, 4 * kn), 1) - 2 * kn * up
        is_k = (l_i >= 0) & (l_i < kn) & (m_i == l_i + kn * r)
        is_v = (l_i >= kn) & (l_i < 2 * kn) & (m_i == hd + kn * r + l_i - kn)
        return jnp.where(is_k | is_v, 1.0, 0.0).astype(BF)

    def to_side(b, p):
        return rdma(pk.at[b, 2 * p + 1 - core], rk1.at[b, p], p1s.at[0], p1r.at[b], sib)

    def to_far2(b):
        return rdma(fk.at[b], rk2.at[b], p2s.at[0], p2r.at[b], far)

    def kv_one(b):
        dk = (dk_acc[...] * scale).astype(BF).astype(F32)
        dx, dg = pull(kv_tok[span(b * seq, seq), :hd], dk, kg[...])
        kga[...] += dg
        gkv = jnp.concatenate([dx, dv_acc[...].astype(BF)], axis=1)
        for r in range(4):
            pk[b, r] = (dotf(gkv[:blk], pick(r, 0)) + dotf(gkv[blk:], pick(r, 1))).astype(BF)
        for p in both:
            to_side(b, p).start()

    def kv_two(b):
        total(rk1.at[b], p1r.at[b])
        fk[b] = (pk[b, 2 * (1 - par) + core].astype(F32) + rk1[b, 1 - par].astype(F32)).astype(BF)
        hk[b] = pk[b, 2 * par + core].astype(F32) + rk1[b, par].astype(F32)
        to_far2(b).start()

    def kv_three(b):
        to_far2(b).wait_recv()
        t = hk[b] + rk2[b].astype(F32)
        low = lax.broadcasted_iota(jnp.int32, t.shape, 1) < 2 * kn
        kvt[b, :blk, :] = jnp.where(low, t, 0.0).astype(BF)
        kvt[b, blk:, :] = jnp.where(low, pltpu.roll(t, 2 * kn, 1), 0.0).astype(BF)

    def fold(b, tile):
        rows = span(tile * seq, seq)
        ids = tile * seq + lax.broadcasted_iota(jnp.int32, (seq, seq), 0)
        hot = jnp.where(ids == tok_seq[pl.ds(b, 1), :], 1.0, 0.0).astype(BF)
        d_rows[rows, :qn] += dotf(hot, gd[span(b * seq, seq), :])
        d_rows[rows, qn:] += dotf(hot, kvt[b])

    tiles = vocab // seq

    def run_unit(u):
        unit(u)

        @pl.when(lax.rem(u, heads) == heads - 1)
        def _():
            kv_one(u // heads)

        @pl.when((u >= heads) & (lax.rem(u, heads) == 1))
        def _():
            kv_two(u // heads - 1)

    def run_fold(f):
        b, tile = f // tiles, lax.rem(f, tiles)

        @pl.when(tile == 0)
        def _():
            kv_three(b)
        fold(b, tile)

    def share(e, first, n, over):
        return jnp.minimum((jnp.maximum(e - first, 0) * n) // over, n)

    def paced(e, first, n, over, f):
        each(share(e, first, n, over), share(e + 1, first, n, over), f)

    def settle(t):
        rows = span(t * vrows, vrows)
        qt[rows, :] = d_rows[rows, :qn].astype(BF)
        kvrow[rows, :] = d_rows[rows, qn:].astype(BF)

    def step_row(k, dr):
        return pl.multiple_of(vrows * lax.rem(z + nz - 1 - k if dr == 0 else k + nz - 1 - z, nz) + 2 * sub_rows * dr, 2 * sub_rows)

    def swap(k, dr, kk):
        src = pl.multiple_of(vrows * (2 * k + 1 - core) + 2 * sub_rows * dr, 2 * sub_rows)
        return rdma((qt, kvrow)[kk].at[pl.ds(src, 2 * sub_rows)], (sq, skv)[kk].at[pl.ds(step_row(k, dr), 2 * sub_rows)], qs.at[0, kk], qs.at[1, kk], sib)

    def gather_h(k):
        for dr in both:
            src = pl.multiple_of(vrows * (2 * k + core) + 2 * sub_rows * dr, 2 * sub_rows)
            dst = pl.ds(step_row(k, dr), 2 * sub_rows)
            o_sib[dst, :] = qt[pl.ds(src, 2 * sub_rows), :]
            kvc[dst, :] = (kvrow[pl.ds(src, 2 * sub_rows), :].astype(F32) + pltpu.roll(skv[dst, :].astype(F32), 2 * kn, 1)).astype(BF)

    hrows = vhalf // 2

    def hstage(j):
        return d_rows.at[pl.ds(pl.multiple_of(vhalf + lax.rem(j, 2) * hrows, hrows), hrows), pl.ds(0, bw)]

    def hstore(j):
        return pltpu.make_async_copy(hstage(j), ph_out.at[span((j // events) * hrows, hrows), span(lax.rem(j, events) * bw, bw)], pt_sem.at[lax.rem(j, 2)])

    def hblock(j):
        @pl.when(lax.rem(j, events) >= 2)
        def _():
            hstore(j - 2).wait()
        rows = span((j // events) * hrows, hrows)
        cols = span(lax.rem(j, events) * bw, bw)
        hstage(j)[...] = dotf(o_sib[rows, :], wpair[:qn, cols]) + dotf(sq[rows, :], wpair[qn:2 * qn, cols]) + dotf(kvc[rows, :], wpair[2 * qn:2 * qn + 4 * kn, cols])
        hstore(j).start()

    def final_y(dr, sub, acc):
        rows = span((2 * dr + sub) * pos, pos)
        y_v[rows, :] = (y_v[rows, :].astype(F32) + acc).astype(BF)

    def step_c(e):
        with jax.named_scope('c_first'):
            @pl.when(e == events - 2)
            def _():
                first_sends(1)

        with jax.named_scope('c_serve'):
            @pl.when(e >= 2)
            def _():
                serve(0, e, final_y)

        @pl.when(e == 0)
        def _():
            total(gown, b_s.at[0])
            total(gown, b_s.at[2])
            total(wqts_out, wq_r.at[0])
            total(wpair.at[pl.ds(0, qn)], w_s.at[0])
            for c in ld2:
                c.start()
            d_rows[...] = jnp.zeros_like(d_rows)
            gn[...] = jnp.zeros_like(gn)
            qga[...] = jnp.zeros_like(qga)
            kga[...] = jnp.zeros_like(kga)

        with jax.named_scope('c_unit'):
            paced(e, 2, units, 6, run_unit)

        with jax.named_scope('c_kv2'):
            @pl.when(e == 8)
            def _():
                kv_two(batch - 1)
        with jax.named_scope('c_fold'):
            paced(e, 8, batch * tiles, 3, run_fold)

        with jax.named_scope('c_settle'):
            @pl.when(e == 10)
            def _():
                each(0, 2 * nz, settle)
                each(0, nz, lambda k: [swap(k, dr, kk).start() for dr in both for kk in both])

        with jax.named_scope('c_swap'):
            @pl.when(e == 11)
            def _():
                for c in ld2:
                    c.wait()
                total(sq, qs.at[1, 0])
                total(skv, qs.at[1, 1])
                each(0, nz, gather_h)
        with jax.named_scope('c_part'):
            paced(e, 11, events, 2, hblock)

        @pl.when(e == 12)
        def _():
            for j in (events - 2, events - 1):
                hstore(j).wait()
            first_fetch(1)

    each(0, events, step_c)

    def gblk(j):
        return qr.at[:, span(lax.rem(j, 2) * bw, bw)]

    def hblk(j):
        return gd.at[:, span(lax.rem(j, 2) * bw, bw)]

    def swo(j):
        return d_rows.at[pl.ds(0, qn), span(lax.rem(j, 2) * bw, bw)]

    def swq(j):
        return d_rows.at[pl.ds(pl.multiple_of(qn + lax.rem(j, 2) * bw, bw), bw), pl.ds(0, qn)]

    def g_load(j):
        return pltpu.make_async_copy(gy_out.at[:, span(j * bw, bw)], gblk(j), gls.at[lax.rem(j, 2)])

    def h_load(j):
        return pltpu.make_async_copy(hid.at[:, span(j * bw, bw)], hblk(j), hls.at[lax.rem(j, 2)])

    def wo_store(j):
        return pltpu.make_async_copy(swo(j), gwo_hbm.at[:, span(j * bw, bw)], swos.at[lax.rem(j, 2)])

    def wq_store(j):
        return pltpu.make_async_copy(swq(j), gq_hbm.at[span(j * bw, bw)], swqs.at[lax.rem(j, 2)])

    def block(j):
        g_load(j).wait()
        h_load(j).wait()

        @pl.when(j + 1 < events)
        def _():
            g_load(j + 1).start()
            h_load(j + 1).start()

        @pl.when(j >= 2)
        def _():
            wo_store(j - 2).wait()
            wq_store(j - 2).wait()
        cols = span(j * bw, bw)
        swo(j)[...] = dotf(o_own[...], gblk(j)[...], TN)
        ge_v[:, cols] = dotf(hotm[...], gblk(j)[...])
        wo_store(j).start()
        swq(j)[...] = dotf(hblk(j)[...], qt[...], TN)
        gkv_v[:, cols] = dotf(kvrow[...], hblk(j)[...], TN)[:2 * kn]
        wq_store(j).start()

    def final_h(dr, sub, gh):
        rows = span((2 * dr + sub) * sub_rows, sub_rows)
        x = gown[rows, :].astype(F32)
        r = lax.rsqrt(jnp.mean(x * x, axis=-1, keepdims=True) + EPS)
        ge_v[rows, :] += rms_pull(x, gh * gain[...], r)

    outs = [pltpu.make_async_copy(s, t, out_sem.at[i]) for i, (s, t) in enumerate((
        (y_v, y_hbm), (gkv_v.at[pl.ds(0, kn)], gk_hbm), (gkv_v.at[pl.ds(kn, kn)], gv_hbm)))]

    def ge_store(dr, sub):
        rows = pl.ds((2 * dr + sub) * sub_rows, sub_rows)
        return pltpu.make_async_copy(ge_v.at[rows], ge_hbm.at[rows], out_sem.at[3])

    g_load(0).start()
    h_load(0).start()
    outs[0].start()
    work_d = events - 3

    wide = gn_out.shape[1]
    gtop = d // wide
    mrow = gtop // 2

    def to_sib(t):
        if t:
            return rdma(gfin.at[core], gfin.at[core], gs.at[4], gs.at[5], sib)
        return rdma(gmine.at[1 - core], gsib, gs.at[0], gs.at[1], sib)

    def to_col(k):
        return rdma(gcol.at[z], gcol.at[z], gs.at[2], gs.at[3], 2 * lax.rem(z + k, nz) + core)

    def step_d(e):
        with jax.named_scope('d_serve'):
            @pl.when(e >= 2)
            def _():
                serve(1, e, final_h)

        @pl.when(e == 0)
        def _():
            for k in both:
                for c in item(k):
                    c.start()

        with jax.named_scope('d_part'):
            paced(e, 0, events, 5, lambda j: hblock(j + events))

        @pl.when(e == 5)
        def _():
            for j in (events - 2, events - 1):
                hstore(j + events).wait()
        with jax.named_scope('d_gain'):
            paced(e, 2, events, 8, gain_part)
        with jax.named_scope('d_block'):
            paced(e, 1, events, work_d - 1, block)

        @pl.when(e == 10)
        def _():
            whole = jnp.sum(gn[...], axis=0, keepdims=True)
            for k, extra in ((0, qga), (1, kga)):
                for j in range(mrow):
                    c0 = (k * mrow + j) * wide
                    gmine[k, j:j + 1, :] = whole[:, c0:c0 + wide].astype(BF)
                gmine[k, mrow:mrow + 1, :] = extra[...].astype(BF)
            to_sib(0).start()

        @pl.when(e == 11)
        def _():
            total(gsib, gs.at[1])
            gcol[z] = (gmine[core].astype(F32) + gsib[...].astype(F32)).astype(BF)
            for k in range(1, nz):
                to_col(k).start()

        @pl.when(e == 13)
        def _():
            total(gcol.at[pl.ds(0, nz - 1)], gs.at[3])
            gfin[core] = sum(gcol[k].astype(F32) for k in range(nz))
            to_sib(1).start()

        @pl.when(e == events - 3)
        def _():
            outs[1].start()
            outs[2].start()

        @pl.when(e == events - 2)
        def _():
            for dr in both:
                ge_store(dr, 0).start()

    each(0, events, step_d)

    for dr in both:
        ge_store(dr, 1).start()
    for ph in both:
        for k in range(4):
            arrived(rs.at[ph, k])

    total(gy_out.at[pl.ds(0, 2 * (events - 4) * pos)], b_s.at[1])
    total(gy_out.at[pl.ds(0, 2 * (events - 2) * pos)], b_s.at[3])
    to_far.wait_send()
    relay.wait_send()
    total(wpair.at[pl.ds(2 * qn, 2 * kn)], w_s.at[2])
    total(o_sib, o_s.at[0])
    total(pk.at[pl.ds(0, batch // 2)], p1s.at[0])
    total(fk, p2s.at[0])
    total(sq, qs.at[0, 0])
    total(skv, qs.at[0, 1])
    with jax.named_scope('gain_wait'):
        total(gfin.at[0], gs.at[5])
    gn_out[0:mrow, :] = gfin[0, 0:mrow, :]
    gn_out[mrow:, :] = gfin[1, 0:mrow, :]
    gqg_out[...] = gfin[0, mrow:mrow + 1, :]
    gkg_out[...] = gfin[1, mrow:mrow + 1, :]
    total(gsib, gs.at[0])
    total(gcol.at[pl.ds(0, nz - 1)], gs.at[2])
    total(gfin.at[0], gs.at[4])
    for j in (events - 2, events - 1):
        wo_store(j).wait()
        wq_store(j).wait()
    with jax.named_scope('t_outs'):
        total(ge_v, out_sem.at[3])
        for c in outs:
            c.wait()


def step_kernel(nz, embed, gy, wq, wk_t, wv_t, wo, gain, qg, kg, cos, sin_s, tok_seq):
    vrows, d = embed.shape
    vocab = vrows * 2 * nz
    qn, kn = wq.shape[1], wk_t.shape[0]
    hd = qg.shape[1]
    batch, seq = tok_seq.shape
    toks = batch * seq
    ev = 2 * nz
    sr, hb, vh = vrows // 4, seq // 2, vocab // 2
    mr = (d // hd // 2 + 1 + 15) // 16 * 16
    dma = pltpu.SemaphoreType.DMA
    v = pltpu.VMEM

    def arr(dt, *shape):
        return jax.ShapeDtypeStruct(shape, dt)

    outs = (arr(BF, vrows, d), arr(F32, vrows, d), arr(F32, d, qn), arr(F32, kn, d), arr(F32, kn, d), arr(F32, qn, d), arr(F32, d // hd, hd), arr(F32, 1, hd), arr(F32, 1, hd), arr(BF, vh, d),
            arr(BF, vocab, d), arr(BF, toks, d), arr(BF, qn, d), arr(BF, qn, d), arr(F32, vh, d), arr(F32, vh, d))
    return pl.pallas_call(
        functools.partial(body, nz),
        name='step_kernel',
        out_shape=outs,
        in_specs=[ANY] * 6 + [VM] * 6,
        out_specs=(ANY,) * 6 + (VM,) * 3 + (ANY,) * 7,
        scratch_shapes=[v((vocab, d), BF), v((2 * qn + 4 * kn, d), BF), v((max(d, 2 * toks), qn), BF), v((vocab, qn), BF), v((toks, qn), BF), v((vh, qn), BF), v((vh, qn), BF),
                        v((toks, 2 * hd), BF), v((toks, hd), BF), v((2, toks // 2, 4 * kn), BF), v((2, toks // 2, 4 * kn), BF), v((vocab, 4 * kn), BF), v((vh, 4 * kn), BF), v((vh, 4 * kn), BF),
                        v((vocab, qn + 4 * kn), F32), v((4, 2, sr, d), F32), v((2, vrows, d), BF), v((vrows, d), BF), v((vrows, toks), BF),
                        v((seq, hd), F32), v((seq, hd), F32), v((batch, 4, hb, 4 * kn), BF), v((batch, 2, hb, 4 * kn), BF), v((batch, hb, 4 * kn), BF), v((batch, hb, 4 * kn), F32),
                        v((batch, hb, 4 * kn), BF), v((batch, seq, 4 * kn), BF), v((8, d), F32), v((1, hd), F32), v((1, hd), F32), v((2, mr, hd), BF), v((mr, hd), BF), v((nz, mr, hd), BF), v((2, mr, hd), F32), v((vrows, d), BF), v((vrows, d), F32), v((2 * kn, d), F32),
                        dma((12,)), dma((2,)), dma((1,)), dma((ev,)), dma((ev,)), dma((2,)), dma((4,)), dma((2,)), dma((2,)), dma((2, 2)), dma((1,)), dma((4,)), dma((2,)),
                        dma((2,)), dma((2, 2)), dma((2, 4)), dma((1,)), dma((batch,)), dma((1,)), dma((batch,)), dma((2, 2)),
                        dma((2,)), dma((2,)), dma((2,)), dma((2,)), dma((6,)), dma((4,)), dma((3,))],
        compiler_params=pltpu.CompilerParams(collective_id=0, has_side_effects=True, vmem_limit_bytes=67043328),
        cost_estimate=pl.CostEstimate(flops=2 * vocab * d * 8 * qn, bytes_accessed=20 * vocab * d, transcendentals=0),
    )(embed, gy, wq, wk_t, wv_t, wo, gain, qg, kg, cos, sin_s, tok_seq)


def emit_body(cuts, *refs):
    n = len(cuts)
    src, dst = refs[:n], refs[n:2 * n]
    bufs, s_in, s_out = refs[2 * n:-2], refs[-2], refs[-1]
    ins, outs = [], []
    for i, c in enumerate(cuts):
        step = src[i].shape[0] // c
        for j in range(c):
            b = bufs[i].at[pl.ds(j * step, step)]
            ins.append(pltpu.make_async_copy(src[i].at[pl.ds(j * step, step)], b, s_in.at[len(ins)]))
            outs.append(pltpu.make_async_copy(b, dst[i].at[pl.ds(j * step, step)], s_out.at[len(outs)]))
    for c in ins:
        c.start()
    for a, b in zip(ins, outs):
        a.wait()
        b.start()
    for b in outs:
        b.wait()


def emit(*arrays):
    size = 1 << 20
    cuts = tuple(max(1, a.size * a.dtype.itemsize // size) for a in arrays)
    return pl.pallas_call(
        functools.partial(emit_body, cuts),
        name='emit',
        out_shape=tuple(jax.ShapeDtypeStruct(a.shape, a.dtype) for a in arrays),
        in_specs=[ANY] * len(arrays),
        out_specs=(ANY,) * len(arrays),
        scratch_shapes=[pltpu.VMEM(a.shape, a.dtype) for a in arrays] + [pltpu.SemaphoreType.DMA((sum(cuts),))] * 2,
        compiler_params=pltpu.CompilerParams(vmem_limit_bytes=60 * 1024 * 1024),
        cost_estimate=pl.CostEstimate(flops=0, bytes_accessed=2 * sum(a.size * a.dtype.itemsize for a in arrays), transcendentals=0),
    )(*arrays)


def rope_consts(seq, hd):
    inv = np.float32(ROPE_BASE) ** (np.float32(-2.0) * np.arange(hd // 2, dtype=np.float32) / np.float32(hd))
    ang = np.arange(seq, dtype=np.float32)[:, None] * inv.astype(np.float32)[None, :]
    ang = np.concatenate([ang, ang], axis=-1)
    sign = np.where(np.arange(hd) < hd // 2, -1.0, 1.0).astype(np.float32)
    return np.cos(ang).astype(np.float32), (np.sin(ang) * sign).astype(np.float32)


def solution(mesh):
    tp = mesh.shape['tp']
    nz = tp // 2

    def local_step(tok_ids, embed_loc, norm_gain, q_gain, k_gain, wq, wk, wv, wo, gy_loc):
        d_model = embed_loc.shape[1]
        batch, seq = tok_ids.shape
        seq_dev = seq // tp
        hd = q_gain.shape[0]
        cos_c, sin_c = (jnp.asarray(t) for t in rope_consts(seq, hd))
        r = step_kernel(nz, embed_loc, gy_loc.reshape(batch * seq_dev, d_model), wq, wk.T, wv.T, wo, norm_gain[None, :], q_gain[None, :], k_gain[None, :], cos_c, sin_c, tok_ids)
        y, g_embed, g_wq, g_wk, g_wv, g_wo, g_n, g_q, g_k = emit(*r[:9])
        return (y.reshape(batch, seq_dev, d_model), g_embed, g_n.reshape(d_model), g_q.reshape(hd), g_k.reshape(hd), g_wq, g_wk.T, g_wv.T, g_wo)

    in_specs = (P('dp', None), P('tp', None), P(), P(), P(), P(None, 'tp'), P(None, 'tp'), P(None, 'tp'), P('tp', None), P('dp', 'tp', None))
    out_specs = (P('dp', 'tp', None), P(('dp', 'tp'), None), P('dp'), P('dp'), P('dp'), P('dp', 'tp'), P('dp', 'tp'), P('dp', 'tp'), P(('dp', 'tp'), None))
    return jax.shard_map(local_step, mesh=mesh, in_specs=in_specs, out_specs=out_specs, check_vma=False)
```

```python
import functools
import jax
import jax.numpy as jnp
import numpy as np
from jax import lax
from jax.experimental import pallas as pl
from jax.experimental.pallas import tpu as pltpu
from jax.sharding import PartitionSpec as P

BF = jnp.bfloat16
F32 = jnp.float32
EPS = 1.0e-6
ROPE_BASE = 1.0e6
NEG_BIG = -1.0e30
LOG2E = 1.4426950408889634
MESH = pl.DeviceIdType.MESH
ANY = pl.BlockSpec(memory_space=pl.ANY)
VM = pl.BlockSpec(memory_space=pltpu.VMEM)
NT = (((1,), (1,)), ((), ()))
NN = (((1,), (0,)), ((), ()))
TN = (((0,), (0,)), ((), ()))


def dotf(a, b, dims=NN):
    return lax.dot_general(a, b, dims, preferred_element_type=F32)


def rdma(src, dst, ssem, rsem, dev):
    return pltpu.make_async_remote_copy(src_ref=src, dst_ref=dst, send_sem=ssem, recv_sem=rsem, device_id={'tp': dev}, device_id_type=MESH)


def span(start, size):
    return pl.ds(pl.multiple_of(start, size), size)


def each(lo, hi, f):
    def go(j, _):
        f(j)
        return 0
    lax.fori_loop(lo, hi, go, 0)


def total(ref, sem):
    pltpu.make_async_copy(ref, ref, sem).wait()


def rms_f32(x, gain):
    return x * lax.rsqrt(jnp.mean(x * x, axis=-1, keepdims=True) + EPS) * gain


def rms_pull(x, dxr, r):
    return r * dxr - x * (r * r * r * jnp.mean(x * dxr, axis=-1, keepdims=True))


def causal_blocks(q, keys, i, blk):
    r_i = lax.broadcasted_iota(jnp.int32, (blk, blk), 0)
    c_i = lax.broadcasted_iota(jnp.int32, (blk, blk), 1)
    s = [dotf(q, keys[j * blk:(j + 1) * blk], NT) for j in range(i + 1)]
    s[i] = jnp.where(r_i >= c_i, s[i], NEG_BIG)
    top = functools.reduce(jnp.maximum, [jnp.max(t, axis=-1, keepdims=True) for t in s])
    c = q.shape[-1] ** -0.5 * LOG2E
    e = [jnp.exp2((t - top) * c) for t in s]
    inv = 1.0 / sum(jnp.sum(t, axis=-1, keepdims=True) for t in e)
    return [t * inv for t in e]


def body(nz, embed, gy, wq, wk_t, wv_t, wo, gain, qg, kg, cos, sin_s, tok_seq,
         y_hbm, ge_hbm, gq_hbm, gk_hbm, gv_hbm, gwo_hbm, gn_out, gqg_out, gkg_out, erows, hid, gy_out, wqt_out, wqts_out, py_out, ph_out,
         table, wpair, wq_v, qt, o_own, o_sib, sq, kv_tok, k_rot, kvacc, farkv, kvrow, skv, kvc, d_rows, pbuf, hbuf, gown, hotm,
         dk_acc, dv_acc, pk, rk1, fk, hk, rk2, kvt, gn, qga, kga, gmine, gsib, gcol, gfin, y_v, ge_v, gkv_v,
         in_sem, h_sem, g_sem, r_sem, s_sem, a_s, b_s, xs, xr, wq_s, wq_r, w_s, o_s, pt_sem, pl_sem, rs, p1s, p1r, p2s, p2r, qs, gls, hls, swos, swqs, gs, out_sem, e_sem):
    rank = lax.axis_index('tp')
    z, core = rank // 2, lax.rem(rank, 2)
    right = 2 * lax.rem(z + 1, nz) + core
    left = 2 * lax.rem(z + nz - 1, nz) + core
    sib = rank + 1 - 2 * core
    par = lax.rem(z, 2)
    far = rank + 2 - 4 * par
    vrows, d = embed.shape
    kn = wk_t.shape[0]
    sub_rows = vrows // 4
    vocab = vrows * 2 * nz
    vhalf = vocab // 2
    batch, seq = tok_seq.shape
    toks = batch * seq
    qn = wq.shape[1]
    hd = qg.shape[1]
    heads = qn // hd
    events = 2 * nz
    pos = seq // events
    blk = seq // 2
    bw = d // events
    scale = hd ** -0.5
    units = batch * heads
    parts = 8
    wo_p, wq_p = qn // parts, d // parts
    both = (0, 1)
    places = [(dr, c) for dr in both for c in both]
    qr = wq_v.at[pl.ds(0, toks)]
    gd = wq_v.at[pl.ds(toks, toks)]
    w_q = wq_v.at[pl.ds(0, d)]

    ld = [pltpu.make_async_copy(s, t, in_sem.at[i]) for i, (s, t) in enumerate((
        (embed, table.at[span(rank * vrows, vrows)]), (gy, gown), (wq, w_q), (wo, wpair.at[pl.ds(0, qn)]),
        (wk_t, wpair.at[pl.ds(2 * qn, kn)]), (wv_t, wpair.at[pl.ds(2 * qn + kn, kn)])))]
    ld2 = [pltpu.make_async_copy(s, t, in_sem.at[i]) for i, (s, t) in enumerate((
        (wqt_out, wpair.at[pl.ds(0, qn)]), (wqts_out, wpair.at[pl.ds(qn, qn)]), (embed, gown)))]
    ld[0].start()
    barrier = pltpu.get_barrier_semaphore()
    for dev in (right, left, sib):
        pl.semaphore_signal(barrier, inc=1, device_id={'tp': dev}, device_id_type=MESH)
    pl.semaphore_wait(barrier, 3)
    ld[0].wait()

    def nbr(dr):
        return right if dr == 0 else left

    def arrived(sem):
        total(table.at[pl.ds(0, 2 * sub_rows)], sem)

    def zd_of(dr, e):
        s = e // 2
        return lax.rem(z + (nz - s if dr == 0 else s), nz)

    def row_of(dr, e, c):
        return pl.multiple_of(vrows * (2 * zd_of(dr, e) + c) + sub_rows * (2 * dr + lax.rem(e, 2)), sub_rows)

    def ring(dr, e, recv_e):
        a = table.at[pl.ds(row_of(dr, e, core), sub_rows)]
        return rdma(a, a, a_s.at[0], r_sem.at[recv_e], nbr(dr))

    def side(dr, e):
        a = table.at[pl.ds(row_of(dr, e, core), sub_rows)]
        return rdma(a, a, a_s.at[1], s_sem.at[e], sib)

    def e_keep(dr, e):
        dst = pl.multiple_of(vrows * lax.rem(e // 2 + nz - 1, nz) + sub_rows * (2 * dr + lax.rem(e, 2)), sub_rows)
        return pltpu.make_async_copy(table.at[pl.ds(row_of(dr, e, core), sub_rows)], erows.at[pl.ds(dst, sub_rows)], e_sem.at[0])

    def h_copy(slot, i, row):
        return pltpu.make_async_copy(hbuf.at[slot, pl.ds(i * sub_rows, sub_rows)], hid.at[pl.ds(row, sub_rows)], h_sem.at[slot])

    def g_row(dr, e, c):
        return pl.multiple_of(seq * (2 * dr + lax.rem(e, 2)) + pos * (2 * zd_of(dr, e) + c), pos)

    def g_piece(dr, e, c):
        return gy_out.at[pl.ds(g_row(dr, e, c), pos)]

    def g_own(dr, e):
        return gown.at[span(pos * (2 * dr + lax.rem(e, 2)), pos)]

    def g_ring(dr, e, recv_e, first):
        a = g_piece(dr, e, core)
        return rdma(g_own(dr, e) if first else a, a, b_s.at[0 if first else 1], r_sem.at[recv_e], nbr(dr))

    def g_side(dr, e, first):
        a = g_piece(dr, e, core)
        return rdma(g_own(dr, e) if first else a, a, b_s.at[2 if first else 3], s_sem.at[e], sib)

    def g_home(dr, e):
        return pltpu.make_async_copy(g_own(dr, e), g_piece(dr, e, core), in_sem.at[8 + 2 * dr + e])

    def g_fetch(slot, i, dr, c, e):
        return pltpu.make_async_copy(g_piece(dr, e, c), hbuf.at[slot, pl.ds(i * pos, pos)], g_sem.at[0])

    def wo_push(k):
        return rdma(wpair.at[span(k * wo_p, wo_p)], wpair.at[pl.ds(pl.multiple_of(qn + k * wo_p, wo_p), wo_p)], w_s.at[0], w_s.at[1], sib)

    def tb(k):
        return o_own.at[span(lax.rem(k, 2) * qn, qn), pl.ds(0, wq_p)]

    def wq_push(k):
        return rdma(tb(k), wqts_out.at[:, span(k * wq_p, wq_p)], wq_s.at[0, lax.rem(k, 2)], wq_r.at[0], sib)

    def wq_home(k):
        return pltpu.make_async_copy(tb(k), wqt_out.at[:, span(k * wq_p, wq_p)], wq_s.at[1, lax.rem(k, 2)])

    def wk_push(k):
        return rdma((wk_t, wv_t)[k], wpair.at[pl.ds(2 * qn + (2 + k) * kn, kn)], w_s.at[2], w_s.at[3], sib)

    def o_push(b, k):
        src = pl.multiple_of(b * seq + pos * (2 * k + 1 - core), pos)
        dst = pl.multiple_of(vrows * k + pos * b, pos)
        return rdma(o_own.at[pl.ds(src, pos)], o_sib.at[pl.ds(dst, pos)], o_s.at[0], o_s.at[1], sib)

    def project(e):
        slot = lax.rem(e, 2)

        @pl.when(e >= 2)
        def _():
            total(hbuf.at[slot], h_sem.at[slot])

        rows = [row_of(dr, e, c) for dr, c in places]
        for i, row in enumerate(rows):
            x = table[pl.ds(row, sub_rows), :].astype(F32)
            ids = row + lax.broadcasted_iota(jnp.int32, (sub_rows, seq), 0)
            hit = jnp.zeros((sub_rows, seq), F32)
            for b in range(batch):
                hit = jnp.maximum(hit, jnp.where(tok_seq[b:b + 1, :] == ids, 1.0, 0.0))
            used = jnp.max(hit, axis=1, keepdims=True)
            h = jnp.where(used > 0.5, rms_f32(x, gain[...]), 0.0)
            hbuf[slot, pl.ds(i * sub_rows, sub_rows), :] = h.astype(BF)
            h_copy(slot, i, row).start()
        hb = hbuf[slot]
        qkv = jnp.concatenate([dotf(hb, w_q[...]).astype(BF), dotf(hb, wpair[2 * qn:2 * qn + 4 * kn, :], NT).astype(BF)], axis=1)
        lane = lax.broadcasted_iota(jnp.int32, (1, vrows), 1)
        rowid = jnp.zeros((1, vrows), jnp.int32)
        for i, row in enumerate(rows):
            rowid = jnp.where(lane // sub_rows == i, row + lane - i * sub_rows, rowid)
        rowid = rowid.astype(F32)
        for b in range(batch):
            sl = slice(b * seq, (b + 1) * seq)
            hot = jnp.where(d_rows[sl, :vrows] == rowid, 1.0, 0.0).astype(BF)
            got = dotf(hot, qkv)
            qt[sl, :] = (qt[sl, :].astype(F32) + got[:, :qn]).astype(BF)
            at = slice((b % 2) * seq, (b % 2 + 1) * seq)
            kvacc[b // 2, at, :] = (kvacc[b // 2, at, :].astype(F32) + got[:, qn:]).astype(BF)

    def step_a(e):
        @pl.when((e >= 2) & (e < events))
        def _():
            arrived(r_sem.at[e])

        @pl.when(e < events - 2)
        def _():
            for dr in both:
                ring(dr, e, e + 2).start()

        @pl.when(e < events)
        def _():
            for dr in both:
                side(dr, e).start()
                e_keep(dr, e).start()

        @pl.when(e == 0)
        def _():
            for c in ld[1:]:
                c.start()
            for k in both:
                wk_push(k).start()
            for b in range(batch):
                wide = jnp.broadcast_to(tok_seq[b:b + 1, :].astype(F32), (vrows, seq))
                d_rows[b * seq:(b + 1) * seq, :vrows] = wide.T
            qt[...] = jnp.zeros_like(qt)
            kvacc[...] = jnp.zeros_like(kvacc)

        @pl.when(e == 1)
        def _():
            for c in ld[1:]:
                c.wait()
            total(wpair.at[pl.ds(2 * qn, 2 * kn)], w_s.at[3])
            for dr in both:
                for k in both:
                    g_home(dr, k).start()

        @pl.when((e >= events - 2) & (e < events))
        def _():
            for dr in both:
                g_ring(dr, e - events + 2, e - events + 4, True).start()

        @pl.when((e >= 2) & (e < 4 + parts))
        def _():
            @pl.when(e >= 4)
            def _():
                wq_push(e - 4).wait_send()
                wq_home(e - 4).wait()

            @pl.when(e < 2 + parts)
            def _():
                k = e - 2
                block = wq_v[span(k * wq_p, wq_p), :]
                tb(k)[...] = block.astype(F32).T.astype(BF)
                wo_push(k).start()
                wq_push(k).start()
                wq_home(k).start()

        @pl.when(e >= 1)
        def _():
            arrived(s_sem.at[e - 1])
            project(e - 1)

    each(0, events + 1, step_a)

    to_far = rdma(kvacc.at[core], farkv.at[core], xs.at[0], xr.at[0], far)
    relay = rdma(farkv.at[core], farkv.at[core], xs.at[1], xr.at[1], sib)
    at_i = lax.broadcasted_iota(jnp.int32, (pos, seq), 1) - pos * rank
    own_i = lax.broadcasted_iota(jnp.int32, (pos, seq), 0)
    col = jnp.concatenate([jnp.sum(jnp.where(at_i == own_i, tok_seq[b:b + 1, :].astype(F32), 0.0), axis=1, keepdims=True) for b in range(batch)], axis=0).astype(jnp.int32)
    lanes = lax.broadcasted_iota(jnp.int32, (vrows, vrows), 1)
    hot_mine = jnp.concatenate([jnp.where(col == lanes + j * vrows, 1.0, 0.0).astype(BF) for j in range(vocab // vrows)], axis=1)
    to_far.start()
    for dr in both:
        for k in both:
            g_side(dr, k, True).start()
            g_home(dr, k).wait()
    cw = min(512, d)

    def own_rows(j):
        y_v[:, span(j * cw, cw)] = dotf(hot_mine, table[:, span(j * cw, cw)]).astype(BF)

    each(0, d // cw, own_rows)
    for b in range(batch):
        ids = rank * vrows + lax.broadcasted_iota(jnp.int32, (vrows, seq), 0)
        hotm[:, b * seq:(b + 1) * seq] = jnp.where(ids == tok_seq[b:b + 1, :], 1.0, 0.0).astype(BF)

    def place(p, first):
        l_i = lax.broadcasted_iota(jnp.int32, (4 * kn, 2 * hd), 0)
        m_i = lax.broadcasted_iota(jnp.int32, (4 * kn, 2 * hd), 1)
        upper = jnp.where(l_i >= 2 * kn, 1, 0)
        owner = jnp.where(upper == 1, 1 - first, first)
        l_i = l_i - 2 * kn * upper
        base = kn * (2 * p + owner)
        want = jnp.where(l_i < kn, base + l_i, hd + base + l_i - kn)
        return jnp.where(m_i == want, 1.0, 0.0).astype(BF)

    def rope(raw, g):
        n = rms_f32(raw.astype(F32), g)
        return (n * cos[...] + pltpu.roll(n, hd // 2, 1) * sin_s[...]).astype(BF)

    def attend(u):
        base = (u // heads) * seq
        rows = span(base, seq)
        cols = span(lax.rem(u, heads) * hd, hd)
        q = rope(qt[rows, cols], qg[...])
        qr[rows, cols] = q
        kr = k_rot[rows, :]
        v = kv_tok[rows, hd:]
        for i in both:
            p = causal_blocks(q[i * blk:(i + 1) * blk], kr, i, blk)
            o = sum(dotf(t.astype(BF), v[j * blk:(j + 1) * blk]) for j, t in enumerate(p))
            o_own[pl.ds(pl.multiple_of(base + i * blk, blk), blk), cols] = o.astype(BF)

    def grad_attend(e):
        total(hbuf, g_sem.at[0])
        r = dotf(hbuf[...].reshape(2 * vrows, d), wpair[:qn, :], NT).astype(BF)
        for k in both:
            for i, (dr, c) in enumerate(places):
                n = (4 * k + i) * pos
                gd[pl.ds(g_row(dr, e + k, c), pos), :] = r[n:n + pos]

    def pstage(j):
        return d_rows.at[span(lax.rem(j, 2) * vhalf, vhalf), pl.ds(0, bw)]

    def pstore(dst, j):
        return pltpu.make_async_copy(pstage(j), dst.at[:, span(j * bw, bw)], pt_sem.at[lax.rem(j, 2)])

    def pblock(dst, j, pairs):
        @pl.when(j >= 2)
        def _():
            pstore(dst, j - 2).wait()
        cols = span(j * bw, bw)
        acc = None
        for a, lo, n in pairs:
            t = dotf(a[...], wpair[lo:lo + n, cols])
            acc = t if acc is None else acc + t
        pstage(j)[...] = acc
        pstore(dst, j).start()

    y_pairs = [(sq, 0, qn), (o_sib, qn, qn)]

    def pslot(ph, e, dr):
        return pbuf.at[2 * ph + lax.rem(e, 2), dr]

    def pfetch(ph, e, dr):
        s = e // 2
        step = s if ph else lax.rem(z + (2 * nz - 1 - s if dr == 0 else 1 + s), nz)
        row = pl.multiple_of(vrows * step + sub_rows * (2 * dr + lax.rem(e, 2)), sub_rows)
        return pltpu.make_async_copy((py_out, ph_out)[ph].at[pl.ds(row, sub_rows)], pslot(ph, e, dr), pl_sem.at[ph, lax.rem(e, 2)])

    def item(i):
        row = vrows * (i // 2)
        cps = []
        for dr in both:
            at = pl.ds(pl.multiple_of(row + sub_rows * (2 * dr + lax.rem(i, 2)), sub_rows), sub_rows)
            cps.append(pltpu.make_async_copy(ph_out.at[at], pbuf.at[lax.rem(i, 2), dr], pl_sem.at[0, lax.rem(i, 2)]))
            cps.append(pltpu.make_async_copy(erows.at[at], hbuf.at[lax.rem(i, 2), pl.ds(dr * sub_rows, sub_rows)], e_sem.at[1 + lax.rem(i, 2)]))
        return cps

    def gain_part(i):
        total(pbuf.at[lax.rem(i, 2)], pl_sem.at[0, lax.rem(i, 2)])
        total(hbuf.at[lax.rem(i, 2), pl.ds(0, 2 * sub_rows)], e_sem.at[1 + lax.rem(i, 2)])
        for dr in both:
            x = hbuf[lax.rem(i, 2), dr * sub_rows:(dr + 1) * sub_rows, :].astype(F32)
            t = pbuf[lax.rem(i, 2), dr] * (x * lax.rsqrt(jnp.mean(x * x, axis=-1, keepdims=True) + EPS))
            gn[...] += sum(t[k:k + 8] for k in range(0, sub_rows, 8))

        @pl.when(i + 2 < events)
        def _():
            for c in item(i + 2):
                c.start()

    def fetched(ph, e):
        total(pbuf.at[2 * ph + lax.rem(e, 2)], pl_sem.at[ph, lax.rem(e, 2)])

    def rslot(dr, e):
        return table.at[span((dr * (events - 2) + e) * sub_rows, sub_rows)]

    def sslot(ph, dr, e):
        k = 2 * (events - 2) + 8 * ph + 4 * lax.rem(e // 2, 2) + 2 * dr + lax.rem(e, 2)
        return table.at[span(k * sub_rows, sub_rows)]

    def send(ph, dr, e):
        return rdma(sslot(ph, dr, e), rslot(dr, e), rs.at[ph, lax.rem(e, 4)], r_sem.at[e + 2], nbr(dr))

    def first_fetch(ph):
        for e in both:
            for dr in both:
                pfetch(ph, e, dr).start()

    def first_sends(ph):
        for e in both:
            fetched(ph, e)
            for dr in both:
                sslot(ph, dr, e)[...] = pslot(ph, e, dr)[...].astype(BF)
        for e in both:
            for dr in both:
                send(ph, dr, e).start()
                pfetch(ph, e + 2, dr).start()

    def serve(ph, e, final):
        arrived(r_sem.at[e])
        fetched(ph, e)

        @pl.when(e < events - 2)
        def _():
            @pl.when(e >= 4)
            def _():
                arrived(rs.at[ph, lax.rem(e, 4)])
            for dr in both:
                sslot(ph, dr, e)[...] = (pslot(ph, e, dr)[...] + rslot(dr, e - 2)[...].astype(F32)).astype(BF)
            for dr in both:
                send(ph, dr, e).start()
                pfetch(ph, e + 2, dr).start()

        @pl.when(e >= events - 2)
        def _():
            for dr in both:
                final(dr, lax.rem(e, 2), pslot(ph, e, dr)[...] + rslot(dr, e - 2)[...].astype(F32))

    slots = 9

    def gather_o(k):
        for b in range(batch):
            src = pl.multiple_of(b * seq + pos * (2 * k + core), pos)
            sq[pl.ds(pl.multiple_of(vrows * k + pos * b, pos), pos), :] = o_own[pl.ds(src, pos), :]

    def upto(e, n, over):
        return jnp.minimum((e * n) // over, n)

    def step_b(e):
        @pl.when(e == events - 2)
        def _():
            first_sends(0)

        @pl.when((e >= 2) & (e < events))
        def _():
            arrived(r_sem.at[e])

        @pl.when((e >= 2) & (e < events - 2))
        def _():
            for dr in both:
                g_ring(dr, e, e + 2, False).start()

        @pl.when((e >= 2) & (e < events))
        def _():
            for dr in both:
                g_side(dr, e, False).start()

        @pl.when((e >= 1) & (e <= events))
        def _():
            arrived(s_sem.at[e - 1])

        @pl.when(e == 2)
        def _():
            to_far.wait_recv()
            relay.start()

        @pl.when(e == 3)
        def _():
            rdma(farkv.at[1 - core], farkv.at[1 - core], xs.at[1], xr.at[1], sib).wait_recv()
            for hf in both:
                kv_tok[hf * (toks // 2):(hf + 1) * (toks // 2), :] = (dotf(kvacc[hf], place(par, core)) + dotf(farkv[hf], place(1 - par, hf))).astype(BF)
            for b in range(batch):
                sl = slice(b * seq, (b + 1) * seq)
                k_rot[sl, :] = rope(kv_tok[sl, :hd], kg[...])

        @pl.when((e >= 2) & (lax.rem(e, 2) == 0))
        def _():
            for k in both:
                for i, (dr, c) in enumerate(places):
                    g_fetch(k, i, dr, c, e - 2 + k).start()

        def give(b):
            each(0, nz, lambda k: o_push(b, k).start())

        def seen(t):
            return jnp.minimum((jnp.maximum(t - 3, 0) * units) // (slots - 3), units)

        each(seen(e - 1) // heads, seen(e) // heads, give)
        each(seen(e), seen(e + 1), attend)

        @pl.when(e == 4)
        def _():
            total(table.at[pl.ds(0, 2 * (events - 2) * sub_rows)], a_s.at[0])
            total(table.at[pl.ds(0, 2 * events * sub_rows)], a_s.at[1])
            total(erows, e_sem.at[0])

        @pl.when(e == slots + 1)
        def _():
            total(wpair.at[pl.ds(0, qn)], w_s.at[1])
            total(o_sib, o_s.at[1])
            each(0, nz, gather_o)

        @pl.when((e > slots) & (e <= slots + 4))
        def _():
            each(4 * (e - slots - 1), 4 * (e - slots), lambda j: pblock(py_out, j, y_pairs))

        @pl.when(e == slots + 4)
        def _():
            for j in (events - 2, events - 1):
                pstore(py_out, j).wait()
            first_fetch(0)

        @pl.when((e >= 3) & (lax.rem(e, 2) == 1))
        def _():
            grad_attend(e - 3)

    for slot in both:
        total(hbuf.at[slot], h_sem.at[slot])
    each(0, events + 2, step_b)

    def pull(raw, dout, g):
        x = raw.astype(F32)
        r = lax.rsqrt(jnp.mean(x * x, axis=-1, keepdims=True) + EPS)
        dn = dout * cos[...] + pltpu.roll(dout * sin_s[...], hd // 2, 1)
        return rms_pull(x, dn * g, r).astype(BF), jnp.sum(dn * (x * r), axis=0, keepdims=True)

    def unit(u):
        b, h = u // heads, lax.rem(u, heads)
        rows = span(b * seq, seq)
        cols = span(h * hd, hd)

        @pl.when(h == 0)
        def _():
            dk_acc[...] = jnp.zeros_like(dk_acc)
            dv_acc[...] = jnp.zeros_like(dv_acc)
        q, g = qr[rows, cols], gd[rows, cols]
        kr, v = k_rot[rows, :], kv_tok[rows, hd:]
        dqs = []
        for i in both:
            qi, gi = q[i * blk:(i + 1) * blk], g[i * blk:(i + 1) * blk]
            p = causal_blocks(qi, kr, i, blk)
            dp = [dotf(gi, v[j * blk:(j + 1) * blk], NT) for j in range(i + 1)]
            tot = sum(jnp.sum(a * b, axis=-1, keepdims=True) for a, b in zip(p, dp))
            dq = None
            for j in range(i + 1):
                at = slice(j * blk, (j + 1) * blk)
                dv_acc[at, :] += dotf(p[j].astype(BF), gi, TN)
                ds = (p[j] * (dp[j] - tot)).astype(BF)
                t = dotf(ds, kr[at])
                dq = t if dq is None else dq + t
                dk_acc[at, :] += dotf(ds, qi, TN)
            dqs.append(dq * scale)
        dq = jnp.concatenate(dqs, axis=0).astype(BF).astype(F32)
        dx, dg = pull(qt[rows, cols], dq, qg[...])
        gd[rows, cols] = dx
        qga[...] += dg

    def pick(r, up):
        m_i = lax.broadcasted_iota(jnp.int32, (2 * hd, 4 * kn), 0)
        l_i = lax.broadcasted_iota(jnp.int32, (2 * hd, 4 * kn), 1) - 2 * kn * up
        is_k = (l_i >= 0) & (l_i < kn) & (m_i == l_i + kn * r)
        is_v = (l_i >= kn) & (l_i < 2 * kn) & (m_i == hd + kn * r + l_i - kn)
        return jnp.where(is_k | is_v, 1.0, 0.0).astype(BF)

    def to_side(b, p):
        return rdma(pk.at[b, 2 * p + 1 - core], rk1.at[b, p], p1s.at[0], p1r.at[b], sib)

    def to_far2(b):
        return rdma(fk.at[b], rk2.at[b], p2s.at[0], p2r.at[b], far)

    def kv_one(b):
        dk = (dk_acc[...] * scale).astype(BF).astype(F32)
        dx, dg = pull(kv_tok[span(b * seq, seq), :hd], dk, kg[...])
        kga[...] += dg
        gkv = jnp.concatenate([dx, dv_acc[...].astype(BF)], axis=1)
        for r in range(4):
            pk[b, r] = (dotf(gkv[:blk], pick(r, 0)) + dotf(gkv[blk:], pick(r, 1))).astype(BF)
        for p in both:
            to_side(b, p).start()

    def kv_two(b):
        total(rk1.at[b], p1r.at[b])
        fk[b] = (pk[b, 2 * (1 - par) + core].astype(F32) + rk1[b, 1 - par].astype(F32)).astype(BF)
        hk[b] = pk[b, 2 * par + core].astype(F32) + rk1[b, par].astype(F32)
        to_far2(b).start()

    def kv_three(b):
        to_far2(b).wait_recv()
        t = hk[b] + rk2[b].astype(F32)
        low = lax.broadcasted_iota(jnp.int32, t.shape, 1) < 2 * kn
        kvt[b, :blk, :] = jnp.where(low, t, 0.0).astype(BF)
        kvt[b, blk:, :] = jnp.where(low, pltpu.roll(t, 2 * kn, 1), 0.0).astype(BF)

    def fold(b, tile):
        rows = span(tile * seq, seq)
        ids = tile * seq + lax.broadcasted_iota(jnp.int32, (seq, seq), 0)
        hot = jnp.where(ids == tok_seq[pl.ds(b, 1), :], 1.0, 0.0).astype(BF)
        d_rows[rows, :qn] += dotf(hot, gd[span(b * seq, seq), :])
        d_rows[rows, qn:] += dotf(hot, kvt[b])

    tiles = vocab // seq

    def run_unit(u):
        unit(u)

        @pl.when(lax.rem(u, heads) == heads - 1)
        def _():
            kv_one(u // heads)

        @pl.when((u >= heads) & (lax.rem(u, heads) == 1))
        def _():
            kv_two(u // heads - 1)

    def run_fold(f):
        b, tile = f // tiles, lax.rem(f, tiles)

        @pl.when(tile == 0)
        def _():
            kv_three(b)
        fold(b, tile)

    def share(e, first, n, over):
        return jnp.minimum((jnp.maximum(e - first, 0) * n) // over, n)

    def paced(e, first, n, over, f):
        each(share(e, first, n, over), share(e + 1, first, n, over), f)

    def settle(t):
        rows = span(t * vrows, vrows)
        qt[rows, :] = d_rows[rows, :qn].astype(BF)
        kvrow[rows, :] = d_rows[rows, qn:].astype(BF)

    def step_row(k, dr):
        return pl.multiple_of(vrows * lax.rem(z + nz - 1 - k if dr == 0 else k + nz - 1 - z, nz) + 2 * sub_rows * dr, 2 * sub_rows)

    def swap(k, dr, kk):
        src = pl.multiple_of(vrows * (2 * k + 1 - core) + 2 * sub_rows * dr, 2 * sub_rows)
        return rdma((qt, kvrow)[kk].at[pl.ds(src, 2 * sub_rows)], (sq, skv)[kk].at[pl.ds(step_row(k, dr), 2 * sub_rows)], qs.at[0, kk], qs.at[1, kk], sib)

    def gather_h(k):
        for dr in both:
            src = pl.multiple_of(vrows * (2 * k + core) + 2 * sub_rows * dr, 2 * sub_rows)
            dst = pl.ds(step_row(k, dr), 2 * sub_rows)
            o_sib[dst, :] = qt[pl.ds(src, 2 * sub_rows), :]
            kvc[dst, :] = (kvrow[pl.ds(src, 2 * sub_rows), :].astype(F32) + pltpu.roll(skv[dst, :].astype(F32), 2 * kn, 1)).astype(BF)

    hrows = vhalf // 2

    def hstage(j):
        return d_rows.at[pl.ds(pl.multiple_of(vhalf + lax.rem(j, 2) * hrows, hrows), hrows), pl.ds(0, bw)]

    def hstore(j):
        return pltpu.make_async_copy(hstage(j), ph_out.at[span((j // events) * hrows, hrows), span(lax.rem(j, events) * bw, bw)], pt_sem.at[lax.rem(j, 2)])

    def hblock(j):
        @pl.when(lax.rem(j, events) >= 2)
        def _():
            hstore(j - 2).wait()
        rows = span((j // events) * hrows, hrows)
        cols = span(lax.rem(j, events) * bw, bw)
        hstage(j)[...] = dotf(o_sib[rows, :], wpair[:qn, cols]) + dotf(sq[rows, :], wpair[qn:2 * qn, cols]) + dotf(kvc[rows, :], wpair[2 * qn:2 * qn + 4 * kn, cols])
        hstore(j).start()

    def final_y(dr, sub, acc):
        rows = span((2 * dr + sub) * pos, pos)
        y_v[rows, :] = (y_v[rows, :].astype(F32) + acc).astype(BF)

    def step_c(e):
        @pl.when(e == events - 2)
        def _():
            first_sends(1)

        @pl.when(e >= 2)
        def _():
            serve(0, e, final_y)

        @pl.when(e == 0)
        def _():
            total(gown, b_s.at[0])
            total(gown, b_s.at[2])
            total(wqts_out, wq_r.at[0])
            total(wpair.at[pl.ds(0, qn)], w_s.at[0])
            for c in ld2:
                c.start()
            d_rows[...] = jnp.zeros_like(d_rows)
            gn[...] = jnp.zeros_like(gn)
            qga[...] = jnp.zeros_like(qga)
            kga[...] = jnp.zeros_like(kga)

        paced(e, 2, units, 6, run_unit)

        @pl.when(e == 8)
        def _():
            kv_two(batch - 1)
        paced(e, 8, batch * tiles, 3, run_fold)

        @pl.when(e == 10)
        def _():
            each(0, 2 * nz, settle)
            each(0, nz, lambda k: [swap(k, dr, kk).start() for dr in both for kk in both])

        @pl.when(e == 11)
        def _():
            for c in ld2:
                c.wait()
            total(sq, qs.at[1, 0])
            total(skv, qs.at[1, 1])
            each(0, nz, gather_h)
        paced(e, 11, events, 2, hblock)

        @pl.when(e == 12)
        def _():
            for j in (events - 2, events - 1):
                hstore(j).wait()
            first_fetch(1)

    each(0, events, step_c)

    def gblk(j):
        return qr.at[:, span(lax.rem(j, 2) * bw, bw)]

    def hblk(j):
        return gd.at[:, span(lax.rem(j, 2) * bw, bw)]

    def swo(j):
        return d_rows.at[pl.ds(0, qn), span(lax.rem(j, 2) * bw, bw)]

    def swq(j):
        return d_rows.at[pl.ds(pl.multiple_of(qn + lax.rem(j, 2) * bw, bw), bw), pl.ds(0, qn)]

    def g_load(j):
        return pltpu.make_async_copy(gy_out.at[:, span(j * bw, bw)], gblk(j), gls.at[lax.rem(j, 2)])

    def h_load(j):
        return pltpu.make_async_copy(hid.at[:, span(j * bw, bw)], hblk(j), hls.at[lax.rem(j, 2)])

    def wo_store(j):
        return pltpu.make_async_copy(swo(j), gwo_hbm.at[:, span(j * bw, bw)], swos.at[lax.rem(j, 2)])

    def wq_store(j):
        return pltpu.make_async_copy(swq(j), gq_hbm.at[span(j * bw, bw)], swqs.at[lax.rem(j, 2)])

    def block(j):
        g_load(j).wait()
        h_load(j).wait()

        @pl.when(j + 1 < events)
        def _():
            g_load(j + 1).start()
            h_load(j + 1).start()

        @pl.when(j >= 2)
        def _():
            wo_store(j - 2).wait()
            wq_store(j - 2).wait()
        cols = span(j * bw, bw)
        swo(j)[...] = dotf(o_own[...], gblk(j)[...], TN)
        ge_v[:, cols] = dotf(hotm[...], gblk(j)[...])
        wo_store(j).start()
        swq(j)[...] = dotf(hblk(j)[...], qt[...], TN)
        gkv_v[:, cols] = dotf(kvrow[...], hblk(j)[...], TN)[:2 * kn]
        wq_store(j).start()

    def final_h(dr, sub, gh):
        rows = span((2 * dr + sub) * sub_rows, sub_rows)
        x = gown[rows, :].astype(F32)
        r = lax.rsqrt(jnp.mean(x * x, axis=-1, keepdims=True) + EPS)
        ge_v[rows, :] += rms_pull(x, gh * gain[...], r)

    outs = [pltpu.make_async_copy(s, t, out_sem.at[i]) for i, (s, t) in enumerate((
        (y_v, y_hbm), (gkv_v.at[pl.ds(0, kn)], gk_hbm), (gkv_v.at[pl.ds(kn, kn)], gv_hbm)))]

    def ge_store(dr, sub):
        rows = pl.ds((2 * dr + sub) * sub_rows, sub_rows)
        return pltpu.make_async_copy(ge_v.at[rows], ge_hbm.at[rows], out_sem.at[3])

    g_load(0).start()
    h_load(0).start()
    outs[0].start()
    work_d = events - 3

    wide = gn_out.shape[1]
    gtop = d // wide
    mrow = gtop // 2

    def to_sib(t):
        if t:
            return rdma(gfin.at[core], gfin.at[core], gs.at[4], gs.at[5], sib)
        return rdma(gmine.at[1 - core], gsib, gs.at[0], gs.at[1], sib)

    def to_col(k):
        return rdma(gcol.at[z], gcol.at[z], gs.at[2], gs.at[3], 2 * lax.rem(z + k, nz) + core)

    def step_d(e):
        @pl.when(e >= 2)
        def _():
            serve(1, e, final_h)

        @pl.when(e == 0)
        def _():
            for k in both:
                for c in item(k):
                    c.start()

        paced(e, 2, events, 4, lambda j: hblock(j + events))

        @pl.when(e == 5)
        def _():
            for j in (events - 2, events - 1):
                hstore(j + events).wait()
        paced(e, 2, events, 8, gain_part)
        paced(e, 5, events, work_d - 5, block)

        @pl.when(e == 10)
        def _():
            whole = jnp.sum(gn[...], axis=0, keepdims=True)
            for k, extra in ((0, qga), (1, kga)):
                for j in range(mrow):
                    c0 = (k * mrow + j) * wide
                    gmine[k, j:j + 1, :] = whole[:, c0:c0 + wide].astype(BF)
                gmine[k, mrow:mrow + 1, :] = extra[...].astype(BF)
            to_sib(0).start()

        @pl.when(e == 11)
        def _():
            total(gsib, gs.at[1])
            gcol[z] = (gmine[core].astype(F32) + gsib[...].astype(F32)).astype(BF)
            for k in range(1, nz):
                to_col(k).start()

        @pl.when(e == 13)
        def _():
            total(gcol.at[pl.ds(0, nz - 1)], gs.at[3])
            gfin[core] = sum(gcol[k].astype(F32) for k in range(nz))
            to_sib(1).start()

        @pl.when(e == events - 3)
        def _():
            outs[1].start()
            outs[2].start()

        @pl.when(e == events - 2)
        def _():
            for dr in both:
                ge_store(dr, 0).start()

    each(0, events, step_d)

    for dr in both:
        ge_store(dr, 1).start()
    for ph in both:
        for k in range(4):
            arrived(rs.at[ph, k])

    total(gy_out.at[pl.ds(0, 2 * (events - 4) * pos)], b_s.at[1])
    total(gy_out.at[pl.ds(0, 2 * (events - 2) * pos)], b_s.at[3])
    to_far.wait_send()
    relay.wait_send()
    total(wpair.at[pl.ds(2 * qn, 2 * kn)], w_s.at[2])
    total(o_sib, o_s.at[0])
    total(pk.at[pl.ds(0, batch // 2)], p1s.at[0])
    total(fk, p2s.at[0])
    total(sq, qs.at[0, 0])
    total(skv, qs.at[0, 1])
    total(gfin.at[0], gs.at[5])
    gn_out[0:mrow, :] = gfin[0, 0:mrow, :]
    gn_out[mrow:, :] = gfin[1, 0:mrow, :]
    gqg_out[...] = gfin[0, mrow:mrow + 1, :]
    gkg_out[...] = gfin[1, mrow:mrow + 1, :]
    total(gsib, gs.at[0])
    total(gcol.at[pl.ds(0, nz - 1)], gs.at[2])
    total(gfin.at[0], gs.at[4])
    for j in (events - 2, events - 1):
        wo_store(j).wait()
        wq_store(j).wait()
    total(ge_v, out_sem.at[3])
    for c in outs:
        c.wait()


def step_kernel(nz, embed, gy, wq, wk_t, wv_t, wo, gain, qg, kg, cos, sin_s, tok_seq):
    vrows, d = embed.shape
    vocab = vrows * 2 * nz
    qn, kn = wq.shape[1], wk_t.shape[0]
    hd = qg.shape[1]
    batch, seq = tok_seq.shape
    toks = batch * seq
    ev = 2 * nz
    sr, hb, vh = vrows // 4, seq // 2, vocab // 2
    mr = (d // hd // 2 + 1 + 15) // 16 * 16
    dma = pltpu.SemaphoreType.DMA
    v = pltpu.VMEM

    def arr(dt, *shape):
        return jax.ShapeDtypeStruct(shape, dt)

    outs = (arr(BF, vrows, d), arr(F32, vrows, d), arr(F32, d, qn), arr(F32, kn, d), arr(F32, kn, d), arr(F32, qn, d), arr(F32, d // hd, hd), arr(F32, 1, hd), arr(F32, 1, hd), arr(BF, vh, d),
            arr(BF, vocab, d), arr(BF, toks, d), arr(BF, qn, d), arr(BF, qn, d), arr(F32, vh, d), arr(F32, vh, d))
    return pl.pallas_call(
        functools.partial(body, nz),
        name='step_kernel',
        out_shape=outs,
        in_specs=[ANY] * 6 + [VM] * 6,
        out_specs=(ANY,) * 6 + (VM,) * 3 + (ANY,) * 7,
        scratch_shapes=[v((vocab, d), BF), v((2 * qn + 4 * kn, d), BF), v((max(d, 2 * toks), qn), BF), v((vocab, qn), BF), v((toks, qn), BF), v((vh, qn), BF), v((vh, qn), BF),
                        v((toks, 2 * hd), BF), v((toks, hd), BF), v((2, toks // 2, 4 * kn), BF), v((2, toks // 2, 4 * kn), BF), v((vocab, 4 * kn), BF), v((vh, 4 * kn), BF), v((vh, 4 * kn), BF),
                        v((vocab, qn + 4 * kn), F32), v((4, 2, sr, d), F32), v((2, vrows, d), BF), v((vrows, d), BF), v((vrows, toks), BF),
                        v((seq, hd), F32), v((seq, hd), F32), v((batch, 4, hb, 4 * kn), BF), v((batch, 2, hb, 4 * kn), BF), v((batch, hb, 4 * kn), BF), v((batch, hb, 4 * kn), F32),
                        v((batch, hb, 4 * kn), BF), v((batch, seq, 4 * kn), BF), v((8, d), F32), v((1, hd), F32), v((1, hd), F32), v((2, mr, hd), BF), v((mr, hd), BF), v((nz, mr, hd), BF), v((2, mr, hd), F32), v((vrows, d), BF), v((vrows, d), F32), v((2 * kn, d), F32),
                        dma((12,)), dma((2,)), dma((1,)), dma((ev,)), dma((ev,)), dma((2,)), dma((4,)), dma((2,)), dma((2,)), dma((2, 2)), dma((1,)), dma((4,)), dma((2,)),
                        dma((2,)), dma((2, 2)), dma((2, 4)), dma((1,)), dma((batch,)), dma((1,)), dma((batch,)), dma((2, 2)),
                        dma((2,)), dma((2,)), dma((2,)), dma((2,)), dma((6,)), dma((4,)), dma((3,))],
        compiler_params=pltpu.CompilerParams(collective_id=0, has_side_effects=True, vmem_limit_bytes=67043328),
        cost_estimate=pl.CostEstimate(flops=2 * vocab * d * 8 * qn, bytes_accessed=20 * vocab * d, transcendentals=0),
    )(embed, gy, wq, wk_t, wv_t, wo, gain, qg, kg, cos, sin_s, tok_seq)


def emit_body(cuts, *refs):
    n = len(cuts)
    src, dst = refs[:n], refs[n:2 * n]
    bufs, s_in, s_out = refs[2 * n:-2], refs[-2], refs[-1]
    ins, outs = [], []
    for i, c in enumerate(cuts):
        step = src[i].shape[0] // c
        for j in range(c):
            b = bufs[i].at[pl.ds(j * step, step)]
            ins.append(pltpu.make_async_copy(src[i].at[pl.ds(j * step, step)], b, s_in.at[len(ins)]))
            outs.append(pltpu.make_async_copy(b, dst[i].at[pl.ds(j * step, step)], s_out.at[len(outs)]))
    for c in ins:
        c.start()
    for a, b in zip(ins, outs):
        a.wait()
        b.start()
    for b in outs:
        b.wait()


def emit(*arrays):
    size = 1 << 20
    cuts = tuple(max(1, a.size * a.dtype.itemsize // size) for a in arrays)
    return pl.pallas_call(
        functools.partial(emit_body, cuts),
        name='emit',
        out_shape=tuple(jax.ShapeDtypeStruct(a.shape, a.dtype) for a in arrays),
        in_specs=[ANY] * len(arrays),
        out_specs=(ANY,) * len(arrays),
        scratch_shapes=[pltpu.VMEM(a.shape, a.dtype) for a in arrays] + [pltpu.SemaphoreType.DMA((sum(cuts),))] * 2,
        compiler_params=pltpu.CompilerParams(vmem_limit_bytes=60 * 1024 * 1024),
        cost_estimate=pl.CostEstimate(flops=0, bytes_accessed=2 * sum(a.size * a.dtype.itemsize for a in arrays), transcendentals=0),
    )(*arrays)


def rope_consts(seq, hd):
    inv = np.float32(ROPE_BASE) ** (np.float32(-2.0) * np.arange(hd // 2, dtype=np.float32) / np.float32(hd))
    ang = np.arange(seq, dtype=np.float32)[:, None] * inv.astype(np.float32)[None, :]
    ang = np.concatenate([ang, ang], axis=-1)
    sign = np.where(np.arange(hd) < hd // 2, -1.0, 1.0).astype(np.float32)
    return np.cos(ang).astype(np.float32), (np.sin(ang) * sign).astype(np.float32)


def solution(mesh):
    tp = mesh.shape['tp']
    nz = tp // 2

    def local_step(tok_ids, embed_loc, norm_gain, q_gain, k_gain, wq, wk, wv, wo, gy_loc):
        d_model = embed_loc.shape[1]
        batch, seq = tok_ids.shape
        seq_dev = seq // tp
        hd = q_gain.shape[0]
        cos_c, sin_c = (jnp.asarray(t) for t in rope_consts(seq, hd))
        r = step_kernel(nz, embed_loc, gy_loc.reshape(batch * seq_dev, d_model), wq, wk.T, wv.T, wo, norm_gain[None, :], q_gain[None, :], k_gain[None, :], cos_c, sin_c, tok_ids)
        y, g_embed, g_wq, g_wk, g_wv, g_wo, g_n, g_q, g_k = emit(*r[:9])
        return (y.reshape(batch, seq_dev, d_model), g_embed, g_n.reshape(d_model), g_q.reshape(hd), g_k.reshape(hd), g_wq, g_wk.T, g_wv.T, g_wo)

    in_specs = (P('dp', None), P('tp', None), P(), P(), P(), P(None, 'tp'), P(None, 'tp'), P(None, 'tp'), P('tp', None), P('dp', 'tp', None))
    out_specs = (P('dp', 'tp', None), P(('dp', 'tp'), None), P('dp'), P('dp'), P('dp'), P('dp', 'tp'), P('dp', 'tp'), P('dp', 'tp'), P(('dp', 'tp'), None))
    return jax.shard_map(local_step, mesh=mesh, in_specs=in_specs, out_specs=out_specs, check_vma=False)
```

```python
import functools
import jax
import jax.numpy as jnp
import numpy as np
from jax import lax
from jax.experimental import pallas as pl
from jax.experimental.pallas import tpu as pltpu
from jax.sharding import PartitionSpec as P

BF = jnp.bfloat16
F32 = jnp.float32
EPS = 1.0e-6
ROPE_BASE = 1.0e6
NEG_BIG = -1.0e30
LOG2E = 1.4426950408889634
MESH = pl.DeviceIdType.MESH
ANY = pl.BlockSpec(memory_space=pl.ANY)
VM = pl.BlockSpec(memory_space=pltpu.VMEM)
NT = (((1,), (1,)), ((), ()))
NN = (((1,), (0,)), ((), ()))
TN = (((0,), (0,)), ((), ()))


def dotf(a, b, dims=NN):
    return lax.dot_general(a, b, dims, preferred_element_type=F32)


def rdma(src, dst, ssem, rsem, dev):
    return pltpu.make_async_remote_copy(src_ref=src, dst_ref=dst, send_sem=ssem, recv_sem=rsem, device_id={'tp': dev}, device_id_type=MESH)


def span(start, size):
    return pl.ds(pl.multiple_of(start, size), size)


def each(lo, hi, f):
    def go(j, _):
        f(j)
        return 0
    lax.fori_loop(lo, hi, go, 0)


def total(ref, sem):
    pltpu.make_async_copy(ref, ref, sem).wait()


def odd(e):
    return lax.rem(e, 2)


def piece(dr, e):
    return 2 * dr + lax.rem(e, 2)


def lead(n):
    return pl.ds(0, n)


def half(n):
    return n // 2


def row_sum(t):
    return jnp.sum(t, axis=-1, keepdims=True)


def row_mean(t):
    return jnp.mean(t, axis=-1, keepdims=True)


def row_ids(shape):
    return lax.broadcasted_iota(jnp.int32, shape, 0)


def col_ids(shape):
    return lax.broadcasted_iota(jnp.int32, shape, 1)


def chosen(mask):
    return jnp.where(mask, 1.0, 0.0).astype(BF)


def rms_f32(x, gain):
    return x * lax.rsqrt(row_mean(x * x) + EPS) * gain


def rms_pull(x, dxr, r):
    return r * dxr - x * (r * r * r * row_mean(x * dxr))


def causal_blocks(q, keys, i, blk):
    r_i = row_ids((blk, blk))
    c_i = col_ids((blk, blk))
    s = [dotf(q, keys[j * blk:(j + 1) * blk], NT) for j in range(i + 1)]
    s[i] = jnp.where(r_i >= c_i, s[i], NEG_BIG)
    top = functools.reduce(jnp.maximum, [jnp.max(t, axis=-1, keepdims=True) for t in s])
    c = q.shape[-1] ** -0.5 * LOG2E
    e = [jnp.exp2((t - top) * c) for t in s]
    inv = 1.0 / sum(row_sum(t) for t in e)
    return [t * inv for t in e]


def body(nz, embed, gy, wq, wk_t, wv_t, wo, gain, qg, kg, cos, sin_s, tok_seq,
         y_hbm, ge_hbm, gq_hbm, gk_hbm, gv_hbm, gwo_hbm, gn_out, gqg_out, gkg_out, erows, hid, gy_out, wqt_out, wqts_out, py_out, ph_out,
         table, wpair, wq_v, qt, o_own, o_sib, sq, kv_tok, k_rot, kvacc, farkv, kvrow, skv, kvc, d_rows, pbuf, hbuf, gown, hotm,
         dk_acc, dv_acc, pk, rk1, fk, hk, rk2, kvt, gn, qga, kga, gmine, gsib, gcol, gfin, y_v, ge_v, gkv_v,
         in_sem, h_sem, g_sem, r_sem, s_sem, a_s, b_s, xs, xr, wq_s, wq_r, w_s, o_s, pt_sem, pl_sem, rs, p1s, p1r, p2s, p2r, qs, gls, hls, swos, swqs, gs, out_sem, e_sem):
    rank = lax.axis_index('tp')
    z, core = half(rank), odd(rank)
    right = 2 * lax.rem(z + 1, nz) + core
    left = 2 * lax.rem(z + nz - 1, nz) + core
    sib = rank + 1 - 2 * core
    par = odd(z)
    far = rank + 2 - 4 * par
    vrows, d = embed.shape
    kn = wk_t.shape[0]
    sub_rows = vrows // 4
    events = 2 * nz
    vocab = vrows * events
    last, final_e = events - 2, events - 1
    kw, kh, sr2 = 4 * kn, 2 * kn, vrows // 2
    vhalf = half(vocab)
    batch, seq = tok_seq.shape
    toks = batch * seq
    qn = wq.shape[1]
    q2 = 2 * qn
    hd = qg.shape[1]
    heads = qn // hd
    pos = seq // events
    blk = half(seq)
    bw = d // events
    scale = hd ** -0.5
    units = batch * heads
    parts = 8
    wo_p, wq_p = qn // parts, d // parts
    both = (0, 1)
    places = [(dr, c) for dr in both for c in both]
    qr = wq_v.at[lead(toks)]
    gd = wq_v.at[pl.ds(toks, toks)]
    w_q = wq_v.at[lead(d)]

    ld = [pltpu.make_async_copy(s, t, in_sem.at[i]) for i, (s, t) in enumerate((
        (embed, table.at[span(rank * vrows, vrows)]), (gy, gown), (wq, w_q), (wo, wpair.at[lead(qn)]),
        (wk_t, wpair.at[pl.ds(q2, kn)]), (wv_t, wpair.at[pl.ds(q2 + kn, kn)])))]
    ld2 = [pltpu.make_async_copy(s, t, in_sem.at[i]) for i, (s, t) in enumerate((
        (wqt_out, wpair.at[lead(qn)]), (wqts_out, wpair.at[pl.ds(qn, qn)]), (embed, gown)))]
    ld[0].start()
    barrier = pltpu.get_barrier_semaphore()
    for dev in (right, left, sib):
        pl.semaphore_signal(barrier, inc=1, device_id={'tp': dev}, device_id_type=MESH)
    pl.semaphore_wait(barrier, 3)
    ld[0].wait()

    def nbr(dr):
        return right if dr == 0 else left

    def arrived(sem):
        total(table.at[lead(sr2)], sem)

    def zd_of(dr, e):
        s = half(e)
        return lax.rem(z + (nz - s if dr == 0 else s), nz)

    def row_of(dr, e, c):
        return pl.multiple_of(vrows * (2 * zd_of(dr, e) + c) + sub_rows * (piece(dr, e)), sub_rows)

    def ring(dr, e, recv_e):
        a = table.at[pl.ds(row_of(dr, e, core), sub_rows)]
        return rdma(a, a, a_s.at[0], r_sem.at[recv_e], nbr(dr))

    def side(dr, e):
        a = table.at[pl.ds(row_of(dr, e, core), sub_rows)]
        return rdma(a, a, a_s.at[1], s_sem.at[e], sib)

    def e_keep(dr, e):
        dst = pl.multiple_of(vrows * lax.rem(half(e) + nz - 1, nz) + sub_rows * (piece(dr, e)), sub_rows)
        return pltpu.make_async_copy(table.at[pl.ds(row_of(dr, e, core), sub_rows)], erows.at[pl.ds(dst, sub_rows)], e_sem.at[0])

    def h_copy(slot, i, row):
        return pltpu.make_async_copy(hbuf.at[slot, pl.ds(i * sub_rows, sub_rows)], hid.at[pl.ds(row, sub_rows)], h_sem.at[slot])

    def g_row(dr, e, c):
        return pl.multiple_of(seq * (piece(dr, e)) + pos * (2 * zd_of(dr, e) + c), pos)

    def g_piece(dr, e, c):
        return gy_out.at[pl.ds(g_row(dr, e, c), pos)]

    def g_own(dr, e):
        return gown.at[span(pos * (piece(dr, e)), pos)]

    def g_ring(dr, e, recv_e, first):
        a = g_piece(dr, e, core)
        return rdma(g_own(dr, e) if first else a, a, b_s.at[0 if first else 1], r_sem.at[recv_e], nbr(dr))

    def g_side(dr, e, first):
        a = g_piece(dr, e, core)
        return rdma(g_own(dr, e) if first else a, a, b_s.at[2 if first else 3], s_sem.at[e], sib)

    def g_home(dr, e):
        return pltpu.make_async_copy(g_own(dr, e), g_piece(dr, e, core), in_sem.at[8 + 2 * dr + e])

    def g_fetch(slot, i, dr, c, e):
        return pltpu.make_async_copy(g_piece(dr, e, c), hbuf.at[slot, pl.ds(i * pos, pos)], g_sem.at[0])

    def wo_push(k):
        return rdma(wpair.at[span(k * wo_p, wo_p)], wpair.at[pl.ds(pl.multiple_of(qn + k * wo_p, wo_p), wo_p)], w_s.at[0], w_s.at[1], sib)

    def tb(k):
        return o_own.at[span(odd(k) * qn, qn), lead(wq_p)]

    def wq_push(k):
        return rdma(tb(k), wqts_out.at[:, span(k * wq_p, wq_p)], wq_s.at[0, odd(k)], wq_r.at[0], sib)

    def wq_home(k):
        return pltpu.make_async_copy(tb(k), wqt_out.at[:, span(k * wq_p, wq_p)], wq_s.at[1, odd(k)])

    def wk_push(k):
        return rdma((wk_t, wv_t)[k], wpair.at[pl.ds(q2 + (2 + k) * kn, kn)], w_s.at[2], w_s.at[3], sib)

    def o_push(b, k):
        src = pl.multiple_of(b * seq + pos * (2 * k + 1 - core), pos)
        dst = pl.multiple_of(vrows * k + pos * b, pos)
        return rdma(o_own.at[pl.ds(src, pos)], o_sib.at[pl.ds(dst, pos)], o_s.at[0], o_s.at[1], sib)

    def project(e):
        slot = odd(e)

        @pl.when(e >= 2)
        def _():
            total(hbuf.at[slot], h_sem.at[slot])

        rows = [row_of(dr, e, c) for dr, c in places]
        for i, row in enumerate(rows):
            x = table[pl.ds(row, sub_rows), :].astype(F32)
            ids = row + row_ids((sub_rows, seq))
            hit = jnp.zeros((sub_rows, seq), F32)
            for b in range(batch):
                hit = jnp.maximum(hit, jnp.where(tok_seq[b:b + 1, :] == ids, 1.0, 0.0))
            used = jnp.max(hit, axis=1, keepdims=True)
            h = jnp.where(used > 0.5, rms_f32(x, gain[:]), 0.0)
            hbuf[slot, pl.ds(i * sub_rows, sub_rows), :] = h.astype(BF)
            h_copy(slot, i, row).start()
        hb = hbuf[slot]
        qkv = jnp.concatenate([dotf(hb, w_q[:]).astype(BF), dotf(hb, wpair[q2:q2 + kw, :], NT).astype(BF)], axis=1)
        lane = col_ids((1, vrows))
        rowid = jnp.zeros((1, vrows), jnp.int32)
        for i, row in enumerate(rows):
            rowid = jnp.where(lane // sub_rows == i, row + lane - i * sub_rows, rowid)
        rowid = rowid.astype(F32)
        for b in range(batch):
            sl = slice(b * seq, (b + 1) * seq)
            hot = chosen(d_rows[sl, :vrows] == rowid)
            got = dotf(hot, qkv)
            qt[sl, :] = (qt[sl, :].astype(F32) + got[:, :qn]).astype(BF)
            at = slice((b % 2) * seq, (b % 2 + 1) * seq)
            kvacc[b // 2, at, :] = (kvacc[b // 2, at, :].astype(F32) + got[:, qn:]).astype(BF)

    def step_a(e):
        @pl.when((e >= 2) & (e < events))
        def _():
            arrived(r_sem.at[e])

        @pl.when(e < last)
        def _():
            for dr in both:
                ring(dr, e, e + 2).start()

        @pl.when(e < events)
        def _():
            for dr in both:
                side(dr, e).start()
                e_keep(dr, e).start()

        @pl.when(e == 0)
        def _():
            for c in ld[1:]:
                c.start()
            for k in both:
                wk_push(k).start()
            for b in range(batch):
                wide = jnp.broadcast_to(tok_seq[b:b + 1, :].astype(F32), (vrows, seq))
                d_rows[b * seq:(b + 1) * seq, :vrows] = wide.T
            qt[:] = jnp.zeros_like(qt)
            kvacc[:] = jnp.zeros_like(kvacc)

        @pl.when(e == 1)
        def _():
            for c in ld[1:]:
                c.wait()
            total(wpair.at[pl.ds(q2, kh)], w_s.at[3])
            for dr in both:
                for k in both:
                    g_home(dr, k).start()

        @pl.when((e >= last) & (e < events))
        def _():
            for dr in both:
                g_ring(dr, e - events + 2, e - events + 4, True).start()

        @pl.when((e >= 2) & (e < 4 + parts))
        def _():
            @pl.when(e >= 4)
            def _():
                wq_push(e - 4).wait_send()
                wq_home(e - 4).wait()

            @pl.when(e < 2 + parts)
            def _():
                k = e - 2
                block = wq_v[span(k * wq_p, wq_p), :]
                tb(k)[:] = block.astype(F32).T.astype(BF)
                wo_push(k).start()
                wq_push(k).start()
                wq_home(k).start()

        @pl.when(e >= 1)
        def _():
            arrived(s_sem.at[e - 1])
            project(e - 1)

    each(0, events + 1, step_a)

    to_far = rdma(kvacc.at[core], farkv.at[core], xs.at[0], xr.at[0], far)
    relay = rdma(farkv.at[core], farkv.at[core], xs.at[1], xr.at[1], sib)
    at_i = col_ids((pos, seq)) - pos * rank
    own_i = row_ids((pos, seq))
    col = jnp.concatenate([jnp.sum(jnp.where(at_i == own_i, tok_seq[b:b + 1, :].astype(F32), 0.0), axis=1, keepdims=True) for b in range(batch)], axis=0).astype(jnp.int32)
    lanes = col_ids((vrows, vrows))
    hot_mine = jnp.concatenate([chosen(col == lanes + j * vrows) for j in range(vocab // vrows)], axis=1)
    to_far.start()
    for dr in both:
        for k in both:
            g_side(dr, k, True).start()
            g_home(dr, k).wait()
    cw = min(512, d)

    def own_rows(j):
        y_v[:, span(j * cw, cw)] = dotf(hot_mine, table[:, span(j * cw, cw)]).astype(BF)

    each(0, d // cw, own_rows)
    for b in range(batch):
        ids = rank * vrows + row_ids((vrows, seq))
        hotm[:, b * seq:(b + 1) * seq] = chosen(ids == tok_seq[b:b + 1, :])

    def place(p, first):
        l_i = row_ids((kw, 2 * hd))
        m_i = col_ids((kw, 2 * hd))
        upper = jnp.where(l_i >= kh, 1, 0)
        owner = jnp.where(upper == 1, 1 - first, first)
        l_i = l_i - kh * upper
        base = kn * (2 * p + owner)
        want = jnp.where(l_i < kn, base + l_i, hd + base + l_i - kn)
        return chosen(m_i == want)

    def rope(raw, g):
        n = rms_f32(raw.astype(F32), g)
        return (n * cos[:] + pltpu.roll(n, half(hd), 1) * sin_s[:]).astype(BF)

    def attend(u):
        base = (u // heads) * seq
        rows = span(base, seq)
        cols = span(lax.rem(u, heads) * hd, hd)
        q = rope(qt[rows, cols], qg[:])
        qr[rows, cols] = q
        kr = k_rot[rows, :]
        v = kv_tok[rows, hd:]
        for i in both:
            p = causal_blocks(q[i * blk:(i + 1) * blk], kr, i, blk)
            o = sum(dotf(t.astype(BF), v[j * blk:(j + 1) * blk]) for j, t in enumerate(p))
            o_own[pl.ds(pl.multiple_of(base + i * blk, blk), blk), cols] = o.astype(BF)

    def grad_attend(e):
        total(hbuf, g_sem.at[0])
        r = dotf(hbuf[:].reshape(2 * vrows, d), wpair[:qn, :], NT).astype(BF)
        for k in both:
            for i, (dr, c) in enumerate(places):
                n = (4 * k + i) * pos
                gd[pl.ds(g_row(dr, e + k, c), pos), :] = r[n:n + pos]

    def pstage(j):
        return d_rows.at[span(odd(j) * vhalf, vhalf), lead(bw)]

    def pstore(dst, j):
        return pltpu.make_async_copy(pstage(j), dst.at[:, span(j * bw, bw)], pt_sem.at[odd(j)])

    def pblock(dst, j, pairs):
        @pl.when(j >= 2)
        def _():
            pstore(dst, j - 2).wait()
        cols = span(j * bw, bw)
        acc = None
        for a, lo, n in pairs:
            t = dotf(a[:], wpair[lo:lo + n, cols])
            acc = t if acc is None else acc + t
        pstage(j)[:] = acc
        pstore(dst, j).start()

    y_pairs = [(sq, 0, qn), (o_sib, qn, qn)]

    def pslot(ph, e, dr):
        return pbuf.at[2 * ph + odd(e), dr]

    def pfetch(ph, e, dr):
        s = half(e)
        step = s if ph else lax.rem(z + (final_e - s if dr == 0 else 1 + s), nz)
        row = pl.multiple_of(vrows * step + sub_rows * (piece(dr, e)), sub_rows)
        return pltpu.make_async_copy((py_out, ph_out)[ph].at[pl.ds(row, sub_rows)], pslot(ph, e, dr), pl_sem.at[ph, odd(e)])

    def item(i):
        row = vrows * (half(i))
        cps = []
        for dr in both:
            at = pl.ds(pl.multiple_of(row + sub_rows * (2 * dr + odd(i)), sub_rows), sub_rows)
            cps.append(pltpu.make_async_copy(ph_out.at[at], pbuf.at[odd(i), dr], pl_sem.at[0, odd(i)]))
            cps.append(pltpu.make_async_copy(erows.at[at], hbuf.at[odd(i), pl.ds(dr * sub_rows, sub_rows)], e_sem.at[1 + odd(i)]))
        return cps

    def gain_part(i):
        total(pbuf.at[odd(i)], pl_sem.at[0, odd(i)])
        total(hbuf.at[odd(i), lead(sr2)], e_sem.at[1 + odd(i)])
        for dr in both:
            x = hbuf[odd(i), dr * sub_rows:(dr + 1) * sub_rows, :].astype(F32)
            t = pbuf[odd(i), dr] * (x * lax.rsqrt(row_mean(x * x) + EPS))
            gn[:] += sum(t[k:k + 8] for k in range(0, sub_rows, 8))

        @pl.when(i + 2 < events)
        def _():
            for c in item(i + 2):
                c.start()

    def fetched(ph, e):
        total(pbuf.at[2 * ph + odd(e)], pl_sem.at[ph, odd(e)])

    def rslot(dr, e):
        return table.at[span((dr * (last) + e) * sub_rows, sub_rows)]

    def sslot(ph, dr, e):
        k = 2 * (last) + 8 * ph + 4 * odd(half(e)) + piece(dr, e)
        return table.at[span(k * sub_rows, sub_rows)]

    def send(ph, dr, e):
        return rdma(sslot(ph, dr, e), rslot(dr, e), rs.at[ph, lax.rem(e, 4)], r_sem.at[e + 2], nbr(dr))

    def first_fetch(ph):
        for e in both:
            for dr in both:
                pfetch(ph, e, dr).start()

    def first_sends(ph):
        for e in both:
            fetched(ph, e)
            for dr in both:
                sslot(ph, dr, e)[:] = pslot(ph, e, dr)[:].astype(BF)
        for e in both:
            for dr in both:
                send(ph, dr, e).start()
                pfetch(ph, e + 2, dr).start()

    def serve(ph, e, final):
        arrived(r_sem.at[e])
        fetched(ph, e)

        @pl.when(e < last)
        def _():
            @pl.when(e >= 4)
            def _():
                arrived(rs.at[ph, lax.rem(e, 4)])
            for dr in both:
                sslot(ph, dr, e)[:] = (pslot(ph, e, dr)[:] + rslot(dr, e - 2)[:].astype(F32)).astype(BF)
            for dr in both:
                send(ph, dr, e).start()
                pfetch(ph, e + 2, dr).start()

        @pl.when(e >= last)
        def _():
            for dr in both:
                final(dr, odd(e), pslot(ph, e, dr)[:] + rslot(dr, e - 2)[:].astype(F32))

    slots = 9

    def gather_o(k):
        for b in range(batch):
            src = pl.multiple_of(b * seq + pos * (2 * k + core), pos)
            sq[pl.ds(pl.multiple_of(vrows * k + pos * b, pos), pos), :] = o_own[pl.ds(src, pos), :]

    def upto(e, n, over):
        return jnp.minimum((e * n) // over, n)

    def step_b(e):
        @pl.when(e == last)
        def _():
            first_sends(0)

        @pl.when((e >= 2) & (e < events))
        def _():
            arrived(r_sem.at[e])

        @pl.when((e >= 2) & (e < last))
        def _():
            for dr in both:
                g_ring(dr, e, e + 2, False).start()

        @pl.when((e >= 2) & (e < events))
        def _():
            for dr in both:
                g_side(dr, e, False).start()

        @pl.when((e >= 1) & (e <= events))
        def _():
            arrived(s_sem.at[e - 1])

        @pl.when(e == 2)
        def _():
            to_far.wait_recv()
            relay.start()

        @pl.when(e == 3)
        def _():
            rdma(farkv.at[1 - core], farkv.at[1 - core], xs.at[1], xr.at[1], sib).wait_recv()
            for hf in both:
                kv_tok[hf * (half(toks)):(hf + 1) * (half(toks)), :] = (dotf(kvacc[hf], place(par, core)) + dotf(farkv[hf], place(1 - par, hf))).astype(BF)
            for b in range(batch):
                sl = slice(b * seq, (b + 1) * seq)
                k_rot[sl, :] = rope(kv_tok[sl, :hd], kg[:])

        @pl.when((e >= 2) & (odd(e) == 0))
        def _():
            for k in both:
                for i, (dr, c) in enumerate(places):
                    g_fetch(k, i, dr, c, e - 2 + k).start()

        def give(b):
            each(0, nz, lambda k: o_push(b, k).start())

        def seen(t):
            return jnp.minimum((jnp.maximum(t - 3, 0) * units) // (slots - 3), units)

        each(seen(e - 1) // heads, seen(e) // heads, give)
        each(seen(e), seen(e + 1), attend)

        @pl.when(e == 4)
        def _():
            total(table.at[lead(2 * (last) * sub_rows)], a_s.at[0])
            total(table.at[lead(2 * events * sub_rows)], a_s.at[1])
            total(erows, e_sem.at[0])

        @pl.when(e == slots + 1)
        def _():
            total(wpair.at[lead(qn)], w_s.at[1])
            total(o_sib, o_s.at[1])
            each(0, nz, gather_o)

        @pl.when((e > slots) & (e <= slots + 4))
        def _():
            each(4 * (e - slots - 1), 4 * (e - slots), lambda j: pblock(py_out, j, y_pairs))

        @pl.when(e == slots + 4)
        def _():
            for j in (last, final_e):
                pstore(py_out, j).wait()
            first_fetch(0)

        @pl.when((e >= 3) & (odd(e) == 1))
        def _():
            grad_attend(e - 3)

    for slot in both:
        total(hbuf.at[slot], h_sem.at[slot])
    each(0, events + 2, step_b)

    def pull(raw, dout, g):
        x = raw.astype(F32)
        r = lax.rsqrt(row_mean(x * x) + EPS)
        dn = dout * cos[:] + pltpu.roll(dout * sin_s[:], half(hd), 1)
        return rms_pull(x, dn * g, r).astype(BF), jnp.sum(dn * (x * r), axis=0, keepdims=True)

    def unit(u):
        b, h = u // heads, lax.rem(u, heads)
        rows = span(b * seq, seq)
        cols = span(h * hd, hd)

        @pl.when(h == 0)
        def _():
            dk_acc[:] = jnp.zeros_like(dk_acc)
            dv_acc[:] = jnp.zeros_like(dv_acc)
        q, g = qr[rows, cols], gd[rows, cols]
        kr, v = k_rot[rows, :], kv_tok[rows, hd:]
        dqs = []
        for i in both:
            qi, gi = q[i * blk:(i + 1) * blk], g[i * blk:(i + 1) * blk]
            p = causal_blocks(qi, kr, i, blk)
            dp = [dotf(gi, v[j * blk:(j + 1) * blk], NT) for j in range(i + 1)]
            tot = sum(row_sum(a * b) for a, b in zip(p, dp))
            dq = None
            for j in range(i + 1):
                at = slice(j * blk, (j + 1) * blk)
                dv_acc[at, :] += dotf(p[j].astype(BF), gi, TN)
                ds = (p[j] * (dp[j] - tot)).astype(BF)
                t = dotf(ds, kr[at])
                dq = t if dq is None else dq + t
                dk_acc[at, :] += dotf(ds, qi, TN)
            dqs.append(dq * scale)
        dq = jnp.concatenate(dqs, axis=0).astype(BF).astype(F32)
        dx, dg = pull(qt[rows, cols], dq, qg[:])
        gd[rows, cols] = dx
        qga[:] += dg

    def pick(r, up):
        m_i = row_ids((2 * hd, kw))
        l_i = col_ids((2 * hd, kw)) - kh * up
        is_k = (l_i >= 0) & (l_i < kn) & (m_i == l_i + kn * r)
        is_v = (l_i >= kn) & (l_i < kh) & (m_i == hd + kn * r + l_i - kn)
        return chosen(is_k | is_v)

    def to_side(b, p):
        return rdma(pk.at[b, 2 * p + 1 - core], rk1.at[b, p], p1s.at[0], p1r.at[b], sib)

    def to_far2(b):
        return rdma(fk.at[b], rk2.at[b], p2s.at[0], p2r.at[b], far)

    def kv_one(b):
        dk = (dk_acc[:] * scale).astype(BF).astype(F32)
        dx, dg = pull(kv_tok[span(b * seq, seq), :hd], dk, kg[:])
        kga[:] += dg
        gkv = jnp.concatenate([dx, dv_acc[:].astype(BF)], axis=1)
        for r in range(4):
            pk[b, r] = (dotf(gkv[:blk], pick(r, 0)) + dotf(gkv[blk:], pick(r, 1))).astype(BF)
        for p in both:
            to_side(b, p).start()

    def kv_two(b):
        total(rk1.at[b], p1r.at[b])
        fk[b] = (pk[b, 2 * (1 - par) + core].astype(F32) + rk1[b, 1 - par].astype(F32)).astype(BF)
        hk[b] = pk[b, 2 * par + core].astype(F32) + rk1[b, par].astype(F32)
        to_far2(b).start()

    def kv_three(b):
        to_far2(b).wait_recv()
        t = hk[b] + rk2[b].astype(F32)
        low = col_ids(t.shape) < kh
        kvt[b, :blk, :] = jnp.where(low, t, 0.0).astype(BF)
        kvt[b, blk:, :] = jnp.where(low, pltpu.roll(t, kh, 1), 0.0).astype(BF)

    def fold(b, tile):
        rows = span(tile * seq, seq)
        ids = tile * seq + row_ids((seq, seq))
        hot = chosen(ids == tok_seq[pl.ds(b, 1), :])
        d_rows[rows, :qn] += dotf(hot, gd[span(b * seq, seq), :])
        d_rows[rows, qn:] += dotf(hot, kvt[b])

    tiles = vocab // seq

    def run_unit(u):
        unit(u)

        @pl.when(lax.rem(u, heads) == heads - 1)
        def _():
            kv_one(u // heads)

        @pl.when((u >= heads) & (lax.rem(u, heads) == 1))
        def _():
            kv_two(u // heads - 1)

    def run_fold(f):
        b, tile = f // tiles, lax.rem(f, tiles)

        @pl.when(tile == 0)
        def _():
            kv_three(b)
        fold(b, tile)

    def share(e, first, n, over):
        return jnp.minimum((jnp.maximum(e - first, 0) * n) // over, n)

    def paced(e, first, n, over, f):
        each(share(e, first, n, over), share(e + 1, first, n, over), f)

    def settle(t):
        rows = span(t * vrows, vrows)
        qt[rows, :] = d_rows[rows, :qn].astype(BF)
        kvrow[rows, :] = d_rows[rows, qn:].astype(BF)

    def step_row(k, dr):
        return pl.multiple_of(vrows * lax.rem(z + nz - 1 - k if dr == 0 else k + nz - 1 - z, nz) + sr2 * dr, sr2)

    def swap(k, dr, kk):
        src = pl.multiple_of(vrows * (2 * k + 1 - core) + sr2 * dr, sr2)
        return rdma((qt, kvrow)[kk].at[pl.ds(src, sr2)], (sq, skv)[kk].at[pl.ds(step_row(k, dr), sr2)], qs.at[0, kk], qs.at[1, kk], sib)

    def gather_h(k):
        for dr in both:
            src = pl.multiple_of(vrows * (2 * k + core) + sr2 * dr, sr2)
            dst = pl.ds(step_row(k, dr), sr2)
            o_sib[dst, :] = qt[pl.ds(src, sr2), :]
            kvc[dst, :] = (kvrow[pl.ds(src, sr2), :].astype(F32) + pltpu.roll(skv[dst, :].astype(F32), kh, 1)).astype(BF)

    hrows = half(vhalf)

    def hstage(j):
        return d_rows.at[pl.ds(pl.multiple_of(vhalf + odd(j) * hrows, hrows), hrows), lead(bw)]

    def hstore(j):
        return pltpu.make_async_copy(hstage(j), ph_out.at[span((j // events) * hrows, hrows), span(lax.rem(j, events) * bw, bw)], pt_sem.at[odd(j)])

    def hblock(j):
        @pl.when(lax.rem(j, events) >= 2)
        def _():
            hstore(j - 2).wait()
        rows = span((j // events) * hrows, hrows)
        cols = span(lax.rem(j, events) * bw, bw)
        hstage(j)[:] = dotf(o_sib[rows, :], wpair[:qn, cols]) + dotf(sq[rows, :], wpair[qn:q2, cols]) + dotf(kvc[rows, :], wpair[q2:q2 + kw, cols])
        hstore(j).start()

    def final_y(dr, sub, acc):
        rows = span((2 * dr + sub) * pos, pos)
        y_v[rows, :] = (y_v[rows, :].astype(F32) + acc).astype(BF)

    def step_c(e):
        @pl.when(e == last)
        def _():
            first_sends(1)

        @pl.when(e >= 2)
        def _():
            serve(0, e, final_y)

        @pl.when(e == 0)
        def _():
            total(gown, b_s.at[0])
            total(gown, b_s.at[2])
            total(wqts_out, wq_r.at[0])
            total(wpair.at[lead(qn)], w_s.at[0])
            for c in ld2:
                c.start()
            d_rows[:] = jnp.zeros_like(d_rows)
            gn[:] = jnp.zeros_like(gn)
            qga[:] = jnp.zeros_like(qga)
            kga[:] = jnp.zeros_like(kga)

        paced(e, 2, units, 6, run_unit)

        @pl.when(e == 8)
        def _():
            kv_two(batch - 1)
        paced(e, 8, batch * tiles, 3, run_fold)

        @pl.when(e == 10)
        def _():
            each(0, events, settle)
            each(0, nz, lambda k: [swap(k, dr, kk).start() for dr in both for kk in both])

        @pl.when(e == 11)
        def _():
            for c in ld2:
                c.wait()
            total(sq, qs.at[1, 0])
            total(skv, qs.at[1, 1])
            each(0, nz, gather_h)
        paced(e, 11, events, 2, hblock)

        @pl.when(e == 12)
        def _():
            for j in (last, final_e):
                hstore(j).wait()
            first_fetch(1)

    each(0, events, step_c)

    def gblk(j):
        return qr.at[:, span(odd(j) * bw, bw)]

    def hblk(j):
        return gd.at[:, span(odd(j) * bw, bw)]

    def swo(j):
        return d_rows.at[lead(qn), span(odd(j) * bw, bw)]

    def swq(j):
        return d_rows.at[pl.ds(pl.multiple_of(qn + odd(j) * bw, bw), bw), lead(qn)]

    def g_load(j):
        return pltpu.make_async_copy(gy_out.at[:, span(j * bw, bw)], gblk(j), gls.at[odd(j)])

    def h_load(j):
        return pltpu.make_async_copy(hid.at[:, span(j * bw, bw)], hblk(j), hls.at[odd(j)])

    def wo_store(j):
        return pltpu.make_async_copy(swo(j), gwo_hbm.at[:, span(j * bw, bw)], swos.at[odd(j)])

    def wq_store(j):
        return pltpu.make_async_copy(swq(j), gq_hbm.at[span(j * bw, bw)], swqs.at[odd(j)])

    def block(j):
        g_load(j).wait()
        h_load(j).wait()

        @pl.when(j + 1 < events)
        def _():
            g_load(j + 1).start()
            h_load(j + 1).start()

        @pl.when(j >= 2)
        def _():
            wo_store(j - 2).wait()
            wq_store(j - 2).wait()
        cols = span(j * bw, bw)
        swo(j)[:] = dotf(o_own[:], gblk(j)[:], TN)
        ge_v[:, cols] = dotf(hotm[:], gblk(j)[:])
        wo_store(j).start()
        swq(j)[:] = dotf(hblk(j)[:], qt[:], TN)
        gkv_v[:, cols] = dotf(kvrow[:], hblk(j)[:], TN)[:kh]
        wq_store(j).start()

    def final_h(dr, sub, gh):
        rows = span((2 * dr + sub) * sub_rows, sub_rows)
        x = gown[rows, :].astype(F32)
        r = lax.rsqrt(row_mean(x * x) + EPS)
        ge_v[rows, :] += rms_pull(x, gh * gain[:], r)

    outs = [pltpu.make_async_copy(s, t, out_sem.at[i]) for i, (s, t) in enumerate((
        (y_v, y_hbm), (gkv_v.at[lead(kn)], gk_hbm), (gkv_v.at[pl.ds(kn, kn)], gv_hbm)))]

    def ge_store(dr, sub):
        rows = pl.ds((2 * dr + sub) * sub_rows, sub_rows)
        return pltpu.make_async_copy(ge_v.at[rows], ge_hbm.at[rows], out_sem.at[3])

    g_load(0).start()
    h_load(0).start()
    outs[0].start()
    work_d = events - 3

    wide = gn_out.shape[1]
    gtop = d // wide
    mrow = half(gtop)

    def to_sib(t):
        if t:
            return rdma(gfin.at[core], gfin.at[core], gs.at[4], gs.at[5], sib)
        return rdma(gmine.at[1 - core], gsib, gs.at[0], gs.at[1], sib)

    def to_col(k):
        return rdma(gcol.at[z], gcol.at[z], gs.at[2], gs.at[3], 2 * lax.rem(z + k, nz) + core)

    def step_d(e):
        @pl.when(e >= 2)
        def _():
            serve(1, e, final_h)

        @pl.when(e == 0)
        def _():
            for k in both:
                for c in item(k):
                    c.start()

        paced(e, 2, events, 4, lambda j: hblock(j + events))

        @pl.when(e == 5)
        def _():
            for j in (last, final_e):
                hstore(j + events).wait()
        paced(e, 2, events, 8, gain_part)
        paced(e, 5, events, work_d - 5, block)

        @pl.when(e == 10)
        def _():
            whole = jnp.sum(gn[:], axis=0, keepdims=True)
            for k, extra in ((0, qga), (1, kga)):
                for j in range(mrow):
                    c0 = (k * mrow + j) * wide
                    gmine[k, j:j + 1, :] = whole[:, c0:c0 + wide].astype(BF)
                gmine[k, mrow:mrow + 1, :] = extra[:].astype(BF)
            to_sib(0).start()

        @pl.when(e == 11)
        def _():
            total(gsib, gs.at[1])
            gcol[z] = (gmine[core].astype(F32) + gsib[:].astype(F32)).astype(BF)
            for k in range(1, nz):
                to_col(k).start()

        @pl.when(e == 13)
        def _():
            total(gcol.at[lead(nz - 1)], gs.at[3])
            gfin[core] = sum(gcol[k].astype(F32) for k in range(nz))
            to_sib(1).start()

        @pl.when(e == events - 3)
        def _():
            outs[1].start()
            outs[2].start()

        @pl.when(e == last)
        def _():
            for dr in both:
                ge_store(dr, 0).start()

    each(0, events, step_d)

    for dr in both:
        ge_store(dr, 1).start()
    for ph in both:
        for k in range(4):
            arrived(rs.at[ph, k])

    total(gy_out.at[lead(2 * (events - 4) * pos)], b_s.at[1])
    total(gy_out.at[lead(2 * (last) * pos)], b_s.at[3])
    to_far.wait_send()
    relay.wait_send()
    total(wpair.at[pl.ds(q2, kh)], w_s.at[2])
    total(o_sib, o_s.at[0])
    total(pk.at[lead(half(batch))], p1s.at[0])
    total(fk, p2s.at[0])
    total(sq, qs.at[0, 0])
    total(skv, qs.at[0, 1])
    total(gfin.at[0], gs.at[5])
    gn_out[:mrow] = gfin[0, :mrow]
    gn_out[mrow:] = gfin[1, :mrow]
    gqg_out[:] = gfin[0, mrow:mrow + 1, :]
    gkg_out[:] = gfin[1, mrow:mrow + 1, :]
    total(gsib, gs.at[0])
    total(gcol.at[lead(nz - 1)], gs.at[2])
    total(gfin.at[0], gs.at[4])
    for j in (last, final_e):
        wo_store(j).wait()
        wq_store(j).wait()
    total(ge_v, out_sem.at[3])
    for c in outs:
        c.wait()


def step_kernel(nz, embed, gy, wq, wk_t, wv_t, wo, gain, qg, kg, cos, sin_s, tok_seq):
    vrows, d = embed.shape
    vocab = vrows * 2 * nz
    qn, kn = wq.shape[1], wk_t.shape[0]
    hd = qg.shape[1]
    batch, seq = tok_seq.shape
    toks = batch * seq
    ev = 2 * nz
    kw, kh, q2, th = 4 * kn, 2 * kn, 2 * qn, toks // 2
    two = pltpu.SemaphoreType.DMA((2,))
    one = pltpu.SemaphoreType.DMA((1,))
    four = pltpu.SemaphoreType.DMA((4,))
    sr, hb, vh = vrows // 4, half(seq), half(vocab)
    mr = (d // half(hd) + 1 + 15) // 16 * 16
    dma = pltpu.SemaphoreType.DMA
    v = pltpu.VMEM

    def arr(dt, *shape):
        return jax.ShapeDtypeStruct(shape, dt)

    outs = (arr(BF, vrows, d), arr(F32, vrows, d), arr(F32, d, qn), arr(F32, kn, d), arr(F32, kn, d), arr(F32, qn, d), arr(F32, d // hd, hd), arr(F32, 1, hd), arr(F32, 1, hd), arr(BF, vh, d),
            arr(BF, vocab, d), arr(BF, toks, d), arr(BF, qn, d), arr(BF, qn, d), arr(F32, vh, d), arr(F32, vh, d))
    return pl.pallas_call(
        functools.partial(body, nz),
        name='step_kernel',
        out_shape=outs,
        in_specs=[ANY] * 6 + [VM] * 6,
        out_specs=(ANY,) * 6 + (VM,) * 3 + (ANY,) * 7,
        scratch_shapes=[v((vocab, d), BF), v((q2 + kw, d), BF), v((max(d, 2 * toks), qn), BF), v((vocab, qn), BF), v((toks, qn), BF), v((vh, qn), BF), v((vh, qn), BF),
                        v((toks, 2 * hd), BF), v((toks, hd), BF), v((2, th, kw), BF), v((2, th, kw), BF), v((vocab, kw), BF), v((vh, kw), BF), v((vh, kw), BF),
                        v((vocab, qn + kw), F32), v((4, 2, sr, d), F32), v((2, vrows, d), BF), v((vrows, d), BF), v((vrows, toks), BF),
                        v((seq, hd), F32), v((seq, hd), F32), v((batch, 4, hb, kw), BF), v((batch, 2, hb, kw), BF), v((batch, hb, kw), BF), v((batch, hb, kw), F32),
                        v((batch, hb, kw), BF), v((batch, seq, kw), BF), v((8, d), F32), v((1, hd), F32), v((1, hd), F32), v((2, mr, hd), BF), v((mr, hd), BF), v((nz, mr, hd), BF), v((2, mr, hd), F32), v((vrows, d), BF), v((vrows, d), F32), v((kh, d), F32),
                        dma((12,)), two, one, dma((ev,)), dma((ev,)), two, four, two, two, dma((2, 2)), one, four, two,
                        two, dma((2, 2)), dma((2, 4)), one, dma((batch,)), one, dma((batch,)), dma((2, 2)),
                        two, two, two, two, dma((6,)), four, dma((3,))],
        compiler_params=pltpu.CompilerParams(collective_id=0, has_side_effects=True, vmem_limit_bytes=67043328),
        cost_estimate=pl.CostEstimate(flops=2 * vocab * d * 8 * qn, bytes_accessed=20 * vocab * d, transcendentals=0),
    )(embed, gy, wq, wk_t, wv_t, wo, gain, qg, kg, cos, sin_s, tok_seq)


def emit_body(cuts, *refs):
    n = len(cuts)
    src, dst = refs[:n], refs[n:2 * n]
    bufs, s_in, s_out = refs[2 * n:-2], refs[-2], refs[-1]
    ins, outs = [], []
    for i, c in enumerate(cuts):
        step = src[i].shape[0] // c
        for j in range(c):
            b = bufs[i].at[pl.ds(j * step, step)]
            ins.append(pltpu.make_async_copy(src[i].at[pl.ds(j * step, step)], b, s_in.at[len(ins)]))
            outs.append(pltpu.make_async_copy(b, dst[i].at[pl.ds(j * step, step)], s_out.at[len(outs)]))
    for c in ins:
        c.start()
    for a, b in zip(ins, outs):
        a.wait()
        b.start()
    for b in outs:
        b.wait()


def emit(*arrays):
    size = 1 << 20
    cuts = tuple(max(1, a.size * a.dtype.itemsize // size) for a in arrays)
    return pl.pallas_call(
        functools.partial(emit_body, cuts),
        name='emit',
        out_shape=tuple(jax.ShapeDtypeStruct(a.shape, a.dtype) for a in arrays),
        in_specs=[ANY] * len(arrays),
        out_specs=(ANY,) * len(arrays),
        scratch_shapes=[pltpu.VMEM(a.shape, a.dtype) for a in arrays] + [pltpu.SemaphoreType.DMA((sum(cuts),))] * 2,
        compiler_params=pltpu.CompilerParams(vmem_limit_bytes=60 * 1024 * 1024),
        cost_estimate=pl.CostEstimate(flops=0, bytes_accessed=2 * sum(a.size * a.dtype.itemsize for a in arrays), transcendentals=0),
    )(*arrays)


def rope_consts(seq, hd):
    inv = np.float32(ROPE_BASE) ** (np.float32(-2.0) * np.arange(half(hd), dtype=np.float32) / np.float32(hd))
    ang = np.arange(seq, dtype=np.float32)[:, None] * inv.astype(np.float32)[None, :]
    ang = np.concatenate([ang, ang], axis=-1)
    sign = np.where(np.arange(hd) < half(hd), -1.0, 1.0).astype(np.float32)
    return np.cos(ang).astype(np.float32), (np.sin(ang) * sign).astype(np.float32)


def solution(mesh):
    tp = mesh.shape['tp']
    nz = tp // 2

    def local_step(tok_ids, embed_loc, norm_gain, q_gain, k_gain, wq, wk, wv, wo, gy_loc):
        d_model = embed_loc.shape[1]
        batch, seq = tok_ids.shape
        seq_dev = seq // tp
        hd = q_gain.shape[0]
        cos_c, sin_c = (jnp.asarray(t) for t in rope_consts(seq, hd))
        r = step_kernel(nz, embed_loc, gy_loc.reshape(batch * seq_dev, d_model), wq, wk.T, wv.T, wo, *(t[None, :] for t in (norm_gain, q_gain, k_gain)), cos_c, sin_c, tok_ids)
        y, g_embed, g_wq, g_wk, g_wv, g_wo, g_n, g_q, g_k = emit(*r[:9])
        return (y.reshape(batch, seq_dev, d_model), g_embed, g_n.reshape(d_model), g_q.reshape(hd), g_k.reshape(hd), g_wq, g_wk.T, g_wv.T, g_wo)

    cols = P(None, 'tp')
    in_specs = (P('dp', None), P('tp', None), P(), P(), P(), cols, cols, cols, P('tp', None), P('dp', 'tp', None))
    out_specs = (P('dp', 'tp', None), P(('dp', 'tp'), None), P('dp'), P('dp'), P('dp'), P('dp', 'tp'), P('dp', 'tp'), P('dp', 'tp'), P(('dp', 'tp'), None))
    return jax.shard_map(local_step, mesh=mesh, in_specs=in_specs, out_specs=out_specs, check_vma=False)
```
